8 devices in a mesh: dp: 1 (over z), pp: 2 (over y), ep: 4 (over x, core).
Axes of the slice: x: 2, y: 2, z: 1, core: 2. Of those that a mesh axis runs over, the one named last changes fastest.
Arguments:
- hidden_in: bfloat16 [64, 128, 1024], P(None, ('dp', 'ep'))
- seq_pos: int32 [64, 128], P(None, ('dp', 'ep'))
- k_cache: bfloat16 [2, 64, 128, 16, 8, 64], P('pp', None, ('dp', 'ep'))
- v_cache: bfloat16 [2, 64, 128, 16, 8, 64], P('pp', None, ('dp', 'ep'))
- expert_ids: int32 [2, 64, 128, 8], P('pp', None, ('dp', 'ep'))
- w_query: bfloat16 [2, 1024, 1024], P('pp')
- w_key: bfloat16 [2, 1024, 512], P('pp')
- w_value: bfloat16 [2, 1024, 512], P('pp')
- w_out: bfloat16 [2, 1024, 1024], P('pp')
- attn_gain: bfloat16 [2, 1024], P('pp')
- mlp_gain: bfloat16 [2, 1024], P('pp')
- w_router: bfloat16 [2, 1024, 32], P('pp')
- w_gate: bfloat16 [2, 32, 1024, 512], P('pp', 'ep')
- w_up: bfloat16 [2, 32, 1024, 512], P('pp', 'ep')
- w_down: bfloat16 [2, 32, 512, 1024], P('pp', 'ep')
- final_gain: bfloat16 [1024], replicated
Outputs:
- output 1: bfloat16 [64, 128, 1024], P(None, ('dp', 'ep'))
- output 2: bfloat16 [2, 64, 128, 8, 64], P('pp', None, ('dp', 'ep'))
- output 3: bfloat16 [2, 64, 128, 8, 64], P('pp', None, ('dp', 'ep'))
All inputs are finite; a program needn't handle non-finite values.
Results may differ from the reference program's by a relative error of at most 0.0174593.
Values are sent between devices in bfloat16 or wider.
A program may use at most 1 GiB of HBM per device.

```python
import jax
import jax.numpy as jnp
from jax import lax

D = 1024
HEADS = 16
KV_HEADS = 8
HEAD = 64
EXPERTS = 32
FF = 512
TOP = 8
LAYERS = 2
EP_SIZE = 4
MICRO_COUNT = 64
TOK_DEV = 32
CONTEXT = 16
MICRO_ROWS = EP_SIZE * TOK_DEV
LOCAL_EXPERTS = EXPERTS // EP_SIZE
THETA = 1000000.0
EPS = 1e-05


def draw_routes(route_key):
    hot_key, perm_key, local_key = jax.random.split(route_key, 3)
    hot_dev = jax.random.randint(hot_key, (LAYERS, MICRO_COUNT, 1, 1), 0, EP_SIZE)
    perm_keys = jax.random.split(perm_key, LAYERS * MICRO_COUNT * EP_SIZE)
    slot_pos = jax.vmap(lambda one_key: jax.random.permutation(one_key, TOK_DEV))(perm_keys)
    slot_pos = slot_pos.reshape(LAYERS, MICRO_COUNT, EP_SIZE, TOK_DEV)
    first_dev = jnp.where(slot_pos < TOK_DEV // 2, hot_dev, (hot_dev + slot_pos) % EP_SIZE)
    local_base = jax.random.randint(local_key, (LAYERS, MICRO_COUNT, EP_SIZE, TOK_DEV, 1), 0, LOCAL_EXPERTS)
    choice = jnp.arange(TOP)
    dest_dev = (first_dev[..., None] + choice) % EP_SIZE
    local_idx = (local_base + choice // EP_SIZE) % LOCAL_EXPERTS
    route_ids = dest_dev * LOCAL_EXPERTS + local_idx
    return route_ids.reshape(LAYERS, MICRO_COUNT, MICRO_ROWS, TOP).astype(jnp.int32)


def draw_normal(one_key, arr_shape, std_scale):
    return (jax.random.normal(one_key, arr_shape, jnp.float32) * std_scale).astype(jnp.bfloat16)


def draw_gain(one_key, arr_shape):
    return (1.0 + 0.3 * jax.random.normal(one_key, arr_shape, jnp.float32)).astype(jnp.bfloat16)


def setup_inputs(seed: int = 0, part: int = 0) -> dict:
    shared_keys = jax.random.split(jax.random.key(seed), 11)
    part_keys = jax.random.split(jax.random.fold_in(jax.random.key(seed + 1), part), 5)
    pos_draw = jax.random.randint(part_keys[1], (MICRO_COUNT, MICRO_ROWS), 1, CONTEXT + 1)
    first_row = jnp.arange(MICRO_COUNT * MICRO_ROWS).reshape(MICRO_COUNT, MICRO_ROWS) == 0
    seq_pos = jnp.where(first_row, CONTEXT, pos_draw).astype(jnp.int32)
    cache_shape = (LAYERS, MICRO_COUNT, MICRO_ROWS, CONTEXT, KV_HEADS, HEAD)
    out_scale = 0.5 * (CONTEXT ** 0.5) * (HEADS * HEAD) ** -0.5
    return {
        "hidden_in": draw_normal(part_keys[0], (MICRO_COUNT, MICRO_ROWS, D), 1.0),
        "seq_pos": seq_pos,
        "k_cache": draw_normal(part_keys[2], cache_shape, 1.0),
        "v_cache": draw_normal(part_keys[3], cache_shape, 1.0),
        "expert_ids": draw_routes(part_keys[4]),
        "w_query": draw_normal(shared_keys[0], (LAYERS, D, HEADS * HEAD), D ** -0.5),
        "w_key": draw_normal(shared_keys[1], (LAYERS, D, KV_HEADS * HEAD), D ** -0.5),
        "w_value": draw_normal(shared_keys[2], (LAYERS, D, KV_HEADS * HEAD), D ** -0.5),
        "w_out": draw_normal(shared_keys[3], (LAYERS, HEADS * HEAD, D), out_scale),
        "attn_gain": draw_gain(shared_keys[4], (LAYERS, D)),
        "mlp_gain": draw_gain(shared_keys[5], (LAYERS, D)),
        "w_router": draw_normal(shared_keys[6], (LAYERS, D, EXPERTS), 2.0 * D ** -0.5),
        "w_gate": draw_normal(shared_keys[7], (LAYERS, EXPERTS, D, FF), D ** -0.5),
        "w_up": draw_normal(shared_keys[8], (LAYERS, EXPERTS, D, FF), D ** -0.5),
        "w_down": draw_normal(shared_keys[9], (LAYERS, EXPERTS, FF, D), FF ** -0.5),
        "final_gain": draw_gain(shared_keys[10], (D,)),
    }


def rms_norm(in_vals, gain_vec):
    vals_f32 = in_vals.astype(jnp.float32)
    inv_rms = lax.rsqrt(jnp.mean(vals_f32 * vals_f32, axis=-1, keepdims=True) + EPS)
    return (vals_f32 * inv_rms * gain_vec.astype(jnp.float32)).astype(jnp.bfloat16)


def rotate(head_vecs, positions):
    half_dim = head_vecs.shape[-1] // 2
    inv_freq = THETA ** (-jnp.arange(half_dim, dtype=jnp.float32) / half_dim)
    angles = positions.astype(jnp.float32)[:, None, None] * inv_freq
    cos_ang = jnp.cos(angles)
    sin_ang = jnp.sin(angles)
    first_half = head_vecs[..., :half_dim].astype(jnp.float32)
    second_half = head_vecs[..., half_dim:].astype(jnp.float32)
    return jnp.concatenate([first_half * cos_ang - second_half * sin_ang, second_half * cos_ang + first_half * sin_ang], axis=-1).astype(jnp.bfloat16)


def attend(q_heads, key_new, val_new, k_rows, v_rows, positions):
    tokens = key_new.shape[0]
    q_groups = q_heads.reshape(tokens, KV_HEADS, HEADS // KV_HEADS, HEAD).astype(jnp.float32)
    score_scale = HEAD ** -0.5
    cache_scores = jnp.einsum("bkgh,btkh->bkgt", q_groups, k_rows.astype(jnp.float32)) * score_scale
    is_valid = jnp.arange(CONTEXT)[None, None, None, :] < positions[:, None, None, None]
    cache_scores = jnp.where(is_valid, cache_scores, -jnp.inf)
    self_score = jnp.einsum("bkgh,bkh->bkg", q_groups, key_new.astype(jnp.float32))[..., None] * score_scale
    top_score = jnp.maximum(jnp.max(cache_scores, axis=-1, keepdims=True), self_score)
    cache_w = jnp.exp(cache_scores - top_score)
    self_w = jnp.exp(self_score - top_score)
    weight_sum = jnp.sum(cache_w, axis=-1, keepdims=True) + self_w
    cache_w = (cache_w / weight_sum).astype(jnp.bfloat16).astype(jnp.float32)
    self_w = (self_w / weight_sum).astype(jnp.bfloat16).astype(jnp.float32)
    attn_out = jnp.einsum("bkgt,btkh->bkgh", cache_w, v_rows.astype(jnp.float32)) + self_w * val_new.astype(jnp.float32)[:, :, None, :]
    return attn_out.astype(jnp.bfloat16).reshape(tokens, HEADS * HEAD)


def one_micro(hidden, positions, k_rows, v_rows, choice_ids, layer_w):
    w_q, w_k, w_v, w_o, a_gain, m_gain, w_r, w_g, w_u, w_d = layer_w
    tokens = hidden.shape[0]
    normed = rms_norm(hidden, a_gain)
    q_heads = jnp.dot(normed, w_q, preferred_element_type=jnp.float32).astype(jnp.bfloat16).reshape(tokens, HEADS, HEAD)
    key_new = jnp.dot(normed, w_k, preferred_element_type=jnp.float32).astype(jnp.bfloat16).reshape(tokens, KV_HEADS, HEAD)
    val_new = jnp.dot(normed, w_v, preferred_element_type=jnp.float32).astype(jnp.bfloat16).reshape(tokens, KV_HEADS, HEAD)
    q_heads = rotate(q_heads, positions)
    key_new = rotate(key_new, positions)
    attn_out = attend(q_heads, key_new, val_new, k_rows, v_rows, positions)
    hidden = (hidden.astype(jnp.float32) + jnp.dot(attn_out, w_o, preferred_element_type=jnp.float32)).astype(jnp.bfloat16)
    normed = rms_norm(hidden, m_gain)
    logits = jnp.dot(normed, w_r, preferred_element_type=jnp.float32)
    gate_vals = jax.nn.softmax(jnp.take_along_axis(logits, choice_ids, axis=1), axis=-1)
    coef_mat = jnp.sum(gate_vals[:, :, None] * (choice_ids[:, :, None] == jnp.arange(EXPERTS)[None, None, :]), axis=1)

    def expert_body(acc_sum, expert_args):
        gate_w, up_w, down_w, coef_col = expert_args
        act_rows = (jax.nn.silu(jnp.dot(normed, gate_w, preferred_element_type=jnp.float32)) * jnp.dot(normed, up_w, preferred_element_type=jnp.float32)).astype(jnp.bfloat16)
        down_h = jnp.dot(act_rows, down_w, preferred_element_type=jnp.float32)
        return acc_sum + (coef_col[:, None] * down_h).astype(jnp.bfloat16).astype(jnp.float32), None

    moe_sum, _ = lax.scan(expert_body, jnp.zeros(hidden.shape, jnp.float32), (w_g, w_u, w_d, coef_mat.T))
    hidden = (hidden.astype(jnp.float32) + moe_sum.astype(jnp.bfloat16).astype(jnp.float32)).astype(jnp.bfloat16)
    return hidden, key_new, val_new


def reference(hidden_in, seq_pos, k_cache, v_cache, expert_ids, w_query, w_key, w_value, w_out, attn_gain, mlp_gain, w_router, w_gate, w_up, w_down, final_gain):
    def layer_body(hidden, layer_args):
        layer_w = layer_args[3:]

        def micro_body(micro_args):
            return one_micro(micro_args[0], micro_args[1], micro_args[2], micro_args[3], micro_args[4], layer_w)

        hidden, k_rows, v_rows = lax.map(micro_body, (hidden, seq_pos, layer_args[0], layer_args[1], layer_args[2]))
        return hidden, (k_rows, v_rows)

    hidden, new_rows = lax.scan(layer_body, hidden_in, (k_cache, v_cache, expert_ids, w_query, w_key, w_value, w_out, attn_gain, mlp_gain, w_router, w_gate, w_up, w_down))
    return rms_norm(hidden, final_gain), new_rows[0], new_rows[1]
```

```python
import functools

import jax
import jax.numpy as jnp
from jax import lax
from jax.experimental import pallas as pl
from jax.experimental.pallas import tpu as pltpu
from jax.sharding import PartitionSpec as P

THETA = 1000000.0
EPS = 1e-05
F32 = jnp.float32
BF16 = jnp.bfloat16
TILE = 128
GROUP = 16


def rms(vals, gain_row):
    inv = lax.rsqrt(jnp.mean(vals * vals, axis=-1, keepdims=True) + EPS)
    return (vals * inv * gain_row).astype(BF16)


def dot_nt(lhs, rhs):
    return lax.dot_general(lhs, rhs, (((1,), (1,)), ((), ())), preferred_element_type=F32)


def dot_tn(lhs, rhs):
    return lax.dot_general(lhs, rhs, (((0,), (0,)), ((), ())), preferred_element_type=F32)


def dot(lhs, rhs):
    return jnp.dot(lhs, rhs, preferred_element_type=F32)


def rope_table(pos, table_ref):
    picked = jnp.zeros(pos.shape, F32)
    for t in range(table_ref.shape[0]):
        picked = jnp.where(pos == t + 1, table_ref[t:t + 1, :], picked)
    return picked


def rope(vals, cos_t, sin_t):
    lane = lax.broadcasted_iota(jnp.int32, (1, 128), 1)
    first = (lane % 64) < 32
    parts = []
    for j in range(vals.shape[1] // 128):
        block = vals[:, j * 128:(j + 1) * 128]
        swapped = jnp.where(first, pltpu.roll(block, 96, 1), pltpu.roll(block, 32, 1))
        parts.append(block * cos_t + swapped * sin_t)
    return jnp.concatenate(parts, axis=1)


def attn_project(hidden, pos, w_q, w_k, w_v, gain, cos_ref, sin_ref, q3, k3, v3):
    tokens = hidden.shape[0]
    normed = rms(hidden.astype(F32), gain[...].astype(F32))
    cos_t = rope_table(pos, cos_ref)
    sin_t = rope_table(pos, sin_ref)
    q = rope(dot(normed, w_q[...]).astype(BF16).astype(F32), cos_t, sin_t)
    q3[...] = q.astype(BF16).astype(F32).reshape(tokens, -1, 128)
    k = rope(dot(normed, w_k[...]).astype(BF16).astype(F32), cos_t, sin_t)
    k3[...] = k.astype(BF16).astype(F32).reshape(tokens, -1, 128)
    v3[...] = dot(normed, w_v[...]).astype(BF16).astype(F32).reshape(tokens, -1, 128)


def attn_group(idx, q3, k3, v3, o3, pos_ref, k_rows, v_rows):
    base = pl.multiple_of(idx * GROUP, GROUP)
    span = pl.ds(base, GROUP)
    q = q3[span]
    lane3 = lax.broadcasted_iota(jnp.int32, (1, 1, 128), 2)
    prod = q * k3[span]
    self_a = jnp.sum(jnp.where(lane3 < 64, prod, 0.0), axis=-1, keepdims=True)
    self_b = jnp.sum(jnp.where(lane3 < 64, 0.0, prod), axis=-1, keepdims=True)
    self_s = jnp.concatenate([self_a, self_b], axis=1) * 0.125
    q_rows = jnp.concatenate([q, pltpu.roll(q, 64, 2)], axis=1).astype(BF16)[:, :, :64].reshape(GROUP * 16, 64)
    row0 = idx * (GROUP * 128)
    blocks = []
    for p in range(GROUP // 2):
        keys = k_rows[pl.ds(pl.multiple_of(row0 + p * 256, 256), 256), :]
        both = dot_nt(q_rows[p * 32:(p + 1) * 32], keys)
        blocks.append(both[:16, :128].reshape(1, 16, 128))
        blocks.append(both[16:, 128:].reshape(1, 16, 128))
    scores = jnp.concatenate(blocks, axis=0)
    row_i = lax.broadcasted_iota(jnp.int32, (16, 128), 0)
    lane_i = lax.broadcasted_iota(jnp.int32, (16, 128), 1)
    step = jnp.where((row_i % 8) == (lane_i % 8), lane_i // 8, 1000)
    pos = pos_ref[span, :].reshape(GROUP, 1, 128)
    scores = jnp.where(step.reshape(1, 16, 128) < pos, scores * 0.125, -jnp.inf)
    top = jnp.maximum(jnp.max(scores, axis=-1, keepdims=True), self_s)
    weights = jnp.exp(scores - top)
    self_w = jnp.exp(self_s - top)
    inv = 1.0 / (jnp.sum(weights, axis=-1, keepdims=True) + self_w)
    weights = (weights * inv).astype(BF16)
    self_w = (self_w * inv).astype(BF16).astype(F32)
    zeros = jnp.zeros((16, 128), BF16)
    outs = []
    for p in range(GROUP // 2):
        vals = v_rows[pl.ds(pl.multiple_of(row0 + p * 256, 256), 256), :]
        upper = jnp.concatenate([weights[2 * p], zeros], axis=1)
        lower = jnp.concatenate([zeros, weights[2 * p + 1]], axis=1)
        outs.append(dot(jnp.concatenate([upper, lower], axis=0), vals).reshape(2, 16, 64))
    out = jnp.concatenate(outs, axis=0)
    v_new = v3[span][:, :, :64]
    out_a = out[:, :8] + self_w[:, :8] * v_new
    out_b = out[:, 8:] + self_w[:, 8:] * v_new
    o3[span] = jnp.concatenate([out_a, out_b], axis=-1)


def attn_finish(hidden, o3, w_o, gain):
    tokens = hidden.shape[0]
    out = o3[...].reshape(tokens, 1024).astype(BF16)
    mid = (hidden.astype(F32) + dot(out, w_o[...])).astype(BF16)
    return mid, rms(mid.astype(F32), gain[...].astype(F32))


def attn_kernel(h_ref, pos_ref, k_rows, v_rows, w_q, w_k, w_v, w_o, a_gain, m_gain, cos_ref, sin_ref, mid_ref, n_ref, kn_ref, vn_ref, q3, k3, v3, o3):
    hidden = h_ref[...]
    attn_project(hidden, pos_ref[...], w_q, w_k, w_v, a_gain, cos_ref, sin_ref, q3, k3, v3)
    kn_ref[...] = k3[...][:, :, :64].astype(BF16)
    vn_ref[...] = v3[...][:, :, :64].astype(BF16)

    def body(idx, carry):
        attn_group(idx, q3, k3, v3, o3, pos_ref, k_rows, v_rows)
        return carry

    lax.fori_loop(0, hidden.shape[0] // GROUP, body, 0)
    mid, normed = attn_finish(hidden, o3, w_o, m_gain)
    mid_ref[...] = mid
    n_ref[...] = normed


def moe_route(ids, first, normed, w_r, tri, rank_ref, gate_ref):
    tokens = ids.shape[1]
    expert_i = lax.broadcasted_iota(jnp.int32, (32, tokens), 0)
    chosen = jnp.zeros((32, tokens), F32)
    for s in range(ids.shape[0]):
        chosen = jnp.where(ids[s:s + 1, :] == expert_i, 1.0, chosen)
    rank = dot(chosen.astype(BF16), tri[...])
    rank_ref[...] = jnp.where(chosen > 0.0, rank, -1.0)
    logits = dot_nt(w_r[...], normed)
    top = jnp.max(jnp.where(chosen > 0.0, logits, -jnp.inf), axis=0, keepdims=True)
    gates = jnp.where(chosen > 0.0, jnp.exp(logits - top), 0.0)
    gate_ref[...] = gates / jnp.sum(gates, axis=0, keepdims=True)


def moe_tile(expert, sub, first, n_ref, rank_ref, gate_ref, w_g, w_u, w_d, acc):
    tokens = n_ref.shape[0]
    ranks = rank_ref[pl.ds(first + expert, 1), :]
    wanted = (lax.broadcasted_iota(jnp.int32, (TILE, 1), 0) + sub * TILE).astype(F32)
    picked = jnp.where(ranks == wanted, 1.0, 0.0)
    gate = jnp.sum(picked * gate_ref[pl.ds(first + expert, 1), :], axis=-1, keepdims=True)
    onehot = picked.astype(BF16)
    rows = dot(onehot, n_ref[...]).astype(BF16)
    up = jax.nn.silu(dot(rows, w_g[expert])) * dot(rows, w_u[expert])
    term = (gate * dot(up.astype(BF16), w_d[expert])).astype(BF16)
    acc[...] += dot_tn(onehot, term)


def moe_kernel(te_ref, tk_ref, first_ref, n_ref, ids_ref, w_r, w_g, w_u, w_d, tri, out_ref, rank_ref, gate_ref):
    first = first_ref[0]
    moe_route(ids_ref[...], first, n_ref[...], w_r, tri, rank_ref, gate_ref)
    out_ref[...] = jnp.zeros_like(out_ref)

    def body(idx, carry):
        moe_tile(te_ref[idx], tk_ref[idx], first, n_ref, rank_ref, gate_ref, w_g, w_u, w_d, out_ref)
        return carry

    lax.fori_loop(0, te_ref.shape[0], body, 0)


def vmem_spec():
    return pl.BlockSpec(memory_space=pltpu.VMEM)


def smem_spec():
    return pl.BlockSpec(memory_space=pltpu.SMEM)


def attn_call(hidden, pos, k_rows, v_rows, consts):
    tokens = hidden.shape[0]
    big = pltpu.VMEM((tokens, 8, 128), F32)
    return pl.pallas_call(
        attn_kernel,
        out_shape=(
            jax.ShapeDtypeStruct((tokens, 1024), BF16),
            jax.ShapeDtypeStruct((tokens, 1024), BF16),
            jax.ShapeDtypeStruct((tokens, 8, 64), BF16),
            jax.ShapeDtypeStruct((tokens, 8, 64), BF16),
        ),
        in_specs=[vmem_spec()] * 12,
        out_specs=(vmem_spec(),) * 4,
        scratch_shapes=[big, big, big, big],
        name="attn_chunk",
        cost_estimate=pl.CostEstimate(flops=4 * 10**9, bytes_accessed=20 * 10**6, transcendentals=0),
    )(hidden, pos, k_rows, v_rows, *consts)


def moe_call(normed, ids, te, tk, first, w_r, w_g, w_u, w_d, tri):
    tokens = normed.shape[0]
    return pl.pallas_call(
        moe_kernel,
        out_shape=jax.ShapeDtypeStruct((tokens, 1024), F32),
        in_specs=[smem_spec()] * 3 + [vmem_spec()] * 7,
        out_specs=vmem_spec(),
        scratch_shapes=[pltpu.VMEM((32, tokens), F32), pltpu.VMEM((32, tokens), F32)],
        name="moe_chunk",
        cost_estimate=pl.CostEstimate(flops=10**10, bytes_accessed=30 * 10**6, transcendentals=0),
    )(te, tk, first, normed, ids, w_r, w_g, w_u, w_d, tri)


def dup_heads(w):
    rows = w.shape[0]
    heads = w.reshape(rows, -1, 1, 64)
    return jnp.broadcast_to(heads, (rows, heads.shape[1], 2, 64)).reshape(rows, -1)


def tile_tables(ids, first, tile_count):
    local = first + jnp.arange(8, dtype=jnp.int32)
    counts = jnp.sum((ids[:, None] == local[None, :, None, None]).astype(jnp.int32), axis=(2, 3))
    tiles = (counts + TILE - 1) // TILE
    ends = jnp.cumsum(tiles, axis=1)
    idx = jnp.arange(tile_count, dtype=jnp.int32)
    expert = jnp.sum((idx[None, :, None] >= ends[:, None, :]).astype(jnp.int32), axis=-1)
    safe = jnp.minimum(expert, 7)
    starts = ends - tiles
    start = jnp.sum(jnp.where(safe[:, :, None] == jnp.arange(8)[None, None, :], starts[:, None, :], 0), axis=-1)
    sub = jnp.where(expert < 8, idx[None, :] - start, 1000)
    return safe, sub.astype(jnp.int32)


def solution(mesh):
    ep_size = mesh.shape["ep"]
    stage_count = mesh.shape["pp"]
    rows_spec = ("dp", "ep")
    three_dim = P("pp", None, None)
    two_dim = P("pp", None)
    expert_spec = P("pp", "ep", None, None)
    cache_spec = P("pp", None, rows_spec, None, None, None)
    new_spec = P("pp", None, rows_spec, None, None)
    in_specs = (P(None, rows_spec, None), P(None, rows_spec), cache_spec, cache_spec, P("pp", None, rows_spec, None), three_dim, three_dim, three_dim, three_dim, two_dim, two_dim, three_dim, expert_spec, expert_spec, expert_spec, P(None))
    out_specs = (P(None, rows_spec, None), new_spec, new_spec)
    shift_perm = [(s, s + 1) for s in range(stage_count - 1)]
    per_chunk = 4

    def device_fn(hidden_in, seq_pos, k_cache, v_cache, expert_ids, w_query, w_key, w_value, w_out, attn_gain, mlp_gain, w_router, w_gate, w_up, w_down, final_gain):
        stage = lax.axis_index("pp")
        ep_idx = lax.axis_index("ep")
        micro, rows = seq_pos.shape
        chunks = micro // per_chunk
        tokens = per_chunk * rows
        gathered = ep_size * tokens
        tile_count = gathered * 2 // TILE + 7
        hid = hidden_in.reshape(chunks, tokens, 1024)
        pos = jnp.broadcast_to(seq_pos.reshape(micro * rows, 1), (micro * rows, 128)).reshape(chunks, tokens, 128)
        k_rows = k_cache.reshape(chunks, tokens * 128, 64)
        v_rows = v_cache.reshape(chunks, tokens * 128, 64)
        inv_freq = THETA ** (-jnp.arange(32, dtype=F32) / 32)
        angles = jnp.arange(1, 17, dtype=F32)[:, None] * inv_freq
        cos_t = jnp.tile(jnp.cos(angles), (1, 4))
        sin_t = jnp.tile(jnp.concatenate([-jnp.sin(angles), jnp.sin(angles)], axis=1), (1, 2))
        consts = (w_query[0], dup_heads(w_key[0]), dup_heads(w_value[0]), w_out[0], attn_gain, mlp_gain, cos_t, sin_t)
        first = (ep_idx * 8).astype(jnp.int32).reshape(1)
        ids = lax.all_gather(expert_ids[0].reshape(chunks, tokens, 8), "ep", axis=1, tiled=True)
        ids = jnp.swapaxes(ids, 1, 2)
        te, tk = tile_tables(ids, first[0], tile_count)
        ti = jnp.arange(gathered)
        tri = (ti[:, None] < ti[None, :]).astype(BF16)
        router_t = w_router[0].T

        def tick(t, state):
            incoming, out_buf, k_buf, v_buf = state
            c = jnp.clip(t - stage, 0, chunks - 1)
            at = lambda arr: lax.dynamic_index_in_dim(arr, c, 0, keepdims=False)
            stage_in = jnp.where(stage == 0, at(hid), incoming)
            mid, normed, k_new, v_new = attn_call(stage_in, at(pos), at(k_rows), at(v_rows), consts)
            n_all = lax.all_gather(normed, "ep", axis=0, tiled=True)
            part = moe_call(n_all, at(ids), at(te), at(tk), first, router_t, w_gate[0], w_up[0], w_down[0], tri)
            mixed = lax.psum_scatter(part, "ep", scatter_dimension=0, tiled=True).astype(BF16)
            result = (mid.astype(F32) + mixed.astype(F32)).astype(BF16)
            k_buf = lax.dynamic_update_index_in_dim(k_buf, k_new, c, 0)
            v_buf = lax.dynamic_update_index_in_dim(v_buf, v_new, c, 0)
            out_buf = lax.dynamic_update_index_in_dim(out_buf, result, c, 0)
            return lax.ppermute(result, "pp", shift_perm), out_buf, k_buf, v_buf

        state = (jnp.zeros((tokens, 1024), BF16), jnp.zeros(hid.shape, BF16), jnp.zeros((chunks, tokens, 8, 64), BF16), jnp.zeros((chunks, tokens, 8, 64), BF16))
        _, out_buf, k_buf, v_buf = lax.fori_loop(0, chunks + stage_count - 1, tick, state)
        x = out_buf.reshape(hidden_in.shape).astype(F32)
        final = rms(x, final_gain.astype(F32))
        final = jnp.where(stage == stage_count - 1, final, jnp.zeros((), BF16))
        shape = (1,) + seq_pos.shape + (8, 64)
        return lax.psum(final, "pp"), k_buf.reshape(shape), v_buf.reshape(shape)

    return jax.shard_map(device_fn, mesh=mesh, in_specs=in_specs, out_specs=out_specs, check_vma=False)
```

```python
import functools

import jax
import jax.numpy as jnp
from jax import lax
from jax.experimental import pallas as pl
from jax.experimental.pallas import tpu as pltpu
from jax.sharding import PartitionSpec as P

THETA = 1000000.0
EPS = 1e-05
F32 = jnp.float32
BF16 = jnp.bfloat16
TILE = 128
GROUP = 16
PER_CHUNK = 4
HIN_SLOTS = 4
MESH = pl.DeviceIdType.MESH


def rms(vals, gain_row):
    inv = lax.rsqrt(jnp.mean(vals * vals, axis=-1, keepdims=True) + EPS)
    return (vals * inv * gain_row).astype(BF16)


def dot(lhs, rhs):
    return jnp.dot(lhs, rhs, preferred_element_type=F32)


def dot_nt(lhs, rhs):
    return lax.dot_general(lhs, rhs, (((1,), (1,)), ((), ())), preferred_element_type=F32)


def rope_table(pos, table_ref):
    picked = jnp.zeros(pos.shape, F32)
    for t in range(table_ref.shape[0]):
        picked = jnp.where(pos == t + 1, table_ref[t:t + 1, :], picked)
    return picked


def rope(vals, cos_t, sin_t):
    lane = lax.broadcasted_iota(jnp.int32, (1, 128), 1)
    first = (lane % 64) < 32
    parts = []
    for j in range(vals.shape[1] // 128):
        block = vals[:, j * 128:(j + 1) * 128]
        swapped = jnp.where(first, pltpu.roll(block, 96, 1), pltpu.roll(block, 32, 1))
        parts.append(block * cos_t + swapped * sin_t)
    return jnp.concatenate(parts, axis=1)


def dup_heads(vals):
    low = lax.broadcasted_iota(jnp.int32, (1, 128), 1) < 64
    parts = []
    for j in range(vals.shape[1] // 128):
        block = vals[:, j * 128:(j + 1) * 128]
        other = pltpu.roll(block, 64, 1)
        parts.append(jnp.where(low, block, other))
        parts.append(jnp.where(low, other, block))
    return jnp.concatenate(parts, axis=1)


def attn_project(hidden, pos, w, q3, k3, v3):
    tokens = hidden.shape[0]
    normed = rms(hidden.astype(F32), w["a_gain"][...].astype(F32))
    cos_t = rope_table(pos, w["cos"])
    sin_t = rope_table(pos, w["sin"])
    q = rope(dot(normed, w["q"][...]).astype(BF16).astype(F32), cos_t, sin_t)
    q3[...] = q.astype(BF16).astype(F32).reshape(tokens, -1, 128)
    k = rope(dot(normed, w["k"][...]).astype(BF16).astype(F32), cos_t, sin_t)
    k3[...] = dup_heads(k.astype(BF16).astype(F32)).reshape(tokens, -1, 128)
    v3[...] = dup_heads(dot(normed, w["v"][...]).astype(BF16).astype(F32)).reshape(tokens, -1, 128)


def attn_group(idx, q3, k3, v3, o3, pos_ref, k_rows, v_rows):
    base = pl.multiple_of(idx * GROUP, GROUP)
    span = pl.ds(base, GROUP)
    q = q3[span]
    lane3 = lax.broadcasted_iota(jnp.int32, (1, 1, 128), 2)
    prod = q * k3[span]
    self_a = jnp.sum(jnp.where(lane3 < 64, prod, 0.0), axis=-1, keepdims=True)
    self_b = jnp.sum(jnp.where(lane3 < 64, 0.0, prod), axis=-1, keepdims=True)
    self_s = jnp.concatenate([self_a, self_b], axis=1) * 0.125
    q_rows = jnp.concatenate([q, pltpu.roll(q, 64, 2)], axis=1).astype(BF16)[:, :, :64].reshape(GROUP * 16, 64)
    row0 = idx * (GROUP * 128)
    blocks = []
    for p in range(GROUP // 2):
        keys = k_rows[pl.ds(pl.multiple_of(row0 + p * 256, 256), 256), :]
        both = dot_nt(q_rows[p * 32:(p + 1) * 32], keys)
        blocks.append(both[:16, :128].reshape(1, 16, 128))
        blocks.append(both[16:, 128:].reshape(1, 16, 128))
    scores = jnp.concatenate(blocks, axis=0)
    row_i = lax.broadcasted_iota(jnp.int32, (16, 128), 0)
    lane_i = lax.broadcasted_iota(jnp.int32, (16, 128), 1)
    step = jnp.where((row_i % 8) == (lane_i % 8), lane_i // 8, 1000)
    pos = pos_ref[span, :].reshape(GROUP, 1, 128)
    scores = jnp.where(step.reshape(1, 16, 128) < pos, scores * 0.125, -jnp.inf)
    top = jnp.maximum(jnp.max(scores, axis=-1, keepdims=True), self_s)
    weights = jnp.exp(scores - top)
    self_w = jnp.exp(self_s - top)
    inv = 1.0 / (jnp.sum(weights, axis=-1, keepdims=True) + self_w)
    weights = (weights * inv).astype(BF16)
    self_w = (self_w * inv).astype(BF16).astype(F32)
    zeros = jnp.zeros((16, 128), BF16)
    outs = []
    for p in range(GROUP // 2):
        vals = v_rows[pl.ds(pl.multiple_of(row0 + p * 256, 256), 256), :]
        upper = jnp.concatenate([weights[2 * p], zeros], axis=1)
        lower = jnp.concatenate([zeros, weights[2 * p + 1]], axis=1)
        outs.append(dot(jnp.concatenate([upper, lower], axis=0), vals).reshape(2, 16, 64))
    out = jnp.concatenate(outs, axis=0)
    v_new = v3[span][:, :, :64]
    out_a = out[:, :8] + self_w[:, :8] * v_new
    out_b = out[:, 8:] + self_w[:, 8:] * v_new
    o3[span] = jnp.concatenate([out_a, out_b], axis=-1)


def moe_route(ids, normed, w_r, tri, rank_ref, gate_ref):
    tokens = ids.shape[1]
    expert_i = lax.broadcasted_iota(jnp.int32, (32, tokens), 0)
    chosen = jnp.zeros((32, tokens), F32)
    for s in range(ids.shape[0]):
        chosen = jnp.where(ids[s:s + 1, :] == expert_i, 1.0, chosen)
    rank = dot(chosen.astype(BF16), tri[...])
    rank_ref[...] = jnp.where(chosen > 0.0, rank, -1.0)
    logits = dot_nt(w_r[...], normed)
    top = jnp.max(jnp.where(chosen > 0.0, logits, -jnp.inf), axis=0, keepdims=True)
    gates = jnp.where(chosen > 0.0, jnp.exp(logits - top), 0.0)
    gate_ref[...] = gates / jnp.sum(gates, axis=0, keepdims=True)


def moe_tile(idx, expert, sub, first, normed, rank_ref, gate_ref, w, picks, terms):
    ranks = rank_ref[pl.ds(first + expert, 1), :]
    wanted = (lax.broadcasted_iota(jnp.int32, (TILE, 1), 0) + sub * TILE).astype(F32)
    picked = jnp.where(ranks == wanted, 1.0, 0.0)
    gate = jnp.sum(picked * gate_ref[pl.ds(first + expert, 1), :], axis=-1, keepdims=True)
    at = pl.ds(pl.multiple_of(idx * TILE, TILE), TILE)
    picks[:, at] = picked.T.astype(BF16)
    rows = dot(picked.astype(BF16), normed[...]).astype(BF16)
    act = jax.nn.silu(dot(rows, w["gate"][expert])) * dot(rows, w["up"][expert])
    terms[at, :] = (gate * dot(act.astype(BF16), w["down"][expert])).astype(BF16)


def step_kernel(
    tile_count,
    te_ref, tk_ref, hid, pos, k_cache, v_cache, ids, wq_h, wk_h, wv_h, wo_h, a_gain, m_gain, f_gain, cos_ref, sin_ref, w_r, wg_h, wu_h, wd_h, tri,
    out, kn_out, vn_out,
    n_buf, hin, mid, ho, k_buf, v_buf, wq, wk, wv, wo, wg, wu, wd, part, own, xsum, rb1, rb2, picks, terms, q3, k3, v3, o3, kn, vn, rank_ref, gate_ref,
    w_sem, hin_sem, kv_sem, new_sem, dx_send, dx_recv, dc_send, dc_recv, dr_send, dr_recv, r1_send, r1_recv, r2_send, r2_recv, hop_send, out_loc, out_recv, credit,
):
    chunks, tokens = hid.shape[0], hid.shape[1]
    gathered = 4 * tokens
    dp = lax.axis_index("dp")
    pp = lax.axis_index("pp")
    ep = lax.axis_index("ep")
    other_pp = (dp, 1 - pp, ep)
    across = (dp, pp, lax.rem(ep + 2, 4))
    beside = (dp, pp, ep + 1 - 2 * lax.rem(ep, 2))
    first = ep * 8

    barrier = pltpu.get_barrier_semaphore()
    for peer in (other_pp, across, beside):
        pl.semaphore_signal(barrier, inc=1, device_id=peer, device_id_type=MESH)
    pl.semaphore_wait(barrier, 3)

    attn_w = [(wq_h, wq), (wk_h, wk), (wv_h, wv), (wo_h, wo)]
    moe_w = [(wg_h, wg), (wu_h, wu), (wd_h, wd)]
    weight_copies = [pltpu.make_async_copy(s, d, w_sem.at[j]) for j, (s, d) in enumerate(attn_w + moe_w)]

    def hin_copy(c):
        return pltpu.make_async_copy(hid.at[c], hin.at[lax.rem(c, HIN_SLOTS)], hin_sem.at[lax.rem(c, HIN_SLOTS)])

    def kv_copies(c):
        return (pltpu.make_async_copy(k_cache.at[c], k_buf, kv_sem.at[0]), pltpu.make_async_copy(v_cache.at[c], v_buf, kv_sem.at[1]))

    def new_copies(c):
        return (pltpu.make_async_copy(kn, kn_out.at[c], new_sem.at[0]), pltpu.make_async_copy(vn, vn_out.at[c], new_sem.at[1]))

    def remote(src, dst, send, recv, peer):
        return pltpu.make_async_remote_copy(src_ref=src, dst_ref=dst, send_sem=send, recv_sem=recv, device_id=peer, device_id_type=MESH)

    def rows_at(slot, part_idx):
        return n_buf.at[slot, pl.ds(part_idx * tokens, tokens)]

    def dx_copy(c):
        s = lax.rem(c, 3)
        return remote(rows_at(s, 0), rows_at(s, 1), dx_send.at[s], dx_recv.at[s], across)

    def dc_copy(c):
        s = lax.rem(c, 3)
        return remote(rows_at(s, 0), rows_at(s, 2), dc_send.at[s], dc_recv.at[s], beside)

    def dr_copy(c):
        s = lax.rem(c, 3)
        return remote(rows_at(s, 1), rows_at(s, 3), dr_send.at[s], dr_recv.at[s], beside)

    def r1_copy(c):
        s = lax.rem(c, 2)
        return remote(part.at[pl.ds(2 * tokens, 2 * tokens)], rb1.at[s], r1_send.at[s], r1_recv.at[s], beside)

    def r2_copy(c):
        s = lax.rem(c, 3)
        return remote(xsum, rb2.at[s], r2_send.at[s], r2_recv.at[s], across)

    def hop_copy(c):
        s = lax.rem(c, 2)
        h = lax.rem(c, HIN_SLOTS)
        return remote(ho.at[s], hin.at[h], hop_send.at[s], hin_sem.at[h], other_pp)

    def out_copy(c):
        s = lax.rem(c, 2)
        return remote(ho.at[s], out.at[c], hop_send.at[s], out_recv.at[c], other_pp)

    def out_local(c):
        s = lax.rem(c, 2)
        return pltpu.make_async_copy(ho.at[s], out.at[c], out_loc.at[s])

    for copy in weight_copies[:3]:
        copy.start()

    @pl.when(pp == 0)
    def _():
        hin_copy(0).start()

    for copy in kv_copies(0):
        copy.start()
    for copy in weight_copies[3:]:
        copy.start()

    @pl.when(pp == 0)
    def _():
        hin_copy(1).start()

    w = {"a_gain": a_gain, "cos": cos_ref, "sin": sin_ref, "q": wq, "k": wk, "v": wv, "gate": wg, "up": wu, "down": wd}

    def project(c):
        hin_copy(c).wait()

        @pl.when(c == 0)
        def _():
            for copy in weight_copies[:3]:
                copy.wait()

        @pl.when(jnp.logical_and(pp == 0, c + 2 < chunks))
        def _():
            hin_copy(c + 2).start()

        @pl.when(c > 0)
        def _():
            for copy in new_copies(c - 1):
                copy.wait()

        attn_project(hin[lax.rem(c, HIN_SLOTS)], pos[c], w, q3, k3, v3)
        kn[...] = k3[...][:, :, :64].astype(BF16)
        vn[...] = v3[...][:, :, :64].astype(BF16)
        for copy in new_copies(c):
            copy.start()

    def reduce_pair(c):
        copy = r1_copy(c)
        copy.wait_send()
        copy.wait_recv()
        s = lax.rem(c, 2)
        xsum[...] = part[pl.ds(tokens, tokens), :] + rb1[s, pl.ds(tokens, tokens), :]
        r2_copy(c).start()
        own[...] = part[pl.ds(0, tokens), :] + rb1[s, pl.ds(0, tokens), :]

    def relay(c):
        copy = dx_copy(c)
        copy.wait_recv()
        dr_copy(c).start()
        copy.wait_send()
        dc_copy(c).wait_send()

    def attend(c):
        for copy in kv_copies(c):
            copy.wait()

        def body(idx, carry):
            attn_group(idx, q3, k3, v3, o3, pos.at[c], k_buf, v_buf)
            return carry

        lax.fori_loop(0, tokens // GROUP, body, 0)

        @pl.when(c + 1 < chunks)
        def _():
            for copy in kv_copies(c + 1):
                copy.start()

        @pl.when(c == 0)
        def _():
            weight_copies[3].wait()

        hidden = hin[lax.rem(c, HIN_SLOTS)].astype(F32)
        attn_out = o3[...].reshape(tokens, 1024).astype(BF16)
        new_mid = (hidden + dot(attn_out, wo[...])).astype(BF16)
        mid[lax.rem(c, 3)] = new_mid
        n_buf[lax.rem(c, 3), pl.ds(0, tokens), :] = rms(new_mid.astype(F32), m_gain[...].astype(F32))
        dx_copy(c).start()
        dc_copy(c).start()

        @pl.when(jnp.logical_and(pp == 1, c + HIN_SLOTS < chunks))
        def _():
            pl.semaphore_signal(credit, inc=1, device_id=other_pp, device_id_type=MESH)

    def experts(c):
        s = lax.rem(c, 3)
        dc_copy(c).wait_recv()
        relayed = dr_copy(c)
        relayed.wait_recv()
        normed = n_buf.at[s]
        moe_route(ids[c], normed[...], w_r, tri, rank_ref, gate_ref)

        @pl.when(c == 0)
        def _():
            for copy in weight_copies[4:]:
                copy.wait()

        def body(idx, carry):
            moe_tile(idx, te_ref[c, idx], tk_ref[c, idx], first, normed, rank_ref, gate_ref, w, picks, terms)
            return carry

        lax.fori_loop(0, tile_count, body, 0)

        def combine(idx, carry):
            cols = pl.ds(pl.multiple_of(idx * 256, 256), 256)
            part[:, cols] = dot(picks[...], terms[:, cols])
            return carry

        lax.fori_loop(0, 4, combine, 0)
        relayed.wait_send()
        r1_copy(c).start()

    def finish(c):
        s = lax.rem(c, 2)
        copy = r2_copy(c)
        copy.wait_recv()
        copy.wait_send()
        mixed = (own[...] + rb2[lax.rem(c, 3)]).astype(BF16)
        result = (mid[lax.rem(c, 3)].astype(F32) + mixed.astype(F32)).astype(BF16)

        @pl.when(pp == 0)
        def _():
            @pl.when(c >= 2)
            def _():
                hop_copy(c - 2).wait_send()

            @pl.when(c >= HIN_SLOTS)
            def _():
                pl.semaphore_wait(credit, 1)

            ho[s] = result
            hop_copy(c).start()

        @pl.when(pp == 1)
        def _():
            @pl.when(c >= 2)
            def _():
                out_copy(c - 2).wait_send()
                out_local(c - 2).wait()

            ho[s] = rms(result.astype(F32), f_gain[...].astype(F32))
            out_copy(c).start()
            out_local(c).start()

    def step(i, carry):
        @pl.when(i < chunks)
        def _():
            project(i)

        @pl.when(jnp.logical_and(i >= 1, i <= chunks))
        def _():
            relay(i - 1)

        @pl.when(i >= 2)
        def _():
            reduce_pair(i - 2)

        @pl.when(i < chunks)
        def _():
            attend(i)

        @pl.when(jnp.logical_and(i >= 1, i <= chunks))
        def _():
            experts(i - 1)

        @pl.when(i >= 2)
        def _():
            finish(i - 2)

        return carry

    lax.fori_loop(0, chunks + 2, step, 0)

    for copy in new_copies(chunks - 1):
        copy.wait()

    @pl.when(pp == 0)
    def _():
        for c in (chunks - 2, chunks - 1):
            hop_copy(c).wait_send()

        def arrived(c, carry):
            out_copy(c).wait_recv()
            return carry

        lax.fori_loop(0, chunks, arrived, 0)

    @pl.when(pp == 1)
    def _():
        for c in (chunks - 2, chunks - 1):
            out_copy(c).wait_send()
            out_local(c).wait()


def step_call(args, chunks, tokens, tile_count):
    vmem = pl.BlockSpec(memory_space=pltpu.VMEM)
    smem = pl.BlockSpec(memory_space=pltpu.SMEM)
    hbm = pl.BlockSpec(memory_space=pl.ANY)
    wide = 4 * tokens
    dma = pltpu.SemaphoreType.DMA
    return pl.pallas_call(
        functools.partial(step_kernel, tile_count),
        out_shape=(
            jax.ShapeDtypeStruct((chunks, tokens, 1024), BF16),
            jax.ShapeDtypeStruct((chunks, tokens, 8, 64), BF16),
            jax.ShapeDtypeStruct((chunks, tokens, 8, 64), BF16),
        ),
        in_specs=[smem, smem, hbm, vmem, hbm, hbm, vmem, hbm, hbm, hbm, hbm, vmem, vmem, vmem, vmem, vmem, vmem, hbm, hbm, hbm, vmem],
        out_specs=(hbm, hbm, hbm),
        scratch_shapes=[
            pltpu.VMEM((3, wide, 1024), BF16),
            pltpu.VMEM((HIN_SLOTS, tokens, 1024), BF16),
            pltpu.VMEM((3, tokens, 1024), BF16),
            pltpu.VMEM((2, tokens, 1024), BF16),
            pltpu.VMEM((tokens * 128, 64), BF16),
            pltpu.VMEM((tokens * 128, 64), BF16),
            pltpu.VMEM((1024, 1024), BF16),
            pltpu.VMEM((1024, 512), BF16),
            pltpu.VMEM((1024, 512), BF16),
            pltpu.VMEM((1024, 1024), BF16),
            pltpu.VMEM((8, 1024, 512), BF16),
            pltpu.VMEM((8, 1024, 512), BF16),
            pltpu.VMEM((8, 512, 1024), BF16),
            pltpu.VMEM((wide, 1024), F32),
            pltpu.VMEM((tokens, 1024), F32),
            pltpu.VMEM((tokens, 1024), F32),
            pltpu.VMEM((2, 2 * tokens, 1024), F32),
            pltpu.VMEM((3, tokens, 1024), F32),
            pltpu.VMEM((wide, tile_count * TILE), BF16),
            pltpu.VMEM((tile_count * TILE, 1024), BF16),
            pltpu.VMEM((tokens, 8, 128), F32),
            pltpu.VMEM((tokens, 8, 128), F32),
            pltpu.VMEM((tokens, 8, 128), F32),
            pltpu.VMEM((tokens, 8, 128), F32),
            pltpu.VMEM((tokens, 8, 64), BF16),
            pltpu.VMEM((tokens, 8, 64), BF16),
            pltpu.VMEM((32, wide), F32),
            pltpu.VMEM((32, wide), F32),
            dma((7,)), dma((HIN_SLOTS,)), dma((2,)), dma((2,)),
            dma((3,)), dma((3,)), dma((3,)), dma((3,)), dma((3,)), dma((3,)),
            dma((2,)), dma((2,)), dma((3,)), dma((3,)),
            dma((2,)), dma((2,)), dma((chunks,)),
            pltpu.SemaphoreType.REGULAR,
        ],
        compiler_params=pltpu.CompilerParams(collective_id=0, has_side_effects=True, vmem_limit_bytes=67043328),
        name="decode_step",
        cost_estimate=pl.CostEstimate(flops=2 * 10**11, bytes_accessed=2 * 10**8, transcendentals=0),
    )(*args)


def tile_tables(ids, first, tile_count):
    local = first + jnp.arange(8, dtype=jnp.int32)
    counts = jnp.sum((ids[:, None] == local[None, :, None, None]).astype(jnp.int32), axis=(2, 3))
    tiles = (counts + TILE - 1) // TILE
    ends = jnp.cumsum(tiles, axis=1)
    idx = jnp.arange(tile_count, dtype=jnp.int32)
    expert = jnp.sum((idx[None, :, None] >= ends[:, None, :]).astype(jnp.int32), axis=-1)
    safe = jnp.minimum(expert, 7)
    starts = ends - tiles
    start = jnp.sum(jnp.where(safe[:, :, None] == jnp.arange(8)[None, None, :], starts[:, None, :], 0), axis=-1)
    sub = jnp.where(expert < 8, idx[None, :] - start, 1000)
    return safe, sub.astype(jnp.int32)


def solution(mesh):
    rows_spec = ("dp", "ep")
    three_dim = P("pp", None, None)
    two_dim = P("pp", None)
    expert_spec = P("pp", "ep", None, None)
    cache_spec = P("pp", None, rows_spec, None, None, None)
    new_spec = P("pp", None, rows_spec, None, None)
    in_specs = (P(None, rows_spec, None), P(None, rows_spec), cache_spec, cache_spec, P("pp", None, rows_spec, None), three_dim, three_dim, three_dim, three_dim, two_dim, two_dim, three_dim, expert_spec, expert_spec, expert_spec, P(None))
    out_specs = (P(None, rows_spec, None), new_spec, new_spec)

    def device_fn(hidden_in, seq_pos, k_cache, v_cache, expert_ids, w_query, w_key, w_value, w_out, attn_gain, mlp_gain, w_router, w_gate, w_up, w_down, final_gain):
        ep_idx = lax.axis_index("ep")
        micro, rows = seq_pos.shape
        chunks = micro // PER_CHUNK
        tokens = PER_CHUNK * rows
        wide = 4 * tokens
        tile_count = (wide * 2 - 8) // TILE + 8
        pos = jnp.broadcast_to(seq_pos.reshape(micro * rows, 1), (micro * rows, 128)).reshape(chunks, tokens, 128)
        angles = jnp.arange(1, 17, dtype=F32)[:, None] * THETA ** (-jnp.arange(32, dtype=F32) / 32)
        cos_t = jnp.tile(jnp.cos(angles), (1, 4))
        sin_t = jnp.tile(jnp.concatenate([-jnp.sin(angles), jnp.sin(angles)], axis=1), (1, 2))
        beside = ep_idx + 1 - 2 * (ep_idx % 2)
        order = jnp.stack([ep_idx, (ep_idx + 2) % 4, beside, (beside + 2) % 4])
        ids = lax.all_gather(expert_ids[0].reshape(chunks, tokens, 8), "ep", axis=0, tiled=False)
        ids = jnp.transpose(ids[order], (1, 3, 0, 2)).reshape(chunks, 8, wide)
        te, tk = tile_tables(ids, ep_idx * 8, tile_count)
        ti = jnp.arange(wide)
        tri = (ti[:, None] < ti[None, :]).astype(BF16)
        args = (
            te, tk, hidden_in.reshape(chunks, tokens, 1024), pos, k_cache.reshape(chunks, tokens * 128, 64), v_cache.reshape(chunks, tokens * 128, 64),
            ids, w_query[0], w_key[0], w_value[0], w_out[0], attn_gain, mlp_gain, final_gain.reshape(1, -1), cos_t, sin_t, w_router[0].T,
            w_gate[0], w_up[0], w_down[0], tri,
        )
        out, k_new, v_new = step_call(args, chunks, tokens, tile_count)
        shape = (1,) + seq_pos.shape + (8, 64)
        return out.reshape(hidden_in.shape), k_new.reshape(shape), v_new.reshape(shape)

    return jax.shard_map(device_fn, mesh=mesh, in_specs=in_specs, out_specs=out_specs, check_vma=False)
```

```python
import functools

import jax
import jax.numpy as jnp
from jax import lax
from jax.experimental import pallas as pl
from jax.experimental.pallas import tpu as pltpu
from jax.sharding import PartitionSpec as P

THETA = 1000000.0
EPS = 1e-05
F32 = jnp.float32
BF16 = jnp.bfloat16
TILE = 128
GROUP = 16
GROUP_UNROLL = 4
TILE_UNROLL = 3
PER_CHUNK = 4
HIN_SLOTS = 4
MESH = pl.DeviceIdType.MESH


def rms(vals, gain_row):
    inv = lax.rsqrt(jnp.mean(vals * vals, axis=-1, keepdims=True) + EPS)
    return (vals * inv * gain_row).astype(BF16)


def dot(lhs, rhs):
    return jnp.dot(lhs, rhs, preferred_element_type=F32)


def dot_nt(lhs, rhs):
    return lax.dot_general(lhs, rhs, (((1,), (1,)), ((), ())), preferred_element_type=F32)


def rope_table(pos, table_ref):
    picked = jnp.zeros(pos.shape, F32)
    for t in range(table_ref.shape[0]):
        picked = jnp.where(pos == t + 1, table_ref[t:t + 1, :], picked)
    return picked


def rope(vals, cos_t, sin_t):
    lane = lax.broadcasted_iota(jnp.int32, (1, 128), 1)
    first = (lane % 64) < 32
    parts = []
    for j in range(vals.shape[1] // 128):
        block = vals[:, j * 128:(j + 1) * 128]
        swapped = jnp.where(first, pltpu.roll(block, 96, 1), pltpu.roll(block, 32, 1))
        parts.append(block * cos_t + swapped * sin_t)
    return jnp.concatenate(parts, axis=1)


def spread(ref, vals):
    tokens = vals.shape[0]
    for g in range(8):
        ref[pl.ds(g, tokens, stride=8), :] = vals[:, g * 128:(g + 1) * 128]


def spread_heads(ref, vals):
    tokens = vals.shape[0]
    low = lax.broadcasted_iota(jnp.int32, (1, 128), 1) < 64
    for j in range(4):
        block = vals[:, j * 128:(j + 1) * 128]
        other = pltpu.roll(block, 64, 1)
        ref[pl.ds(2 * j, tokens, stride=8), :] = jnp.where(low, block, other)
        ref[pl.ds(2 * j + 1, tokens, stride=8), :] = jnp.where(low, other, block)


def rows_of(ref, idx):
    return ref[pl.ds(pl.multiple_of(idx * GROUP * 8, GROUP * 8), GROUP * 8), :].reshape(GROUP, 8, 128)


def attn_project(hidden, pos, w, q3, k3, v3):
    normed = rms(hidden.astype(F32), w["a_gain"][...].astype(F32))
    cos_t = rope_table(pos, w["cos"])
    sin_t = rope_table(pos, w["sin"])
    k = rope(dot(normed, w["k"][...]).astype(BF16).astype(F32), cos_t, sin_t)
    spread_heads(k3, k.astype(BF16).astype(F32))
    spread_heads(v3, dot(normed, w["v"][...]).astype(BF16).astype(F32))
    q = rope(dot(normed, w["q"][...]).astype(BF16).astype(F32), cos_t, sin_t)
    spread(q3, q.astype(BF16).astype(F32))


def attn_scores(idx, q3, k3, k_rows):
    q = rows_of(q3, idx)
    lane3 = lax.broadcasted_iota(jnp.int32, (1, 1, 128), 2)
    prod = q * rows_of(k3, idx)
    self_a = jnp.sum(jnp.where(lane3 < 64, prod, 0.0), axis=-1, keepdims=True)
    self_b = jnp.sum(jnp.where(lane3 < 64, 0.0, prod), axis=-1, keepdims=True)
    self_s = jnp.concatenate([self_a, self_b], axis=1) * 0.125
    q_rows = jnp.concatenate([q, pltpu.roll(q, 64, 2)], axis=1).astype(BF16)[:, :, :64].reshape(GROUP * 16, 64)
    row0 = idx * (GROUP * 128)
    blocks = []
    for p in range(GROUP // 2):
        keys = k_rows[pl.ds(pl.multiple_of(row0 + p * 256, 256), 256), :]
        both = dot_nt(q_rows[p * 32:(p + 1) * 32], keys)
        blocks.append(both[:16, :128].reshape(1, 16, 128))
        blocks.append(both[16:, 128:].reshape(1, 16, 128))
    return jnp.concatenate(blocks, axis=0), self_s


def attn_weights(idx, scores, self_s, pos_ref):
    row_i = lax.broadcasted_iota(jnp.int32, (16, 128), 0)
    lane_i = lax.broadcasted_iota(jnp.int32, (16, 128), 1)
    step = jnp.where((row_i % 8) == (lane_i % 8), lane_i // 8, 1000)
    pos = pos_ref[pl.ds(pl.multiple_of(idx * GROUP, GROUP), GROUP), :].reshape(GROUP, 1, 128)
    scores = jnp.where(step.reshape(1, 16, 128) < pos, scores * 0.125, -jnp.inf)
    top = jnp.maximum(jnp.max(scores, axis=-1, keepdims=True), self_s)
    weights = jnp.exp(scores - top)
    self_w = jnp.exp(self_s - top)
    inv = 1.0 / (jnp.sum(weights, axis=-1, keepdims=True) + self_w)
    return (weights * inv).astype(BF16), (self_w * inv).astype(BF16).astype(F32)


def attn_mix(idx, weights, self_w, v3, o3, v_rows):
    row0 = idx * (GROUP * 128)
    zeros = jnp.zeros((16, 128), BF16)
    outs = []
    for p in range(GROUP // 2):
        vals = v_rows[pl.ds(pl.multiple_of(row0 + p * 256, 256), 256), :]
        upper = jnp.concatenate([weights[2 * p], zeros], axis=1)
        lower = jnp.concatenate([zeros, weights[2 * p + 1]], axis=1)
        outs.append(dot(jnp.concatenate([upper, lower], axis=0), vals).reshape(2, 16, 64))
    out = jnp.concatenate(outs, axis=0)
    v_new = rows_of(v3, idx)[:, :, :64]
    out_a = out[:, :8] + self_w[:, :8] * v_new
    out_b = out[:, 8:] + self_w[:, 8:] * v_new
    o3[pl.ds(pl.multiple_of(idx * GROUP * 8, GROUP * 8), GROUP * 8), :] = jnp.concatenate([out_a, out_b], axis=-1).reshape(GROUP * 8, 128)


def moe_route(ids, normed, w_r, tri, rank_ref, gate_ref):
    tokens = ids.shape[1]
    expert_i = lax.broadcasted_iota(jnp.int32, (32, tokens), 0)
    chosen = jnp.zeros((32, tokens), F32)
    for s in range(ids.shape[0]):
        chosen = jnp.where(ids[s:s + 1, :] == expert_i, 1.0, chosen)
    rank = dot(chosen.astype(BF16), tri[...])
    rank_ref[...] = jnp.where(chosen > 0.0, rank, -1.0)
    logits = dot_nt(w_r[...], normed)
    top = jnp.max(jnp.where(chosen > 0.0, logits, -jnp.inf), axis=0, keepdims=True)
    gates = jnp.where(chosen > 0.0, jnp.exp(logits - top), 0.0)
    gate_ref[...] = gates / jnp.sum(gates, axis=0, keepdims=True)


def moe_gather(j, slot, expert, sub, first, normed, rank_ref, gate_ref, picks, x_buf, g_buf):
    ranks = rank_ref[pl.ds(first + expert, 1), :]
    wanted = (lax.broadcasted_iota(jnp.int32, (TILE, 1), 0) + sub * TILE).astype(F32)
    picked = jnp.where(ranks == wanted, 1.0, 0.0)
    gate = jnp.sum(picked * gate_ref[pl.ds(first + expert, 1), :], axis=-1, keepdims=True)
    g_buf[slot] = jnp.broadcast_to(gate, (TILE, 128))
    picks[:, pl.ds(pl.multiple_of(j * TILE, TILE), TILE)] = picked.T.astype(BF16)
    x_buf[slot] = dot(picked.astype(BF16), normed[...]).astype(BF16)


def moe_expand(slot, expert, w, x_buf, a_buf):
    rows = x_buf[slot]
    a_buf[slot] = (jax.nn.silu(dot(rows, w["gate"][expert])) * dot(rows, w["up"][expert])).astype(BF16)


def moe_contract(j, slot, expert, w, a_buf, g_buf, terms):
    y = dot(a_buf[slot], w["down"][expert])
    gate = g_buf[slot]
    at = pl.ds(pl.multiple_of(j * TILE, TILE), TILE)
    for p in range(8):
        terms[at, p * 128:(p + 1) * 128] = (gate * y[:, p * 128:(p + 1) * 128]).astype(BF16)


def step_kernel(
    tile_count,
    te_ref, tk_ref, hid, pos, k_cache, v_cache, ids, wq_h, wk_h, wv_h, wo_h, a_gain, m_gain, f_gain, cos_ref, sin_ref, w_r, wg_h, wu_h, wd_h, tri,
    out, kn_out, vn_out,
    n_buf, hin, mid, ho, k_buf, v_buf, wq, wk, wv, wo, wg, wu, wd, part, own, xsum, rb1, rb2, picks, terms, x_buf, a_buf, g_buf, q3, k3, v3, o3, kn, vn, rank_ref, gate_ref,
    w_sem, hin_sem, kv_sem, new_sem, dx_send, dx_recv, dc_send, dc_recv, dr_send, dr_recv, r1_send, r1_recv, r2_send, r2_recv, hop_send, out_loc, out_recv, credit,
):
    chunks, tokens = hid.shape[0], hid.shape[1]
    gathered = 4 * tokens
    dp = lax.axis_index("dp")
    pp = lax.axis_index("pp")
    ep = lax.axis_index("ep")
    other_pp = (dp, 1 - pp, ep)
    across = (dp, pp, lax.rem(ep + 2, 4))
    beside = (dp, pp, ep + 1 - 2 * lax.rem(ep, 2))
    first = ep * 8

    barrier = pltpu.get_barrier_semaphore()
    for peer in (other_pp, across, beside):
        pl.semaphore_signal(barrier, inc=1, device_id=peer, device_id_type=MESH)
    pl.semaphore_wait(barrier, 3)

    attn_w = [(wq_h, wq), (wk_h, wk), (wv_h, wv), (wo_h, wo)]
    moe_w = [(wg_h, wg), (wu_h, wu), (wd_h, wd)]
    weight_copies = [pltpu.make_async_copy(s, d, w_sem.at[j]) for j, (s, d) in enumerate(attn_w + moe_w)]

    def hin_copy(c):
        return pltpu.make_async_copy(hid.at[c], hin.at[lax.rem(c, HIN_SLOTS)], hin_sem.at[lax.rem(c, HIN_SLOTS)])

    def kv_copies(c):
        return (pltpu.make_async_copy(k_cache.at[c], k_buf, kv_sem.at[0]), pltpu.make_async_copy(v_cache.at[c], v_buf, kv_sem.at[1]))

    def new_copies(c):
        return (pltpu.make_async_copy(kn, kn_out.at[c], new_sem.at[0]), pltpu.make_async_copy(vn, vn_out.at[c], new_sem.at[1]))

    def remote(src, dst, send, recv, peer):
        return pltpu.make_async_remote_copy(src_ref=src, dst_ref=dst, send_sem=send, recv_sem=recv, device_id=peer, device_id_type=MESH)

    def rows_at(slot, part_idx):
        return n_buf.at[slot, pl.ds(part_idx * tokens, tokens)]

    def dx_copy(c):
        s = lax.rem(c, 3)
        return remote(rows_at(s, 0), rows_at(s, 1), dx_send.at[s], dx_recv.at[s], across)

    def dc_copy(c):
        s = lax.rem(c, 3)
        return remote(rows_at(s, 0), rows_at(s, 2), dc_send.at[s], dc_recv.at[s], beside)

    def dr_copy(c):
        s = lax.rem(c, 3)
        return remote(rows_at(s, 1), rows_at(s, 3), dr_send.at[s], dr_recv.at[s], beside)

    def r1_copy(c):
        s = lax.rem(c, 2)
        return remote(part.at[pl.ds(2 * tokens, 2 * tokens)], rb1.at[s], r1_send.at[s], r1_recv.at[s], beside)

    def r2_copy(c):
        s = lax.rem(c, 3)
        return remote(xsum, rb2.at[s], r2_send.at[s], r2_recv.at[s], across)

    def hop_copy(c):
        s = lax.rem(c, 2)
        h = lax.rem(c, HIN_SLOTS)
        return remote(ho.at[s], hin.at[h], hop_send.at[s], hin_sem.at[h], other_pp)

    def out_copy(c):
        s = lax.rem(c, 2)
        return remote(ho.at[s], out.at[c], hop_send.at[s], out_recv.at[c], other_pp)

    def out_local(c):
        s = lax.rem(c, 2)
        return pltpu.make_async_copy(ho.at[s], out.at[c], out_loc.at[s])

    @pl.when(pp == 0)
    def _():
        hin_copy(0).start()

    for copy in weight_copies[:3]:
        copy.start()
    for copy in kv_copies(0):
        copy.start()
    weight_copies[3].start()

    @pl.when(pp == 0)
    def _():
        hin_copy(1).start()

    w = {"a_gain": a_gain, "cos": cos_ref, "sin": sin_ref, "q": wq, "k": wk, "v": wv, "gate": wg, "up": wu, "down": wd}

    def project(c):
        hin_copy(c).wait()

        @pl.when(c == 0)
        def _():
            for copy in weight_copies[:3]:
                copy.wait()

        @pl.when(jnp.logical_and(pp == 0, c + 2 < chunks))
        def _():
            hin_copy(c + 2).start()

        @pl.when(c > 0)
        def _():
            for copy in new_copies(c - 1):
                copy.wait()

        attn_project(hin[lax.rem(c, HIN_SLOTS)], pos[c], w, q3, k3, v3)
        kn[...] = k3[...].reshape(tokens, 8, 128)[:, :, :64].astype(BF16)
        vn[...] = v3[...].reshape(tokens, 8, 128)[:, :, :64].astype(BF16)
        for copy in new_copies(c):
            copy.start()

    def reduce_pair(c):
        copy = r1_copy(c)
        copy.wait_send()
        copy.wait_recv()
        s = lax.rem(c, 2)
        xsum[...] = part[pl.ds(tokens, tokens), :] + rb1[s, pl.ds(tokens, tokens), :]
        r2_copy(c).start()
        own[...] = part[pl.ds(0, tokens), :] + rb1[s, pl.ds(0, tokens), :]

    def relay(c):
        copy = dx_copy(c)
        copy.wait_recv()
        dr_copy(c).start()
        copy.wait_send()
        dc_copy(c).wait_send()

    def attend(c):
        for copy in kv_copies(c):
            copy.wait()

        @pl.when(c == 0)
        def _():
            for copy in weight_copies[4:]:
                copy.start()

        def body(idx, carry):
            base = idx * GROUP_UNROLL
            ahead = attn_scores(base, q3, k3, k_buf)
            for u in range(GROUP_UNROLL):
                scores = ahead
                if u + 1 < GROUP_UNROLL:
                    ahead = attn_scores(base + u + 1, q3, k3, k_buf)
                attn_mix(base + u, *attn_weights(base + u, *scores, pos.at[c]), v3, o3, v_buf)
            return carry

        lax.fori_loop(0, tokens // (GROUP * GROUP_UNROLL), body, 0)

        @pl.when(c + 1 < chunks)
        def _():
            for copy in kv_copies(c + 1):
                copy.start()

        @pl.when(c == 0)
        def _():
            weight_copies[3].wait()

        hidden = hin[lax.rem(c, HIN_SLOTS)].astype(F32)
        attn_out = jnp.concatenate([o3[pl.ds(g, tokens, stride=8), :].astype(BF16) for g in range(8)], axis=1)
        new_mid = (hidden + dot(attn_out, wo[...])).astype(BF16)
        mid[lax.rem(c, 3)] = new_mid
        n_buf[lax.rem(c, 3), pl.ds(0, tokens), :] = rms(new_mid.astype(F32), m_gain[...].astype(F32))
        dx_copy(c).start()
        dc_copy(c).start()

        @pl.when(jnp.logical_and(pp == 1, c + HIN_SLOTS < chunks))
        def _():
            pl.semaphore_signal(credit, inc=1, device_id=other_pp, device_id_type=MESH)

    def experts(c):
        s = lax.rem(c, 3)
        dc_copy(c).wait_recv()
        relayed = dr_copy(c)
        relayed.wait_recv()
        normed = n_buf.at[s]
        moe_route(ids[c], normed[...], w_r, tri, rank_ref, gate_ref)

        @pl.when(c == 0)
        def _():
            for copy in weight_copies[4:]:
                copy.wait()

        def gather(j, slot):
            moe_gather(j, slot, te_ref[c, j], tk_ref[c, j], first, normed, rank_ref, gate_ref, picks, x_buf, g_buf)

        def expand(j, slot):
            moe_expand(slot, te_ref[c, j], w, x_buf, a_buf)

        def contract(j, slot):
            moe_contract(j, slot, te_ref[c, j], w, a_buf, g_buf, terms)

        last = tile_count // TILE_UNROLL

        def body(idx, carry):
            base = idx * TILE_UNROLL
            expand(base, 0)
            gather(base + 1, 1)
            for u in range(1, TILE_UNROLL):
                expand(base + u, u)
                if u + 1 < TILE_UNROLL:
                    gather(base + u + 1, u + 1)
                else:
                    gather(lax.rem(base + TILE_UNROLL, tile_count), 0)
                contract(base + u - 1, u - 1)
            contract(base + TILE_UNROLL - 1, TILE_UNROLL - 1)
            return carry

        gather(0, 0)
        lax.fori_loop(0, last, body, 0)
        half = 2 * tokens
        part[pl.ds(half, half), :] = dot(picks[pl.ds(half, half), :], terms[...])
        relayed.wait_send()
        r1_copy(c).start()
        part[pl.ds(0, half), :] = dot(picks[pl.ds(0, half), :], terms[...])

    def finish(c):
        s = lax.rem(c, 2)
        copy = r2_copy(c)
        copy.wait_recv()
        copy.wait_send()
        mixed = (own[...] + rb2[lax.rem(c, 3)]).astype(BF16)
        result = (mid[lax.rem(c, 3)].astype(F32) + mixed.astype(F32)).astype(BF16)

        @pl.when(pp == 0)
        def _():
            @pl.when(c >= 2)
            def _():
                hop_copy(c - 2).wait_send()

            @pl.when(c >= HIN_SLOTS)
            def _():
                pl.semaphore_wait(credit, 1)

            ho[s] = result
            hop_copy(c).start()

        @pl.when(pp == 1)
        def _():
            @pl.when(c >= 2)
            def _():
                out_copy(c - 2).wait_send()
                out_local(c - 2).wait()

            ho[s] = rms(result.astype(F32), f_gain[...].astype(F32))
            out_copy(c).start()
            out_local(c).start()

    def step(i, carry):
        @pl.when(i < chunks)
        def _():
            project(i)

        @pl.when(jnp.logical_and(i >= 1, i <= chunks))
        def _():
            relay(i - 1)

        @pl.when(i >= 2)
        def _():
            reduce_pair(i - 2)

        @pl.when(i < chunks)
        def _():
            attend(i)

        @pl.when(jnp.logical_and(i >= 1, i <= chunks))
        def _():
            experts(i - 1)

        @pl.when(i >= 2)
        def _():
            finish(i - 2)

        return carry

    lax.fori_loop(0, chunks + 2, step, 0)

    for copy in new_copies(chunks - 1):
        copy.wait()

    @pl.when(pp == 0)
    def _():
        for c in (chunks - 2, chunks - 1):
            hop_copy(c).wait_send()

        def arrived(c, carry):
            out_copy(c).wait_recv()
            return carry

        lax.fori_loop(0, chunks, arrived, 0)

    @pl.when(pp == 1)
    def _():
        for c in (chunks - 2, chunks - 1):
            out_copy(c).wait_send()
            out_local(c).wait()


def step_call(args, chunks, tokens, tile_count):
    vmem = pl.BlockSpec(memory_space=pltpu.VMEM)
    smem = pl.BlockSpec(memory_space=pltpu.SMEM)
    hbm = pl.BlockSpec(memory_space=pl.ANY)
    wide = 4 * tokens
    dma = pltpu.SemaphoreType.DMA
    return pl.pallas_call(
        functools.partial(step_kernel, tile_count),
        out_shape=(
            jax.ShapeDtypeStruct((chunks, tokens, 1024), BF16),
            jax.ShapeDtypeStruct((chunks, tokens, 8, 64), BF16),
            jax.ShapeDtypeStruct((chunks, tokens, 8, 64), BF16),
        ),
        in_specs=[smem, smem, hbm, vmem, hbm, hbm, vmem, hbm, hbm, hbm, hbm, vmem, vmem, vmem, vmem, vmem, vmem, hbm, hbm, hbm, vmem],
        out_specs=(hbm, hbm, hbm),
        scratch_shapes=[
            pltpu.VMEM((3, wide, 1024), BF16),
            pltpu.VMEM((HIN_SLOTS, tokens, 1024), BF16),
            pltpu.VMEM((3, tokens, 1024), BF16),
            pltpu.VMEM((2, tokens, 1024), BF16),
            pltpu.VMEM((tokens * 128, 64), BF16),
            pltpu.VMEM((tokens * 128, 64), BF16),
            pltpu.VMEM((1024, 1024), BF16),
            pltpu.VMEM((1024, 512), BF16),
            pltpu.VMEM((1024, 512), BF16),
            pltpu.VMEM((1024, 1024), BF16),
            pltpu.VMEM((8, 1024, 512), BF16),
            pltpu.VMEM((8, 1024, 512), BF16),
            pltpu.VMEM((8, 512, 1024), BF16),
            pltpu.VMEM((wide, 1024), F32),
            pltpu.VMEM((tokens, 1024), F32),
            pltpu.VMEM((tokens, 1024), F32),
            pltpu.VMEM((2, 2 * tokens, 1024), F32),
            pltpu.VMEM((3, tokens, 1024), F32),
            pltpu.VMEM((wide, tile_count * TILE), BF16),
            pltpu.VMEM((tile_count * TILE, 1024), BF16),
            pltpu.VMEM((TILE_UNROLL, TILE, 1024), BF16),
            pltpu.VMEM((TILE_UNROLL, TILE, 512), BF16),
            pltpu.VMEM((TILE_UNROLL, TILE, 128), F32),
            pltpu.VMEM((tokens * 8, 128), F32),
            pltpu.VMEM((tokens * 8, 128), F32),
            pltpu.VMEM((tokens * 8, 128), F32),
            pltpu.VMEM((tokens * 8, 128), F32),
            pltpu.VMEM((tokens, 8, 64), BF16),
            pltpu.VMEM((tokens, 8, 64), BF16),
            pltpu.VMEM((32, wide), F32),
            pltpu.VMEM((32, wide), F32),
            dma((7,)), dma((HIN_SLOTS,)), dma((2,)), dma((2,)),
            dma((3,)), dma((3,)), dma((3,)), dma((3,)), dma((3,)), dma((3,)),
            dma((2,)), dma((2,)), dma((3,)), dma((3,)),
            dma((2,)), dma((2,)), dma((chunks,)),
            pltpu.SemaphoreType.REGULAR,
        ],
        compiler_params=pltpu.CompilerParams(collective_id=0, has_side_effects=True, vmem_limit_bytes=67043328),
        name="decode_step",
        cost_estimate=pl.CostEstimate(flops=2 * 10**11, bytes_accessed=2 * 10**8, transcendentals=0),
    )(*args)


def tile_tables(ids, first, tile_count):
    local = first + jnp.arange(8, dtype=jnp.int32)
    counts = jnp.sum((ids[:, None] == local[None, :, None, None]).astype(jnp.int32), axis=(2, 3))
    tiles = (counts + TILE - 1) // TILE
    ends = jnp.cumsum(tiles, axis=1)
    idx = jnp.arange(tile_count, dtype=jnp.int32)
    expert = jnp.sum((idx[None, :, None] >= ends[:, None, :]).astype(jnp.int32), axis=-1)
    safe = jnp.minimum(expert, 7)
    starts = ends - tiles
    start = jnp.sum(jnp.where(safe[:, :, None] == jnp.arange(8)[None, None, :], starts[:, None, :], 0), axis=-1)
    sub = jnp.where(expert < 8, idx[None, :] - start, 1000)
    return safe, sub.astype(jnp.int32)


def solution(mesh):
    rows_spec = ("dp", "ep")
    three_dim = P("pp", None, None)
    two_dim = P("pp", None)
    expert_spec = P("pp", "ep", None, None)
    cache_spec = P("pp", None, rows_spec, None, None, None)
    new_spec = P("pp", None, rows_spec, None, None)
    in_specs = (P(None, rows_spec, None), P(None, rows_spec), cache_spec, cache_spec, P("pp", None, rows_spec, None), three_dim, three_dim, three_dim, three_dim, two_dim, two_dim, three_dim, expert_spec, expert_spec, expert_spec, P(None))
    out_specs = (P(None, rows_spec, None), new_spec, new_spec)

    def device_fn(hidden_in, seq_pos, k_cache, v_cache, expert_ids, w_query, w_key, w_value, w_out, attn_gain, mlp_gain, w_router, w_gate, w_up, w_down, final_gain):
        ep_idx = lax.axis_index("ep")
        micro, rows = seq_pos.shape
        chunks = micro // PER_CHUNK
        tokens = PER_CHUNK * rows
        wide = 4 * tokens
        tile_count = (wide * 2 - 8) // TILE + 8
        pos = jnp.broadcast_to(seq_pos.reshape(micro * rows, 1), (micro * rows, 128)).reshape(chunks, tokens, 128)
        angles = jnp.arange(1, 17, dtype=F32)[:, None] * THETA ** (-jnp.arange(32, dtype=F32) / 32)
        cos_t = jnp.tile(jnp.cos(angles), (1, 4))
        sin_t = jnp.tile(jnp.concatenate([-jnp.sin(angles), jnp.sin(angles)], axis=1), (1, 2))
        beside = ep_idx + 1 - 2 * (ep_idx % 2)
        order = jnp.stack([ep_idx, (ep_idx + 2) % 4, beside, (beside + 2) % 4])
        ids = lax.all_gather(expert_ids[0].reshape(chunks, tokens, 8), "ep", axis=0, tiled=False)
        ids = jnp.transpose(ids[order], (1, 3, 0, 2)).reshape(chunks, 8, wide)
        te, tk = tile_tables(ids, ep_idx * 8, tile_count)
        ti = jnp.arange(wide)
        tri = (ti[:, None] < ti[None, :]).astype(BF16)
        args = (
            te, tk, hidden_in.reshape(chunks, tokens, 1024), pos, k_cache.reshape(chunks, tokens * 128, 64), v_cache.reshape(chunks, tokens * 128, 64),
            ids, w_query[0], w_key[0], w_value[0], w_out[0], attn_gain, mlp_gain, final_gain.reshape(1, -1), cos_t, sin_t, w_router[0].T,
            w_gate[0], w_up[0], w_down[0], tri,
        )
        out, k_new, v_new = step_call(args, chunks, tokens, tile_count)
        shape = (1,) + seq_pos.shape + (8, 64)
        return out.reshape(hidden_in.shape), k_new.reshape(shape), v_new.reshape(shape)

    return jax.shard_map(device_fn, mesh=mesh, in_specs=in_specs, out_specs=out_specs, check_vma=False)
```

```python
import functools

import jax
import jax.numpy as jnp
import numpy as np
from jax import lax
from jax.experimental import pallas as pl
from jax.experimental.pallas import tpu as pltpu
from jax.sharding import PartitionSpec as P

THETA = 1000000.0
EPS = 1e-05
F32 = jnp.float32
BF16 = jnp.bfloat16
TILE = 128
GROUP = 16
GROUP_UNROLL = 4
TILE_UNROLL = 3
PER_CHUNK = 4
HIN_SLOTS = 4
PIECES = 4
MESH = pl.DeviceIdType.MESH


def rms(vals, gain_row):
    inv = lax.rsqrt(jnp.mean(vals * vals, axis=-1, keepdims=True) + EPS)
    return (vals * inv * gain_row).astype(BF16)


def dot(lhs, rhs):
    return jnp.dot(lhs, rhs, preferred_element_type=F32)


def dot_nt(lhs, rhs):
    return lax.dot_general(lhs, rhs, (((1,), (1,)), ((), ())), preferred_element_type=F32)


def rope_table(pos, table_ref):
    picked = jnp.zeros(pos.shape, F32)
    for t in range(table_ref.shape[0]):
        picked = jnp.where(pos == float(t + 1), table_ref[t:t + 1, :], picked)
    return picked


def rope(vals, cos_t, sin_t):
    lane = lax.broadcasted_iota(jnp.int32, (1, 128), 1)
    first = (lane % 64) < 32
    parts = []
    for j in range(vals.shape[1] // 128):
        block = vals[:, j * 128:(j + 1) * 128]
        swapped = jnp.where(first, pltpu.roll(block, 96, 1), pltpu.roll(block, 32, 1))
        parts.append(block * cos_t + swapped * sin_t)
    return jnp.concatenate(parts, axis=1)


def spread(ref, vals):
    tokens = vals.shape[0]
    for g in range(8):
        ref[pl.ds(g, tokens, stride=8), :] = vals[:, g * 128:(g + 1) * 128]


def spread_heads(ref, vals):
    tokens = vals.shape[0]
    low = lax.broadcasted_iota(jnp.int32, (1, 128), 1) < 64
    for j in range(4):
        block = vals[:, j * 128:(j + 1) * 128]
        other = pltpu.roll(block, 64, 1)
        ref[pl.ds(2 * j, tokens, stride=8), :] = jnp.where(low, block, other)
        ref[pl.ds(2 * j + 1, tokens, stride=8), :] = jnp.where(low, other, block)


def rows_of(ref, idx):
    return ref[pl.ds(pl.multiple_of(idx * GROUP * 8, GROUP * 8), GROUP * 8), :].reshape(GROUP, 8, 128)


def attn_project(hidden, pos, w, q3, k3, v3):
    normed = rms(hidden.astype(F32), w["a_gain"][...].astype(F32))
    cos_t = rope_table(pos, w["cos"])
    sin_t = rope_table(pos, w["sin"])
    k = rope(dot(normed, w["k"][...]).astype(BF16).astype(F32), cos_t, sin_t)
    spread_heads(k3, k.astype(BF16).astype(F32))
    spread_heads(v3, dot(normed, w["v"][...]).astype(BF16).astype(F32))
    q = rope(dot(normed, w["q"][...]).astype(BF16).astype(F32), cos_t, sin_t)
    spread(q3, q.astype(BF16).astype(F32))


def attn_scores(idx, q3, k3, k_rows):
    q = rows_of(q3, idx)
    lane3 = lax.broadcasted_iota(jnp.int32, (1, 1, 128), 2)
    prod = q * rows_of(k3, idx)
    self_a = jnp.sum(jnp.where(lane3 < 64, prod, 0.0), axis=-1, keepdims=True)
    self_b = jnp.sum(jnp.where(lane3 < 64, 0.0, prod), axis=-1, keepdims=True)
    self_s = jnp.concatenate([self_a, self_b], axis=1) * 0.125
    q_rows = jnp.concatenate([q, pltpu.roll(q, 64, 2)], axis=1).astype(BF16)[:, :, :64].reshape(GROUP * 16, 64)
    row0 = idx * (GROUP * 128)
    blocks = []
    for p in range(GROUP // 2):
        keys = k_rows[pl.ds(pl.multiple_of(row0 + p * 256, 256), 256), :]
        both = dot_nt(q_rows[p * 32:(p + 1) * 32], keys)
        blocks.append(both[:16, :128].reshape(1, 16, 128))
        blocks.append(both[16:, 128:].reshape(1, 16, 128))
    return jnp.concatenate(blocks, axis=0), self_s


def attn_weights(idx, scores, self_s, pos_ref):
    row_i = lax.broadcasted_iota(jnp.int32, (16, 128), 0)
    lane_i = lax.broadcasted_iota(jnp.int32, (16, 128), 1)
    step = jnp.where((row_i % 8) == (lane_i % 8), lane_i // 8, 1000).astype(F32)
    pos = pos_ref[pl.ds(pl.multiple_of(idx * GROUP, GROUP), GROUP), :].reshape(GROUP, 1, 128)
    scores = jnp.where(step.reshape(1, 16, 128) < pos, scores * 0.125, -jnp.inf)
    top = jnp.maximum(jnp.max(scores, axis=-1, keepdims=True), self_s)
    weights = jnp.exp(scores - top)
    self_w = jnp.exp(self_s - top)
    inv = 1.0 / (jnp.sum(weights, axis=-1, keepdims=True) + self_w)
    return (weights * inv).astype(BF16), (self_w * inv).astype(BF16).astype(F32)


def attn_mix(idx, weights, self_w, v3, o3, v_rows):
    row0 = idx * (GROUP * 128)
    zeros = jnp.zeros((16, 128), BF16)
    outs = []
    for p in range(GROUP // 2):
        vals = v_rows[pl.ds(pl.multiple_of(row0 + p * 256, 256), 256), :]
        upper = jnp.concatenate([weights[2 * p], zeros], axis=1)
        lower = jnp.concatenate([zeros, weights[2 * p + 1]], axis=1)
        outs.append(dot(jnp.concatenate([upper, lower], axis=0), vals).reshape(2, 16, 64))
    out = jnp.concatenate(outs, axis=0)
    v_new = rows_of(v3, idx)[:, :, :64]
    out_a = out[:, :8] + self_w[:, :8] * v_new
    out_b = out[:, 8:] + self_w[:, 8:] * v_new
    o3[pl.ds(pl.multiple_of(idx * GROUP * 8, GROUP * 8), GROUP * 8), :] = jnp.concatenate([out_a, out_b], axis=-1).reshape(GROUP * 8, 128)


def plan_tiles(ids, first, tri, member_ref, rank_ref, table_ref):
    tokens = ids.shape[1]
    expert_i = lax.broadcasted_iota(jnp.int32, (32, tokens), 0)
    chosen = jnp.zeros((32, tokens), F32)
    for s in range(ids.shape[0]):
        chosen = jnp.where(ids[s:s + 1, :] == expert_i, 1.0, chosen)
    member_ref[...] = chosen
    rank = dot(chosen.astype(BF16), tri[...])
    rank_ref[...] = jnp.where(chosen > 0.0, rank, -1.0)
    local = member_ref[pl.ds(pl.multiple_of(first, 8), 8), :]
    counts = jnp.sum(local, axis=-1, keepdims=True).astype(jnp.int32)
    tiles = jnp.broadcast_to(lax.shift_right_logical(counts + (TILE - 1), 7), (8, 128))
    lane = lax.broadcasted_iota(jnp.int32, (1, 128), 1)
    end = jnp.zeros((1, 128), jnp.int32)
    start = jnp.zeros((1, 128), jnp.int32)
    expert = jnp.zeros((1, 128), jnp.int32)
    for e in range(8):
        end = end + tiles[e:e + 1, :]
        passed = lane >= end
        expert = jnp.where(passed, expert + 1, expert)
        start = jnp.where(passed, end, start)
    sub = jnp.where(expert < 8, lane - start, 1000)
    table_ref[0:1, :] = jnp.minimum(expert, 7)
    table_ref[1:2, :] = sub


def moe_gates(normed, w_r, rank_ref, gate_ref):
    chosen = rank_ref[...] >= 0.0
    logits = dot_nt(w_r[...], normed)
    top = jnp.max(jnp.where(chosen, logits, -jnp.inf), axis=0, keepdims=True)
    gates = jnp.where(chosen, jnp.exp(logits - top), 0.0)
    gate_ref[...] = gates / jnp.sum(gates, axis=0, keepdims=True)


def moe_gather(j, slot, expert, sub, first, normed, rank_ref, gate_ref, picks, x_buf, g_buf):
    ranks = rank_ref[pl.ds(first + expert, 1), :]
    wanted = (lax.broadcasted_iota(jnp.int32, (TILE, 1), 0) + sub * TILE).astype(F32)
    picked = jnp.where(ranks == wanted, 1.0, 0.0)
    gate = jnp.sum(picked * gate_ref[pl.ds(first + expert, 1), :], axis=-1, keepdims=True)
    g_buf[slot] = jnp.broadcast_to(gate, (TILE, 128))
    picks[:, pl.ds(pl.multiple_of(j * TILE, TILE), TILE)] = picked.T.astype(BF16)
    x_buf[slot] = dot(picked.astype(BF16), normed[...]).astype(BF16)


def moe_expand(slot, expert, w, x_buf, a_buf):
    rows = x_buf[slot]
    a_buf[slot] = (jax.nn.silu(dot(rows, w["gate"][expert])) * dot(rows, w["up"][expert])).astype(BF16)


def moe_contract(j, slot, expert, w, a_buf, g_buf, terms):
    y = dot(a_buf[slot], w["down"][expert])
    gate = g_buf[slot]
    at = pl.ds(pl.multiple_of(j * TILE, TILE), TILE)
    for p in range(8):
        terms[at, p * 128:(p + 1) * 128] = (gate * y[:, p * 128:(p + 1) * 128]).astype(BF16)


def step_kernel(
    tile_count,
    hid, seq, k_cache, v_cache, ids_own, wq_h, wk_h, wv_h, wo_h, a_gain, m_gain, f_gain, cos_ref, sin_ref, w_r, wg_h, wu_h, wd_h, tri,
    out, kn_out, vn_out,
    n_buf, hin, mid, ho, k_buf, v_buf, wq, wk, wv, wo, wg, wu, wd, part, own, xsum, rb1, rb2, picks, terms, x_buf, a_buf, g_buf, q3, k3, v3, o3, kn, vn, rank_buf, gate_ref, member, pos, ids, table, smem_table,
    w_sem, ids_send, ids_recv, table_sem, hin_sem, kv_sem, new_sem, dx_send, dx_recv, dc_send, dc_recv, dr_send, dr_recv, r1_send, r1_recv, r2_send, r2_recv, hop_send, out_loc, out_recv, credit,
):
    chunks, tokens = hid.shape[0], hid.shape[1]
    gathered = 4 * tokens
    dp = lax.axis_index("dp")
    pp = lax.axis_index("pp")
    ep = lax.axis_index("ep")
    other_pp = (dp, 1 - pp, ep)
    across = (dp, pp, lax.rem(ep + 2, 4))
    beside = (dp, pp, ep + 1 - 2 * lax.rem(ep, 2))
    first = ep * 8

    diagonal = (dp, pp, lax.rem(ep + 3 - 2 * lax.rem(ep, 2), 4))

    barrier = pltpu.get_barrier_semaphore()
    for peer in (other_pp, across, beside, diagonal):
        pl.semaphore_signal(barrier, inc=1, device_id=peer, device_id_type=MESH)
    pl.semaphore_wait(barrier, 4)

    attn_w = [(wq_h, wq), (wk_h, wk), (wv_h, wv), (wo_h, wo)]
    moe_w = [(wg_h, wg), (wu_h, wu), (wd_h, wd)]
    weight_copies = [pltpu.make_async_copy(s, d, w_sem.at[j]) for j, (s, d) in enumerate(attn_w + moe_w)]

    def hin_copies(c):
        h = lax.rem(c, HIN_SLOTS)
        return [pltpu.make_async_copy(hid.at[c, piece(p)], hin.at[h, piece(p)], hin_sem.at[h, p]) for p in range(PIECES)]

    def kv_copies(c):
        return (pltpu.make_async_copy(k_cache.at[c], k_buf, kv_sem.at[0]), pltpu.make_async_copy(v_cache.at[c], v_buf, kv_sem.at[1]))

    def new_copies(c):
        return (pltpu.make_async_copy(kn, kn_out.at[c], new_sem.at[0]), pltpu.make_async_copy(vn, vn_out.at[c], new_sem.at[1]))

    def remote(src, dst, send, recv, peer):
        return pltpu.make_async_remote_copy(src_ref=src, dst_ref=dst, send_sem=send, recv_sem=recv, device_id=peer, device_id_type=MESH)

    def rows_at(slot, part_idx):
        return n_buf.at[slot, pl.ds(part_idx * tokens, tokens)]

    def dx_copy(c):
        s = lax.rem(c, 3)
        return remote(rows_at(s, 0), rows_at(s, 1), dx_send.at[s], dx_recv.at[s], across)

    def dc_copy(c):
        s = lax.rem(c, 3)
        return remote(rows_at(s, 0), rows_at(s, 2), dc_send.at[s], dc_recv.at[s], beside)

    def dr_copy(c):
        s = lax.rem(c, 3)
        return remote(rows_at(s, 1), rows_at(s, 3), dr_send.at[s], dr_recv.at[s], beside)

    def r1_copy(c):
        s = lax.rem(c, 2)
        return remote(part.at[pl.ds(2 * tokens, 2 * tokens)], rb1.at[s], r1_send.at[s], r1_recv.at[s], beside)

    rows = tokens // PIECES

    def piece(p):
        return pl.ds(p * rows, rows)

    def r2_copy(c, p):
        s = lax.rem(c, 3)
        return remote(xsum.at[piece(p)], rb2.at[s, piece(p)], r2_send.at[s, p], r2_recv.at[s, p], across)

    def hop_copy(c, p):
        s = lax.rem(c, 2)
        h = lax.rem(c, HIN_SLOTS)
        return remote(ho.at[s, piece(p)], hin.at[h, piece(p)], hop_send.at[s, p], hin_sem.at[h, p], other_pp)

    def out_copy(c, p):
        s = lax.rem(c, 2)
        return remote(ho.at[s, piece(p)], out.at[c, piece(p)], hop_send.at[s, p], out_recv.at[c, p], other_pp)

    def out_local(c, p):
        s = lax.rem(c, 2)
        return pltpu.make_async_copy(ho.at[s, piece(p)], out.at[c, piece(p)], out_loc.at[s, p])

    def ids_copies():
        return [remote(ids_own, ids.at[j], ids_send.at[j], ids_recv.at[j], peer) for j, peer in ((1, across), (2, beside), (3, diagonal))]

    def table_copy(c):
        s = lax.rem(c, 2)
        return pltpu.make_async_copy(table, smem_table.at[s], table_sem)

    for copy in ids_copies():
        copy.start()

    @pl.when(pp == 0)
    def _():
        for copy in hin_copies(0):
            copy.start()

    for copy in weight_copies[:3]:
        copy.start()
    for copy in kv_copies(0):
        copy.start()
    weight_copies[3].start()

    @pl.when(pp == 0)
    def _():
        for copy in hin_copies(1):
            copy.start()

    w = {"a_gain": a_gain, "cos": cos_ref, "sin": sin_ref, "q": wq, "k": wk, "v": wv, "gate": wg, "up": wu, "down": wd}

    def plan(c):
        @pl.when(c == 0)
        def _():
            ids[0] = ids_own[...]
            for copy in ids_copies():
                copy.wait()

        chosen_ids = jnp.concatenate([ids[j, c] for j in range(4)], axis=1)
        plan_tiles(chosen_ids, first, tri, member, rank_buf.at[lax.rem(c, 2)], table)
        table_copy(c).start()

    def project(c):
        plan(c)
        for copy in hin_copies(c):
            copy.wait()

        @pl.when(c == 0)
        def _():
            for copy in weight_copies[:3]:
                copy.wait()

        @pl.when(jnp.logical_and(pp == 0, c + 2 < chunks))
        def _():
            for copy in hin_copies(c + 2):
                copy.start()

        @pl.when(c > 0)
        def _():
            for copy in new_copies(c - 1):
                copy.wait()

        seq_row = seq[pl.ds(c, 1), :].astype(F32)
        pos[...] = jnp.broadcast_to(seq_row, (128, 128)).T
        attn_project(hin[lax.rem(c, HIN_SLOTS)], pos[...], w, q3, k3, v3)
        kn[...] = k3[...].reshape(tokens, 8, 128)[:, :, :64].astype(BF16)
        vn[...] = v3[...].reshape(tokens, 8, 128)[:, :, :64].astype(BF16)
        for copy in new_copies(c):
            copy.start()

    def reduce_pair(c):
        copy = r1_copy(c)
        copy.wait_send()
        copy.wait_recv()
        s = lax.rem(c, 2)
        xsum[...] = part[pl.ds(tokens, tokens), :] + rb1[s, pl.ds(tokens, tokens), :]
        for p in range(PIECES):
            r2_copy(c, p).start()
        own[...] = part[pl.ds(0, tokens), :] + rb1[s, pl.ds(0, tokens), :]

    def relay(c):
        copy = dx_copy(c)
        copy.wait_recv()
        dr_copy(c).start()
        copy.wait_send()
        dc_copy(c).wait_send()

    def attend(c):
        table_copy(c).wait()
        for copy in kv_copies(c):
            copy.wait()

        @pl.when(c == 0)
        def _():
            for copy in weight_copies[4:]:
                copy.start()

        def body(idx, carry):
            base = idx * GROUP_UNROLL
            ahead = attn_scores(base, q3, k3, k_buf)
            for u in range(GROUP_UNROLL):
                scores = ahead
                if u + 1 < GROUP_UNROLL:
                    ahead = attn_scores(base + u + 1, q3, k3, k_buf)
                attn_mix(base + u, *attn_weights(base + u, *scores, pos), v3, o3, v_buf)
            return carry

        lax.fori_loop(0, tokens // (GROUP * GROUP_UNROLL), body, 0)

        @pl.when(c + 1 < chunks)
        def _():
            for copy in kv_copies(c + 1):
                copy.start()

        @pl.when(c == 0)
        def _():
            weight_copies[3].wait()

        hidden = hin[lax.rem(c, HIN_SLOTS)].astype(F32)
        attn_out = jnp.concatenate([o3[pl.ds(g, tokens, stride=8), :].astype(BF16) for g in range(8)], axis=1)
        new_mid = (hidden + dot(attn_out, wo[...])).astype(BF16)
        mid[lax.rem(c, 3)] = new_mid
        n_buf[lax.rem(c, 3), pl.ds(0, tokens), :] = rms(new_mid.astype(F32), m_gain[...].astype(F32))
        dx_copy(c).start()
        dc_copy(c).start()

        @pl.when(jnp.logical_and(pp == 1, c + HIN_SLOTS < chunks))
        def _():
            pl.semaphore_signal(credit, inc=1, device_id=other_pp, device_id_type=MESH)

    def experts(c):
        s = lax.rem(c, 3)
        dc_copy(c).wait_recv()
        relayed = dr_copy(c)
        relayed.wait_recv()
        normed = n_buf.at[s]
        rank_ref = rank_buf.at[lax.rem(c, 2)]
        tile_ref = smem_table.at[lax.rem(c, 2)]
        moe_gates(normed[...], w_r, rank_ref, gate_ref)

        @pl.when(c == 0)
        def _():
            for copy in weight_copies[4:]:
                copy.wait()

        def gather(j, slot):
            moe_gather(j, slot, tile_ref[0, j], tile_ref[1, j], first, normed, rank_ref, gate_ref, picks, x_buf, g_buf)

        def expand(j, slot):
            moe_expand(slot, tile_ref[0, j], w, x_buf, a_buf)

        def contract(j, slot):
            moe_contract(j, slot, tile_ref[0, j], w, a_buf, g_buf, terms)

        last = tile_count // TILE_UNROLL

        def body(idx, carry):
            base = idx * TILE_UNROLL
            expand(base, 0)
            gather(base + 1, 1)
            for u in range(1, TILE_UNROLL):
                expand(base + u, u)
                if u + 1 < TILE_UNROLL:
                    gather(base + u + 1, u + 1)
                else:
                    gather(lax.rem(base + TILE_UNROLL, tile_count), 0)
                contract(base + u - 1, u - 1)
            contract(base + TILE_UNROLL - 1, TILE_UNROLL - 1)
            return carry

        gather(0, 0)
        lax.fori_loop(0, last, body, 0)
        half = 2 * tokens
        part[pl.ds(half, half), :] = dot(picks[pl.ds(half, half), :], terms[...])
        relayed.wait_send()
        r1_copy(c).start()
        part[pl.ds(0, half), :] = dot(picks[pl.ds(0, half), :], terms[...])

    def finish(c):
        s = lax.rem(c, 2)

        @pl.when(jnp.logical_and(pp == 0, c >= HIN_SLOTS))
        def _():
            pl.semaphore_wait(credit, 1)

        @pl.when(c >= 2)
        def _():
            for p in range(PIECES):
                @pl.when(pp == 0)
                def _():
                    hop_copy(c - 2, p).wait_send()

                @pl.when(pp == 1)
                def _():
                    out_copy(c - 2, p).wait_send()
                    out_local(c - 2, p).wait()

        for p in range(PIECES):
            r2_copy(c, p).wait_recv()
            at = piece(p)
            mixed = (own[at, :] + rb2[lax.rem(c, 3), at, :]).astype(BF16)
            result = (mid[lax.rem(c, 3), at, :].astype(F32) + mixed.astype(F32)).astype(BF16)

            @pl.when(pp == 0)
            def _():
                ho[s, at, :] = result
                hop_copy(c, p).start()

            @pl.when(pp == 1)
            def _():
                vals = result.astype(F32)
                vals = vals * lax.rsqrt(jnp.mean(vals * vals, axis=-1, keepdims=True) + EPS)
                for g in range(8):
                    ho[s, at, g * 128:(g + 1) * 128] = (vals[:, g * 128:(g + 1) * 128] * f_gain[g:g + 1, :]).astype(BF16)
                out_copy(c, p).start()
                out_local(c, p).start()

        for p in range(PIECES):
            r2_copy(c, p).wait_send()

    def step(i, carry):
        @pl.when(i < chunks)
        def _():
            project(i)

        @pl.when(jnp.logical_and(i >= 1, i <= chunks))
        def _():
            relay(i - 1)

        @pl.when(i >= 2)
        def _():
            reduce_pair(i - 2)

        @pl.when(i < chunks)
        def _():
            attend(i)

        @pl.when(jnp.logical_and(i >= 1, i <= chunks))
        def _():
            experts(i - 1)

        @pl.when(i >= 2)
        def _():
            finish(i - 2)

        return carry

    lax.fori_loop(0, chunks + 2, step, 0)

    for copy in new_copies(chunks - 1):
        copy.wait()

    @pl.when(pp == 0)
    def _():
        for c in (chunks - 2, chunks - 1):
            for p in range(PIECES):
                hop_copy(c, p).wait_send()

        def arrived(c, carry):
            for p in range(PIECES):
                out_copy(c, p).wait_recv()
            return carry

        lax.fori_loop(0, chunks, arrived, 0)

    @pl.when(pp == 1)
    def _():
        for c in (chunks - 2, chunks - 1):
            for p in range(PIECES):
                out_copy(c, p).wait_send()
                out_local(c, p).wait()


def step_call(args, chunks, tokens, tile_count):
    vmem = pl.BlockSpec(memory_space=pltpu.VMEM)
    hbm = pl.BlockSpec(memory_space=pl.ANY)
    wide = 4 * tokens
    dma = pltpu.SemaphoreType.DMA
    return pl.pallas_call(
        functools.partial(step_kernel, tile_count),
        out_shape=(
            jax.ShapeDtypeStruct((chunks, tokens, 1024), BF16),
            jax.ShapeDtypeStruct((chunks, tokens, 8, 64), BF16),
            jax.ShapeDtypeStruct((chunks, tokens, 8, 64), BF16),
        ),
        in_specs=[hbm, vmem, hbm, hbm, vmem, hbm, hbm, hbm, hbm, vmem, vmem, vmem, vmem, vmem, vmem, hbm, hbm, hbm, vmem],
        out_specs=(hbm, hbm, hbm),
        scratch_shapes=[
            pltpu.VMEM((3, wide, 1024), BF16),
            pltpu.VMEM((HIN_SLOTS, tokens, 1024), BF16),
            pltpu.VMEM((3, tokens, 1024), BF16),
            pltpu.VMEM((2, tokens, 1024), BF16),
            pltpu.VMEM((tokens * 128, 64), BF16),
            pltpu.VMEM((tokens * 128, 64), BF16),
            pltpu.VMEM((1024, 1024), BF16),
            pltpu.VMEM((1024, 512), BF16),
            pltpu.VMEM((1024, 512), BF16),
            pltpu.VMEM((1024, 1024), BF16),
            pltpu.VMEM((8, 1024, 512), BF16),
            pltpu.VMEM((8, 1024, 512), BF16),
            pltpu.VMEM((8, 512, 1024), BF16),
            pltpu.VMEM((wide, 1024), F32),
            pltpu.VMEM((tokens, 1024), F32),
            pltpu.VMEM((tokens, 1024), F32),
            pltpu.VMEM((2, 2 * tokens, 1024), F32),
            pltpu.VMEM((3, tokens, 1024), F32),
            pltpu.VMEM((wide, tile_count * TILE), BF16),
            pltpu.VMEM((tile_count * TILE, 1024), BF16),
            pltpu.VMEM((TILE_UNROLL, TILE, 1024), BF16),
            pltpu.VMEM((TILE_UNROLL, TILE, 512), BF16),
            pltpu.VMEM((TILE_UNROLL, TILE, 128), F32),
            pltpu.VMEM((tokens * 8, 128), F32),
            pltpu.VMEM((tokens * 8, 128), F32),
            pltpu.VMEM((tokens * 8, 128), F32),
            pltpu.VMEM((tokens * 8, 128), F32),
            pltpu.VMEM((tokens, 8, 64), BF16),
            pltpu.VMEM((tokens, 8, 64), BF16),
            pltpu.VMEM((2, 32, wide), F32),
            pltpu.VMEM((32, wide), F32),
            pltpu.VMEM((32, wide), F32),
            pltpu.VMEM((tokens, 128), F32),
            pltpu.VMEM((4, chunks, 8, tokens), jnp.int32),
            pltpu.VMEM((8, 128), jnp.int32),
            pltpu.SMEM((2, 8, 128), jnp.int32),
            dma((7,)), dma((4,)), dma((4,)), dma(()), dma((HIN_SLOTS, PIECES)), dma((2,)), dma((2,)),
            dma((3,)), dma((3,)), dma((3,)), dma((3,)), dma((3,)), dma((3,)),
            dma((2,)), dma((2,)), dma((3, PIECES)), dma((3, PIECES)),
            dma((2, PIECES)), dma((2, PIECES)), dma((chunks, PIECES)),
            pltpu.SemaphoreType.REGULAR,
        ],
        compiler_params=pltpu.CompilerParams(collective_id=0, has_side_effects=True, vmem_limit_bytes=67043328),
        name="decode_step",
        cost_estimate=pl.CostEstimate(flops=2 * 10**11, bytes_accessed=2 * 10**8, transcendentals=0),
    )(*args)


def solution(mesh):
    rows_spec = ("dp", "ep")
    three_dim = P("pp", None, None)
    two_dim = P("pp", None)
    expert_spec = P("pp", "ep", None, None)
    cache_spec = P("pp", None, rows_spec, None, None, None)
    new_spec = P("pp", None, rows_spec, None, None)
    in_specs = (P(None, rows_spec, None), P(None, rows_spec), cache_spec, cache_spec, P("pp", None, rows_spec, None), three_dim, three_dim, three_dim, three_dim, two_dim, two_dim, three_dim, expert_spec, expert_spec, expert_spec, P(None))
    out_specs = (P(None, rows_spec, None), new_spec, new_spec)

    def device_fn(hidden_in, seq_pos, k_cache, v_cache, expert_ids, w_query, w_key, w_value, w_out, attn_gain, mlp_gain, w_router, w_gate, w_up, w_down, final_gain):
        micro, rows = seq_pos.shape
        chunks = micro // PER_CHUNK
        tokens = PER_CHUNK * rows
        wide = 4 * tokens
        tile_count = (wide * 2 - 8) // TILE + 8
        angles = np.arange(1, 17)[:, None] * THETA ** (-np.arange(32) / 32)
        cos_t = jnp.asarray(np.tile(np.cos(angles), (1, 4)), F32)
        sin_t = jnp.asarray(np.tile(np.concatenate([-np.sin(angles), np.sin(angles)], axis=1), (1, 2)), F32)
        tri = jnp.asarray(np.triu(np.ones((wide, wide)), 1), BF16)
        ids = jnp.swapaxes(expert_ids[0].reshape(chunks, tokens, 8), 1, 2)
        args = (
            hidden_in.reshape(chunks, tokens, 1024), seq_pos.reshape(chunks, tokens), k_cache.reshape(chunks, tokens * 128, 64), v_cache.reshape(chunks, tokens * 128, 64),
            ids, w_query[0], w_key[0], w_value[0], w_out[0], attn_gain, mlp_gain, final_gain.astype(F32).reshape(8, 128), cos_t, sin_t, w_router[0].T,
            w_gate[0], w_up[0], w_down[0], tri,
        )
        out, k_new, v_new = step_call(args, chunks, tokens, tile_count)
        shape = (1,) + seq_pos.shape + (8, 64)
        return out.reshape(hidden_in.shape), k_new.reshape(shape), v_new.reshape(shape)

    return jax.shard_map(device_fn, mesh=mesh, in_specs=in_specs, out_specs=out_specs, check_vma=False)
```

```python
import functools

import jax
import jax.numpy as jnp
import numpy as np
from jax import lax
from jax.experimental import pallas as pl
from jax.experimental.pallas import tpu as pltpu
from jax.sharding import PartitionSpec as P

THETA = 1000000.0
EPS = 1e-05
F32 = jnp.float32
BF16 = jnp.bfloat16
TILE = 128
GROUP = 16
GROUP_UNROLL = 4
TILE_UNROLL = 3
PER_CHUNK = 4
HIN_SLOTS = 4
PIECES = 4
MESH = pl.DeviceIdType.MESH


def scope(name):
    return jax.named_scope(name)


def rms(vals, gain_row):
    inv = lax.rsqrt(jnp.mean(vals * vals, axis=-1, keepdims=True) + EPS)
    return (vals * inv * gain_row).astype(BF16)


def dot(lhs, rhs):
    return jnp.dot(lhs, rhs, preferred_element_type=F32)


def dot_nt(lhs, rhs):
    return lax.dot_general(lhs, rhs, (((1,), (1,)), ((), ())), preferred_element_type=F32)


def rope_table(pos, table_ref):
    picked = jnp.zeros(pos.shape, F32)
    for t in range(table_ref.shape[0]):
        picked = jnp.where(pos == float(t + 1), table_ref[t:t + 1, :], picked)
    return picked


def rope(vals, cos_t, sin_t):
    lane = lax.broadcasted_iota(jnp.int32, (1, 128), 1)
    first = (lane % 64) < 32
    parts = []
    for j in range(vals.shape[1] // 128):
        block = vals[:, j * 128:(j + 1) * 128]
        swapped = jnp.where(first, pltpu.roll(block, 96, 1), pltpu.roll(block, 32, 1))
        parts.append(block * cos_t + swapped * sin_t)
    return jnp.concatenate(parts, axis=1)


def spread(ref, vals):
    tokens = vals.shape[0]
    for g in range(8):
        ref[pl.ds(g, tokens, stride=8), :] = vals[:, g * 128:(g + 1) * 128]


def spread_heads(ref, vals):
    tokens = vals.shape[0]
    low = lax.broadcasted_iota(jnp.int32, (1, 128), 1) < 64
    for j in range(4):
        block = vals[:, j * 128:(j + 1) * 128]
        other = pltpu.roll(block, 64, 1)
        ref[pl.ds(2 * j, tokens, stride=8), :] = jnp.where(low, block, other)
        ref[pl.ds(2 * j + 1, tokens, stride=8), :] = jnp.where(low, other, block)


def rows_of(ref, idx):
    return ref[pl.ds(pl.multiple_of(idx * GROUP * 8, GROUP * 8), GROUP * 8), :].reshape(GROUP, 8, 128)


def attn_dots(hidden, w, raw):
    normed = rms(hidden.astype(F32), w["a_gain"][...].astype(F32))
    raw[1] = dot(normed, w["q"][...]).astype(BF16)
    raw[2, :, :512] = dot(normed, w["k"][...]).astype(BF16)
    raw[2, :, 512:] = dot(normed, w["v"][...]).astype(BF16)


def attn_rope(pos, w, raw, q3, k3, v3):
    cos_t = rope_table(pos, w["cos"])
    sin_t = rope_table(pos, w["sin"])
    spread(q3, rope(raw[1].astype(F32), cos_t, sin_t).astype(BF16).astype(F32))
    spread_heads(k3, rope(raw[2, :, :512].astype(F32), cos_t, sin_t).astype(BF16).astype(F32))
    spread_heads(v3, raw[2, :, 512:].astype(F32))


def attn_scores(idx, q3, k3, k_rows):
    q = rows_of(q3, idx)
    lane3 = lax.broadcasted_iota(jnp.int32, (1, 1, 128), 2)
    prod = q * rows_of(k3, idx)
    self_a = jnp.sum(jnp.where(lane3 < 64, prod, 0.0), axis=-1, keepdims=True)
    self_b = jnp.sum(jnp.where(lane3 < 64, 0.0, prod), axis=-1, keepdims=True)
    self_s = jnp.concatenate([self_a, self_b], axis=1) * 0.125
    q_rows = jnp.concatenate([q, pltpu.roll(q, 64, 2)], axis=1).astype(BF16)[:, :, :64].reshape(GROUP * 16, 64)
    row0 = idx * (GROUP * 128)
    blocks = []
    for p in range(GROUP // 2):
        keys = k_rows[pl.ds(pl.multiple_of(row0 + p * 256, 256), 256), :]
        both = dot_nt(q_rows[p * 32:(p + 1) * 32], keys)
        blocks.append(both[:16, :128].reshape(1, 16, 128))
        blocks.append(both[16:, 128:].reshape(1, 16, 128))
    return jnp.concatenate(blocks, axis=0), self_s


def attn_weights(idx, scores, self_s, pos_ref):
    row_i = lax.broadcasted_iota(jnp.int32, (16, 128), 0)
    lane_i = lax.broadcasted_iota(jnp.int32, (16, 128), 1)
    step = jnp.where((row_i % 8) == (lane_i % 8), lane_i // 8, 1000).astype(F32)
    pos = pos_ref[pl.ds(pl.multiple_of(idx * GROUP, GROUP), GROUP), :].reshape(GROUP, 1, 128)
    scores = jnp.where(step.reshape(1, 16, 128) < pos, scores * 0.125, -jnp.inf)
    top = jnp.maximum(jnp.max(scores, axis=-1, keepdims=True), self_s)
    weights = jnp.exp(scores - top)
    self_w = jnp.exp(self_s - top)
    inv = 1.0 / (jnp.sum(weights, axis=-1, keepdims=True) + self_w)
    return (weights * inv).astype(BF16), (self_w * inv).astype(BF16).astype(F32)


def attn_mix(idx, weights, self_w, v3, o3, v_rows):
    row0 = idx * (GROUP * 128)
    zeros = jnp.zeros((16, 128), BF16)
    outs = []
    for p in range(GROUP // 2):
        vals = v_rows[pl.ds(pl.multiple_of(row0 + p * 256, 256), 256), :]
        upper = jnp.concatenate([weights[2 * p], zeros], axis=1)
        lower = jnp.concatenate([zeros, weights[2 * p + 1]], axis=1)
        outs.append(dot(jnp.concatenate([upper, lower], axis=0), vals).reshape(2, 16, 64))
    out = jnp.concatenate(outs, axis=0)
    v_new = rows_of(v3, idx)[:, :, :64]
    out_a = out[:, :8] + self_w[:, :8] * v_new
    out_b = out[:, 8:] + self_w[:, 8:] * v_new
    o3[pl.ds(pl.multiple_of(idx * GROUP * 8, GROUP * 8), GROUP * 8), :] = jnp.concatenate([out_a, out_b], axis=-1).reshape(GROUP * 8, 128)


def plan_tiles(ids, first, tri, member_ref, rank_ref, table_ref):
    tokens = ids.shape[1]
    expert_i = lax.broadcasted_iota(jnp.int32, (32, tokens), 0)
    chosen = jnp.zeros((32, tokens), F32)
    for s in range(ids.shape[0]):
        chosen = jnp.where(ids[s:s + 1, :] == expert_i, 1.0, chosen)
    member_ref[...] = chosen
    rank = dot(chosen.astype(BF16), tri[...])
    rank_ref[...] = jnp.where(chosen > 0.0, rank, -1.0)
    local = member_ref[pl.ds(pl.multiple_of(first, 8), 8), :]
    counts = jnp.sum(local, axis=-1, keepdims=True).astype(jnp.int32)
    tiles = jnp.broadcast_to(lax.shift_right_logical(counts + (TILE - 1), 7), (8, 128))
    lane = lax.broadcasted_iota(jnp.int32, (1, 128), 1)
    end = jnp.zeros((1, 128), jnp.int32)
    start = jnp.zeros((1, 128), jnp.int32)
    expert = jnp.zeros((1, 128), jnp.int32)
    for e in range(8):
        end = end + tiles[e:e + 1, :]
        passed = lane >= end
        expert = jnp.where(passed, expert + 1, expert)
        start = jnp.where(passed, end, start)
    sub = jnp.where(expert < 8, lane - start, 1000)
    table_ref[0:1, :] = jnp.minimum(expert, 7)
    table_ref[1:2, :] = sub


def moe_gates(logits, rank_ref, gate_ref):
    chosen = rank_ref[...] >= 0.0
    top = jnp.max(jnp.where(chosen, logits, -jnp.inf), axis=0, keepdims=True)
    gates = jnp.where(chosen, jnp.exp(logits - top), 0.0)
    gate_ref[...] = gates / jnp.sum(gates, axis=0, keepdims=True)


def slot_of(u):
    return 0 if u == 0 else 1 + (u - 1) % 2


def moe_gather(j, u, expert, sub, first, normed, rank_ref, picks, x_buf):
    ranks = rank_ref[pl.ds(first + expert, 1), :]
    wanted = (lax.broadcasted_iota(jnp.int32, (TILE, 1), 0) + sub * TILE).astype(F32)
    picked = jnp.where(ranks == wanted, 1.0, 0.0)
    picks[:, pl.ds(pl.multiple_of(j * TILE, TILE), TILE)] = picked.T.astype(BF16)
    x_buf[slot_of(u)] = dot(picked.astype(BF16), normed[...]).astype(BF16)
    return picked


def moe_gate(picked, u, expert, first, gate_ref, g_buf):
    gate = jnp.sum(picked * gate_ref[pl.ds(first + expert, 1), :], axis=-1, keepdims=True)
    g_buf[u] = jnp.broadcast_to(gate, (TILE, 128))


def moe_expand(u, expert, w, x_buf, a_buf):
    rows = x_buf[slot_of(u)]
    a_buf[slot_of(u)] = (jax.nn.silu(dot(rows, w["gate"][expert])) * dot(rows, w["up"][expert])).astype(BF16)


def moe_contract(j, u, expert, w, a_buf, g_buf, terms):
    y = dot(a_buf[slot_of(u)], w["down"][expert])
    gate = g_buf[u]
    at = pl.ds(pl.multiple_of(j * TILE, TILE), TILE)
    for p in range(8):
        terms[at, p * 128:(p + 1) * 128] = (gate * y[:, p * 128:(p + 1) * 128]).astype(BF16)


def step_kernel(
    tile_count,
    hid, seq, k_cache, v_cache, ids_own, wq_h, wk_h, wv_h, wo_h, a_gain, m_gain, f_gain, cos_ref, sin_ref, w_r, wg_h, wu_h, wd_h, tri,
    out, kn_out, vn_out,
    n_buf, hin, mid, ho, k_buf, v_buf, wq, wk, wv, wo, wg, wu, wd, part, rb1, rb2, picks, terms, x_buf, a_buf, g_buf, q3, k3, v3, o3, kn, vn, rank_buf, gate_ref, member, pos, ids, table, smem_table,
    w_sem, ids_send, ids_recv, table_sem, hin_sem, kv_sem, new_sem, dx_send, dx_recv, dc_send, dc_recv, dr_send, dr_recv, r1_send, r1_recv, r2_send, r2_recv, hop_send, out_loc, out_recv, credit,
):
    chunks, tokens = hid.shape[0], hid.shape[1]
    gathered = 4 * tokens
    dp = lax.axis_index("dp")
    pp = lax.axis_index("pp")
    ep = lax.axis_index("ep")
    other_pp = (dp, 1 - pp, ep)
    across = (dp, pp, lax.rem(ep + 2, 4))
    beside = (dp, pp, ep + 1 - 2 * lax.rem(ep, 2))
    first = ep * 8

    diagonal = (dp, pp, lax.rem(ep + 3 - 2 * lax.rem(ep, 2), 4))

    barrier = pltpu.get_barrier_semaphore()
    for peer in (other_pp, across, beside, diagonal):
        pl.semaphore_signal(barrier, inc=1, device_id=peer, device_id_type=MESH)
    pl.semaphore_wait(barrier, 4)

    attn_w = [(wq_h, wq), (wk_h, wk), (wv_h, wv), (wo_h, wo)]
    moe_w = [(wg_h, wg), (wu_h, wu), (wd_h, wd)]
    weight_copies = [pltpu.make_async_copy(s, d, w_sem.at[j]) for j, (s, d) in enumerate(attn_w + moe_w)]

    def hin_copies(c):
        h = lax.rem(c, HIN_SLOTS)
        return [pltpu.make_async_copy(hid.at[c, piece(p)], hin.at[h, piece(p)], hin_sem.at[h, p]) for p in range(PIECES)]

    def kv_copies(c):
        return (pltpu.make_async_copy(k_cache.at[c], k_buf, kv_sem.at[0]), pltpu.make_async_copy(v_cache.at[c], v_buf, kv_sem.at[1]))

    def new_copies(c):
        return (pltpu.make_async_copy(kn, kn_out.at[c], new_sem.at[0]), pltpu.make_async_copy(vn, vn_out.at[c], new_sem.at[1]))

    def remote(src, dst, send, recv, peer):
        return pltpu.make_async_remote_copy(src_ref=src, dst_ref=dst, send_sem=send, recv_sem=recv, device_id=peer, device_id_type=MESH)

    def rows_at(slot, part_idx):
        return n_buf.at[slot, pl.ds(part_idx * tokens, tokens)]

    def dx_copy(c):
        s = lax.rem(c, 3)
        return remote(rows_at(s, 0), rows_at(s, 1), dx_send.at[s], dx_recv.at[s], across)

    def dc_copy(c):
        s = lax.rem(c, 3)
        return remote(rows_at(s, 0), rows_at(s, 2), dc_send.at[s], dc_recv.at[s], beside)

    def dr_copy(c):
        s = lax.rem(c, 3)
        return remote(rows_at(s, 1), rows_at(s, 3), dr_send.at[s], dr_recv.at[s], beside)

    def r1_copy(c):
        s = lax.rem(c, 2)
        return remote(part.at[pl.ds(2 * tokens, 2 * tokens)], rb1.at[s], r1_send.at[s], r1_recv.at[s], beside)

    rows = tokens // PIECES

    def piece(p):
        return pl.ds(p * rows, rows)

    def r2_copy(c, p):
        s = lax.rem(c, 3)
        return remote(rb1.at[lax.rem(c, 2), pl.ds(tokens + p * rows, rows)], rb2.at[s, piece(p)], r2_send.at[s, p], r2_recv.at[s, p], across)

    def hop_copy(c, p):
        s = lax.rem(c, 2)
        h = lax.rem(c, HIN_SLOTS)
        return remote(ho.at[s, piece(p)], hin.at[h, piece(p)], hop_send.at[s, p], hin_sem.at[h, p], other_pp)

    def out_copy(c, p):
        s = lax.rem(c, 2)
        return remote(ho.at[s, piece(p)], out.at[c, piece(p)], hop_send.at[s, p], out_recv.at[c, p], other_pp)

    def out_local(c, p):
        s = lax.rem(c, 2)
        return pltpu.make_async_copy(ho.at[s, piece(p)], out.at[c, piece(p)], out_loc.at[s, p])

    def ids_copies():
        return [remote(ids_own, ids.at[j], ids_send.at[j], ids_recv.at[j], peer) for j, peer in ((1, across), (2, beside), (3, diagonal))]

    def table_copy(c):
        s = lax.rem(c, 2)
        return pltpu.make_async_copy(table, smem_table.at[s], table_sem)

    smem_table[1, 0, 0] = 0
    smem_table[1, 1, 0] = 0

    for copy in ids_copies():
        copy.start()

    @pl.when(pp == 0)
    def _():
        for copy in hin_copies(0):
            copy.start()

    for copy in weight_copies[:3]:
        copy.start()
    for copy in kv_copies(0):
        copy.start()
    weight_copies[3].start()

    @pl.when(pp == 0)
    def _():
        for copy in hin_copies(1):
            copy.start()

    w = {"a_gain": a_gain, "cos": cos_ref, "sin": sin_ref, "q": wq, "k": wk, "v": wv, "gate": wg, "up": wu, "down": wd}

    def plan(c):
        @pl.when(c == 0)
        def _():
            ids[0] = ids_own[...]
            with scope("w_ids"):
                for copy in ids_copies():
                    copy.wait()

        chosen_ids = jnp.concatenate([ids[j, c] for j in range(4)], axis=1)
        plan_tiles(chosen_ids, first, tri, member, rank_buf.at[lax.rem(c, 2)], table)
        table_copy(c).start()

    def combine_near():
        half = pl.ds(0, 2 * tokens)
        part[half, :] = dot(picks[half, :], terms[...])

    def project(c, with_sums):
        plan(c)
        with scope("w_hin"):
            for copy in hin_copies(c):
                copy.wait()

        @pl.when(c == 0)
        def _():
            for copy in weight_copies[:3]:
                copy.wait()

        @pl.when(jnp.logical_and(pp == 0, c + 2 < chunks))
        def _():
            for copy in hin_copies(c + 2):
                copy.start()

        @pl.when(c > 0)
        def _():
            for copy in new_copies(c - 1):
                copy.wait()

        seq_row = seq[pl.ds(c, 1), :].astype(F32)
        pos[...] = jnp.broadcast_to(seq_row, (128, 128)).T
        if with_sums:
            combine_near()
        attn_dots(hin[lax.rem(c, HIN_SLOTS)], w, x_buf)
        attn_rope(pos[...], w, x_buf, q3, k3, v3)
        kn[...] = k3[...].reshape(tokens, 8, 128)[:, :, :64].astype(BF16)
        vn[...] = v3[...].reshape(tokens, 8, 128)[:, :, :64].astype(BF16)
        for copy in new_copies(c):
            copy.start()

    def reduce_pair(c):
        copy = r1_copy(c)
        with scope("w_r1"):
            copy.wait_send()
            copy.wait_recv()
        s = lax.rem(c, 2)
        far = pl.ds(tokens, tokens)
        near = pl.ds(0, tokens)
        rb1[s, far, :] = rb1[s, far, :] + part[far, :]
        for p in range(PIECES):
            r2_copy(c, p).start()
        rb1[s, near, :] = rb1[s, near, :] + part[near, :]

    def relay(c):
        copy = dx_copy(c)
        with scope("w_dx"):
            copy.wait_recv()
        dr_copy(c).start()
        copy.wait_send()
        dc_copy(c).wait_send()

    def attend(c):
        table_copy(c).wait()
        with scope("w_kv"):
            for copy in kv_copies(c):
                copy.wait()

        @pl.when(c == 0)
        def _():
            for copy in weight_copies[4:]:
                copy.start()

        def body(idx, carry):
            base = idx * GROUP_UNROLL
            ahead = attn_scores(base, q3, k3, k_buf)
            for u in range(GROUP_UNROLL):
                scores = ahead
                if u + 1 < GROUP_UNROLL:
                    ahead = attn_scores(base + u + 1, q3, k3, k_buf)
                attn_mix(base + u, *attn_weights(base + u, *scores, pos), v3, o3, v_buf)
            return carry

        with scope("groups"):
            lax.fori_loop(0, tokens // (GROUP * GROUP_UNROLL), body, 0)

        @pl.when(c + 1 < chunks)
        def _():
            for copy in kv_copies(c + 1):
                copy.start()

        @pl.when(c == 0)
        def _():
            weight_copies[3].wait()

        @pl.when(c >= 1)
        def _():
            dispatched(c - 1)

        hidden = hin[lax.rem(c, HIN_SLOTS)].astype(F32)
        attn_out = jnp.concatenate([o3[pl.ds(g, tokens, stride=8), :].astype(BF16) for g in range(8)], axis=1)
        before = c + 5
        mixed = dot(attn_out, wo[...])
        router = logits(before)
        picked = gather_rows(before, 0, 0)
        new_mid = (hidden + mixed).astype(BF16)
        mid[lax.rem(c, 3)] = new_mid
        n_buf[lax.rem(c, 3), pl.ds(0, tokens), :] = rms(new_mid.astype(F32), m_gain[...].astype(F32))
        gates(before, router)
        gather_gate(picked, before, 0, 0)
        dx_copy(c).start()
        dc_copy(c).start()

        @pl.when(jnp.logical_and(pp == 1, c + HIN_SLOTS < chunks))
        def _():
            pl.semaphore_signal(credit, inc=1, device_id=other_pp, device_id_type=MESH)

    def tile_at(c, row, j):
        return smem_table[lax.rem(c, 2), row, j]

    def gather_rows(c, j, u):
        normed = n_buf.at[lax.rem(c, 3)]
        return moe_gather(j, u, tile_at(c, 0, j), tile_at(c, 1, j), first, normed, rank_buf.at[lax.rem(c, 2)], picks, x_buf)

    def gather_gate(picked, c, j, u):
        moe_gate(picked, u, tile_at(c, 0, j), first, gate_ref, g_buf)

    def gather(c, j, u):
        gather_gate(gather_rows(c, j, u), c, j, u)

    def dispatched(c):
        with scope("w_disp"):
            dc_copy(c).wait_recv()
            dr_copy(c).wait_recv()

    def logits(c):
        return dot_nt(w_r[...], n_buf[lax.rem(c, 3)])

    def gates(c, router):
        moe_gates(router, rank_buf.at[lax.rem(c, 2)], gate_ref)

    def experts(c):
        @pl.when(c == 0)
        def _():
            with scope("w_wts"):
                for copy in weight_copies[4:]:
                    copy.wait()

        def expand(j, u):
            moe_expand(u, tile_at(c, 0, j), w, x_buf, a_buf)

        def contract(j, u):
            moe_contract(j, u, tile_at(c, 0, j), w, a_buf, g_buf, terms)

        def body(idx, carry):
            base = idx * TILE_UNROLL
            expand(base, 0)
            gather(c, base + 1, 1)
            for u in range(1, TILE_UNROLL):
                expand(base + u, u)
                if u + 1 < TILE_UNROLL:
                    gather(c, base + u + 1, u + 1)
                else:
                    gather(c, lax.rem(base + TILE_UNROLL, tile_count), 0)
                contract(base + u - 1, u - 1)
            contract(base + TILE_UNROLL - 1, TILE_UNROLL - 1)
            return carry

        with scope("tiles"):
            lax.fori_loop(0, tile_count // TILE_UNROLL, body, 0)
        half = 2 * tokens
        part[pl.ds(half, half), :] = dot(picks[pl.ds(half, half), :], terms[...])
        dr_copy(c).wait_send()
        r1_copy(c).start()

    def finish(c):
        s = lax.rem(c, 2)

        @pl.when(jnp.logical_and(pp == 0, c >= HIN_SLOTS))
        def _():
            pl.semaphore_wait(credit, 1)

        @pl.when(c >= 2)
        def _():
            for p in range(PIECES):
                @pl.when(pp == 0)
                def _():
                    hop_copy(c - 2, p).wait_send()

                @pl.when(pp == 1)
                def _():
                    out_copy(c - 2, p).wait_send()
                    out_local(c - 2, p).wait()

        for p in range(PIECES):
            with scope("w_r2"):
                r2_copy(c, p).wait_recv()
            at = piece(p)
            mixed = (rb1[s, at, :] + rb2[lax.rem(c, 3), at, :]).astype(BF16)
            result = (mid[lax.rem(c, 3), at, :].astype(F32) + mixed.astype(F32)).astype(BF16)

            @pl.when(pp == 0)
            def _():
                ho[s, at, :] = result
                hop_copy(c, p).start()

            @pl.when(pp == 1)
            def _():
                vals = result.astype(F32)
                vals = vals * lax.rsqrt(jnp.mean(vals * vals, axis=-1, keepdims=True) + EPS)
                for g in range(8):
                    ho[s, at, g * 128:(g + 1) * 128] = (vals[:, g * 128:(g + 1) * 128] * f_gain[g:g + 1, :]).astype(BF16)
                out_copy(c, p).start()
                out_local(c, p).start()

        for p in range(PIECES):
            r2_copy(c, p).wait_send()

    def step(i, carry):
        @pl.when(i < 2)
        def _():
            with scope("project"):
                project(i, False)

        @pl.when(jnp.logical_and(i >= 2, i < chunks))
        def _():
            with scope("project_sum"):
                project(i, True)

        @pl.when(i >= chunks)
        def _():
            combine_near()

        @pl.when(jnp.logical_and(i >= 1, i <= chunks))
        def _():
            with scope("relay"):
                relay(i - 1)

        @pl.when(i >= 2)
        def _():
            with scope("reduce_pair"):
                reduce_pair(i - 2)

        @pl.when(i < chunks)
        def _():
            with scope("attend"):
                attend(i)

        @pl.when(i == chunks)
        def _():
            dispatched(i - 1)
            gates(i - 1, logits(i - 1))
            gather(i - 1, 0, 0)

        @pl.when(jnp.logical_and(i >= 1, i <= chunks))
        def _():
            with scope("experts"):
                experts(i - 1)

        @pl.when(i >= 2)
        def _():
            with scope("finish"):
                finish(i - 2)

        return carry

    lax.fori_loop(0, chunks + 2, step, 0)

    for copy in new_copies(chunks - 1):
        copy.wait()

    @pl.when(pp == 0)
    def _():
        for c in (chunks - 2, chunks - 1):
            for p in range(PIECES):
                hop_copy(c, p).wait_send()

        def arrived(c, carry):
            for p in range(PIECES):
                out_copy(c, p).wait_recv()
            return carry

        with scope("w_out"):
            lax.fori_loop(0, chunks, arrived, 0)

    @pl.when(pp == 1)
    def _():
        for c in (chunks - 2, chunks - 1):
            for p in range(PIECES):
                out_copy(c, p).wait_send()
                out_local(c, p).wait()


def step_call(args, chunks, tokens, tile_count):
    vmem = pl.BlockSpec(memory_space=pltpu.VMEM)
    hbm = pl.BlockSpec(memory_space=pl.ANY)
    wide = 4 * tokens
    dma = pltpu.SemaphoreType.DMA
    return pl.pallas_call(
        functools.partial(step_kernel, tile_count),
        out_shape=(
            jax.ShapeDtypeStruct((chunks, tokens, 1024), BF16),
            jax.ShapeDtypeStruct((chunks, tokens, 8, 64), BF16),
            jax.ShapeDtypeStruct((chunks, tokens, 8, 64), BF16),
        ),
        in_specs=[hbm, vmem, hbm, hbm, vmem, hbm, hbm, hbm, hbm, vmem, vmem, vmem, vmem, vmem, vmem, hbm, hbm, hbm, vmem],
        out_specs=(hbm, hbm, hbm),
        scratch_shapes=[
            pltpu.VMEM((3, wide, 1024), BF16),
            pltpu.VMEM((HIN_SLOTS, tokens, 1024), BF16),
            pltpu.VMEM((3, tokens, 1024), BF16),
            pltpu.VMEM((2, tokens, 1024), BF16),
            pltpu.VMEM((tokens * 128, 64), BF16),
            pltpu.VMEM((tokens * 128, 64), BF16),
            pltpu.VMEM((1024, 1024), BF16),
            pltpu.VMEM((1024, 512), BF16),
            pltpu.VMEM((1024, 512), BF16),
            pltpu.VMEM((1024, 1024), BF16),
            pltpu.VMEM((8, 1024, 512), BF16),
            pltpu.VMEM((8, 1024, 512), BF16),
            pltpu.VMEM((8, 512, 1024), BF16),
            pltpu.VMEM((wide, 1024), F32),
            pltpu.VMEM((2, 2 * tokens, 1024), F32),
            pltpu.VMEM((3, tokens, 1024), F32),
            pltpu.VMEM((wide, tile_count * TILE), BF16),
            pltpu.VMEM((tile_count * TILE, 1024), BF16),
            pltpu.VMEM((3, TILE, 1024), BF16),
            pltpu.VMEM((3, TILE, 512), BF16),
            pltpu.VMEM((TILE_UNROLL, TILE, 128), F32),
            pltpu.VMEM((tokens * 8, 128), F32),
            pltpu.VMEM((tokens * 8, 128), F32),
            pltpu.VMEM((tokens * 8, 128), F32),
            pltpu.VMEM((tokens * 8, 128), F32),
            pltpu.VMEM((tokens, 8, 64), BF16),
            pltpu.VMEM((tokens, 8, 64), BF16),
            pltpu.VMEM((2, 32, wide), F32),
            pltpu.VMEM((32, wide), F32),
            pltpu.VMEM((32, wide), F32),
            pltpu.VMEM((tokens, 128), F32),
            pltpu.VMEM((4, chunks, 8, tokens), jnp.int32),
            pltpu.VMEM((8, 128), jnp.int32),
            pltpu.SMEM((2, 8, 128), jnp.int32),
            dma((7,)), dma((4,)), dma((4,)), dma(()), dma((HIN_SLOTS, PIECES)), dma((2,)), dma((2,)),
            dma((3,)), dma((3,)), dma((3,)), dma((3,)), dma((3,)), dma((3,)),
            dma((2,)), dma((2,)), dma((3, PIECES)), dma((3, PIECES)),
            dma((2, PIECES)), dma((2, PIECES)), dma((chunks, PIECES)),
            pltpu.SemaphoreType.REGULAR,
        ],
        compiler_params=pltpu.CompilerParams(collective_id=0, has_side_effects=True, vmem_limit_bytes=67043328),
        name="decode_step",
        cost_estimate=pl.CostEstimate(flops=2 * 10**11, bytes_accessed=2 * 10**8, transcendentals=0),
    )(*args)


def solution(mesh):
    rows_spec = ("dp", "ep")
    three_dim = P("pp", None, None)
    two_dim = P("pp", None)
    expert_spec = P("pp", "ep", None, None)
    cache_spec = P("pp", None, rows_spec, None, None, None)
    new_spec = P("pp", None, rows_spec, None, None)
    in_specs = (P(None, rows_spec, None), P(None, rows_spec), cache_spec, cache_spec, P("pp", None, rows_spec, None), three_dim, three_dim, three_dim, three_dim, two_dim, two_dim, three_dim, expert_spec, expert_spec, expert_spec, P(None))
    out_specs = (P(None, rows_spec, None), new_spec, new_spec)

    def device_fn(hidden_in, seq_pos, k_cache, v_cache, expert_ids, w_query, w_key, w_value, w_out, attn_gain, mlp_gain, w_router, w_gate, w_up, w_down, final_gain):
        micro, rows = seq_pos.shape
        chunks = micro // PER_CHUNK
        tokens = PER_CHUNK * rows
        wide = 4 * tokens
        tile_count = (wide * 2 - 8) // TILE + 8
        angles = np.arange(1, 17)[:, None] * THETA ** (-np.arange(32) / 32)
        cos_t = jnp.asarray(np.tile(np.cos(angles), (1, 4)), F32)
        sin_t = jnp.asarray(np.tile(np.concatenate([-np.sin(angles), np.sin(angles)], axis=1), (1, 2)), F32)
        tri = jnp.asarray(np.triu(np.ones((wide, wide)), 1), BF16)
        ids = jnp.swapaxes(expert_ids[0].reshape(chunks, tokens, 8), 1, 2)
        args = (
            hidden_in.reshape(chunks, tokens, 1024), seq_pos.reshape(chunks, tokens), k_cache.reshape(chunks, tokens * 128, 64), v_cache.reshape(chunks, tokens * 128, 64),
            ids, w_query[0], w_key[0], w_value[0], w_out[0], attn_gain, mlp_gain, final_gain.astype(F32).reshape(8, 128), cos_t, sin_t, w_router[0].T,
            w_gate[0], w_up[0], w_down[0], tri,
        )
        out, k_new, v_new = step_call(args, chunks, tokens, tile_count)
        shape = (1,) + seq_pos.shape + (8, 64)
        return out.reshape(hidden_in.shape), k_new.reshape(shape), v_new.reshape(shape)

    return jax.shard_map(device_fn, mesh=mesh, in_specs=in_specs, out_specs=out_specs, check_vma=False)
```

```python
import functools

import jax
import jax.numpy as jnp
import numpy as np
from jax import lax
from jax.experimental import pallas as pl
from jax.experimental.pallas import tpu as pltpu
from jax.sharding import PartitionSpec as P

THETA = 1000000.0
EPS = 1e-05
F32 = jnp.float32
BF16 = jnp.bfloat16
TILE = 128
GROUP = 16
GROUP_UNROLL = 8
TILE_UNROLL = 3
PER_CHUNK = 4
HIN_SLOTS = 4
PIECES = 4
MESH = pl.DeviceIdType.MESH


def scope(name):
    return jax.named_scope(name)


def rms(vals, gain_row):
    inv = lax.rsqrt(jnp.mean(vals * vals, axis=-1, keepdims=True) + EPS)
    return (vals * inv * gain_row).astype(BF16)


def dot(lhs, rhs):
    return jnp.dot(lhs, rhs, preferred_element_type=F32)


def dot_nt(lhs, rhs):
    return lax.dot_general(lhs, rhs, (((1,), (1,)), ((), ())), preferred_element_type=F32)


def rope_tables(pos, table):
    lane = lax.broadcasted_iota(jnp.int32, pos.shape, 1).astype(F32)
    both = dot(jnp.where(lane + 1.0 == pos, 1.0, 0.0).astype(BF16), table[...])
    both = both[:, :256] + both[:, 256:512] + both[:, 512:]
    return both


def rope(vals, cos_t, sin_t):
    lane = lax.broadcasted_iota(jnp.int32, (1, 128), 1)
    first = (lane % 64) < 32
    parts = []
    for j in range(vals.shape[1] // 128):
        block = vals[:, j * 128:(j + 1) * 128]
        swapped = jnp.where(first, pltpu.roll(block, 96, 1), pltpu.roll(block, 32, 1))
        parts.append(block * cos_t + swapped * sin_t)
    return jnp.concatenate(parts, axis=1)


def spread(ref, vals):
    tokens = vals.shape[0]
    for g in range(8):
        ref[pl.ds(g, tokens, stride=8), :] = vals[:, g * 128:(g + 1) * 128]


def spread_heads(ref, vals):
    tokens = vals.shape[0]
    low = lax.broadcasted_iota(jnp.int32, (1, 128), 1) < 64
    for j in range(4):
        block = vals[:, j * 128:(j + 1) * 128]
        other = pltpu.roll(block, 64, 1)
        ref[pl.ds(2 * j, tokens, stride=8), :] = jnp.where(low, block, other)
        ref[pl.ds(2 * j + 1, tokens, stride=8), :] = jnp.where(low, other, block)


def rows_of(ref, idx):
    return ref[pl.ds(pl.multiple_of(idx * GROUP * 8, GROUP * 8), GROUP * 8), :].reshape(GROUP, 8, 128)


def attn_dots(hidden, w, raw):
    normed = rms(hidden.astype(F32), w["a_gain"][...].astype(F32))
    raw[1] = dot(normed, w["q"][...]).astype(BF16)
    raw[2, :, :512] = dot(normed, w["k"][...]).astype(BF16)
    raw[2, :, 512:] = dot(normed, w["v"][...]).astype(BF16)


def attn_rope(turn, raw, q3, k3, v3):
    cos_t, sin_t = turn[:, :128], turn[:, 128:]
    spread(q3, rope(raw[1].astype(F32), cos_t, sin_t).astype(BF16).astype(F32))
    spread_heads(k3, rope(raw[2, :, :512].astype(F32), cos_t, sin_t).astype(BF16).astype(F32))
    spread_heads(v3, raw[2, :, 512:].astype(F32))


def attn_scores(idx, q3, k3, k_rows):
    q = rows_of(q3, idx)
    lane3 = lax.broadcasted_iota(jnp.int32, (1, 1, 128), 2)
    prod = q * rows_of(k3, idx)
    self_a = jnp.sum(jnp.where(lane3 < 64, prod, 0.0), axis=-1, keepdims=True)
    self_b = jnp.sum(jnp.where(lane3 < 64, 0.0, prod), axis=-1, keepdims=True)
    wide = (GROUP, 8, 128)
    self_s = jnp.concatenate([jnp.broadcast_to(self_a, wide), jnp.broadcast_to(self_b, wide)], axis=1) * 0.125
    q_rows = jnp.concatenate([q, pltpu.roll(q, 64, 2)], axis=1).astype(BF16)[:, :, :64].reshape(GROUP * 16, 64)
    row0 = idx * (GROUP * 128)
    blocks = []
    for p in range(GROUP // 2):
        keys = k_rows[pl.ds(pl.multiple_of(row0 + p * 256, 256), 256), :]
        both = dot_nt(q_rows[p * 32:(p + 1) * 32], keys)
        blocks.append(both[:16, :128].reshape(1, 16, 128))
        blocks.append(both[16:, 128:].reshape(1, 16, 128))
    return jnp.concatenate(blocks, axis=0), self_s


def attn_weights(idx, scores, self_s, pos_ref):
    row_i = lax.broadcasted_iota(jnp.int32, (16, 128), 0)
    lane_i = lax.broadcasted_iota(jnp.int32, (16, 128), 1)
    step = jnp.where((row_i % 8) == (lane_i % 8), lane_i // 8, 1000).astype(F32)
    pos = pos_ref[pl.ds(pl.multiple_of(idx * GROUP, GROUP), GROUP), :].reshape(GROUP, 1, 128)
    scores = jnp.where(step.reshape(1, 16, 128) < pos, scores * 0.125, -jnp.inf)
    wide = (GROUP, 16, 128)
    top = jnp.maximum(jnp.broadcast_to(jnp.max(scores, axis=-1, keepdims=True), wide), self_s)
    weights = jnp.exp(scores - top)
    self_w = jnp.exp(self_s - top)
    inv = 1.0 / (jnp.broadcast_to(jnp.sum(weights, axis=-1, keepdims=True), wide) + self_w)
    return (weights * inv).astype(BF16), (self_w * inv).astype(BF16).astype(F32)


def attn_mix(idx, weights, self_w, v3, o3, v_rows):
    row0 = idx * (GROUP * 128)
    zeros = jnp.zeros((16, 128), BF16)
    outs = []
    for p in range(GROUP // 2):
        vals = v_rows[pl.ds(pl.multiple_of(row0 + p * 256, 256), 256), :]
        upper = jnp.concatenate([weights[2 * p], zeros], axis=1)
        lower = jnp.concatenate([zeros, weights[2 * p + 1]], axis=1)
        outs.append(dot(jnp.concatenate([upper, lower], axis=0), vals).reshape(2, 16, 64))
    out = jnp.concatenate(outs, axis=0)
    v_new = rows_of(v3, idx)[:, :, :64]
    out_a = out[:, :8] + self_w[:, :8, :64] * v_new
    out_b = out[:, 8:] + self_w[:, 8:, :64] * v_new
    o3[pl.ds(pl.multiple_of(idx * GROUP * 8, GROUP * 8), GROUP * 8), :] = jnp.concatenate([out_a, out_b], axis=-1).reshape(GROUP * 8, 128)


def plan_tiles(ids, first, tri, member_ref, rank_ref, table_ref):
    tokens = ids.shape[1]
    expert_i = lax.broadcasted_iota(jnp.int32, (32, tokens), 0)
    chosen = jnp.zeros((32, tokens), F32)
    for s in range(ids.shape[0]):
        chosen = jnp.where(ids[s:s + 1, :] == expert_i, 1.0, chosen)
    member_ref[...] = chosen
    rank = dot(chosen.astype(BF16), tri[...])
    rank_ref[...] = jnp.where(chosen > 0.0, rank, -1.0)
    local = member_ref[pl.ds(pl.multiple_of(first, 8), 8), :]
    counts = jnp.sum(local, axis=-1, keepdims=True).astype(jnp.int32)
    tiles = jnp.broadcast_to(lax.shift_right_logical(counts + (TILE - 1), 7), (8, 128))
    lane = lax.broadcasted_iota(jnp.int32, (1, 128), 1)
    end = jnp.zeros((1, 128), jnp.int32)
    start = jnp.zeros((1, 128), jnp.int32)
    expert = jnp.zeros((1, 128), jnp.int32)
    for e in range(8):
        end = end + tiles[e:e + 1, :]
        passed = lane >= end
        expert = jnp.where(passed, expert + 1, expert)
        start = jnp.where(passed, end, start)
    sub = jnp.where(expert < 8, lane - start, 1000)
    table_ref[0:1, :] = jnp.minimum(expert, 7)
    table_ref[1:2, :] = sub


def moe_gates(logits, rank_ref, gate_ref):
    chosen = rank_ref[...] >= 0.0
    top = jnp.max(jnp.where(chosen, logits, -jnp.inf), axis=0, keepdims=True)
    gates = jnp.where(chosen, jnp.exp(logits - top), 0.0)
    gate_ref[...] = gates / jnp.sum(gates, axis=0, keepdims=True)


def slot_of(u):
    return 0 if u == 0 else 1 + (u - 1) % 2


def moe_gather(j, u, expert, sub, first, normed, rank_ref, picks, x_buf):
    ranks = rank_ref[pl.ds(first + expert, 1), :]
    wanted = (lax.broadcasted_iota(jnp.int32, (TILE, 1), 0) + sub * TILE).astype(F32)
    picked = jnp.where(ranks == wanted, 1.0, 0.0)
    picks[:, pl.ds(pl.multiple_of(j * TILE, TILE), TILE)] = picked.T.astype(BF16)
    x_buf[slot_of(u)] = dot(picked.astype(BF16), normed[...]).astype(BF16)
    return picked


def moe_gate(picked, u, expert, first, gate_ref, g_buf):
    gate = jnp.sum(picked * gate_ref[pl.ds(first + expert, 1), :], axis=-1, keepdims=True)
    g_buf[u] = jnp.broadcast_to(gate, (TILE, 128))


def moe_expand(u, expert, w, x_buf, a_buf):
    rows = x_buf[slot_of(u)]
    a_buf[slot_of(u)] = (jax.nn.silu(dot(rows, w["gate"][expert])) * dot(rows, w["up"][expert])).astype(BF16)


def moe_contract(j, u, expert, w, a_buf, g_buf, terms):
    y = dot(a_buf[slot_of(u)], w["down"][expert])
    gate = g_buf[u]
    at = pl.ds(pl.multiple_of(j * TILE, TILE), TILE)
    for p in range(8):
        terms[at, p * 128:(p + 1) * 128] = (gate * y[:, p * 128:(p + 1) * 128]).astype(BF16)


def step_kernel(
    tile_count,
    hid, seq, k_cache, v_cache, ids_own, wq_h, wk_h, wv_h, wo_h, a_gain, m_gain, f_gain, rope_ref, w_r, wg_h, wu_h, wd_h, tri,
    out, kn_out, vn_out,
    n_buf, hin, mid, ho, k_buf, v_buf, wq, wk, wv, wo, wg, wu, wd, part, rb1, rb2, picks, terms, x_buf, a_buf, g_buf, q3, k3, v3, o3, kn, vn, rank_buf, gate_ref, member, pos, turn, ids, table, smem_table,
    w_sem, ids_send, ids_recv, table_sem, hin_sem, kv_sem, new_sem, dx_send, dx_recv, dc_send, dc_recv, dr_send, dr_recv, r1_send, r1_recv, r2_send, r2_recv, hop_send, out_loc, out_recv, credit,
):
    chunks, tokens = hid.shape[0], hid.shape[1]
    gathered = 4 * tokens
    dp = lax.axis_index("dp")
    pp = lax.axis_index("pp")
    ep = lax.axis_index("ep")
    other_pp = (dp, 1 - pp, ep)
    across = (dp, pp, lax.rem(ep + 2, 4))
    beside = (dp, pp, ep + 1 - 2 * lax.rem(ep, 2))
    first = ep * 8

    diagonal = (dp, pp, lax.rem(ep + 3 - 2 * lax.rem(ep, 2), 4))

    barrier = pltpu.get_barrier_semaphore()
    for peer in (other_pp, across, beside, diagonal):
        pl.semaphore_signal(barrier, inc=1, device_id=peer, device_id_type=MESH)
    pl.semaphore_wait(barrier, 4)

    attn_w = [(wq_h, wq), (wk_h, wk), (wv_h, wv), (wo_h, wo)]
    moe_w = [(wg_h, wg), (wu_h, wu), (wd_h, wd)]
    weight_copies = [pltpu.make_async_copy(s, d, w_sem.at[j]) for j, (s, d) in enumerate(attn_w + moe_w)]

    def hin_copies(c):
        h = lax.rem(c, HIN_SLOTS)
        return [pltpu.make_async_copy(hid.at[c, piece(p)], hin.at[h, piece(p)], hin_sem.at[h, p]) for p in range(PIECES)]

    def kv_copies(c):
        return (pltpu.make_async_copy(k_cache.at[c], k_buf, kv_sem.at[0]), pltpu.make_async_copy(v_cache.at[c], v_buf, kv_sem.at[1]))

    def new_copies(c):
        return (pltpu.make_async_copy(kn, kn_out.at[c], new_sem.at[0]), pltpu.make_async_copy(vn, vn_out.at[c], new_sem.at[1]))

    def remote(src, dst, send, recv, peer):
        return pltpu.make_async_remote_copy(src_ref=src, dst_ref=dst, send_sem=send, recv_sem=recv, device_id=peer, device_id_type=MESH)

    def rows_at(slot, part_idx):
        return n_buf.at[slot, pl.ds(part_idx * tokens, tokens)]

    def dx_copy(c):
        s = lax.rem(c, 3)
        return remote(rows_at(s, 0), rows_at(s, 1), dx_send.at[s], dx_recv.at[s], across)

    def dc_copy(c):
        s = lax.rem(c, 3)
        return remote(rows_at(s, 0), rows_at(s, 2), dc_send.at[s], dc_recv.at[s], beside)

    def dr_copy(c):
        s = lax.rem(c, 3)
        return remote(rows_at(s, 1), rows_at(s, 3), dr_send.at[s], dr_recv.at[s], beside)

    def r1_copy(c):
        s = lax.rem(c, 2)
        return remote(part.at[pl.ds(2 * tokens, 2 * tokens)], rb1.at[s], r1_send.at[s], r1_recv.at[s], beside)

    rows = tokens // PIECES

    def piece(p):
        return pl.ds(p * rows, rows)

    def r2_copy(c, p):
        s = lax.rem(c, 3)
        return remote(rb1.at[lax.rem(c, 2), pl.ds(tokens + p * rows, rows)], rb2.at[s, piece(p)], r2_send.at[s, p], r2_recv.at[s, p], across)

    def hop_copy(c, p):
        s = lax.rem(c, 2)
        h = lax.rem(c, HIN_SLOTS)
        return remote(ho.at[s, piece(p)], hin.at[h, piece(p)], hop_send.at[s, p], hin_sem.at[h, p], other_pp)

    def out_copy(c, p):
        s = lax.rem(c, 2)
        return remote(ho.at[s, piece(p)], out.at[c, piece(p)], hop_send.at[s, p], out_recv.at[c, p], other_pp)

    def out_local(c, p):
        s = lax.rem(c, 2)
        return pltpu.make_async_copy(ho.at[s, piece(p)], out.at[c, piece(p)], out_loc.at[s, p])

    def ids_copies(part_idx):
        some = pl.ds(0, 1) if part_idx == 0 else pl.ds(1, chunks - 1)
        return [remote(ids_own.at[some], ids.at[j, some], ids_send.at[part_idx, j], ids_recv.at[part_idx, j], peer) for j, peer in ((1, across), (2, beside), (3, diagonal))]

    def table_copy(c):
        s = lax.rem(c, 2)
        return pltpu.make_async_copy(table, smem_table.at[s], table_sem)

    smem_table[1, 0, 0] = 0
    smem_table[1, 1, 0] = 0

    for part_idx in range(2):
        for copy in ids_copies(part_idx):
            copy.start()

    @pl.when(pp == 0)
    def _():
        for copy in hin_copies(0):
            copy.start()

    for copy in weight_copies[:3]:
        copy.start()
    for copy in kv_copies(0):
        copy.start()
    weight_copies[3].start()

    @pl.when(pp == 0)
    def _():
        for copy in hin_copies(1):
            copy.start()

    w = {"a_gain": a_gain, "rope": rope_ref, "q": wq, "k": wk, "v": wv, "gate": wg, "up": wu, "down": wd}

    def plan(c):
        @pl.when(c == 0)
        def _():
            ids[0] = ids_own[...]
            with scope("w_ids"):
                for copy in ids_copies(0):
                    copy.wait()

        @pl.when(c == 1)
        def _():
            for copy in ids_copies(1):
                copy.wait()

        chosen_ids = jnp.concatenate([ids[j, c] for j in range(4)], axis=1)
        plan_tiles(chosen_ids, first, tri, member, rank_buf.at[lax.rem(c, 2)], table)
        table_copy(c).start()

    def combine_near(from_col, to_col):
        half = pl.ds(0, 2 * tokens)
        part[half, from_col:to_col] = dot(picks[half, :], terms[:, from_col:to_col])

    def project(c, with_sums):
        plan(c)
        with scope("w_hin"):
            for copy in hin_copies(c):
                copy.wait()

        @pl.when(c == 0)
        def _():
            for copy in weight_copies[:3]:
                copy.wait()

        @pl.when(jnp.logical_and(pp == 0, c + 2 < chunks))
        def _():
            for copy in hin_copies(c + 2):
                copy.start()

        @pl.when(c > 0)
        def _():
            for copy in new_copies(c - 1):
                copy.wait()

        seq_row = seq[pl.ds(c, 1), :].astype(F32)
        pos[...] = jnp.broadcast_to(seq_row, (128, 128)).T
        turn[...] = rope_tables(pos[...], w["rope"])
        if with_sums:
            combine_near(0, 256)
        attn_dots(hin[lax.rem(c, HIN_SLOTS)], w, x_buf)
        if with_sums:
            combine_near(256, 1024)
        attn_rope(turn, x_buf, q3, k3, v3)
        kn[...] = k3[...].reshape(tokens, 8, 128)[:, :, :64].astype(BF16)
        vn[...] = v3[...].reshape(tokens, 8, 128)[:, :, :64].astype(BF16)
        for copy in new_copies(c):
            copy.start()

    def reduce_pair(c):
        copy = r1_copy(c)
        with scope("w_r1"):
            copy.wait_send()
            copy.wait_recv()
        s = lax.rem(c, 2)
        far = pl.ds(tokens, tokens)
        near = pl.ds(0, tokens)
        rb1[s, far, :] = rb1[s, far, :] + part[far, :]
        for p in range(PIECES):
            r2_copy(c, p).start()
        rb1[s, near, :] = rb1[s, near, :] + part[near, :]

    def relay(c):
        copy = dx_copy(c)
        with scope("w_dx"):
            copy.wait_recv()
        dr_copy(c).start()
        copy.wait_send()
        dc_copy(c).wait_send()

    def attend(c):
        table_copy(c).wait()
        with scope("w_kv"):
            for copy in kv_copies(c):
                copy.wait()

        @pl.when(c == 0)
        def _():
            for copy in weight_copies[4:]:
                copy.start()

        def body(idx, carry):
            base = idx * GROUP_UNROLL
            ahead = attn_scores(base, q3, k3, k_buf)
            for u in range(GROUP_UNROLL):
                scores = ahead
                if u + 1 < GROUP_UNROLL:
                    ahead = attn_scores(base + u + 1, q3, k3, k_buf)
                attn_mix(base + u, *attn_weights(base + u, *scores, pos), v3, o3, v_buf)
            return carry

        with scope("groups"):
            lax.fori_loop(0, tokens // (GROUP * GROUP_UNROLL), body, 0)

        @pl.when(c + 1 < chunks)
        def _():
            for copy in kv_copies(c + 1):
                copy.start()

        @pl.when(c == 0)
        def _():
            weight_copies[3].wait()

        @pl.when(c == 1)
        def _():
            relay(0)

        @pl.when(c >= 1)
        def _():
            dispatched(c - 1)

        hidden = hin[lax.rem(c, HIN_SLOTS)].astype(F32)
        attn_out = jnp.concatenate([o3[pl.ds(g, tokens, stride=8), :].astype(BF16) for g in range(8)], axis=1)
        before = c + 5
        mixed = dot(attn_out, wo[...])
        router = logits(before)
        picked = gather_rows(before, 0, 0)
        new_mid = (hidden + mixed).astype(BF16)
        mid[lax.rem(c, 3)] = new_mid
        n_buf[lax.rem(c, 3), pl.ds(0, tokens), :] = rms(new_mid.astype(F32), m_gain[...].astype(F32))
        gates(before, router)
        gather_gate(picked, before, 0, 0)
        dx_copy(c).start()
        dc_copy(c).start()

        @pl.when(jnp.logical_and(pp == 1, c + HIN_SLOTS < chunks))
        def _():
            pl.semaphore_signal(credit, inc=1, device_id=other_pp, device_id_type=MESH)

    def tile_at(c, row, j):
        return smem_table[lax.rem(c, 2), row, j]

    def gather_rows(c, j, u):
        normed = n_buf.at[lax.rem(c, 3)]
        return moe_gather(j, u, tile_at(c, 0, j), tile_at(c, 1, j), first, normed, rank_buf.at[lax.rem(c, 2)], picks, x_buf)

    def gather_gate(picked, c, j, u):
        moe_gate(picked, u, tile_at(c, 0, j), first, gate_ref, g_buf)

    def gather(c, j, u):
        gather_gate(gather_rows(c, j, u), c, j, u)

    def dispatched(c):
        with scope("w_disp"):
            dc_copy(c).wait_recv()
            dr_copy(c).wait_recv()

    def logits(c):
        return dot_nt(w_r[...], n_buf[lax.rem(c, 3)])

    def gates(c, router):
        moe_gates(router, rank_buf.at[lax.rem(c, 2)], gate_ref)

    def experts(c):
        @pl.when(c == 0)
        def _():
            with scope("w_wts"):
                for copy in weight_copies[4:]:
                    copy.wait()

        def expand(j, u):
            moe_expand(u, tile_at(c, 0, j), w, x_buf, a_buf)

        def contract(j, u):
            moe_contract(j, u, tile_at(c, 0, j), w, a_buf, g_buf, terms)

        def body(idx, carry):
            base = idx * TILE_UNROLL
            expand(base, 0)
            gather(c, base + 1, 1)
            for u in range(1, TILE_UNROLL):
                expand(base + u, u)
                if u + 1 < TILE_UNROLL:
                    gather(c, base + u + 1, u + 1)
                else:
                    gather(c, lax.rem(base + TILE_UNROLL, tile_count), 0)
                contract(base + u - 1, u - 1)
            contract(base + TILE_UNROLL - 1, TILE_UNROLL - 1)
            return carry

        with scope("tiles"):
            lax.fori_loop(0, tile_count // TILE_UNROLL, body, 0)
        half = 2 * tokens
        part[pl.ds(half, half), :] = dot(picks[pl.ds(half, half), :], terms[...])
        dr_copy(c).wait_send()
        r1_copy(c).start()

    def finish(c):
        s = lax.rem(c, 2)

        @pl.when(jnp.logical_and(pp == 0, c >= HIN_SLOTS))
        def _():
            pl.semaphore_wait(credit, 1)

        @pl.when(c >= 2)
        def _():
            for p in range(PIECES):
                @pl.when(pp == 0)
                def _():
                    hop_copy(c - 2, p).wait_send()

                @pl.when(pp == 1)
                def _():
                    out_copy(c - 2, p).wait_send()
                    out_local(c - 2, p).wait()

        def settle(at, pieces):
            mixed = (rb1[s, at, :] + rb2[lax.rem(c, 3), at, :]).astype(BF16)
            result = (mid[lax.rem(c, 3), at, :].astype(F32) + mixed.astype(F32)).astype(BF16)

            @pl.when(pp == 0)
            def _():
                ho[s, at, :] = result
                for p in pieces:
                    hop_copy(c, p).start()

            @pl.when(pp == 1)
            def _():
                vals = result.astype(F32)
                vals = vals * lax.rsqrt(jnp.mean(vals * vals, axis=-1, keepdims=True) + EPS)
                for g in range(8):
                    ho[s, at, g * 128:(g + 1) * 128] = (vals[:, g * 128:(g + 1) * 128] * f_gain[g:g + 1, :]).astype(BF16)
                for p in pieces:
                    out_copy(c, p).start()
                    out_local(c, p).start()

        @pl.when(c < chunks - 1)
        def _():
            with scope("w_r2"):
                for p in range(PIECES):
                    r2_copy(c, p).wait_recv()
            settle(pl.ds(0, tokens), range(PIECES))

        @pl.when(c == chunks - 1)
        def _():
            for p in range(PIECES):
                with scope("w_r2l"):
                    r2_copy(c, p).wait_recv()
                settle(piece(p), (p,))

        for p in range(PIECES):
            r2_copy(c, p).wait_send()

    def step(i, carry):
        @pl.when(i < 2)
        def _():
            with scope("project"):
                project(i, False)

        @pl.when(jnp.logical_and(i >= 2, i < chunks))
        def _():
            with scope("project_sum"):
                project(i, True)

        @pl.when(i >= chunks)
        def _():
            combine_near(0, 1024)

        @pl.when(jnp.logical_and(i >= 2, i <= chunks))
        def _():
            with scope("relay"):
                relay(i - 1)

        @pl.when(i >= 2)
        def _():
            with scope("reduce_pair"):
                reduce_pair(i - 2)

        @pl.when(i < chunks)
        def _():
            with scope("attend"):
                attend(i)

        @pl.when(i == chunks)
        def _():
            dispatched(i - 1)
            gates(i - 1, logits(i - 1))
            gather(i - 1, 0, 0)

        @pl.when(jnp.logical_and(i >= 1, i <= chunks))
        def _():
            with scope("experts"):
                experts(i - 1)

        @pl.when(i >= 2)
        def _():
            with scope("finish"):
                finish(i - 2)

        return carry

    lax.fori_loop(0, chunks + 2, step, 0)

    for copy in new_copies(chunks - 1):
        copy.wait()

    @pl.when(pp == 0)
    def _():
        for c in (chunks - 2, chunks - 1):
            for p in range(PIECES):
                hop_copy(c, p).wait_send()

        def arrived(c, carry):
            for p in range(PIECES):
                out_copy(c, p).wait_recv()
            return carry

        with scope("w_out"):
            lax.fori_loop(0, chunks, arrived, 0)

    @pl.when(pp == 1)
    def _():
        for c in (chunks - 2, chunks - 1):
            for p in range(PIECES):
                out_copy(c, p).wait_send()
                out_local(c, p).wait()


def step_call(args, chunks, tokens, tile_count):
    vmem = pl.BlockSpec(memory_space=pltpu.VMEM)
    hbm = pl.BlockSpec(memory_space=pl.ANY)
    wide = 4 * tokens
    dma = pltpu.SemaphoreType.DMA
    return pl.pallas_call(
        functools.partial(step_kernel, tile_count),
        out_shape=(
            jax.ShapeDtypeStruct((chunks, tokens, 1024), BF16),
            jax.ShapeDtypeStruct((chunks, tokens, 8, 64), BF16),
            jax.ShapeDtypeStruct((chunks, tokens, 8, 64), BF16),
        ),
        in_specs=[hbm, vmem, hbm, hbm, vmem, hbm, hbm, hbm, hbm, vmem, vmem, vmem, vmem, vmem, hbm, hbm, hbm, vmem],
        out_specs=(hbm, hbm, hbm),
        scratch_shapes=[
            pltpu.VMEM((3, wide, 1024), BF16),
            pltpu.VMEM((HIN_SLOTS, tokens, 1024), BF16),
            pltpu.VMEM((3, tokens, 1024), BF16),
            pltpu.VMEM((2, tokens, 1024), BF16),
            pltpu.VMEM((tokens * 128, 64), BF16),
            pltpu.VMEM((tokens * 128, 64), BF16),
            pltpu.VMEM((1024, 1024), BF16),
            pltpu.VMEM((1024, 512), BF16),
            pltpu.VMEM((1024, 512), BF16),
            pltpu.VMEM((1024, 1024), BF16),
            pltpu.VMEM((8, 1024, 512), BF16),
            pltpu.VMEM((8, 1024, 512), BF16),
            pltpu.VMEM((8, 512, 1024), BF16),
            pltpu.VMEM((wide, 1024), F32),
            pltpu.VMEM((2, 2 * tokens, 1024), F32),
            pltpu.VMEM((3, tokens, 1024), F32),
            pltpu.VMEM((wide, tile_count * TILE), BF16),
            pltpu.VMEM((tile_count * TILE, 1024), BF16),
            pltpu.VMEM((3, TILE, 1024), BF16),
            pltpu.VMEM((3, TILE, 512), BF16),
            pltpu.VMEM((TILE_UNROLL, TILE, 128), F32),
            pltpu.VMEM((tokens * 8, 128), F32),
            pltpu.VMEM((tokens * 8, 128), F32),
            pltpu.VMEM((tokens * 8, 128), F32),
            pltpu.VMEM((tokens * 8, 128), F32),
            pltpu.VMEM((tokens, 8, 64), BF16),
            pltpu.VMEM((tokens, 8, 64), BF16),
            pltpu.VMEM((2, 32, wide), F32),
            pltpu.VMEM((32, wide), F32),
            pltpu.VMEM((32, wide), F32),
            pltpu.VMEM((tokens, 128), F32),
            pltpu.VMEM((tokens, 256), F32),
            pltpu.VMEM((4, chunks, 8, tokens), jnp.int32),
            pltpu.VMEM((8, 128), jnp.int32),
            pltpu.SMEM((2, 8, 128), jnp.int32),
            dma((7,)), dma((2, 4)), dma((2, 4)), dma(()), dma((HIN_SLOTS, PIECES)), dma((2,)), dma((2,)),
            dma((3,)), dma((3,)), dma((3,)), dma((3,)), dma((3,)), dma((3,)),
            dma((2,)), dma((2,)), dma((3, PIECES)), dma((3, PIECES)),
            dma((2, PIECES)), dma((2, PIECES)), dma((chunks, PIECES)),
            pltpu.SemaphoreType.REGULAR,
        ],
        compiler_params=pltpu.CompilerParams(collective_id=0, has_side_effects=True, vmem_limit_bytes=67043328),
        name="decode_step",
        cost_estimate=pl.CostEstimate(flops=2 * 10**11, bytes_accessed=2 * 10**8, transcendentals=0),
    )(*args)


def solution(mesh):
    rows_spec = ("dp", "ep")
    three_dim = P("pp", None, None)
    two_dim = P("pp", None)
    expert_spec = P("pp", "ep", None, None)
    cache_spec = P("pp", None, rows_spec, None, None, None)
    new_spec = P("pp", None, rows_spec, None, None)
    in_specs = (P(None, rows_spec, None), P(None, rows_spec), cache_spec, cache_spec, P("pp", None, rows_spec, None), three_dim, three_dim, three_dim, three_dim, two_dim, two_dim, three_dim, expert_spec, expert_spec, expert_spec, P(None))
    out_specs = (P(None, rows_spec, None), new_spec, new_spec)

    def device_fn(hidden_in, seq_pos, k_cache, v_cache, expert_ids, w_query, w_key, w_value, w_out, attn_gain, mlp_gain, w_router, w_gate, w_up, w_down, final_gain):
        micro, rows = seq_pos.shape
        chunks = micro // PER_CHUNK
        tokens = PER_CHUNK * rows
        wide = 4 * tokens
        tile_count = (wide * 2 - 8) // TILE + 8
        angles = np.arange(1, 17)[:, None] * THETA ** (-np.arange(32) / 32)
        both = np.concatenate([np.tile(np.cos(angles), (1, 4)), np.tile(np.concatenate([-np.sin(angles), np.sin(angles)], axis=1), (1, 2))], axis=1)
        both = np.concatenate([both, np.zeros((112, 256))], axis=0).astype(np.float32)
        table = []
        for _ in range(3):
            table.append(both.astype(BF16))
            both = both - table[-1].astype(np.float32)
        table = jnp.asarray(np.concatenate(table, axis=1))
        tri = jnp.asarray(np.triu(np.ones((wide, wide)), 1), BF16)
        ids = jnp.swapaxes(expert_ids[0].reshape(chunks, tokens, 8), 1, 2)
        args = (
            hidden_in.reshape(chunks, tokens, 1024), seq_pos.reshape(chunks, tokens), k_cache.reshape(chunks, tokens * 128, 64), v_cache.reshape(chunks, tokens * 128, 64),
            ids, w_query[0], w_key[0], w_value[0], w_out[0], attn_gain, mlp_gain, final_gain.astype(F32).reshape(8, 128), table, w_router[0].T,
            w_gate[0], w_up[0], w_down[0], tri,
        )
        out, k_new, v_new = step_call(args, chunks, tokens, tile_count)
        shape = (1,) + seq_pos.shape + (8, 64)
        return out.reshape(hidden_in.shape), k_new.reshape(shape), v_new.reshape(shape)

    return jax.shard_map(device_fn, mesh=mesh, in_specs=in_specs, out_specs=out_specs, check_vma=False)
```

```python
import functools

import jax
import jax.numpy as jnp
import numpy as np
from jax import lax
from jax.experimental import pallas as pl
from jax.experimental.pallas import tpu as pltpu
from jax.sharding import PartitionSpec as P

THETA = 1000000.0
EPS = 1e-05
F32 = jnp.float32
BF16 = jnp.bfloat16
TILE = 128
GROUP = 16
GROUP_UNROLL = 8
TILE_UNROLL = 3
PER_CHUNK = 4
HIN_SLOTS = 4
PIECES = 4
MESH = pl.DeviceIdType.MESH


def scope(name):
    return jax.named_scope(name)


def rms(vals, gain_row):
    inv = lax.rsqrt(jnp.mean(vals * vals, axis=-1, keepdims=True) + EPS)
    return (vals * inv * gain_row).astype(BF16)


def dot(lhs, rhs):
    return jnp.dot(lhs, rhs, preferred_element_type=F32)


def dot_nt(lhs, rhs):
    return lax.dot_general(lhs, rhs, (((1,), (1,)), ((), ())), preferred_element_type=F32)


def rope_tables(pos, table):
    lane = lax.broadcasted_iota(jnp.int32, pos.shape, 1).astype(F32)
    both = dot(jnp.where(lane + 1.0 == pos, 1.0, 0.0).astype(BF16), table[...])
    both = both[:, :256] + both[:, 256:512] + both[:, 512:]
    return both


def rope(vals, cos_t, sin_t):
    lane = lax.broadcasted_iota(jnp.int32, (1, 128), 1)
    first = (lane % 64) < 32
    parts = []
    for j in range(vals.shape[1] // 128):
        block = vals[:, j * 128:(j + 1) * 128]
        swapped = jnp.where(first, pltpu.roll(block, 96, 1), pltpu.roll(block, 32, 1))
        parts.append(block * cos_t + swapped * sin_t)
    return jnp.concatenate(parts, axis=1)


def spread(ref, vals):
    tokens = vals.shape[0]
    for g in range(8):
        ref[pl.ds(g, tokens, stride=8), :] = vals[:, g * 128:(g + 1) * 128]


def spread_heads(ref, vals):
    tokens = vals.shape[0]
    low = lax.broadcasted_iota(jnp.int32, (1, 128), 1) < 64
    for j in range(4):
        block = vals[:, j * 128:(j + 1) * 128]
        other = pltpu.roll(block, 64, 1)
        ref[pl.ds(2 * j, tokens, stride=8), :] = jnp.where(low, block, other)
        ref[pl.ds(2 * j + 1, tokens, stride=8), :] = jnp.where(low, other, block)


def rows_of(ref, idx):
    return ref[pl.ds(pl.multiple_of(idx * GROUP * 8, GROUP * 8), GROUP * 8), :].reshape(GROUP, 8, 128)


def attn_dots(hidden, w, raw):
    normed = rms(hidden.astype(F32), w["a_gain"][...].astype(F32))
    raw[1] = dot(normed, w["q"][...]).astype(BF16)
    raw[2, :, :512] = dot(normed, w["k"][...]).astype(BF16)
    raw[2, :, 512:] = dot(normed, w["v"][...]).astype(BF16)


def attn_rope(turn, raw, q3, k3, v3):
    cos_t, sin_t = turn[:, :128], turn[:, 128:]
    spread(q3, rope(raw[1].astype(F32), cos_t, sin_t).astype(BF16).astype(F32))
    spread_heads(k3, rope(raw[2, :, :512].astype(F32), cos_t, sin_t).astype(BF16).astype(F32))
    spread_heads(v3, raw[2, :, 512:].astype(F32))


def attn_scores(idx, q3, k3, k_rows):
    q = rows_of(q3, idx)
    lane3 = lax.broadcasted_iota(jnp.int32, (1, 1, 128), 2)
    prod = q * rows_of(k3, idx)
    self_a = jnp.sum(jnp.where(lane3 < 64, prod, 0.0), axis=-1, keepdims=True)
    self_b = jnp.sum(jnp.where(lane3 < 64, 0.0, prod), axis=-1, keepdims=True)
    wide = (GROUP, 8, 128)
    self_s = jnp.concatenate([jnp.broadcast_to(self_a, wide), jnp.broadcast_to(self_b, wide)], axis=1) * 0.125
    q_rows = jnp.concatenate([q, pltpu.roll(q, 64, 2)], axis=1).astype(BF16)[:, :, :64].reshape(GROUP * 16, 64)
    row0 = idx * (GROUP * 128)
    blocks = []
    for p in range(GROUP // 2):
        keys = k_rows[pl.ds(pl.multiple_of(row0 + p * 256, 256), 256), :]
        both = dot_nt(q_rows[p * 32:(p + 1) * 32], keys)
        blocks.append(both[:16, :128].reshape(1, 16, 128))
        blocks.append(both[16:, 128:].reshape(1, 16, 128))
    return jnp.concatenate(blocks, axis=0), self_s


def attn_weights(idx, scores, self_s, pos_ref):
    row_i = lax.broadcasted_iota(jnp.int32, (16, 128), 0)
    lane_i = lax.broadcasted_iota(jnp.int32, (16, 128), 1)
    step = jnp.where((row_i % 8) == (lane_i % 8), lane_i // 8, 1000).astype(F32)
    pos = pos_ref[pl.ds(pl.multiple_of(idx * GROUP, GROUP), GROUP), :].reshape(GROUP, 1, 128)
    scores = jnp.where(step.reshape(1, 16, 128) < pos, scores * 0.125, -jnp.inf)
    wide = (GROUP, 16, 128)
    top = jnp.maximum(jnp.broadcast_to(jnp.max(scores, axis=-1, keepdims=True), wide), self_s)
    weights = jnp.exp(scores - top)
    self_w = jnp.exp(self_s - top)
    inv = 1.0 / (jnp.broadcast_to(jnp.sum(weights, axis=-1, keepdims=True), wide) + self_w)
    return (weights * inv).astype(BF16), (self_w * inv).astype(BF16).astype(F32)


def attn_mix(idx, weights, self_w, v3, o3, v_rows):
    row0 = idx * (GROUP * 128)
    zeros = jnp.zeros((16, 128), BF16)
    outs = []
    for p in range(GROUP // 2):
        vals = v_rows[pl.ds(pl.multiple_of(row0 + p * 256, 256), 256), :]
        upper = jnp.concatenate([weights[2 * p], zeros], axis=1)
        lower = jnp.concatenate([zeros, weights[2 * p + 1]], axis=1)
        outs.append(dot(jnp.concatenate([upper, lower], axis=0), vals).reshape(2, 16, 64))
    out = jnp.concatenate(outs, axis=0)
    v_new = rows_of(v3, idx)[:, :, :64]
    out_a = out[:, :8] + self_w[:, :8, :64] * v_new
    out_b = out[:, 8:] + self_w[:, 8:, :64] * v_new
    o3[pl.ds(pl.multiple_of(idx * GROUP * 8, GROUP * 8), GROUP * 8), :] = jnp.concatenate([out_a, out_b], axis=-1).reshape(GROUP * 8, 128)


def plan_tiles(ids, first, tri, member_ref, rank_ref, table_ref):
    tokens = ids.shape[1]
    expert_i = lax.broadcasted_iota(jnp.int32, (32, tokens), 0)
    chosen = jnp.zeros((32, tokens), F32)
    for s in range(ids.shape[0]):
        chosen = jnp.where(ids[s:s + 1, :] == expert_i, 1.0, chosen)
    member_ref[...] = chosen
    rank = dot(chosen.astype(BF16), tri[...])
    rank_ref[...] = jnp.where(chosen > 0.0, rank, -1.0)
    local = member_ref[pl.ds(pl.multiple_of(first, 8), 8), :]
    counts = jnp.sum(local, axis=-1, keepdims=True).astype(jnp.int32)
    tiles = jnp.broadcast_to(lax.shift_right_logical(counts + (TILE - 1), 7), (8, 128))
    lane = lax.broadcasted_iota(jnp.int32, (1, 128), 1)
    end = jnp.zeros((1, 128), jnp.int32)
    start = jnp.zeros((1, 128), jnp.int32)
    expert = jnp.zeros((1, 128), jnp.int32)
    for e in range(8):
        end = end + tiles[e:e + 1, :]
        passed = lane >= end
        expert = jnp.where(passed, expert + 1, expert)
        start = jnp.where(passed, end, start)
    sub = jnp.where(expert < 8, lane - start, 1000)
    table_ref[0:1, :] = jnp.minimum(expert, 7)
    table_ref[1:2, :] = sub


def moe_gates(logits, rank_ref, gate_ref):
    chosen = rank_ref[...] >= 0.0
    top = jnp.max(jnp.where(chosen, logits, -jnp.inf), axis=0, keepdims=True)
    gates = jnp.where(chosen, jnp.exp(logits - top), 0.0)
    gate_ref[...] = gates / jnp.sum(gates, axis=0, keepdims=True)


def slot_of(u):
    return 0 if u == 0 else 1 + (u - 1) % 2


def moe_gather(j, u, expert, sub, first, normed, rank_ref, picks, x_buf):
    ranks = rank_ref[pl.ds(first + expert, 1), :]
    wanted = (lax.broadcasted_iota(jnp.int32, (TILE, 1), 0) + sub * TILE).astype(F32)
    picked = jnp.where(ranks == wanted, 1.0, 0.0)
    picks[:, pl.ds(pl.multiple_of(j * TILE, TILE), TILE)] = picked.T.astype(BF16)
    x_buf[slot_of(u)] = dot(picked.astype(BF16), normed[...]).astype(BF16)
    return picked


def moe_gate(picked, u, expert, first, gate_ref, g_buf):
    gate = jnp.sum(picked * gate_ref[pl.ds(first + expert, 1), :], axis=-1, keepdims=True)
    g_buf[u] = jnp.broadcast_to(gate, (TILE, 128))


def moe_expand(u, expert, w, x_buf, a_buf):
    rows = x_buf[slot_of(u)]
    a_buf[slot_of(u)] = (jax.nn.silu(dot(rows, w["gate"][expert])) * dot(rows, w["up"][expert])).astype(BF16)


def moe_contract(j, u, expert, w, a_buf, g_buf, terms):
    y = dot(a_buf[slot_of(u)], w["down"][expert])
    gate = g_buf[u]
    at = pl.ds(pl.multiple_of(j * TILE, TILE), TILE)
    for p in range(8):
        terms[at, p * 128:(p + 1) * 128] = (gate * y[:, p * 128:(p + 1) * 128]).astype(BF16)


def step_kernel(
    tile_count,
    hid, seq, k_cache, v_cache, ids_own, wq_h, wk_h, wv_h, wo_h, a_gain, m_gain, f_gain, rope_ref, w_r, wg_h, wu_h, wd_h, tri,
    out, kn_out, vn_out,
    n_buf, hin, mid, ho, k_buf, v_buf, wq, wk, wv, wo, wg, wu, wd, part, rb1, rb2, picks, terms, x_buf, a_buf, g_buf, q3, k3, v3, o3, kn, vn, rank_buf, gate_ref, member, pos, turn, ids, table, smem_table,
    w_sem, ids_send, ids_recv, table_sem, hin_sem, kv_sem, new_sem, dx_send, dx_recv, dc_send, dc_recv, dr_send, dr_recv, r1_send, r1_recv, r2_send, r2_recv, hop_send, out_loc, out_recv, credit,
):
    chunks, tokens = hid.shape[0], hid.shape[1]
    gathered = 4 * tokens
    dp = lax.axis_index("dp")
    pp = lax.axis_index("pp")
    ep = lax.axis_index("ep")
    other_pp = (dp, 1 - pp, ep)
    across = (dp, pp, lax.rem(ep + 2, 4))
    beside = (dp, pp, ep + 1 - 2 * lax.rem(ep, 2))
    first = ep * 8

    diagonal = (dp, pp, lax.rem(ep + 3 - 2 * lax.rem(ep, 2), 4))

    attn_w = [(wq_h, wq), (wk_h, wk), (wv_h, wv), (wo_h, wo)]
    moe_w = [(wg_h, wg), (wu_h, wu), (wd_h, wd)]
    weight_copies = [pltpu.make_async_copy(s, d, w_sem.at[j]) for j, (s, d) in enumerate(attn_w + moe_w)]

    def hin_copies(c):
        h = lax.rem(c, HIN_SLOTS)
        return [pltpu.make_async_copy(hid.at[c, piece(p)], hin.at[h, piece(p)], hin_sem.at[h, p]) for p in range(PIECES)]

    def kv_copies(c):
        return (pltpu.make_async_copy(k_cache.at[c], k_buf, kv_sem.at[0]), pltpu.make_async_copy(v_cache.at[c], v_buf, kv_sem.at[1]))

    def new_copies(c):
        return (pltpu.make_async_copy(kn, kn_out.at[c], new_sem.at[0]), pltpu.make_async_copy(vn, vn_out.at[c], new_sem.at[1]))

    def remote(src, dst, send, recv, peer):
        return pltpu.make_async_remote_copy(src_ref=src, dst_ref=dst, send_sem=send, recv_sem=recv, device_id=peer, device_id_type=MESH)

    def rows_at(slot, part_idx):
        return n_buf.at[slot, pl.ds(part_idx * tokens, tokens)]

    def dx_copy(c):
        s = lax.rem(c, 3)
        return remote(rows_at(s, 0), rows_at(s, 1), dx_send.at[s], dx_recv.at[s], across)

    def dc_copy(c):
        s = lax.rem(c, 3)
        return remote(rows_at(s, 0), rows_at(s, 2), dc_send.at[s], dc_recv.at[s], beside)

    def dr_copy(c):
        s = lax.rem(c, 3)
        return remote(rows_at(s, 1), rows_at(s, 3), dr_send.at[s], dr_recv.at[s], beside)

    def r1_copy(c, home):
        s = lax.rem(c, 2)
        return remote(part.at[pl.ds((2 + home) * tokens, tokens)], rb1.at[s, pl.ds(home * tokens, tokens)], r1_send.at[s, home], r1_recv.at[s, home], beside)

    rows = tokens // PIECES

    def piece(p):
        return pl.ds(p * rows, rows)

    def r2_copy(c, p):
        s = lax.rem(c, 3)
        return remote(rb1.at[lax.rem(c, 2), pl.ds(tokens + p * rows, rows)], rb2.at[s, piece(p)], r2_send.at[s, p], r2_recv.at[s, p], across)

    def hop_copy(c, p):
        s = lax.rem(c, 2)
        h = lax.rem(c, HIN_SLOTS)
        return remote(ho.at[s, piece(p)], hin.at[h, piece(p)], hop_send.at[s, p], hin_sem.at[h, p], other_pp)

    def out_copy(c, p):
        s = lax.rem(c, 2)
        return remote(ho.at[s, piece(p)], out.at[c, piece(p)], hop_send.at[s, p], out_recv.at[c, p], other_pp)

    def out_local(c, p):
        s = lax.rem(c, 2)
        return pltpu.make_async_copy(ho.at[s, piece(p)], out.at[c, piece(p)], out_loc.at[s, p])

    def ids_copies(part_idx):
        some = pl.ds(0, 1) if part_idx == 0 else pl.ds(1, chunks - 1)
        return [remote(ids_own.at[some], ids.at[j, some], ids_send.at[part_idx, j], ids_recv.at[part_idx, j], peer) for j, peer in ((1, across), (2, beside), (3, diagonal))]

    def table_copy(c):
        s = lax.rem(c, 2)
        return pltpu.make_async_copy(table, smem_table.at[s], table_sem)

    smem_table[1, 0, 0] = 0
    smem_table[1, 1, 0] = 0

    @pl.when(pp == 0)
    def _():
        for copy in hin_copies(0):
            copy.start()

    for copy in weight_copies[:3]:
        copy.start()
    for copy in kv_copies(0):
        copy.start()
    weight_copies[3].start()

    @pl.when(pp == 0)
    def _():
        for copy in hin_copies(1):
            copy.start()

    barrier = pltpu.get_barrier_semaphore()
    for peer in (other_pp, across, beside, diagonal):
        pl.semaphore_signal(barrier, inc=1, device_id=peer, device_id_type=MESH)
    pl.semaphore_wait(barrier, 4)

    for part_idx in range(2):
        for copy in ids_copies(part_idx):
            copy.start()

    w = {"a_gain": a_gain, "rope": rope_ref, "q": wq, "k": wk, "v": wv, "gate": wg, "up": wu, "down": wd}

    def plan(c):
        @pl.when(c == 0)
        def _():
            ids[0] = ids_own[...]
            with scope("w_ids"):
                for copy in ids_copies(0):
                    copy.wait()

        @pl.when(c == 1)
        def _():
            for copy in ids_copies(1):
                copy.wait()

        chosen_ids = jnp.concatenate([ids[j, c] for j in range(4)], axis=1)
        plan_tiles(chosen_ids, first, tri, member, rank_buf.at[lax.rem(c, 2)], table)
        table_copy(c).start()

    def combine_near(from_col, to_col):
        half = pl.ds(0, 2 * tokens)
        part[half, from_col:to_col] = dot(picks[half, :], terms[:, from_col:to_col])

    def project(c, with_sums):
        plan(c)
        with scope("w_hin"):
            for copy in hin_copies(c):
                copy.wait()

        @pl.when(c == 0)
        def _():
            for copy in weight_copies[:3]:
                copy.wait()

        @pl.when(jnp.logical_and(pp == 0, c + 2 < chunks))
        def _():
            for copy in hin_copies(c + 2):
                copy.start()

        @pl.when(c > 0)
        def _():
            for copy in new_copies(c - 1):
                copy.wait()

        seq_row = seq[pl.ds(c, 1), :].astype(F32)
        pos[...] = jnp.broadcast_to(seq_row, (128, 128)).T
        turn[...] = rope_tables(pos[...], w["rope"])
        if with_sums:
            combine_near(0, 256)
        attn_dots(hin[lax.rem(c, HIN_SLOTS)], w, x_buf)
        if with_sums:
            combine_near(256, 1024)
        attn_rope(turn, x_buf, q3, k3, v3)
        kn[...] = k3[...].reshape(tokens, 8, 128)[:, :, :64].astype(BF16)
        vn[...] = v3[...].reshape(tokens, 8, 128)[:, :, :64].astype(BF16)
        for copy in new_copies(c):
            copy.start()

    def reduce_pair(c):
        s = lax.rem(c, 2)
        far = pl.ds(tokens, tokens)
        near = pl.ds(0, tokens)
        with scope("w_r1"):
            r1_copy(c, 1).wait_recv()
        rb1[s, far, :] = rb1[s, far, :] + part[far, :]
        for p in range(PIECES):
            r2_copy(c, p).start()
        r1_copy(c, 0).wait_recv()
        rb1[s, near, :] = rb1[s, near, :] + part[near, :]
        for home in (1, 0):
            r1_copy(c, home).wait_send()

    def relay(c):
        copy = dx_copy(c)
        with scope("w_dx"):
            copy.wait_recv()
        dr_copy(c).start()
        copy.wait_send()
        dc_copy(c).wait_send()

    def attend(c):
        table_copy(c).wait()
        with scope("w_kv"):
            for copy in kv_copies(c):
                copy.wait()

        def body(idx, carry):
            base = idx * GROUP_UNROLL
            ahead = attn_scores(base, q3, k3, k_buf)
            for u in range(GROUP_UNROLL):
                scores = ahead
                if u + 1 < GROUP_UNROLL:
                    ahead = attn_scores(base + u + 1, q3, k3, k_buf)
                attn_mix(base + u, *attn_weights(base + u, *scores, pos), v3, o3, v_buf)
            return carry

        with scope("groups"):
            lax.fori_loop(0, tokens // (GROUP * GROUP_UNROLL), body, 0)

        @pl.when(c + 1 < chunks)
        def _():
            for copy in kv_copies(c + 1):
                copy.start()

        @pl.when(c == 0)
        def _():
            for copy in weight_copies[4:]:
                copy.start()

        @pl.when(c == 0)
        def _():
            weight_copies[3].wait()

        @pl.when(c == 1)
        def _():
            relay(0)

        @pl.when(c >= 1)
        def _():
            dispatched(c - 1)

        hidden = hin[lax.rem(c, HIN_SLOTS)].astype(F32)
        attn_out = jnp.concatenate([o3[pl.ds(g, tokens, stride=8), :].astype(BF16) for g in range(8)], axis=1)
        before = c + 5
        mixed = dot(attn_out, wo[...])
        router = logits(before)
        picked = gather_rows(before, 0, 0)
        new_mid = (hidden + mixed).astype(BF16)
        mid[lax.rem(c, 3)] = new_mid
        n_buf[lax.rem(c, 3), pl.ds(0, tokens), :] = rms(new_mid.astype(F32), m_gain[...].astype(F32))
        gates(before, router)
        gather_gate(picked, before, 0, 0)
        dx_copy(c).start()
        dc_copy(c).start()

        @pl.when(jnp.logical_and(pp == 1, c + HIN_SLOTS < chunks))
        def _():
            pl.semaphore_signal(credit, inc=1, device_id=other_pp, device_id_type=MESH)

    def tile_at(c, row, j):
        return smem_table[lax.rem(c, 2), row, j]

    def gather_rows(c, j, u):
        normed = n_buf.at[lax.rem(c, 3)]
        return moe_gather(j, u, tile_at(c, 0, j), tile_at(c, 1, j), first, normed, rank_buf.at[lax.rem(c, 2)], picks, x_buf)

    def gather_gate(picked, c, j, u):
        moe_gate(picked, u, tile_at(c, 0, j), first, gate_ref, g_buf)

    def gather(c, j, u):
        gather_gate(gather_rows(c, j, u), c, j, u)

    def dispatched(c):
        with scope("w_disp"):
            dc_copy(c).wait_recv()
            dr_copy(c).wait_recv()

    def logits(c):
        return dot_nt(w_r[...], n_buf[lax.rem(c, 3)])

    def gates(c, router):
        moe_gates(router, rank_buf.at[lax.rem(c, 2)], gate_ref)

    def experts(c):
        @pl.when(c == 0)
        def _():
            with scope("w_wts"):
                for copy in weight_copies[4:]:
                    copy.wait()

        def expand(j, u):
            moe_expand(u, tile_at(c, 0, j), w, x_buf, a_buf)

        def contract(j, u):
            moe_contract(j, u, tile_at(c, 0, j), w, a_buf, g_buf, terms)

        def body(idx, carry):
            base = idx * TILE_UNROLL
            expand(base, 0)
            gather(c, base + 1, 1)
            for u in range(1, TILE_UNROLL):
                expand(base + u, u)
                if u + 1 < TILE_UNROLL:
                    gather(c, base + u + 1, u + 1)
                else:
                    gather(c, lax.rem(base + TILE_UNROLL, tile_count), 0)
                contract(base + u - 1, u - 1)
            contract(base + TILE_UNROLL - 1, TILE_UNROLL - 1)
            return carry

        with scope("tiles"):
            lax.fori_loop(0, tile_count // TILE_UNROLL, body, 0)
        half = 2 * tokens
        part[pl.ds(half, half), :] = dot(picks[pl.ds(half, half), :], terms[...])
        dr_copy(c).wait_send()
        r1_copy(c, 1).start()
        r1_copy(c, 0).start()

    def finish(c):
        s = lax.rem(c, 2)

        @pl.when(jnp.logical_and(pp == 0, c >= HIN_SLOTS))
        def _():
            pl.semaphore_wait(credit, 1)

        @pl.when(c >= 2)
        def _():
            for p in range(PIECES):
                @pl.when(pp == 0)
                def _():
                    hop_copy(c - 2, p).wait_send()

                @pl.when(pp == 1)
                def _():
                    out_copy(c - 2, p).wait_send()
                    out_local(c - 2, p).wait()

        def settle(at, pieces):
            mixed = (rb1[s, at, :] + rb2[lax.rem(c, 3), at, :]).astype(BF16)
            result = (mid[lax.rem(c, 3), at, :].astype(F32) + mixed.astype(F32)).astype(BF16)

            @pl.when(pp == 0)
            def _():
                ho[s, at, :] = result
                for p in pieces:
                    hop_copy(c, p).start()

            @pl.when(pp == 1)
            def _():
                vals = result.astype(F32)
                vals = vals * lax.rsqrt(jnp.mean(vals * vals, axis=-1, keepdims=True) + EPS)
                for g in range(8):
                    ho[s, at, g * 128:(g + 1) * 128] = (vals[:, g * 128:(g + 1) * 128] * f_gain[g:g + 1, :]).astype(BF16)
                for p in pieces:
                    out_copy(c, p).start()
                    out_local(c, p).start()

        @pl.when(c < chunks - 1)
        def _():
            with scope("w_r2"):
                for p in range(PIECES):
                    r2_copy(c, p).wait_recv()
            settle(pl.ds(0, tokens), range(PIECES))

        @pl.when(c == chunks - 1)
        def _():
            for p in range(PIECES):
                with scope("w_r2l"):
                    r2_copy(c, p).wait_recv()
                settle(piece(p), (p,))

        for p in range(PIECES):
            r2_copy(c, p).wait_send()

    def step(i, carry):
        @pl.when(i < 2)
        def _():
            with scope("project"):
                project(i, False)

        @pl.when(jnp.logical_and(i >= 2, i < chunks))
        def _():
            with scope("project_sum"):
                project(i, True)

        @pl.when(i >= chunks)
        def _():
            combine_near(0, 1024)

        @pl.when(i >= 2)
        def _():
            with scope("reduce_pair"):
                reduce_pair(i - 2)

        @pl.when(jnp.logical_and(i >= 2, i <= chunks))
        def _():
            with scope("relay"):
                relay(i - 1)

        @pl.when(i < chunks)
        def _():
            with scope("attend"):
                attend(i)

        @pl.when(i == chunks)
        def _():
            dispatched(i - 1)
            gates(i - 1, logits(i - 1))
            gather(i - 1, 0, 0)

        @pl.when(jnp.logical_and(i >= 1, i <= chunks))
        def _():
            with scope("experts"):
                experts(i - 1)

        @pl.when(i >= 2)
        def _():
            with scope("finish"):
                finish(i - 2)

        return carry

    lax.fori_loop(0, chunks + 2, step, 0)

    for copy in new_copies(chunks - 1):
        copy.wait()

    @pl.when(pp == 0)
    def _():
        for c in (chunks - 2, chunks - 1):
            for p in range(PIECES):
                hop_copy(c, p).wait_send()

        def arrived(c, carry):
            for p in range(PIECES):
                out_copy(c, p).wait_recv()
            return carry

        with scope("w_out"):
            lax.fori_loop(0, chunks, arrived, 0)

    @pl.when(pp == 1)
    def _():
        for c in (chunks - 2, chunks - 1):
            for p in range(PIECES):
                out_copy(c, p).wait_send()
                out_local(c, p).wait()


def step_call(args, chunks, tokens, tile_count):
    vmem = pl.BlockSpec(memory_space=pltpu.VMEM)
    hbm = pl.BlockSpec(memory_space=pl.ANY)
    wide = 4 * tokens
    dma = pltpu.SemaphoreType.DMA
    return pl.pallas_call(
        functools.partial(step_kernel, tile_count),
        out_shape=(
            jax.ShapeDtypeStruct((chunks, tokens, 1024), BF16),
            jax.ShapeDtypeStruct((chunks, tokens, 8, 64), BF16),
            jax.ShapeDtypeStruct((chunks, tokens, 8, 64), BF16),
        ),
        in_specs=[hbm, vmem, hbm, hbm, vmem, hbm, hbm, hbm, hbm, vmem, vmem, vmem, vmem, vmem, hbm, hbm, hbm, vmem],
        out_specs=(hbm, hbm, hbm),
        scratch_shapes=[
            pltpu.VMEM((3, wide, 1024), BF16),
            pltpu.VMEM((HIN_SLOTS, tokens, 1024), BF16),
            pltpu.VMEM((3, tokens, 1024), BF16),
            pltpu.VMEM((2, tokens, 1024), BF16),
            pltpu.VMEM((tokens * 128, 64), BF16),
            pltpu.VMEM((tokens * 128, 64), BF16),
            pltpu.VMEM((1024, 1024), BF16),
            pltpu.VMEM((1024, 512), BF16),
            pltpu.VMEM((1024, 512), BF16),
            pltpu.VMEM((1024, 1024), BF16),
            pltpu.VMEM((8, 1024, 512), BF16),
            pltpu.VMEM((8, 1024, 512), BF16),
            pltpu.VMEM((8, 512, 1024), BF16),
            pltpu.VMEM((wide, 1024), F32),
            pltpu.VMEM((2, 2 * tokens, 1024), F32),
            pltpu.VMEM((3, tokens, 1024), F32),
            pltpu.VMEM((wide, tile_count * TILE), BF16),
            pltpu.VMEM((tile_count * TILE, 1024), BF16),
            pltpu.VMEM((3, TILE, 1024), BF16),
            pltpu.VMEM((3, TILE, 512), BF16),
            pltpu.VMEM((TILE_UNROLL, TILE, 128), F32),
            pltpu.VMEM((tokens * 8, 128), F32),
            pltpu.VMEM((tokens * 8, 128), F32),
            pltpu.VMEM((tokens * 8, 128), F32),
            pltpu.VMEM((tokens * 8, 128), F32),
            pltpu.VMEM((tokens, 8, 64), BF16),
            pltpu.VMEM((tokens, 8, 64), BF16),
            pltpu.VMEM((2, 32, wide), F32),
            pltpu.VMEM((32, wide), F32),
            pltpu.VMEM((32, wide), F32),
            pltpu.VMEM((tokens, 128), F32),
            pltpu.VMEM((tokens, 256), F32),
            pltpu.VMEM((4, chunks, 8, tokens), jnp.int32),
            pltpu.VMEM((8, 128), jnp.int32),
            pltpu.SMEM((2, 8, 128), jnp.int32),
            dma((7,)), dma((2, 4)), dma((2, 4)), dma(()), dma((HIN_SLOTS, PIECES)), dma((2,)), dma((2,)),
            dma((3,)), dma((3,)), dma((3,)), dma((3,)), dma((3,)), dma((3,)),
            dma((2, 2)), dma((2, 2)), dma((3, PIECES)), dma((3, PIECES)),
            dma((2, PIECES)), dma((2, PIECES)), dma((chunks, PIECES)),
            pltpu.SemaphoreType.REGULAR,
        ],
        compiler_params=pltpu.CompilerParams(collective_id=0, has_side_effects=True, vmem_limit_bytes=67043328),
        name="decode_step",
        cost_estimate=pl.CostEstimate(flops=2 * 10**11, bytes_accessed=2 * 10**8, transcendentals=0),
    )(*args)


def solution(mesh):
    rows_spec = ("dp", "ep")
    three_dim = P("pp", None, None)
    two_dim = P("pp", None)
    expert_spec = P("pp", "ep", None, None)
    cache_spec = P("pp", None, rows_spec, None, None, None)
    new_spec = P("pp", None, rows_spec, None, None)
    in_specs = (P(None, rows_spec, None), P(None, rows_spec), cache_spec, cache_spec, P("pp", None, rows_spec, None), three_dim, three_dim, three_dim, three_dim, two_dim, two_dim, three_dim, expert_spec, expert_spec, expert_spec, P(None))
    out_specs = (P(None, rows_spec, None), new_spec, new_spec)

    def device_fn(hidden_in, seq_pos, k_cache, v_cache, expert_ids, w_query, w_key, w_value, w_out, attn_gain, mlp_gain, w_router, w_gate, w_up, w_down, final_gain):
        micro, rows = seq_pos.shape
        chunks = micro // PER_CHUNK
        tokens = PER_CHUNK * rows
        wide = 4 * tokens
        tile_count = (wide * 2 - 8) // TILE + 8
        angles = np.arange(1, 17)[:, None] * THETA ** (-np.arange(32) / 32)
        both = np.concatenate([np.tile(np.cos(angles), (1, 4)), np.tile(np.concatenate([-np.sin(angles), np.sin(angles)], axis=1), (1, 2))], axis=1)
        both = np.concatenate([both, np.zeros((112, 256))], axis=0).astype(np.float32)
        table = []
        for _ in range(3):
            table.append(both.astype(BF16))
            both = both - table[-1].astype(np.float32)
        table = jnp.asarray(np.concatenate(table, axis=1))
        tri = jnp.asarray(np.triu(np.ones((wide, wide)), 1), BF16)
        ids = jnp.swapaxes(expert_ids[0].reshape(chunks, tokens, 8), 1, 2)
        args = (
            hidden_in.reshape(chunks, tokens, 1024), seq_pos.reshape(chunks, tokens), k_cache.reshape(chunks, tokens * 128, 64), v_cache.reshape(chunks, tokens * 128, 64),
            ids, w_query[0], w_key[0], w_value[0], w_out[0], attn_gain, mlp_gain, final_gain.astype(F32).reshape(8, 128), table, w_router[0].T,
            w_gate[0], w_up[0], w_down[0], tri,
        )
        out, k_new, v_new = step_call(args, chunks, tokens, tile_count)
        shape = (1,) + seq_pos.shape + (8, 64)
        return out.reshape(hidden_in.shape), k_new.reshape(shape), v_new.reshape(shape)

    return jax.shard_map(device_fn, mesh=mesh, in_specs=in_specs, out_specs=out_specs, check_vma=False)
```

```python
import functools

import jax
import jax.numpy as jnp
import numpy as np
from jax import lax
from jax.experimental import pallas as pl
from jax.experimental.pallas import tpu as pltpu
from jax.sharding import PartitionSpec as P

THETA = 1000000.0
EPS = 1e-05
F32 = jnp.float32
BF16 = jnp.bfloat16
TILE = 128
GROUP = 16
GROUP_UNROLL = 8
TILE_UNROLL = 3
PER_CHUNK = 4
HIN_SLOTS = 4
PIECES = 4
MESH = pl.DeviceIdType.MESH


def scope(name):
    return jax.named_scope(name)


def rms(vals, gain_row):
    inv = lax.rsqrt(jnp.mean(vals * vals, axis=-1, keepdims=True) + EPS)
    return (vals * inv * gain_row).astype(BF16)


def dot(lhs, rhs):
    return jnp.dot(lhs, rhs, preferred_element_type=F32)


def dot_nt(lhs, rhs):
    return lax.dot_general(lhs, rhs, (((1,), (1,)), ((), ())), preferred_element_type=F32)


def rope_tables(pos, table):
    lane = lax.broadcasted_iota(jnp.int32, pos.shape, 1).astype(F32)
    both = dot(jnp.where(lane + 1.0 == pos, 1.0, 0.0).astype(BF16), table[...])
    both = both[:, :256] + both[:, 256:512] + both[:, 512:]
    return both


def rope(vals, cos_t, sin_t):
    lane = lax.broadcasted_iota(jnp.int32, (1, 128), 1)
    first = (lane % 64) < 32
    parts = []
    for j in range(vals.shape[1] // 128):
        block = vals[:, j * 128:(j + 1) * 128]
        swapped = jnp.where(first, pltpu.roll(block, 96, 1), pltpu.roll(block, 32, 1))
        parts.append(block * cos_t + swapped * sin_t)
    return jnp.concatenate(parts, axis=1)


def spread(ref, vals):
    tokens = vals.shape[0]
    for g in range(8):
        ref[pl.ds(g, tokens, stride=8), :] = vals[:, g * 128:(g + 1) * 128]


def spread_heads(ref, vals):
    tokens = vals.shape[0]
    low = lax.broadcasted_iota(jnp.int32, (1, 128), 1) < 64
    for j in range(4):
        block = vals[:, j * 128:(j + 1) * 128]
        other = pltpu.roll(block, 64, 1)
        ref[pl.ds(2 * j, tokens, stride=8), :] = jnp.where(low, block, other)
        ref[pl.ds(2 * j + 1, tokens, stride=8), :] = jnp.where(low, other, block)


def rows_of(ref, idx):
    return ref[pl.ds(pl.multiple_of(idx * GROUP * 8, GROUP * 8), GROUP * 8), :].reshape(GROUP, 8, 128)


def attn_dots(hidden, w, raw):
    normed = rms(hidden.astype(F32), w["a_gain"][...].astype(F32))
    raw[1] = dot(normed, w["q"][...]).astype(BF16)
    raw[2, :, :512] = dot(normed, w["k"][...]).astype(BF16)
    raw[2, :, 512:] = dot(normed, w["v"][...]).astype(BF16)


def attn_rope(turn, raw, q3, k3, v3, kn, vn):
    cos_t, sin_t = turn[:, :128], turn[:, 128:]
    spread(q3, rope(raw[1].astype(F32), cos_t, sin_t).astype(BF16).astype(F32))
    k = rope(raw[2, :, :512].astype(F32), cos_t, sin_t).astype(BF16)
    kn[...] = k
    spread_heads(k3, k.astype(F32))
    v = raw[2, :, 512:]
    vn[...] = v
    spread_heads(v3, v.astype(F32))


def attn_scores(idx, q3, k3, k_rows):
    q = rows_of(q3, idx)
    lane3 = lax.broadcasted_iota(jnp.int32, (1, 1, 128), 2)
    prod = q * rows_of(k3, idx)
    self_a = jnp.sum(jnp.where(lane3 < 64, prod, 0.0), axis=-1, keepdims=True)
    self_b = jnp.sum(jnp.where(lane3 < 64, 0.0, prod), axis=-1, keepdims=True)
    wide = (GROUP, 8, 128)
    self_s = jnp.concatenate([jnp.broadcast_to(self_a, wide), jnp.broadcast_to(self_b, wide)], axis=1) * 0.125
    q_rows = jnp.concatenate([q, pltpu.roll(q, 64, 2)], axis=1).astype(BF16)[:, :, :64].reshape(GROUP * 16, 64)
    row0 = idx * (GROUP * 128)
    blocks = []
    for p in range(GROUP // 2):
        keys = k_rows[pl.ds(pl.multiple_of(row0 + p * 256, 256), 256), :]
        both = dot_nt(q_rows[p * 32:(p + 1) * 32], keys)
        blocks.append(both[:16, :128].reshape(1, 16, 128))
        blocks.append(both[16:, 128:].reshape(1, 16, 128))
    return jnp.concatenate(blocks, axis=0), self_s


def attn_weights(idx, scores, self_s, pos_ref):
    row_i = lax.broadcasted_iota(jnp.int32, (16, 128), 0)
    lane_i = lax.broadcasted_iota(jnp.int32, (16, 128), 1)
    step = jnp.where((row_i % 8) == (lane_i % 8), lane_i // 8, 1000).astype(F32)
    pos = pos_ref[pl.ds(pl.multiple_of(idx * GROUP, GROUP), GROUP), :].reshape(GROUP, 1, 128)
    scores = jnp.where(step.reshape(1, 16, 128) < pos, scores * 0.125, -jnp.inf)
    wide = (GROUP, 16, 128)
    top = jnp.maximum(jnp.broadcast_to(jnp.max(scores, axis=-1, keepdims=True), wide), self_s)
    weights = jnp.exp(scores - top)
    self_w = jnp.exp(self_s - top)
    inv = 1.0 / (jnp.broadcast_to(jnp.sum(weights, axis=-1, keepdims=True), wide) + self_w)
    return (weights * inv).astype(BF16), (self_w * inv).astype(BF16).astype(F32)


def attn_mix(idx, weights, self_w, v3, o3, v_rows):
    row0 = idx * (GROUP * 128)
    zeros = jnp.zeros((16, 128), BF16)
    outs = []
    for p in range(GROUP // 2):
        vals = v_rows[pl.ds(pl.multiple_of(row0 + p * 256, 256), 256), :]
        upper = jnp.concatenate([weights[2 * p], zeros], axis=1)
        lower = jnp.concatenate([zeros, weights[2 * p + 1]], axis=1)
        outs.append(dot(jnp.concatenate([upper, lower], axis=0), vals).reshape(2, 16, 64))
    out = jnp.concatenate(outs, axis=0)
    v_new = rows_of(v3, idx)[:, :, :64]
    out_a = out[:, :8] + self_w[:, :8, :64] * v_new
    out_b = out[:, 8:] + self_w[:, 8:, :64] * v_new
    o3[pl.ds(pl.multiple_of(idx * GROUP * 8, GROUP * 8), GROUP * 8), :] = jnp.concatenate([out_a, out_b], axis=-1).reshape(GROUP * 8, 128)


def plan_tiles(ids, first, tri, member_ref, rank_ref, table_ref):
    tokens = ids.shape[1]
    expert_i = lax.broadcasted_iota(jnp.int32, (32, tokens), 0)
    chosen = jnp.zeros((32, tokens), F32)
    for s in range(ids.shape[0]):
        chosen = jnp.where(ids[s:s + 1, :] == expert_i, 1.0, chosen)
    member_ref[...] = chosen
    rank = dot(chosen.astype(BF16), tri[...])
    rank_ref[...] = jnp.where(chosen > 0.0, rank, -1.0)
    local = member_ref[pl.ds(pl.multiple_of(first, 8), 8), :]
    counts = jnp.sum(local, axis=-1, keepdims=True).astype(jnp.int32)
    tiles = jnp.broadcast_to(lax.shift_right_logical(counts + (TILE - 1), 7), (8, 128))
    lane = lax.broadcasted_iota(jnp.int32, (1, 128), 1)
    end = jnp.zeros((1, 128), jnp.int32)
    start = jnp.zeros((1, 128), jnp.int32)
    expert = jnp.zeros((1, 128), jnp.int32)
    for e in range(8):
        end = end + tiles[e:e + 1, :]
        passed = lane >= end
        expert = jnp.where(passed, expert + 1, expert)
        start = jnp.where(passed, end, start)
    sub = jnp.where(expert < 8, lane - start, 1000)
    table_ref[0:1, :] = jnp.minimum(expert, 7)
    table_ref[1:2, :] = sub


def moe_gates(logits, rank_ref, gate_ref):
    chosen = rank_ref[...] >= 0.0
    top = jnp.max(jnp.where(chosen, logits, -jnp.inf), axis=0, keepdims=True)
    gates = jnp.where(chosen, jnp.exp(logits - top), 0.0)
    gate_ref[...] = gates / jnp.sum(gates, axis=0, keepdims=True)


def slot_of(u):
    return 0 if u == 0 else 1 + (u - 1) % 2


def moe_gather(j, u, expert, sub, first, normed, rank_ref, picks, x_buf):
    ranks = rank_ref[pl.ds(first + expert, 1), :]
    wanted = (lax.broadcasted_iota(jnp.int32, (TILE, 1), 0) + sub * TILE).astype(F32)
    picked = jnp.where(ranks == wanted, 1.0, 0.0)
    picks[:, pl.ds(pl.multiple_of(j * TILE, TILE), TILE)] = picked.T.astype(BF16)
    x_buf[slot_of(u)] = dot(picked.astype(BF16), normed[...]).astype(BF16)
    return picked


def moe_gate(picked, u, expert, first, gate_ref, g_buf):
    gate = jnp.sum(picked * gate_ref[pl.ds(first + expert, 1), :], axis=-1, keepdims=True)
    g_buf[u] = jnp.broadcast_to(gate, (TILE, 128))


def moe_expand(u, expert, w, x_buf, a_buf):
    rows = x_buf[slot_of(u)]
    a_buf[slot_of(u)] = (jax.nn.silu(dot(rows, w["gate"][expert])) * dot(rows, w["up"][expert])).astype(BF16)


def moe_contract(j, u, expert, w, a_buf, g_buf, terms):
    y = dot(a_buf[slot_of(u)], w["down"][expert])
    gate = g_buf[u]
    at = pl.ds(pl.multiple_of(j * TILE, TILE), TILE)
    for p in range(8):
        terms[at, p * 128:(p + 1) * 128] = (gate * y[:, p * 128:(p + 1) * 128]).astype(BF16)


def step_kernel(
    tile_count,
    hid, seq, k_cache, v_cache, ids_own, wq_h, wk_h, wv_h, wo_h, a_gain, m_gain, rope_ref, w_r, wg_h, wu_h, wd_h, tri,
    out, kn_out, vn_out,
    n_buf, hin, mid, ho, k_buf, v_buf, wq, wk, wv, wo, wg, wu, wd, part, rb1, rb2, picks, terms, x_buf, a_buf, g_buf, q3, k3, v3, o3, kn, vn, rank_buf, gate_ref, member, pos, turn, ids, table, smem_table,
    w_sem, ids_send, ids_recv, table_sem, hin_sem, kv_sem, new_sem, dx_send, dx_recv, dc_send, dc_recv, dr_send, dr_recv, r1_send, r1_recv, r2_send, r2_recv, hop_send, out_loc, out_recv, credit,
):
    chunks, tokens = hid.shape[0], hid.shape[1]
    gathered = 4 * tokens
    dp = lax.axis_index("dp")
    pp = lax.axis_index("pp")
    ep = lax.axis_index("ep")
    other_pp = (dp, 1 - pp, ep)
    across = (dp, pp, lax.rem(ep + 2, 4))
    beside = (dp, pp, ep + 1 - 2 * lax.rem(ep, 2))
    first = ep * 8

    diagonal = (dp, pp, lax.rem(ep + 3 - 2 * lax.rem(ep, 2), 4))

    attn_w = [(wq_h, wq), (wk_h, wk), (wv_h, wv), (wo_h, wo)]
    moe_w = [(wg_h, wg), (wu_h, wu), (wd_h, wd)]
    weight_copies = [pltpu.make_async_copy(s, d, w_sem.at[j]) for j, (s, d) in enumerate(attn_w + moe_w)]

    def hin_copies(c):
        h = lax.rem(c, HIN_SLOTS)
        return [pltpu.make_async_copy(hid.at[c, piece(p)], hin.at[h, piece(p)], hin_sem.at[h, p]) for p in range(PIECES)]

    def kv_copies(c):
        return (pltpu.make_async_copy(k_cache.at[c], k_buf, kv_sem.at[0]), pltpu.make_async_copy(v_cache.at[c], v_buf, kv_sem.at[1]))

    def new_copies(c):
        return (pltpu.make_async_copy(kn, kn_out.at[c], new_sem.at[0]), pltpu.make_async_copy(vn, vn_out.at[c], new_sem.at[1]))

    def remote(src, dst, send, recv, peer):
        return pltpu.make_async_remote_copy(src_ref=src, dst_ref=dst, send_sem=send, recv_sem=recv, device_id=peer, device_id_type=MESH)

    def rows_at(slot, part_idx):
        return n_buf.at[slot, pl.ds(part_idx * tokens, tokens)]

    def dx_copy(c):
        s = lax.rem(c, 3)
        return remote(rows_at(s, 0), rows_at(s, 1), dx_send.at[s], dx_recv.at[s], across)

    def dc_copy(c):
        s = lax.rem(c, 3)
        return remote(rows_at(s, 0), rows_at(s, 2), dc_send.at[s], dc_recv.at[s], beside)

    def dr_copy(c):
        s = lax.rem(c, 3)
        return remote(rows_at(s, 1), rows_at(s, 3), dr_send.at[s], dr_recv.at[s], beside)

    def r1_copy(c, home):
        s = lax.rem(c, 2)
        return remote(part.at[pl.ds((2 + home) * tokens, tokens)], rb1.at[s, pl.ds(home * tokens, tokens)], r1_send.at[s, home], r1_recv.at[s, home], beside)

    rows = tokens // PIECES

    def piece(p):
        return pl.ds(p * rows, rows)

    def r2_copy(c, p):
        s = lax.rem(c, 3)
        return remote(rb1.at[lax.rem(c, 2), pl.ds(tokens + p * rows, rows)], rb2.at[s, piece(p)], r2_send.at[s, p], r2_recv.at[s, p], across)

    def hop_copy(c, p):
        s = lax.rem(c, 2)
        h = lax.rem(c, HIN_SLOTS)
        return remote(ho.at[s, piece(p)], hin.at[h, piece(p)], hop_send.at[s, p], hin_sem.at[h, p], other_pp)

    def out_copy(c, p):
        s = lax.rem(c, 2)
        return remote(ho.at[s, piece(p)], out.at[c, piece(p)], hop_send.at[s, p], out_recv.at[c, p], other_pp)

    def out_local(c, p):
        s = lax.rem(c, 2)
        return pltpu.make_async_copy(ho.at[s, piece(p)], out.at[c, piece(p)], out_loc.at[s, p])

    def ids_copies(part_idx):
        some = pl.ds(0, 1) if part_idx == 0 else pl.ds(1, chunks - 1)
        return [remote(ids_own.at[some], ids.at[j, some], ids_send.at[part_idx, j], ids_recv.at[part_idx, j], peer) for j, peer in ((1, across), (2, beside), (3, diagonal))]

    def table_copy(c):
        s = lax.rem(c, 2)
        return pltpu.make_async_copy(table, smem_table.at[s], table_sem)

    smem_table[1, 0, 0] = 0
    smem_table[1, 1, 0] = 0

    @pl.when(pp == 0)
    def _():
        for copy in hin_copies(0):
            copy.start()

    for copy in weight_copies[:3]:
        copy.start()
    for copy in kv_copies(0):
        copy.start()
    weight_copies[3].start()

    @pl.when(pp == 0)
    def _():
        for copy in hin_copies(1):
            copy.start()

    barrier = pltpu.get_barrier_semaphore()
    for peer in (other_pp, across, beside, diagonal):
        pl.semaphore_signal(barrier, inc=1, device_id=peer, device_id_type=MESH)
    pl.semaphore_wait(barrier, 4)

    for part_idx in range(2):
        for copy in ids_copies(part_idx):
            copy.start()

    w = {"a_gain": a_gain, "rope": rope_ref, "q": wq, "k": wk, "v": wv, "gate": wg, "up": wu, "down": wd}

    def plan(c):
        @pl.when(c == 0)
        def _():
            ids[0] = ids_own[...]
            with scope("w_ids"):
                for copy in ids_copies(0):
                    copy.wait()

        @pl.when(c == 1)
        def _():
            for copy in ids_copies(1):
                copy.wait()

        chosen_ids = jnp.concatenate([ids[j, c] for j in range(4)], axis=1)
        plan_tiles(chosen_ids, first, tri, member, rank_buf.at[lax.rem(c, 2)], table)
        table_copy(c).start()

    def combine_near(from_col, to_col):
        half = pl.ds(0, 2 * tokens)
        part[half, from_col:to_col] = dot(picks[half, :], terms[:, from_col:to_col])

    def project(c, with_sums):
        plan(c)
        with scope("w_hin"):
            for copy in hin_copies(c):
                copy.wait()

        @pl.when(c == 0)
        def _():
            for copy in weight_copies[:3]:
                copy.wait()

        @pl.when(jnp.logical_and(pp == 0, c + 2 < chunks))
        def _():
            for copy in hin_copies(c + 2):
                copy.start()

        @pl.when(c > 0)
        def _():
            for copy in new_copies(c - 1):
                copy.wait()

        seq_row = seq[pl.ds(c, 1), :].astype(F32)
        pos[...] = jnp.broadcast_to(seq_row, (128, 128)).T
        turn[...] = rope_tables(pos[...], w["rope"])
        if with_sums:
            combine_near(0, 256)
        attn_dots(hin[lax.rem(c, HIN_SLOTS)], w, x_buf)
        if with_sums:
            combine_near(256, 1024)
        attn_rope(turn, x_buf, q3, k3, v3, kn, vn)
        for copy in new_copies(c):
            copy.start()

    def reduce_pair(c):
        s = lax.rem(c, 2)
        far = pl.ds(tokens, tokens)
        near = pl.ds(0, tokens)
        with scope("w_r1"):
            r1_copy(c, 1).wait_recv()
        rb1[s, far, :] = rb1[s, far, :] + part[far, :]
        for p in range(PIECES):
            r2_copy(c, p).start()
        r1_copy(c, 0).wait_recv()
        rb1[s, near, :] = rb1[s, near, :] + part[near, :]
        for home in (1, 0):
            r1_copy(c, home).wait_send()

    def relay(c):
        copy = dx_copy(c)
        with scope("w_dx"):
            copy.wait_recv()
        dr_copy(c).start()
        copy.wait_send()
        dc_copy(c).wait_send()

    def attend(c):
        table_copy(c).wait()
        with scope("w_kv"):
            for copy in kv_copies(c):
                copy.wait()

        @pl.when(c == 0)
        def _():
            weight_copies[4].start()

        @pl.when(c == 1)
        def _():
            for copy in weight_copies[5:]:
                copy.start()

        def body(idx, carry):
            base = idx * GROUP_UNROLL
            ahead = attn_scores(base, q3, k3, k_buf)
            for u in range(GROUP_UNROLL):
                scores = ahead
                if u + 1 < GROUP_UNROLL:
                    ahead = attn_scores(base + u + 1, q3, k3, k_buf)
                attn_mix(base + u, *attn_weights(base + u, *scores, pos), v3, o3, v_buf)
            return carry

        with scope("groups"):
            lax.fori_loop(0, tokens // (GROUP * GROUP_UNROLL), body, 0)

        @pl.when(c + 1 < chunks)
        def _():
            for copy in kv_copies(c + 1):
                copy.start()

        @pl.when(c == 0)
        def _():
            weight_copies[3].wait()

        @pl.when(c == 1)
        def _():
            relay(0)

        @pl.when(c >= 1)
        def _():
            dispatched(c - 1)

        hidden = hin[lax.rem(c, HIN_SLOTS)].astype(F32)
        attn_out = jnp.concatenate([o3[pl.ds(g, tokens, stride=8), :].astype(BF16) for g in range(8)], axis=1)
        before = c + 5
        mixed = dot(attn_out, wo[...])
        router = logits(before)
        picked = gather_rows(before, 0, 0)
        new_mid = (hidden + mixed).astype(BF16)
        mid[lax.rem(c, 3)] = new_mid
        n_buf[lax.rem(c, 3), pl.ds(0, tokens), :] = rms(new_mid.astype(F32), m_gain[...].astype(F32))
        gates(before, router)
        gather_gate(picked, before, 0, 0)
        dx_copy(c).start()
        dc_copy(c).start()

        @pl.when(jnp.logical_and(pp == 1, c + HIN_SLOTS < chunks))
        def _():
            pl.semaphore_signal(credit, inc=1, device_id=other_pp, device_id_type=MESH)

    def tile_at(c, row, j):
        return smem_table[lax.rem(c, 2), row, j]

    def gather_rows(c, j, u):
        normed = n_buf.at[lax.rem(c, 3)]
        return moe_gather(j, u, tile_at(c, 0, j), tile_at(c, 1, j), first, normed, rank_buf.at[lax.rem(c, 2)], picks, x_buf)

    def gather_gate(picked, c, j, u):
        moe_gate(picked, u, tile_at(c, 0, j), first, gate_ref, g_buf)

    def gather(c, j, u):
        gather_gate(gather_rows(c, j, u), c, j, u)

    def dispatched(c):
        with scope("w_disp"):
            dc_copy(c).wait_recv()
            dr_copy(c).wait_recv()

    def logits(c):
        return dot_nt(w_r[...], n_buf[lax.rem(c, 3)])

    def gates(c, router):
        moe_gates(router, rank_buf.at[lax.rem(c, 2)], gate_ref)

    def experts(c):
        @pl.when(c == 0)
        def _():
            with scope("w_wts"):
                for copy in weight_copies[4:]:
                    copy.wait()

        def expand(j, u):
            moe_expand(u, tile_at(c, 0, j), w, x_buf, a_buf)

        def contract(j, u):
            moe_contract(j, u, tile_at(c, 0, j), w, a_buf, g_buf, terms)

        def body(idx, carry):
            base = idx * TILE_UNROLL
            expand(base, 0)
            gather(c, base + 1, 1)
            for u in range(1, TILE_UNROLL):
                expand(base + u, u)
                if u + 1 < TILE_UNROLL:
                    gather(c, base + u + 1, u + 1)
                else:
                    gather(c, lax.rem(base + TILE_UNROLL, tile_count), 0)
                contract(base + u - 1, u - 1)
            contract(base + TILE_UNROLL - 1, TILE_UNROLL - 1)
            return carry

        with scope("tiles"):
            lax.fori_loop(0, tile_count // TILE_UNROLL, body, 0)
        half = 2 * tokens
        part[pl.ds(half, half), :] = dot(picks[pl.ds(half, half), :], terms[...])
        dr_copy(c).wait_send()
        r1_copy(c, 1).start()
        r1_copy(c, 0).start()

    def finish(c):
        s = lax.rem(c, 2)

        @pl.when(jnp.logical_and(pp == 0, c >= HIN_SLOTS))
        def _():
            pl.semaphore_wait(credit, 1)

        @pl.when(c >= 2)
        def _():
            for p in range(PIECES):
                @pl.when(pp == 0)
                def _():
                    hop_copy(c - 2, p).wait_send()

                @pl.when(pp == 1)
                def _():
                    out_copy(c - 2, p).wait_send()
                    out_local(c - 2, p).wait()

        def settle(at, pieces):
            mixed = (rb1[s, at, :] + rb2[lax.rem(c, 3), at, :]).astype(BF16)
            result = (mid[lax.rem(c, 3), at, :].astype(F32) + mixed.astype(F32)).astype(BF16)

            @pl.when(pp == 0)
            def _():
                ho[s, at, :] = result
                for p in pieces:
                    hop_copy(c, p).start()

            @pl.when(pp == 1)
            def _():
                ho[s, at, :] = result
                for p in pieces:
                    out_copy(c, p).start()
                    out_local(c, p).start()

        @pl.when(c < chunks - 1)
        def _():
            with scope("w_r2"):
                for p in range(PIECES):
                    r2_copy(c, p).wait_recv()
            settle(pl.ds(0, tokens), range(PIECES))

        @pl.when(c == chunks - 1)
        def _():
            for p in range(PIECES):
                with scope("w_r2l"):
                    r2_copy(c, p).wait_recv()
                settle(piece(p), (p,))

        for p in range(PIECES):
            r2_copy(c, p).wait_send()

    def step(i, carry):
        @pl.when(i < 2)
        def _():
            with scope("project"):
                project(i, False)

        @pl.when(jnp.logical_and(i >= 2, i < chunks))
        def _():
            with scope("project_sum"):
                project(i, True)

        @pl.when(i >= chunks)
        def _():
            combine_near(0, 1024)

        @pl.when(i >= 2)
        def _():
            with scope("reduce_pair"):
                reduce_pair(i - 2)

        @pl.when(jnp.logical_and(i >= 2, i <= chunks))
        def _():
            with scope("relay"):
                relay(i - 1)

        @pl.when(i < chunks)
        def _():
            with scope("attend"):
                attend(i)

        @pl.when(i == chunks)
        def _():
            dispatched(i - 1)
            gates(i - 1, logits(i - 1))
            gather(i - 1, 0, 0)

        @pl.when(jnp.logical_and(i >= 1, i <= chunks))
        def _():
            with scope("experts"):
                experts(i - 1)

        @pl.when(i >= 2)
        def _():
            with scope("finish"):
                finish(i - 2)

        return carry

    lax.fori_loop(0, chunks + 2, step, 0)

    for copy in new_copies(chunks - 1):
        copy.wait()

    @pl.when(pp == 0)
    def _():
        for c in (chunks - 2, chunks - 1):
            for p in range(PIECES):
                hop_copy(c, p).wait_send()

        def arrived(c, carry):
            for p in range(PIECES):
                out_copy(c, p).wait_recv()
            return carry

        with scope("w_out"):
            lax.fori_loop(0, chunks, arrived, 0)

    @pl.when(pp == 1)
    def _():
        for c in (chunks - 2, chunks - 1):
            for p in range(PIECES):
                out_copy(c, p).wait_send()
                out_local(c, p).wait()


def step_call(args, chunks, tokens, tile_count):
    vmem = pl.BlockSpec(memory_space=pltpu.VMEM)
    hbm = pl.BlockSpec(memory_space=pl.ANY)
    wide = 4 * tokens
    dma = pltpu.SemaphoreType.DMA
    return pl.pallas_call(
        functools.partial(step_kernel, tile_count),
        out_shape=(
            jax.ShapeDtypeStruct((chunks, tokens, 1024), BF16),
            jax.ShapeDtypeStruct((chunks, tokens, 512), BF16),
            jax.ShapeDtypeStruct((chunks, tokens, 512), BF16),
        ),
        in_specs=[hbm, vmem, hbm, hbm, vmem, hbm, hbm, hbm, hbm, vmem, vmem, vmem, vmem, hbm, hbm, hbm, vmem],
        out_specs=(hbm, hbm, hbm),
        scratch_shapes=[
            pltpu.VMEM((3, wide, 1024), BF16),
            pltpu.VMEM((HIN_SLOTS, tokens, 1024), BF16),
            pltpu.VMEM((3, tokens, 1024), BF16),
            pltpu.VMEM((2, tokens, 1024), BF16),
            pltpu.VMEM((tokens * 128, 64), BF16),
            pltpu.VMEM((tokens * 128, 64), BF16),
            pltpu.VMEM((1024, 1024), BF16),
            pltpu.VMEM((1024, 512), BF16),
            pltpu.VMEM((1024, 512), BF16),
            pltpu.VMEM((1024, 1024), BF16),
            pltpu.VMEM((8, 1024, 512), BF16),
            pltpu.VMEM((8, 1024, 512), BF16),
            pltpu.VMEM((8, 512, 1024), BF16),
            pltpu.VMEM((wide, 1024), F32),
            pltpu.VMEM((2, 2 * tokens, 1024), F32),
            pltpu.VMEM((3, tokens, 1024), F32),
            pltpu.VMEM((wide, tile_count * TILE), BF16),
            pltpu.VMEM((tile_count * TILE, 1024), BF16),
            pltpu.VMEM((3, TILE, 1024), BF16),
            pltpu.VMEM((3, TILE, 512), BF16),
            pltpu.VMEM((TILE_UNROLL, TILE, 128), F32),
            pltpu.VMEM((tokens * 8, 128), F32),
            pltpu.VMEM((tokens * 8, 128), F32),
            pltpu.VMEM((tokens * 8, 128), F32),
            pltpu.VMEM((tokens * 8, 128), F32),
            pltpu.VMEM((tokens, 512), BF16),
            pltpu.VMEM((tokens, 512), BF16),
            pltpu.VMEM((2, 32, wide), F32),
            pltpu.VMEM((32, wide), F32),
            pltpu.VMEM((32, wide), F32),
            pltpu.VMEM((tokens, 128), F32),
            pltpu.VMEM((tokens, 256), F32),
            pltpu.VMEM((4, chunks, 8, tokens), jnp.int32),
            pltpu.VMEM((8, 128), jnp.int32),
            pltpu.SMEM((2, 8, 128), jnp.int32),
            dma((7,)), dma((2, 4)), dma((2, 4)), dma(()), dma((HIN_SLOTS, PIECES)), dma((2,)), dma((2,)),
            dma((3,)), dma((3,)), dma((3,)), dma((3,)), dma((3,)), dma((3,)),
            dma((2, 2)), dma((2, 2)), dma((3, PIECES)), dma((3, PIECES)),
            dma((2, PIECES)), dma((2, PIECES)), dma((chunks, PIECES)),
            pltpu.SemaphoreType.REGULAR,
        ],
        compiler_params=pltpu.CompilerParams(collective_id=0, has_side_effects=True, vmem_limit_bytes=67043328),
        name="decode_step",
        cost_estimate=pl.CostEstimate(flops=2 * 10**11, bytes_accessed=2 * 10**8, transcendentals=0),
    )(*args)


def result_kernel(h_ref, k_ref, v_ref, gain_ref, out_ref, kn_ref, vn_ref, rows):
    tokens = h_ref.shape[1]
    vals = h_ref[0].astype(F32)
    vals = vals * lax.rsqrt(jnp.mean(vals * vals, axis=-1, keepdims=True) + EPS)
    for g in range(8):
        out_ref[0, :, g * 128:(g + 1) * 128] = (vals[:, g * 128:(g + 1) * 128] * gain_ref[g:g + 1, :]).astype(BF16)
    for j, (src, dst) in enumerate(((k_ref, kn_ref), (v_ref, vn_ref))):
        spread_heads(rows.at[j], src[0].astype(F32))
        dst[0] = rows[j].reshape(tokens, 8, 128)[:, :, :64].astype(BF16)


def result_call(hidden, k_rows, v_rows, gain):
    chunks, tokens = hidden.shape[0], hidden.shape[1]
    wide = pl.BlockSpec((1, tokens, 1024), lambda i: (i, 0, 0))
    dense = pl.BlockSpec((1, tokens, 512), lambda i: (i, 0, 0))
    heads = pl.BlockSpec((1, tokens, 8, 64), lambda i: (i, 0, 0, 0))
    return pl.pallas_call(
        result_kernel,
        grid=(chunks,),
        out_shape=(
            jax.ShapeDtypeStruct((chunks, tokens, 1024), BF16),
            jax.ShapeDtypeStruct((chunks, tokens, 8, 64), BF16),
            jax.ShapeDtypeStruct((chunks, tokens, 8, 64), BF16),
        ),
        in_specs=[wide, dense, dense, pl.BlockSpec((8, 128), lambda i: (0, 0))],
        out_specs=(wide, heads, heads),
        scratch_shapes=[pltpu.VMEM((2, tokens * 8, 128), F32)],
        name="results",
        cost_estimate=pl.CostEstimate(flops=10**7, bytes_accessed=2 * 10**7, transcendentals=0),
    )(hidden, k_rows, v_rows, gain)


def solution(mesh):
    rows_spec = ("dp", "ep")
    three_dim = P("pp", None, None)
    two_dim = P("pp", None)
    expert_spec = P("pp", "ep", None, None)
    cache_spec = P("pp", None, rows_spec, None, None, None)
    new_spec = P("pp", None, rows_spec, None, None)
    in_specs = (P(None, rows_spec, None), P(None, rows_spec), cache_spec, cache_spec, P("pp", None, rows_spec, None), three_dim, three_dim, three_dim, three_dim, two_dim, two_dim, three_dim, expert_spec, expert_spec, expert_spec, P(None))
    out_specs = (P(None, rows_spec, None), new_spec, new_spec)

    def device_fn(hidden_in, seq_pos, k_cache, v_cache, expert_ids, w_query, w_key, w_value, w_out, attn_gain, mlp_gain, w_router, w_gate, w_up, w_down, final_gain):
        micro, rows = seq_pos.shape
        chunks = micro // PER_CHUNK
        tokens = PER_CHUNK * rows
        wide = 4 * tokens
        tile_count = (wide * 2 - 8) // TILE + 8
        angles = np.arange(1, 17)[:, None] * THETA ** (-np.arange(32) / 32)
        both = np.concatenate([np.tile(np.cos(angles), (1, 4)), np.tile(np.concatenate([-np.sin(angles), np.sin(angles)], axis=1), (1, 2))], axis=1)
        both = np.concatenate([both, np.zeros((112, 256))], axis=0).astype(np.float32)
        table = []
        for _ in range(3):
            table.append(both.astype(BF16))
            both = both - table[-1].astype(np.float32)
        table = jnp.asarray(np.concatenate(table, axis=1))
        tri = jnp.asarray(np.triu(np.ones((wide, wide)), 1), BF16)
        ids = jnp.swapaxes(expert_ids[0].reshape(chunks, tokens, 8), 1, 2)
        args = (
            hidden_in.reshape(chunks, tokens, 1024), seq_pos.reshape(chunks, tokens), k_cache.reshape(chunks, tokens * 128, 64), v_cache.reshape(chunks, tokens * 128, 64),
            ids, w_query[0], w_key[0], w_value[0], w_out[0], attn_gain, mlp_gain, table, w_router[0].T,
            w_gate[0], w_up[0], w_down[0], tri,
        )
        out, k_new, v_new = result_call(*step_call(args, chunks, tokens, tile_count), final_gain.astype(F32).reshape(8, 128))
        shape = (1,) + seq_pos.shape + (8, 64)
        return out.reshape(hidden_in.shape), k_new.reshape(shape), v_new.reshape(shape)

    return jax.shard_map(device_fn, mesh=mesh, in_specs=in_specs, out_specs=out_specs, check_vma=False)
```

```python
import functools

import jax
import jax.numpy as jnp
import numpy as np
from jax import lax
from jax.experimental import pallas as pl
from jax.experimental.pallas import tpu as pltpu
from jax.sharding import PartitionSpec as P

THETA = 1000000.0
EPS = 1e-05
F32 = jnp.float32
BF16 = jnp.bfloat16
TILE = 128
GROUP = 16
GROUP_UNROLL = 8
TILE_UNROLL = 3
PER_CHUNK = 4
HIN_SLOTS = 4
PIECES = 4
MESH = pl.DeviceIdType.MESH


def scope(name):
    return jax.named_scope(name)


def rms(vals, gain_row):
    inv = lax.rsqrt(jnp.mean(vals * vals, axis=-1, keepdims=True) + EPS)
    return (vals * inv * gain_row).astype(BF16)


def dot(lhs, rhs):
    return jnp.dot(lhs, rhs, preferred_element_type=F32)


def dot_nt(lhs, rhs):
    return lax.dot_general(lhs, rhs, (((1,), (1,)), ((), ())), preferred_element_type=F32)


def rope_tables(pos, table):
    lane = lax.broadcasted_iota(jnp.int32, pos.shape, 1).astype(F32)
    both = dot(jnp.where(lane + 1.0 == pos, 1.0, 0.0).astype(BF16), table[...])
    both = both[:, :256] + both[:, 256:512] + both[:, 512:]
    return both


def rope(vals, cos_t, sin_t):
    lane = lax.broadcasted_iota(jnp.int32, (1, 128), 1)
    first = (lane % 64) < 32
    parts = []
    for j in range(vals.shape[1] // 128):
        block = vals[:, j * 128:(j + 1) * 128]
        swapped = jnp.where(first, pltpu.roll(block, 96, 1), pltpu.roll(block, 32, 1))
        parts.append(block * cos_t + swapped * sin_t)
    return jnp.concatenate(parts, axis=1)


def spread(ref, vals):
    tokens = vals.shape[0]
    for g in range(8):
        ref[pl.ds(g, tokens, stride=8), :] = vals[:, g * 128:(g + 1) * 128]


def spread_heads(ref, vals):
    tokens = vals.shape[0]
    low = lax.broadcasted_iota(jnp.int32, (1, 128), 1) < 64
    for j in range(4):
        block = vals[:, j * 128:(j + 1) * 128]
        other = pltpu.roll(block, 64, 1)
        ref[pl.ds(2 * j, tokens, stride=8), :] = jnp.where(low, block, other)
        ref[pl.ds(2 * j + 1, tokens, stride=8), :] = jnp.where(low, other, block)


def rows_of(ref, idx):
    return ref[pl.ds(pl.multiple_of(idx * GROUP * 8, GROUP * 8), GROUP * 8), :].reshape(GROUP, 8, 128)


def attn_dots(hidden, w, raw):
    normed = rms(hidden.astype(F32), w["a_gain"][...].astype(F32))
    raw[1] = dot(normed, w["q"][...]).astype(BF16)
    raw[2, :, :512] = dot(normed, w["k"][...]).astype(BF16)
    raw[2, :, 512:] = dot(normed, w["v"][...]).astype(BF16)


def attn_rope(turn, raw, q3, k3, v3, kn, vn):
    cos_t, sin_t = turn[:, :128], turn[:, 128:]
    spread(q3, rope(raw[1].astype(F32), cos_t, sin_t).astype(BF16).astype(F32))
    k = rope(raw[2, :, :512].astype(F32), cos_t, sin_t).astype(BF16)
    kn[...] = k
    spread_heads(k3, k.astype(F32))
    v = raw[2, :, 512:]
    vn[...] = v
    spread_heads(v3, v.astype(F32))


def attn_scores(idx, q3, k3, k_rows):
    q = rows_of(q3, idx)
    lane3 = lax.broadcasted_iota(jnp.int32, (1, 1, 128), 2)
    prod = q * rows_of(k3, idx)
    self_a = jnp.sum(jnp.where(lane3 < 64, prod, 0.0), axis=-1, keepdims=True)
    self_b = jnp.sum(jnp.where(lane3 < 64, 0.0, prod), axis=-1, keepdims=True)
    wide = (GROUP, 8, 128)
    self_s = jnp.concatenate([jnp.broadcast_to(self_a, wide), jnp.broadcast_to(self_b, wide)], axis=1) * 0.125
    q_rows = jnp.concatenate([q, pltpu.roll(q, 64, 2)], axis=1).astype(BF16)[:, :, :64].reshape(GROUP * 16, 64)
    row0 = idx * (GROUP * 128)
    blocks = []
    for p in range(GROUP // 2):
        keys = k_rows[pl.ds(pl.multiple_of(row0 + p * 256, 256), 256), :]
        both = dot_nt(q_rows[p * 32:(p + 1) * 32], keys)
        blocks.append(both[:16, :128].reshape(1, 16, 128))
        blocks.append(both[16:, 128:].reshape(1, 16, 128))
    return jnp.concatenate(blocks, axis=0), self_s


def attn_weights(idx, scores, self_s, pos_ref):
    row_i = lax.broadcasted_iota(jnp.int32, (16, 128), 0)
    lane_i = lax.broadcasted_iota(jnp.int32, (16, 128), 1)
    step = jnp.where((row_i % 8) == (lane_i % 8), lane_i // 8, 1000).astype(F32)
    pos = pos_ref[pl.ds(pl.multiple_of(idx * GROUP, GROUP), GROUP), :].reshape(GROUP, 1, 128)
    scores = jnp.where(step.reshape(1, 16, 128) < pos, scores * 0.125, -jnp.inf)
    wide = (GROUP, 16, 128)
    top = jnp.maximum(jnp.broadcast_to(jnp.max(scores, axis=-1, keepdims=True), wide), self_s)
    weights = jnp.exp(scores - top)
    self_w = jnp.exp(self_s - top)
    inv = 1.0 / (jnp.broadcast_to(jnp.sum(weights, axis=-1, keepdims=True), wide) + self_w)
    return (weights * inv).astype(BF16), (self_w * inv).astype(BF16).astype(F32)


def attn_mix(idx, weights, self_w, v3, o3, v_rows):
    row0 = idx * (GROUP * 128)
    zeros = jnp.zeros((16, 128), BF16)
    outs = []
    for p in range(GROUP // 2):
        vals = v_rows[pl.ds(pl.multiple_of(row0 + p * 256, 256), 256), :]
        upper = jnp.concatenate([weights[2 * p], zeros], axis=1)
        lower = jnp.concatenate([zeros, weights[2 * p + 1]], axis=1)
        outs.append(dot(jnp.concatenate([upper, lower], axis=0), vals).reshape(2, 16, 64))
    out = jnp.concatenate(outs, axis=0)
    v_new = rows_of(v3, idx)[:, :, :64]
    out_a = out[:, :8] + self_w[:, :8, :64] * v_new
    out_b = out[:, 8:] + self_w[:, 8:, :64] * v_new
    o3[pl.ds(pl.multiple_of(idx * GROUP * 8, GROUP * 8), GROUP * 8), :] = jnp.concatenate([out_a, out_b], axis=-1).reshape(GROUP * 8, 128)


def plan_tiles(ids, first, tri, member_ref, rank_ref, table_ref):
    tokens = ids.shape[1]
    expert_i = lax.broadcasted_iota(jnp.int32, (32, tokens), 0)
    chosen = jnp.zeros((32, tokens), F32)
    for s in range(ids.shape[0]):
        chosen = jnp.where(ids[s:s + 1, :] == expert_i, 1.0, chosen)
    member_ref[...] = chosen
    rank = dot(chosen.astype(BF16), tri[...])
    rank_ref[...] = jnp.where(chosen > 0.0, rank, -1.0)
    local = member_ref[pl.ds(pl.multiple_of(first, 8), 8), :]
    counts = jnp.sum(local, axis=-1, keepdims=True).astype(jnp.int32)
    tiles = jnp.broadcast_to(lax.shift_right_logical(counts + (TILE - 1), 7), (8, 128))
    lane = lax.broadcasted_iota(jnp.int32, (1, 128), 1)
    end = jnp.zeros((1, 128), jnp.int32)
    start = jnp.zeros((1, 128), jnp.int32)
    expert = jnp.zeros((1, 128), jnp.int32)
    for e in range(8):
        end = end + tiles[e:e + 1, :]
        passed = lane >= end
        expert = jnp.where(passed, expert + 1, expert)
        start = jnp.where(passed, end, start)
    sub = jnp.where(expert < 8, lane - start, 1000)
    table_ref[0:1, :] = jnp.minimum(expert, 7)
    table_ref[1:2, :] = sub


def moe_gates(logits, rank_ref, gate_ref):
    chosen = rank_ref[...] >= 0.0
    top = jnp.max(jnp.where(chosen, logits, -jnp.inf), axis=0, keepdims=True)
    gates = jnp.where(chosen, jnp.exp(logits - top), 0.0)
    gate_ref[...] = gates / jnp.sum(gates, axis=0, keepdims=True)


def slot_of(u):
    return 0 if u == 0 else 1 + (u - 1) % 2


def moe_gather(j, u, expert, sub, first, normed, rank_ref, picks, x_buf):
    ranks = rank_ref[pl.ds(first + expert, 1), :]
    wanted = (lax.broadcasted_iota(jnp.int32, (TILE, 1), 0) + sub * TILE).astype(F32)
    picked = jnp.where(ranks == wanted, 1.0, 0.0)
    picks[:, pl.ds(pl.multiple_of(j * TILE, TILE), TILE)] = picked.T.astype(BF16)
    x_buf[slot_of(u)] = dot(picked.astype(BF16), normed[...]).astype(BF16)
    return picked


def moe_gate(picked, u, expert, first, gate_ref, g_buf):
    gate = jnp.sum(picked * gate_ref[pl.ds(first + expert, 1), :], axis=-1, keepdims=True)
    g_buf[u] = jnp.broadcast_to(gate, (TILE, 128))


def moe_expand(u, expert, w, x_buf, a_buf):
    rows = x_buf[slot_of(u)]
    a_buf[slot_of(u)] = (jax.nn.silu(dot(rows, w["gate"][expert])) * dot(rows, w["up"][expert])).astype(BF16)


def moe_contract(j, u, expert, w, a_buf, g_buf, terms):
    y = dot(a_buf[slot_of(u)], w["down"][expert])
    gate = g_buf[u]
    at = pl.ds(pl.multiple_of(j * TILE, TILE), TILE)
    for p in range(8):
        terms[at, p * 128:(p + 1) * 128] = (gate * y[:, p * 128:(p + 1) * 128]).astype(BF16)


def step_kernel(
    tile_count,
    hid, seq, k_cache, v_cache, ids_own, wq_h, wk_h, wv_h, wo_h, a_gain, m_gain, rope_ref, w_r, wg_h, wu_h, wd_h, tri,
    out, kn_out, vn_out,
    n_buf, hin, mid, ho, k_buf, v_buf, wq, wk, wv, wo, wg, wu, wd, part, rb1, rb2, picks, terms, x_buf, a_buf, g_buf, q3, k3, v3, o3, kn, vn, rank_buf, gate_ref, member, pos, turn, ids, table, smem_table,
    w_sem, ids_send, ids_recv, table_sem, hin_sem, kv_sem, new_sem, dx_send, dx_recv, dc_send, dc_recv, dr_send, dr_recv, r1_send, r1_recv, r2_send, r2_recv, hop_send, out_loc, out_recv, credit,
):
    chunks, tokens = hid.shape[0], hid.shape[1]
    gathered = 4 * tokens
    dp = lax.axis_index("dp")
    pp = lax.axis_index("pp")
    ep = lax.axis_index("ep")
    other_pp = (dp, 1 - pp, ep)
    across = (dp, pp, lax.rem(ep + 2, 4))
    beside = (dp, pp, ep + 1 - 2 * lax.rem(ep, 2))
    first = ep * 8

    diagonal = (dp, pp, lax.rem(ep + 3 - 2 * lax.rem(ep, 2), 4))

    attn_w = [(wq_h, wq), (wk_h, wk), (wv_h, wv), (wo_h, wo)]
    moe_w = [(wg_h, wg), (wu_h, wu), (wd_h, wd)]
    weight_copies = [pltpu.make_async_copy(s, d, w_sem.at[j]) for j, (s, d) in enumerate(attn_w + moe_w)]

    def hin_copies(c):
        h = lax.rem(c, HIN_SLOTS)
        return [pltpu.make_async_copy(hid.at[c, piece(p)], hin.at[h, piece(p)], hin_sem.at[h, p]) for p in range(PIECES)]

    def kv_copies(c):
        return (pltpu.make_async_copy(k_cache.at[c], k_buf, kv_sem.at[0]), pltpu.make_async_copy(v_cache.at[c], v_buf, kv_sem.at[1]))

    def new_copies(c):
        return (pltpu.make_async_copy(kn, kn_out.at[c], new_sem.at[0]), pltpu.make_async_copy(vn, vn_out.at[c], new_sem.at[1]))

    def remote(src, dst, send, recv, peer):
        return pltpu.make_async_remote_copy(src_ref=src, dst_ref=dst, send_sem=send, recv_sem=recv, device_id=peer, device_id_type=MESH)

    def rows_at(slot, part_idx):
        return n_buf.at[slot, pl.ds(part_idx * tokens, tokens)]

    def dx_copy(c):
        s = lax.rem(c, 3)
        return remote(rows_at(s, 0), rows_at(s, 1), dx_send.at[s], dx_recv.at[s], across)

    def dc_copy(c):
        s = lax.rem(c, 3)
        return remote(rows_at(s, 0), rows_at(s, 2), dc_send.at[s], dc_recv.at[s], beside)

    def dr_copy(c):
        s = lax.rem(c, 3)
        return remote(rows_at(s, 1), rows_at(s, 3), dr_send.at[s], dr_recv.at[s], beside)

    def r1_copy(c, home):
        s = lax.rem(c, 2)
        return remote(part.at[pl.ds((2 + home) * tokens, tokens)], rb1.at[s, pl.ds(home * tokens, tokens)], r1_send.at[s, home], r1_recv.at[s, home], beside)

    rows = tokens // PIECES

    def piece(p):
        return pl.ds(p * rows, rows)

    def r2_copy(c, p):
        s = lax.rem(c, 3)
        return remote(rb1.at[lax.rem(c, 2), pl.ds(tokens + p * rows, rows)], rb2.at[s, piece(p)], r2_send.at[s, p], r2_recv.at[s, p], across)

    def hop_copy(c, p):
        s = lax.rem(c, 2)
        h = lax.rem(c, HIN_SLOTS)
        return remote(ho.at[s, piece(p)], hin.at[h, piece(p)], hop_send.at[s, p], hin_sem.at[h, p], other_pp)

    def out_copy(c, p):
        s = lax.rem(c, 2)
        return remote(ho.at[s, piece(p)], out.at[c, piece(p)], hop_send.at[s, p], out_recv.at[c, p], other_pp)

    def out_local(c, p):
        s = lax.rem(c, 2)
        return pltpu.make_async_copy(ho.at[s, piece(p)], out.at[c, piece(p)], out_loc.at[s, p])

    def ids_copies(part_idx):
        some = pl.ds(0, 1) if part_idx == 0 else pl.ds(1, chunks - 1)
        return [remote(ids_own.at[some], ids.at[j, some], ids_send.at[part_idx, j], ids_recv.at[part_idx, j], peer) for j, peer in ((1, across), (2, beside), (3, diagonal))]

    def table_copy(c):
        s = lax.rem(c, 2)
        return pltpu.make_async_copy(table, smem_table.at[s], table_sem)

    smem_table[1, 0, 0] = 0
    smem_table[1, 1, 0] = 0

    @pl.when(pp == 0)
    def _():
        for copy in hin_copies(0):
            copy.start()

    for copy in weight_copies[:3]:
        copy.start()
    for copy in kv_copies(0):
        copy.start()
    weight_copies[3].start()

    @pl.when(pp == 0)
    def _():
        for copy in hin_copies(1):
            copy.start()

    barrier = pltpu.get_barrier_semaphore()
    for peer in (other_pp, across, beside, diagonal):
        pl.semaphore_signal(barrier, inc=1, device_id=peer, device_id_type=MESH)
    pl.semaphore_wait(barrier, 4)

    for part_idx in range(2):
        for copy in ids_copies(part_idx):
            copy.start()

    w = {"a_gain": a_gain, "rope": rope_ref, "q": wq, "k": wk, "v": wv, "gate": wg, "up": wu, "down": wd}

    def plan(c):
        @pl.when(c == 0)
        def _():
            ids[0] = ids_own[...]
            with scope("w_ids"):
                for copy in ids_copies(0):
                    copy.wait()

        @pl.when(c == 1)
        def _():
            for copy in ids_copies(1):
                copy.wait()

        chosen_ids = jnp.concatenate([ids[j, c] for j in range(4)], axis=1)
        plan_tiles(chosen_ids, first, tri, member, rank_buf.at[lax.rem(c, 2)], table)
        table_copy(c).start()

    def project(c):
        plan(c)
        with scope("w_hin"):
            for copy in hin_copies(c):
                copy.wait()

        @pl.when(c == 0)
        def _():
            for copy in weight_copies[:3]:
                copy.wait()

        @pl.when(jnp.logical_and(pp == 0, c + 2 < chunks))
        def _():
            for copy in hin_copies(c + 2):
                copy.start()

        @pl.when(c > 0)
        def _():
            for copy in new_copies(c - 1):
                copy.wait()

        seq_row = seq[pl.ds(c, 1), :].astype(F32)
        pos[...] = jnp.broadcast_to(seq_row, (128, 128)).T
        turn[...] = rope_tables(pos[...], w["rope"])
        attn_dots(hin[lax.rem(c, HIN_SLOTS)], w, x_buf)
        attn_rope(turn, x_buf, q3, k3, v3, kn, vn)
        for copy in new_copies(c):
            copy.start()

    def reduce_pair(c):
        s = lax.rem(c, 2)
        far = pl.ds(tokens, tokens)
        near = pl.ds(0, tokens)
        with scope("w_r1"):
            r1_copy(c, 1).wait_recv()
        rb1[s, far, :] = rb1[s, far, :] + part[far, :]
        for p in range(PIECES):
            r2_copy(c, p).start()
        r1_copy(c, 0).wait_recv()
        rb1[s, near, :] = rb1[s, near, :] + part[near, :]
        for home in (1, 0):
            r1_copy(c, home).wait_send()

    def relay(c):
        copy = dx_copy(c)
        with scope("w_dx"):
            copy.wait_recv()
        dr_copy(c).start()
        copy.wait_send()
        dc_copy(c).wait_send()

    def attend(c):
        table_copy(c).wait()
        with scope("w_kv"):
            for copy in kv_copies(c):
                copy.wait()

        @pl.when(c == 0)
        def _():
            weight_copies[4].start()

        @pl.when(c == 1)
        def _():
            for copy in weight_copies[5:]:
                copy.start()

        def body(idx, carry):
            base = idx * GROUP_UNROLL
            ahead = attn_scores(base, q3, k3, k_buf)
            for u in range(GROUP_UNROLL):
                scores = ahead
                if u + 1 < GROUP_UNROLL:
                    ahead = attn_scores(base + u + 1, q3, k3, k_buf)
                attn_mix(base + u, *attn_weights(base + u, *scores, pos), v3, o3, v_buf)
            return carry

        with scope("groups"):
            lax.fori_loop(0, tokens // (GROUP * GROUP_UNROLL), body, 0)

        @pl.when(c + 1 < chunks)
        def _():
            for copy in kv_copies(c + 1):
                copy.start()

        @pl.when(c == 0)
        def _():
            weight_copies[3].wait()

        @pl.when(c == 1)
        def _():
            relay(0)

        @pl.when(c >= 1)
        def _():
            dispatched(c - 1)

        hidden = hin[lax.rem(c, HIN_SLOTS)].astype(F32)
        attn_out = jnp.concatenate([o3[pl.ds(g, tokens, stride=8), :].astype(BF16) for g in range(8)], axis=1)
        before = c + 5
        mixed = dot(attn_out, wo[...])
        router = logits(before)
        picked = gather_rows(before, 0, 0)
        new_mid = (hidden + mixed).astype(BF16)
        mid[lax.rem(c, 3)] = new_mid
        n_buf[lax.rem(c, 3), pl.ds(0, tokens), :] = rms(new_mid.astype(F32), m_gain[...].astype(F32))
        gates(before, router)
        gather_gate(picked, before, 0, 0)
        dx_copy(c).start()
        dc_copy(c).start()

        @pl.when(jnp.logical_and(pp == 1, c + HIN_SLOTS < chunks))
        def _():
            pl.semaphore_signal(credit, inc=1, device_id=other_pp, device_id_type=MESH)

    def tile_at(c, row, j):
        return smem_table[lax.rem(c, 2), row, j]

    def gather_rows(c, j, u):
        normed = n_buf.at[lax.rem(c, 3)]
        return moe_gather(j, u, tile_at(c, 0, j), tile_at(c, 1, j), first, normed, rank_buf.at[lax.rem(c, 2)], picks, x_buf)

    def gather_gate(picked, c, j, u):
        moe_gate(picked, u, tile_at(c, 0, j), first, gate_ref, g_buf)

    def gather(c, j, u):
        gather_gate(gather_rows(c, j, u), c, j, u)

    def dispatched(c):
        with scope("w_disp"):
            dc_copy(c).wait_recv()
            dr_copy(c).wait_recv()

    def logits(c):
        return dot_nt(w_r[...], n_buf[lax.rem(c, 3)])

    def gates(c, router):
        moe_gates(router, rank_buf.at[lax.rem(c, 2)], gate_ref)

    def experts(c):
        @pl.when(c == 0)
        def _():
            with scope("w_wts"):
                for copy in weight_copies[4:]:
                    copy.wait()

        def expand(j, u):
            moe_expand(u, tile_at(c, 0, j), w, x_buf, a_buf)

        def contract(j, u):
            moe_contract(j, u, tile_at(c, 0, j), w, a_buf, g_buf, terms)

        def body(idx, carry):
            base = idx * TILE_UNROLL
            expand(base, 0)
            gather(c, base + 1, 1)
            for u in range(1, TILE_UNROLL):
                expand(base + u, u)
                if u + 1 < TILE_UNROLL:
                    gather(c, base + u + 1, u + 1)
                else:
                    gather(c, lax.rem(base + TILE_UNROLL, tile_count), 0)
                contract(base + u - 1, u - 1)
            contract(base + TILE_UNROLL - 1, TILE_UNROLL - 1)
            return carry

        with scope("tiles"):
            lax.fori_loop(0, tile_count // TILE_UNROLL, body, 0)
        @pl.when(c >= 1)
        def _():
            with scope("finish"):
                finish(c - 1, False)

        half = 2 * tokens
        part[pl.ds(half, half), :] = dot(picks[pl.ds(half, half), :], terms[...])
        dr_copy(c).wait_send()
        r1_copy(c, 1).start()
        r1_copy(c, 0).start()
        part[pl.ds(0, half), :] = dot(picks[pl.ds(0, half), :], terms[...])

    def finish(c, last):
        s = lax.rem(c, 2)

        @pl.when(jnp.logical_and(pp == 0, c >= HIN_SLOTS))
        def _():
            pl.semaphore_wait(credit, 1)

        @pl.when(c >= 2)
        def _():
            for p in range(PIECES):
                @pl.when(pp == 0)
                def _():
                    hop_copy(c - 2, p).wait_send()

                @pl.when(pp == 1)
                def _():
                    out_copy(c - 2, p).wait_send()
                    out_local(c - 2, p).wait()

        def settle(at, pieces):
            mixed = (rb1[s, at, :] + rb2[lax.rem(c, 3), at, :]).astype(BF16)
            result = (mid[lax.rem(c, 3), at, :].astype(F32) + mixed.astype(F32)).astype(BF16)

            @pl.when(pp == 0)
            def _():
                ho[s, at, :] = result
                for p in pieces:
                    hop_copy(c, p).start()

            @pl.when(pp == 1)
            def _():
                ho[s, at, :] = result
                for p in pieces:
                    out_copy(c, p).start()
                    out_local(c, p).start()

        if last:
            for p in range(PIECES):
                with scope("w_r2l"):
                    r2_copy(c, p).wait_recv()
                settle(piece(p), (p,))
        else:
            with scope("w_r2"):
                for p in range(PIECES):
                    r2_copy(c, p).wait_recv()
            settle(pl.ds(0, tokens), range(PIECES))

        for p in range(PIECES):
            r2_copy(c, p).wait_send()

    def step(i, carry):
        @pl.when(i >= 2)
        def _():
            with scope("reduce_pair"):
                reduce_pair(i - 2)

        @pl.when(i < chunks)
        def _():
            with scope("project"):
                project(i)

        @pl.when(jnp.logical_and(i >= 2, i <= chunks))
        def _():
            with scope("relay"):
                relay(i - 1)

        @pl.when(i < chunks)
        def _():
            with scope("attend"):
                attend(i)

        @pl.when(i == chunks)
        def _():
            dispatched(i - 1)
            gates(i - 1, logits(i - 1))
            gather(i - 1, 0, 0)

        @pl.when(jnp.logical_and(i >= 1, i <= chunks))
        def _():
            with scope("experts"):
                experts(i - 1)

        @pl.when(i == chunks + 1)
        def _():
            with scope("finish_last"):
                finish(i - 2, True)

        return carry

    lax.fori_loop(0, chunks + 2, step, 0)

    for copy in new_copies(chunks - 1):
        copy.wait()

    @pl.when(pp == 0)
    def _():
        for c in (chunks - 2, chunks - 1):
            for p in range(PIECES):
                hop_copy(c, p).wait_send()

        def arrived(c, carry):
            for p in range(PIECES):
                out_copy(c, p).wait_recv()
            return carry

        with scope("w_out"):
            lax.fori_loop(0, chunks, arrived, 0)

    @pl.when(pp == 1)
    def _():
        for c in (chunks - 2, chunks - 1):
            for p in range(PIECES):
                out_copy(c, p).wait_send()
                out_local(c, p).wait()


def step_call(args, chunks, tokens, tile_count):
    vmem = pl.BlockSpec(memory_space=pltpu.VMEM)
    hbm = pl.BlockSpec(memory_space=pl.ANY)
    wide = 4 * tokens
    dma = pltpu.SemaphoreType.DMA
    return pl.pallas_call(
        functools.partial(step_kernel, tile_count),
        out_shape=(
            jax.ShapeDtypeStruct((chunks, tokens, 1024), BF16),
            jax.ShapeDtypeStruct((chunks, tokens, 512), BF16),
            jax.ShapeDtypeStruct((chunks, tokens, 512), BF16),
        ),
        in_specs=[hbm, vmem, hbm, hbm, vmem, hbm, hbm, hbm, hbm, vmem, vmem, vmem, vmem, hbm, hbm, hbm, vmem],
        out_specs=(hbm, hbm, hbm),
        scratch_shapes=[
            pltpu.VMEM((3, wide, 1024), BF16),
            pltpu.VMEM((HIN_SLOTS, tokens, 1024), BF16),
            pltpu.VMEM((3, tokens, 1024), BF16),
            pltpu.VMEM((2, tokens, 1024), BF16),
            pltpu.VMEM((tokens * 128, 64), BF16),
            pltpu.VMEM((tokens * 128, 64), BF16),
            pltpu.VMEM((1024, 1024), BF16),
            pltpu.VMEM((1024, 512), BF16),
            pltpu.VMEM((1024, 512), BF16),
            pltpu.VMEM((1024, 1024), BF16),
            pltpu.VMEM((8, 1024, 512), BF16),
            pltpu.VMEM((8, 1024, 512), BF16),
            pltpu.VMEM((8, 512, 1024), BF16),
            pltpu.VMEM((wide, 1024), F32),
            pltpu.VMEM((2, 2 * tokens, 1024), F32),
            pltpu.VMEM((3, tokens, 1024), F32),
            pltpu.VMEM((wide, tile_count * TILE), BF16),
            pltpu.VMEM((tile_count * TILE, 1024), BF16),
            pltpu.VMEM((3, TILE, 1024), BF16),
            pltpu.VMEM((3, TILE, 512), BF16),
            pltpu.VMEM((TILE_UNROLL, TILE, 128), F32),
            pltpu.VMEM((tokens * 8, 128), F32),
            pltpu.VMEM((tokens * 8, 128), F32),
            pltpu.VMEM((tokens * 8, 128), F32),
            pltpu.VMEM((tokens * 8, 128), F32),
            pltpu.VMEM((tokens, 512), BF16),
            pltpu.VMEM((tokens, 512), BF16),
            pltpu.VMEM((2, 32, wide), F32),
            pltpu.VMEM((32, wide), F32),
            pltpu.VMEM((32, wide), F32),
            pltpu.VMEM((tokens, 128), F32),
            pltpu.VMEM((tokens, 256), F32),
            pltpu.VMEM((4, chunks, 8, tokens), jnp.int32),
            pltpu.VMEM((8, 128), jnp.int32),
            pltpu.SMEM((2, 8, 128), jnp.int32),
            dma((7,)), dma((2, 4)), dma((2, 4)), dma(()), dma((HIN_SLOTS, PIECES)), dma((2,)), dma((2,)),
            dma((3,)), dma((3,)), dma((3,)), dma((3,)), dma((3,)), dma((3,)),
            dma((2, 2)), dma((2, 2)), dma((3, PIECES)), dma((3, PIECES)),
            dma((2, PIECES)), dma((2, PIECES)), dma((chunks, PIECES)),
            pltpu.SemaphoreType.REGULAR,
        ],
        compiler_params=pltpu.CompilerParams(collective_id=0, has_side_effects=True, vmem_limit_bytes=67043328),
        name="decode_step",
        cost_estimate=pl.CostEstimate(flops=2 * 10**11, bytes_accessed=2 * 10**8, transcendentals=0),
    )(*args)


def result_kernel(h_ref, k_ref, v_ref, gain_ref, out_ref, kn_ref, vn_ref, rows):
    tokens = rows.shape[1] // 8
    gain = gain_ref[...].astype(F32).reshape(1, 1024)

    def body(idx, carry):
        at = pl.ds(pl.multiple_of(idx * tokens, tokens), tokens)
        vals = h_ref[0, at, :].astype(F32)
        vals = vals * lax.rsqrt(jnp.mean(vals * vals, axis=-1, keepdims=True) + EPS)
        for g in range(8):
            out_ref[0, at, g * 128:(g + 1) * 128] = (vals[:, g * 128:(g + 1) * 128] * gain[:, g * 128:(g + 1) * 128]).astype(BF16)
        for j, (src, dst) in enumerate(((k_ref, kn_ref), (v_ref, vn_ref))):
            spread_heads(rows.at[j], src[0, at, :].astype(F32))
            dst[0, at] = rows[j].reshape(tokens, 8, 128)[:, :, :64].astype(BF16)
        return carry

    lax.fori_loop(0, h_ref.shape[1] // tokens, body, 0)


def result_call(hidden, k_rows, v_rows, gain):
    blocks = 4
    step = hidden.shape[1]
    tokens = hidden.shape[0] * step // blocks
    hidden, k_rows, v_rows = (x.reshape(blocks, tokens, x.shape[-1]) for x in (hidden, k_rows, v_rows))
    chunks = blocks
    wide = pl.BlockSpec((1, tokens, 1024), lambda i: (i, 0, 0))
    dense = pl.BlockSpec((1, tokens, 512), lambda i: (i, 0, 0))
    heads = pl.BlockSpec((1, tokens, 8, 64), lambda i: (i, 0, 0, 0))
    return pl.pallas_call(
        result_kernel,
        grid=(chunks,),
        out_shape=(
            jax.ShapeDtypeStruct((chunks, tokens, 1024), BF16),
            jax.ShapeDtypeStruct((chunks, tokens, 8, 64), BF16),
            jax.ShapeDtypeStruct((chunks, tokens, 8, 64), BF16),
        ),
        in_specs=[wide, dense, dense, pl.BlockSpec((1024,), lambda i: (0,))],
        out_specs=(wide, heads, heads),
        scratch_shapes=[pltpu.VMEM((2, step * 8, 128), F32)],
        name="results",
        cost_estimate=pl.CostEstimate(flops=10**7, bytes_accessed=2 * 10**7, transcendentals=0),
    )(hidden, k_rows, v_rows, gain)


def solution(mesh):
    rows_spec = ("dp", "ep")
    three_dim = P("pp", None, None)
    two_dim = P("pp", None)
    expert_spec = P("pp", "ep", None, None)
    cache_spec = P("pp", None, rows_spec, None, None, None)
    new_spec = P("pp", None, rows_spec, None, None)
    in_specs = (P(None, rows_spec, None), P(None, rows_spec), cache_spec, cache_spec, P("pp", None, rows_spec, None), three_dim, three_dim, three_dim, three_dim, two_dim, two_dim, three_dim, expert_spec, expert_spec, expert_spec, P(None))
    out_specs = (P(None, rows_spec, None), new_spec, new_spec)

    def device_fn(hidden_in, seq_pos, k_cache, v_cache, expert_ids, w_query, w_key, w_value, w_out, attn_gain, mlp_gain, w_router, w_gate, w_up, w_down, final_gain):
        micro, rows = seq_pos.shape
        chunks = micro // PER_CHUNK
        tokens = PER_CHUNK * rows
        wide = 4 * tokens
        tile_count = (wide * 2 - 8) // TILE + 8
        angles = np.arange(1, 17)[:, None] * THETA ** (-np.arange(32) / 32)
        both = np.concatenate([np.tile(np.cos(angles), (1, 4)), np.tile(np.concatenate([-np.sin(angles), np.sin(angles)], axis=1), (1, 2))], axis=1)
        both = np.concatenate([both, np.zeros((112, 256))], axis=0).astype(np.float32)
        table = []
        for _ in range(3):
            table.append(both.astype(BF16))
            both = both - table[-1].astype(np.float32)
        table = jnp.asarray(np.concatenate(table, axis=1))
        tri = jnp.asarray(np.triu(np.ones((wide, wide)), 1), BF16)
        ids = jnp.swapaxes(expert_ids[0].reshape(chunks, tokens, 8), 1, 2)
        args = (
            hidden_in.reshape(chunks, tokens, 1024), seq_pos.reshape(chunks, tokens), k_cache.reshape(chunks, tokens * 128, 64), v_cache.reshape(chunks, tokens * 128, 64),
            ids, w_query[0], w_key[0], w_value[0], w_out[0], attn_gain, mlp_gain, table, w_router[0].T,
            w_gate[0], w_up[0], w_down[0], tri,
        )
        out, k_new, v_new = result_call(*step_call(args, chunks, tokens, tile_count), final_gain)
        shape = (1,) + seq_pos.shape + (8, 64)
        return out.reshape(hidden_in.shape), k_new.reshape(shape), v_new.reshape(shape)

    return jax.shard_map(device_fn, mesh=mesh, in_specs=in_specs, out_specs=out_specs, check_vma=False)
```

```python
import functools

import jax
import jax.numpy as jnp
import numpy as np
from jax import lax
from jax.experimental import pallas as pl
from jax.experimental.pallas import tpu as pltpu
from jax.sharding import PartitionSpec as P

THETA = 1000000.0
EPS = 1e-05
F32 = jnp.float32
BF16 = jnp.bfloat16
TILE = 128
GROUP = 16
GROUP_UNROLL = 8
TILE_UNROLL = 3
PER_CHUNK = 4
HIN_SLOTS = 4
PIECES = 4
MESH = pl.DeviceIdType.MESH


def scope(name):
    return jax.named_scope(name)


def rms(vals, gain_row):
    inv = lax.rsqrt(jnp.mean(vals * vals, axis=-1, keepdims=True) + EPS)
    return (vals * inv * gain_row).astype(BF16)


def dot(lhs, rhs):
    return jnp.dot(lhs, rhs, preferred_element_type=F32)


def dot_nt(lhs, rhs):
    return lax.dot_general(lhs, rhs, (((1,), (1,)), ((), ())), preferred_element_type=F32)


def rope_tables(pos, table):
    lane = lax.broadcasted_iota(jnp.int32, pos.shape, 1).astype(F32)
    both = dot(jnp.where(lane + 1.0 == pos, 1.0, 0.0).astype(BF16), table[...])
    both = both[:, :256] + both[:, 256:512] + both[:, 512:]
    return both


def rope(vals, cos_t, sin_t):
    lane = lax.broadcasted_iota(jnp.int32, (1, 128), 1)
    first = (lane % 64) < 32
    parts = []
    for j in range(vals.shape[1] // 128):
        block = vals[:, j * 128:(j + 1) * 128]
        swapped = jnp.where(first, pltpu.roll(block, 96, 1), pltpu.roll(block, 32, 1))
        parts.append(block * cos_t + swapped * sin_t)
    return jnp.concatenate(parts, axis=1)


def spread(ref, vals):
    tokens = vals.shape[0]
    for g in range(8):
        ref[pl.ds(g, tokens, stride=8), :] = vals[:, g * 128:(g + 1) * 128]


def spread_heads(ref, vals):
    tokens = vals.shape[0]
    low = lax.broadcasted_iota(jnp.int32, (1, 128), 1) < 64
    for j in range(4):
        block = vals[:, j * 128:(j + 1) * 128]
        other = pltpu.roll(block, 64, 1)
        ref[pl.ds(2 * j, tokens, stride=8), :] = jnp.where(low, block, other)
        ref[pl.ds(2 * j + 1, tokens, stride=8), :] = jnp.where(low, other, block)


def rows_of(ref, idx):
    return ref[pl.ds(pl.multiple_of(idx * GROUP * 8, GROUP * 8), GROUP * 8), :].reshape(GROUP, 8, 128)


def attn_dots(hidden, w, raw):
    normed = rms(hidden.astype(F32), w["a_gain"][...].astype(F32))
    raw[1] = dot(normed, w["q"][...]).astype(BF16)
    raw[2, :, :512] = dot(normed, w["k"][...]).astype(BF16)
    raw[2, :, 512:] = dot(normed, w["v"][...]).astype(BF16)


def attn_rope(turn, raw, q3, k3, v3, kn, vn):
    cos_t, sin_t = turn[:, :128], turn[:, 128:]
    spread(q3, rope(raw[1].astype(F32), cos_t, sin_t).astype(BF16).astype(F32))
    k = rope(raw[2, :, :512].astype(F32), cos_t, sin_t).astype(BF16)
    kn[...] = k
    spread_heads(k3, k.astype(F32))
    v = raw[2, :, 512:]
    vn[...] = v
    spread_heads(v3, v.astype(F32))


def attn_scores(idx, q3, k3, k_rows):
    q = rows_of(q3, idx)
    lane3 = lax.broadcasted_iota(jnp.int32, (1, 1, 128), 2)
    prod = q * rows_of(k3, idx)
    self_a = jnp.sum(jnp.where(lane3 < 64, prod, 0.0), axis=-1, keepdims=True)
    self_b = jnp.sum(jnp.where(lane3 < 64, 0.0, prod), axis=-1, keepdims=True)
    wide = (GROUP, 8, 128)
    self_s = jnp.concatenate([jnp.broadcast_to(self_a, wide), jnp.broadcast_to(self_b, wide)], axis=1) * 0.125
    q_rows = jnp.concatenate([q, pltpu.roll(q, 64, 2)], axis=1).astype(BF16)[:, :, :64].reshape(GROUP * 16, 64)
    row0 = idx * (GROUP * 128)
    blocks = []
    for p in range(GROUP // 2):
        keys = k_rows[pl.ds(pl.multiple_of(row0 + p * 256, 256), 256), :]
        both = dot_nt(q_rows[p * 32:(p + 1) * 32], keys)
        blocks.append(both[:16, :128].reshape(1, 16, 128))
        blocks.append(both[16:, 128:].reshape(1, 16, 128))
    return jnp.concatenate(blocks, axis=0), self_s


def attn_weights(idx, scores, self_s, pos_ref):
    row_i = lax.broadcasted_iota(jnp.int32, (16, 128), 0)
    lane_i = lax.broadcasted_iota(jnp.int32, (16, 128), 1)
    step = jnp.where((row_i % 8) == (lane_i % 8), lane_i // 8, 1000).astype(F32)
    pos = pos_ref[pl.ds(pl.multiple_of(idx * GROUP, GROUP), GROUP), :].reshape(GROUP, 1, 128)
    scores = jnp.where(step.reshape(1, 16, 128) < pos, scores * 0.125, -jnp.inf)
    wide = (GROUP, 16, 128)
    top = jnp.maximum(jnp.broadcast_to(jnp.max(scores, axis=-1, keepdims=True), wide), self_s)
    weights = jnp.exp(scores - top)
    self_w = jnp.exp(self_s - top)
    inv = 1.0 / (jnp.broadcast_to(jnp.sum(weights, axis=-1, keepdims=True), wide) + self_w)
    return (weights * inv).astype(BF16), (self_w * inv).astype(BF16).astype(F32)


def attn_mix(idx, weights, self_w, v3, o3, v_rows):
    row0 = idx * (GROUP * 128)
    zeros = jnp.zeros((16, 128), BF16)
    outs = []
    for p in range(GROUP // 2):
        vals = v_rows[pl.ds(pl.multiple_of(row0 + p * 256, 256), 256), :]
        upper = jnp.concatenate([weights[2 * p], zeros], axis=1)
        lower = jnp.concatenate([zeros, weights[2 * p + 1]], axis=1)
        outs.append(dot(jnp.concatenate([upper, lower], axis=0), vals).reshape(2, 16, 64))
    out = jnp.concatenate(outs, axis=0)
    v_new = rows_of(v3, idx)[:, :, :64]
    out_a = out[:, :8] + self_w[:, :8, :64] * v_new
    out_b = out[:, 8:] + self_w[:, 8:, :64] * v_new
    o3[pl.ds(pl.multiple_of(idx * GROUP * 8, GROUP * 8), GROUP * 8), :] = jnp.concatenate([out_a, out_b], axis=-1).reshape(GROUP * 8, 128)


def plan_tiles(ids, first, tri, member_ref, rank_ref, table_ref):
    tokens = ids.shape[1]
    expert_i = lax.broadcasted_iota(jnp.int32, (32, tokens), 0)
    chosen = jnp.zeros((32, tokens), F32)
    for s in range(ids.shape[0]):
        chosen = jnp.where(ids[s:s + 1, :] == expert_i, 1.0, chosen)
    member_ref[...] = chosen
    rank = dot(chosen.astype(BF16), tri[...])
    rank_ref[...] = jnp.where(chosen > 0.0, rank, -1.0)
    local = member_ref[pl.ds(pl.multiple_of(first, 8), 8), :]
    counts = jnp.sum(local, axis=-1, keepdims=True).astype(jnp.int32)
    tiles = jnp.broadcast_to(lax.shift_right_logical(counts + (TILE - 1), 7), (8, 128))
    lane = lax.broadcasted_iota(jnp.int32, (1, 128), 1)
    end = jnp.zeros((1, 128), jnp.int32)
    start = jnp.zeros((1, 128), jnp.int32)
    expert = jnp.zeros((1, 128), jnp.int32)
    for e in range(8):
        end = end + tiles[e:e + 1, :]
        passed = lane >= end
        expert = jnp.where(passed, expert + 1, expert)
        start = jnp.where(passed, end, start)
    sub = jnp.where(expert < 8, lane - start, 1000)
    table_ref[0:1, :] = jnp.minimum(expert, 7)
    table_ref[1:2, :] = sub


def moe_gates(logits, rank_ref, gate_ref):
    chosen = rank_ref[...] >= 0.0
    top = jnp.max(jnp.where(chosen, logits, -jnp.inf), axis=0, keepdims=True)
    gates = jnp.where(chosen, jnp.exp(logits - top), 0.0)
    gate_ref[...] = gates / jnp.sum(gates, axis=0, keepdims=True)


def slot_of(u):
    return 0 if u == 0 else 1 + (u - 1) % 2


def moe_gather(j, u, expert, sub, first, normed, rank_ref, picks, x_buf):
    ranks = rank_ref[pl.ds(first + expert, 1), :]
    wanted = (lax.broadcasted_iota(jnp.int32, (TILE, 1), 0) + sub * TILE).astype(F32)
    picked = jnp.where(ranks == wanted, 1.0, 0.0)
    picks[:, pl.ds(pl.multiple_of(j * TILE, TILE), TILE)] = picked.T.astype(BF16)
    x_buf[slot_of(u)] = dot(picked.astype(BF16), normed[...]).astype(BF16)
    return picked


def moe_gate(picked, u, expert, first, gate_ref, g_buf):
    gate = jnp.sum(picked * gate_ref[pl.ds(first + expert, 1), :], axis=-1, keepdims=True)
    g_buf[u] = jnp.broadcast_to(gate, (TILE, 128))


def moe_expand(u, expert, w, x_buf, a_buf):
    rows = x_buf[slot_of(u)]
    a_buf[slot_of(u)] = (jax.nn.silu(dot(rows, w["gate"][expert])) * dot(rows, w["up"][expert])).astype(BF16)


def moe_contract(j, u, expert, w, a_buf, g_buf, terms):
    y = dot(a_buf[slot_of(u)], w["down"][expert])
    gate = g_buf[u]
    at = pl.ds(pl.multiple_of(j * TILE, TILE), TILE)
    for p in range(8):
        terms[at, p * 128:(p + 1) * 128] = (gate * y[:, p * 128:(p + 1) * 128]).astype(BF16)


def step_kernel(
    tile_count,
    hid, seq, k_cache, v_cache, ids_own, wq_h, wk_h, wv_h, wo_h, a_gain, m_gain, rope_ref, w_r, wg_h, wu_h, wd_h, tri,
    out, kn_out, vn_out,
    n_buf, hin, mid, ho, k_buf, v_buf, wq, wk, wv, wo, wg, wu, wd, part, rb1, rb2, picks, terms, x_buf, a_buf, g_buf, q3, k3, v3, o3, kn, vn, rank_buf, gate_ref, member, pos, turn, ids, table, smem_table,
    w_sem, ids_send, ids_recv, table_sem, hin_sem, kv_sem, new_sem, dx_send, dx_recv, dc_send, dc_recv, dr_send, dr_recv, r1_send, r1_recv, r2_send, r2_recv, hop_send, out_loc, out_recv, credit,
):
    chunks, tokens = hid.shape[0], hid.shape[1]
    gathered = 4 * tokens
    dp = lax.axis_index("dp")
    pp = lax.axis_index("pp")
    ep = lax.axis_index("ep")
    other_pp = (dp, 1 - pp, ep)
    across = (dp, pp, lax.rem(ep + 2, 4))
    beside = (dp, pp, ep + 1 - 2 * lax.rem(ep, 2))
    first = ep * 8

    diagonal = (dp, pp, lax.rem(ep + 3 - 2 * lax.rem(ep, 2), 4))

    attn_w = [(wq_h, wq), (wk_h, wk), (wv_h, wv), (wo_h, wo)]
    moe_w = [(wg_h, wg), (wu_h, wu), (wd_h, wd)]
    weight_copies = [pltpu.make_async_copy(s, d, w_sem.at[j]) for j, (s, d) in enumerate(attn_w + moe_w)]

    def hin_copies(c):
        h = lax.rem(c, HIN_SLOTS)
        return [pltpu.make_async_copy(hid.at[c, piece(p)], hin.at[h, piece(p)], hin_sem.at[h, p]) for p in range(PIECES)]

    def kv_copies(c):
        return (pltpu.make_async_copy(k_cache.at[c], k_buf, kv_sem.at[0]), pltpu.make_async_copy(v_cache.at[c], v_buf, kv_sem.at[1]))

    def new_copies(c):
        return (pltpu.make_async_copy(kn, kn_out.at[c], new_sem.at[0]), pltpu.make_async_copy(vn, vn_out.at[c], new_sem.at[1]))

    def remote(src, dst, send, recv, peer):
        return pltpu.make_async_remote_copy(src_ref=src, dst_ref=dst, send_sem=send, recv_sem=recv, device_id=peer, device_id_type=MESH)

    def rows_at(slot, part_idx):
        return n_buf.at[slot, pl.ds(part_idx * tokens, tokens)]

    def dx_copy(c):
        s = lax.rem(c, 3)
        return remote(rows_at(s, 0), rows_at(s, 1), dx_send.at[s], dx_recv.at[s], across)

    def dc_copy(c):
        s = lax.rem(c, 3)
        return remote(rows_at(s, 0), rows_at(s, 2), dc_send.at[s], dc_recv.at[s], beside)

    def dr_copy(c):
        s = lax.rem(c, 3)
        return remote(rows_at(s, 1), rows_at(s, 3), dr_send.at[s], dr_recv.at[s], beside)

    def r1_copy(c, home):
        s = lax.rem(c, 2)
        return remote(part.at[pl.ds((2 + home) * tokens, tokens)], rb1.at[s, pl.ds(home * tokens, tokens)], r1_send.at[s, home], r1_recv.at[s, home], beside)

    rows = tokens // PIECES

    def piece(p):
        return pl.ds(p * rows, rows)

    def r2_copy(c, p):
        s = lax.rem(c, 3)
        return remote(rb1.at[lax.rem(c, 2), pl.ds(tokens + p * rows, rows)], rb2.at[s, piece(p)], r2_send.at[s, p], r2_recv.at[s, p], across)

    def hop_copy(c, p):
        s = lax.rem(c, 2)
        h = lax.rem(c, HIN_SLOTS)
        return remote(ho.at[s, piece(p)], hin.at[h, piece(p)], hop_send.at[s, p], hin_sem.at[h, p], other_pp)

    def out_copy(c, p):
        s = lax.rem(c, 2)
        return remote(ho.at[s, piece(p)], out.at[c, piece(p)], hop_send.at[s, p], out_recv.at[c, p], other_pp)

    def out_local(c, p):
        s = lax.rem(c, 2)
        return pltpu.make_async_copy(ho.at[s, piece(p)], out.at[c, piece(p)], out_loc.at[s, p])

    def ids_copies(part_idx):
        some = pl.ds(0, 1) if part_idx == 0 else pl.ds(1, chunks - 1)
        return [remote(ids_own.at[some], ids.at[j, some], ids_send.at[part_idx, j], ids_recv.at[part_idx, j], peer) for j, peer in ((1, across), (2, beside), (3, diagonal))]

    def table_copy(c):
        s = lax.rem(c, 2)
        return pltpu.make_async_copy(table, smem_table.at[s], table_sem)

    smem_table[1, 0, 0] = 0
    smem_table[1, 1, 0] = 0

    @pl.when(pp == 0)
    def _():
        for copy in hin_copies(0):
            copy.start()

    for copy in weight_copies[:3]:
        copy.start()
    for copy in kv_copies(0):
        copy.start()
    weight_copies[3].start()

    @pl.when(pp == 0)
    def _():
        for copy in hin_copies(1):
            copy.start()

    barrier = pltpu.get_barrier_semaphore()
    for peer in (other_pp, across, beside, diagonal):
        pl.semaphore_signal(barrier, inc=1, device_id=peer, device_id_type=MESH)
    pl.semaphore_wait(barrier, 4)

    for part_idx in range(2):
        for copy in ids_copies(part_idx):
            copy.start()

    w = {"a_gain": a_gain, "rope": rope_ref, "q": wq, "k": wk, "v": wv, "gate": wg, "up": wu, "down": wd}

    def plan(c):
        @pl.when(c == 0)
        def _():
            ids[0] = ids_own[...]
            with scope("w_ids"):
                for copy in ids_copies(0):
                    copy.wait()

        @pl.when(c == 1)
        def _():
            for copy in ids_copies(1):
                copy.wait()

        chosen_ids = jnp.concatenate([ids[j, c] for j in range(4)], axis=1)
        plan_tiles(chosen_ids, first, tri, member, rank_buf.at[lax.rem(c, 2)], table)
        table_copy(c).start()

    def combine_near(from_col, to_col):
        half = pl.ds(0, 2 * tokens)
        part[half, from_col:to_col] = dot(picks[half, :], terms[:, from_col:to_col])

    def project(c, with_sums):
        plan(c)
        with scope("w_hin"):
            for copy in hin_copies(c):
                copy.wait()

        @pl.when(c == 0)
        def _():
            for copy in weight_copies[:3]:
                copy.wait()

        @pl.when(jnp.logical_and(pp == 0, c + 2 < chunks))
        def _():
            for copy in hin_copies(c + 2):
                copy.start()

        @pl.when(c > 0)
        def _():
            for copy in new_copies(c - 1):
                copy.wait()

        seq_row = seq[pl.ds(c, 1), :].astype(F32)
        pos[...] = jnp.broadcast_to(seq_row, (128, 128)).T
        turn[...] = rope_tables(pos[...], w["rope"])
        if with_sums:
            combine_near(0, 256)
        attn_dots(hin[lax.rem(c, HIN_SLOTS)], w, x_buf)
        if with_sums:
            combine_near(256, 1024)
        attn_rope(turn, x_buf, q3, k3, v3, kn, vn)
        for copy in new_copies(c):
            copy.start()

    def reduce_pair(c):
        s = lax.rem(c, 2)
        far = pl.ds(tokens, tokens)
        near = pl.ds(0, tokens)
        with scope("w_r1"):
            r1_copy(c, 1).wait_recv()
        rb1[s, far, :] = rb1[s, far, :] + part[far, :]
        for p in range(PIECES - 1):
            r2_copy(c, p).start()

        @pl.when(jnp.logical_or(c == 0, c + 2 >= chunks))
        def _():
            r2_copy(c, PIECES - 1).start()

        r1_copy(c, 0).wait_recv()
        rb1[s, near, :] = rb1[s, near, :] + part[near, :]
        for home in (1, 0):
            r1_copy(c, home).wait_send()

    def relay(c):
        copy = dx_copy(c)
        with scope("w_dx"):
            copy.wait_recv()
        dr_copy(c).start()
        copy.wait_send()
        dc_copy(c).wait_send()

    def attend(c):
        table_copy(c).wait()
        with scope("w_kv"):
            for copy in kv_copies(c):
                copy.wait()

        @pl.when(c == 0)
        def _():
            weight_copies[4].start()

        @pl.when(c == 1)
        def _():
            for copy in weight_copies[5:]:
                copy.start()

        def body(idx, carry):
            base = idx * GROUP_UNROLL
            ahead = attn_scores(base, q3, k3, k_buf)
            for u in range(GROUP_UNROLL):
                scores = ahead
                if u + 1 < GROUP_UNROLL:
                    ahead = attn_scores(base + u + 1, q3, k3, k_buf)
                attn_mix(base + u, *attn_weights(base + u, *scores, pos), v3, o3, v_buf)
            return carry

        with scope("groups"):
            lax.fori_loop(0, tokens // (GROUP * GROUP_UNROLL), body, 0)

        @pl.when(c + 1 < chunks)
        def _():
            for copy in kv_copies(c + 1):
                copy.start()

        @pl.when(c == 0)
        def _():
            weight_copies[3].wait()

        @pl.when(c == 1)
        def _():
            relay(0)

        @pl.when(c >= 1)
        def _():
            dispatched(c - 1)

        hidden = hin[lax.rem(c, HIN_SLOTS)].astype(F32)
        attn_out = jnp.concatenate([o3[pl.ds(g, tokens, stride=8), :].astype(BF16) for g in range(8)], axis=1)
        before = c + 5
        mixed = dot(attn_out, wo[...])
        router = logits(before)
        picked = gather_rows(before, 0, 0)
        new_mid = (hidden + mixed).astype(BF16)
        mid[lax.rem(c, 3)] = new_mid
        n_buf[lax.rem(c, 3), pl.ds(0, tokens), :] = rms(new_mid.astype(F32), m_gain[...].astype(F32))
        gates(before, router)
        gather_gate(picked, before, 0, 0)
        dx_copy(c).start()
        dc_copy(c).start()

        @pl.when(c >= 3)
        def _():
            r2_copy(c - 2, PIECES - 1).start()

        @pl.when(jnp.logical_and(pp == 1, c + HIN_SLOTS < chunks))
        def _():
            pl.semaphore_signal(credit, inc=1, device_id=other_pp, device_id_type=MESH)

    def tile_at(c, row, j):
        return smem_table[lax.rem(c, 2), row, j]

    def gather_rows(c, j, u):
        normed = n_buf.at[lax.rem(c, 3)]
        return moe_gather(j, u, tile_at(c, 0, j), tile_at(c, 1, j), first, normed, rank_buf.at[lax.rem(c, 2)], picks, x_buf)

    def gather_gate(picked, c, j, u):
        moe_gate(picked, u, tile_at(c, 0, j), first, gate_ref, g_buf)

    def gather(c, j, u):
        gather_gate(gather_rows(c, j, u), c, j, u)

    def dispatched(c):
        with scope("w_disp"):
            dc_copy(c).wait_recv()
            dr_copy(c).wait_recv()

    def logits(c):
        return dot_nt(w_r[...], n_buf[lax.rem(c, 3)])

    def gates(c, router):
        moe_gates(router, rank_buf.at[lax.rem(c, 2)], gate_ref)

    def experts(c):
        @pl.when(c == 0)
        def _():
            with scope("w_wts"):
                for copy in weight_copies[4:]:
                    copy.wait()

        def expand(j, u):
            moe_expand(u, tile_at(c, 0, j), w, x_buf, a_buf)

        def contract(j, u):
            moe_contract(j, u, tile_at(c, 0, j), w, a_buf, g_buf, terms)

        def body(idx, carry):
            base = idx * TILE_UNROLL
            expand(base, 0)
            gather(c, base + 1, 1)
            for u in range(1, TILE_UNROLL):
                expand(base + u, u)
                if u + 1 < TILE_UNROLL:
                    gather(c, base + u + 1, u + 1)
                else:
                    gather(c, lax.rem(base + TILE_UNROLL, tile_count), 0)
                contract(base + u - 1, u - 1)
            contract(base + TILE_UNROLL - 1, TILE_UNROLL - 1)
            return carry

        with scope("tiles"):
            lax.fori_loop(0, tile_count // TILE_UNROLL, body, 0)
        half = 2 * tokens
        part[pl.ds(half, half), :] = dot(picks[pl.ds(half, half), :], terms[...])
        dr_copy(c).wait_send()
        r1_copy(c, 1).start()
        r1_copy(c, 0).start()

    def finish(c, last):
        s = lax.rem(c, 2)

        @pl.when(jnp.logical_and(pp == 0, c >= HIN_SLOTS))
        def _():
            pl.semaphore_wait(credit, 1)

        @pl.when(c >= 2)
        def _():
            for p in range(PIECES):
                @pl.when(pp == 0)
                def _():
                    hop_copy(c - 2, p).wait_send()

                @pl.when(pp == 1)
                def _():
                    out_copy(c - 2, p).wait_send()
                    out_local(c - 2, p).wait()

        def settle(at, pieces):
            mixed = (rb1[s, at, :] + rb2[lax.rem(c, 3), at, :]).astype(BF16)
            result = (mid[lax.rem(c, 3), at, :].astype(F32) + mixed.astype(F32)).astype(BF16)

            @pl.when(pp == 0)
            def _():
                ho[s, at, :] = result
                for p in pieces:
                    hop_copy(c, p).start()

            @pl.when(pp == 1)
            def _():
                ho[s, at, :] = result
                for p in pieces:
                    out_copy(c, p).start()
                    out_local(c, p).start()

        if last:
            for p in range(PIECES):
                with scope("w_r2l"):
                    r2_copy(c, p).wait_recv()
                settle(piece(p), (p,))
        else:
            with scope("w_r2"):
                for p in range(PIECES):
                    r2_copy(c, p).wait_recv()
            settle(pl.ds(0, tokens), range(PIECES))

        for p in range(PIECES):
            r2_copy(c, p).wait_send()

    def step(i, carry):
        @pl.when(i < 2)
        def _():
            with scope("project"):
                project(i, False)

        @pl.when(jnp.logical_and(i >= 2, i < chunks))
        def _():
            with scope("project_sum"):
                project(i, True)

        @pl.when(i >= chunks)
        def _():
            combine_near(0, 1024)

        @pl.when(i >= 2)
        def _():
            with scope("reduce_pair"):
                reduce_pair(i - 2)

        @pl.when(jnp.logical_and(i >= 4, i <= chunks + 1))
        def _():
            with scope("finish"):
                finish(i - 3, False)

        @pl.when(jnp.logical_and(i >= 2, i <= chunks))
        def _():
            with scope("relay"):
                relay(i - 1)

        @pl.when(i < chunks)
        def _():
            with scope("attend"):
                attend(i)

        @pl.when(i == chunks)
        def _():
            dispatched(i - 1)
            gates(i - 1, logits(i - 1))
            gather(i - 1, 0, 0)

        @pl.when(jnp.logical_and(i >= 1, i <= chunks))
        def _():
            with scope("experts"):
                experts(i - 1)

        @pl.when(i == 2)
        def _():
            with scope("finish_first"):
                finish(0, False)

        @pl.when(i == chunks + 1)
        def _():
            with scope("finish_last"):
                finish(i - 2, True)

        return carry

    lax.fori_loop(0, chunks + 2, step, 0)

    for copy in new_copies(chunks - 1):
        copy.wait()

    @pl.when(pp == 0)
    def _():
        for c in (chunks - 2, chunks - 1):
            for p in range(PIECES):
                hop_copy(c, p).wait_send()

        def arrived(c, carry):
            for p in range(PIECES):
                out_copy(c, p).wait_recv()
            return carry

        with scope("w_out"):
            lax.fori_loop(0, chunks, arrived, 0)

    @pl.when(pp == 1)
    def _():
        for c in (chunks - 2, chunks - 1):
            for p in range(PIECES):
                out_copy(c, p).wait_send()
                out_local(c, p).wait()


def step_call(args, chunks, tokens, tile_count):
    vmem = pl.BlockSpec(memory_space=pltpu.VMEM)
    hbm = pl.BlockSpec(memory_space=pl.ANY)
    wide = 4 * tokens
    dma = pltpu.SemaphoreType.DMA
    return pl.pallas_call(
        functools.partial(step_kernel, tile_count),
        out_shape=(
            jax.ShapeDtypeStruct((chunks, tokens, 1024), BF16),
            jax.ShapeDtypeStruct((chunks, tokens, 512), BF16),
            jax.ShapeDtypeStruct((chunks, tokens, 512), BF16),
        ),
        in_specs=[hbm, vmem, hbm, hbm, vmem, hbm, hbm, hbm, hbm, vmem, vmem, vmem, vmem, hbm, hbm, hbm, vmem],
        out_specs=(hbm, hbm, hbm),
        scratch_shapes=[
            pltpu.VMEM((3, wide, 1024), BF16),
            pltpu.VMEM((HIN_SLOTS, tokens, 1024), BF16),
            pltpu.VMEM((3, tokens, 1024), BF16),
            pltpu.VMEM((2, tokens, 1024), BF16),
            pltpu.VMEM((tokens * 128, 64), BF16),
            pltpu.VMEM((tokens * 128, 64), BF16),
            pltpu.VMEM((1024, 1024), BF16),
            pltpu.VMEM((1024, 512), BF16),
            pltpu.VMEM((1024, 512), BF16),
            pltpu.VMEM((1024, 1024), BF16),
            pltpu.VMEM((8, 1024, 512), BF16),
            pltpu.VMEM((8, 1024, 512), BF16),
            pltpu.VMEM((8, 512, 1024), BF16),
            pltpu.VMEM((wide, 1024), F32),
            pltpu.VMEM((2, 2 * tokens, 1024), F32),
            pltpu.VMEM((3, tokens, 1024), F32),
            pltpu.VMEM((wide, tile_count * TILE), BF16),
            pltpu.VMEM((tile_count * TILE, 1024), BF16),
            pltpu.VMEM((3, TILE, 1024), BF16),
            pltpu.VMEM((3, TILE, 512), BF16),
            pltpu.VMEM((TILE_UNROLL, TILE, 128), F32),
            pltpu.VMEM((tokens * 8, 128), F32),
            pltpu.VMEM((tokens * 8, 128), F32),
            pltpu.VMEM((tokens * 8, 128), F32),
            pltpu.VMEM((tokens * 8, 128), F32),
            pltpu.VMEM((tokens, 512), BF16),
            pltpu.VMEM((tokens, 512), BF16),
            pltpu.VMEM((2, 32, wide), F32),
            pltpu.VMEM((32, wide), F32),
            pltpu.VMEM((32, wide), F32),
            pltpu.VMEM((tokens, 128), F32),
            pltpu.VMEM((tokens, 256), F32),
            pltpu.VMEM((4, chunks, 8, tokens), jnp.int32),
            pltpu.VMEM((8, 128), jnp.int32),
            pltpu.SMEM((2, 8, 128), jnp.int32),
            dma((7,)), dma((2, 4)), dma((2, 4)), dma(()), dma((HIN_SLOTS, PIECES)), dma((2,)), dma((2,)),
            dma((3,)), dma((3,)), dma((3,)), dma((3,)), dma((3,)), dma((3,)),
            dma((2, 2)), dma((2, 2)), dma((3, PIECES)), dma((3, PIECES)),
            dma((2, PIECES)), dma((2, PIECES)), dma((chunks, PIECES)),
            pltpu.SemaphoreType.REGULAR,
        ],
        compiler_params=pltpu.CompilerParams(collective_id=0, has_side_effects=True, vmem_limit_bytes=67043328),
        name="decode_step",
        cost_estimate=pl.CostEstimate(flops=2 * 10**11, bytes_accessed=2 * 10**8, transcendentals=0),
    )(*args)


def result_kernel(h_ref, k_ref, v_ref, gain_ref, out_ref, kn_ref, vn_ref, rows):
    tokens = rows.shape[1] // 8
    gain = gain_ref[...].astype(F32).reshape(1, 1024)

    def body(idx, carry):
        at = pl.ds(pl.multiple_of(idx * tokens, tokens), tokens)
        vals = h_ref[0, at, :].astype(F32)
        vals = vals * lax.rsqrt(jnp.mean(vals * vals, axis=-1, keepdims=True) + EPS)
        for g in range(8):
            out_ref[0, at, g * 128:(g + 1) * 128] = (vals[:, g * 128:(g + 1) * 128] * gain[:, g * 128:(g + 1) * 128]).astype(BF16)
        for j, (src, dst) in enumerate(((k_ref, kn_ref), (v_ref, vn_ref))):
            spread_heads(rows.at[j], src[0, at, :].astype(F32))
            dst[0, at] = rows[j].reshape(tokens, 8, 128)[:, :, :64].astype(BF16)
        return carry

    lax.fori_loop(0, h_ref.shape[1] // tokens, body, 0)


def result_call(hidden, k_rows, v_rows, gain):
    blocks = 4
    step = hidden.shape[1]
    tokens = hidden.shape[0] * step // blocks
    hidden, k_rows, v_rows = (x.reshape(blocks, tokens, x.shape[-1]) for x in (hidden, k_rows, v_rows))
    chunks = blocks
    wide = pl.BlockSpec((1, tokens, 1024), lambda i: (i, 0, 0))
    dense = pl.BlockSpec((1, tokens, 512), lambda i: (i, 0, 0))
    heads = pl.BlockSpec((1, tokens, 8, 64), lambda i: (i, 0, 0, 0))
    return pl.pallas_call(
        result_kernel,
        grid=(chunks,),
        out_shape=(
            jax.ShapeDtypeStruct((chunks, tokens, 1024), BF16),
            jax.ShapeDtypeStruct((chunks, tokens, 8, 64), BF16),
            jax.ShapeDtypeStruct((chunks, tokens, 8, 64), BF16),
        ),
        in_specs=[wide, dense, dense, pl.BlockSpec((1024,), lambda i: (0,))],
        out_specs=(wide, heads, heads),
        scratch_shapes=[pltpu.VMEM((2, step * 8, 128), F32)],
        name="results",
        cost_estimate=pl.CostEstimate(flops=10**7, bytes_accessed=2 * 10**7, transcendentals=0),
    )(hidden, k_rows, v_rows, gain)


def solution(mesh):
    rows_spec = ("dp", "ep")
    three_dim = P("pp", None, None)
    two_dim = P("pp", None)
    expert_spec = P("pp", "ep", None, None)
    cache_spec = P("pp", None, rows_spec, None, None, None)
    new_spec = P("pp", None, rows_spec, None, None)
    in_specs = (P(None, rows_spec, None), P(None, rows_spec), cache_spec, cache_spec, P("pp", None, rows_spec, None), three_dim, three_dim, three_dim, three_dim, two_dim, two_dim, three_dim, expert_spec, expert_spec, expert_spec, P(None))
    out_specs = (P(None, rows_spec, None), new_spec, new_spec)

    def device_fn(hidden_in, seq_pos, k_cache, v_cache, expert_ids, w_query, w_key, w_value, w_out, attn_gain, mlp_gain, w_router, w_gate, w_up, w_down, final_gain):
        micro, rows = seq_pos.shape
        chunks = micro // PER_CHUNK
        tokens = PER_CHUNK * rows
        wide = 4 * tokens
        tile_count = (wide * 2 - 8) // TILE + 8
        angles = np.arange(1, 17)[:, None] * THETA ** (-np.arange(32) / 32)
        both = np.concatenate([np.tile(np.cos(angles), (1, 4)), np.tile(np.concatenate([-np.sin(angles), np.sin(angles)], axis=1), (1, 2))], axis=1)
        both = np.concatenate([both, np.zeros((112, 256))], axis=0).astype(np.float32)
        table = []
        for _ in range(3):
            table.append(both.astype(BF16))
            both = both - table[-1].astype(np.float32)
        table = jnp.asarray(np.concatenate(table, axis=1))
        tri = jnp.asarray(np.triu(np.ones((wide, wide)), 1), BF16)
        ids = jnp.swapaxes(expert_ids[0].reshape(chunks, tokens, 8), 1, 2)
        args = (
            hidden_in.reshape(chunks, tokens, 1024), seq_pos.reshape(chunks, tokens), k_cache.reshape(chunks, tokens * 128, 64), v_cache.reshape(chunks, tokens * 128, 64),
            ids, w_query[0], w_key[0], w_value[0], w_out[0], attn_gain, mlp_gain, table, w_router[0].T,
            w_gate[0], w_up[0], w_down[0], tri,
        )
        out, k_new, v_new = result_call(*step_call(args, chunks, tokens, tile_count), final_gain)
        shape = (1,) + seq_pos.shape + (8, 64)
        return out.reshape(hidden_in.shape), k_new.reshape(shape), v_new.reshape(shape)

    return jax.shard_map(device_fn, mesh=mesh, in_specs=in_specs, out_specs=out_specs, check_vma=False)
```

```python
import functools

import jax
import jax.numpy as jnp
import numpy as np
from jax import lax
from jax.experimental import pallas as pl
from jax.experimental.pallas import tpu as pltpu
from jax.sharding import PartitionSpec as P

THETA = 1000000.0
EPS = 1e-05
F32 = jnp.float32
BF16 = jnp.bfloat16
TILE = 128
GROUP = 16
GROUP_UNROLL = 8
TILE_UNROLL = 3
PER_CHUNK = 4
HIN_SLOTS = 4
PIECES = 4
MESH = pl.DeviceIdType.MESH


def scope(name):
    return jax.named_scope(name)


def rms(vals, gain_row):
    inv = lax.rsqrt(jnp.mean(vals * vals, axis=-1, keepdims=True) + EPS)
    return (vals * inv * gain_row).astype(BF16)


def dot(lhs, rhs):
    return jnp.dot(lhs, rhs, preferred_element_type=F32)


def dot_nt(lhs, rhs):
    return lax.dot_general(lhs, rhs, (((1,), (1,)), ((), ())), preferred_element_type=F32)


def rope_tables(pos, table):
    lane = lax.broadcasted_iota(jnp.int32, pos.shape, 1).astype(F32)
    both = dot(jnp.where(lane + 1.0 == pos, 1.0, 0.0).astype(BF16), table[...])
    both = both[:, :256] + both[:, 256:512] + both[:, 512:]
    return both


def rope(vals, cos_t, sin_t):
    lane = lax.broadcasted_iota(jnp.int32, (1, 128), 1)
    first = (lane % 64) < 32
    parts = []
    for j in range(vals.shape[1] // 128):
        block = vals[:, j * 128:(j + 1) * 128]
        swapped = jnp.where(first, pltpu.roll(block, 96, 1), pltpu.roll(block, 32, 1))
        parts.append(block * cos_t + swapped * sin_t)
    return jnp.concatenate(parts, axis=1)


def spread(ref, vals):
    tokens = vals.shape[0]
    for g in range(8):
        ref[pl.ds(g, tokens, stride=8), :] = vals[:, g * 128:(g + 1) * 128]


def spread_heads(ref, vals):
    tokens = vals.shape[0]
    low = lax.broadcasted_iota(jnp.int32, (1, 128), 1) < 64
    for j in range(4):
        block = vals[:, j * 128:(j + 1) * 128]
        other = pltpu.roll(block, 64, 1)
        ref[pl.ds(2 * j, tokens, stride=8), :] = jnp.where(low, block, other)
        ref[pl.ds(2 * j + 1, tokens, stride=8), :] = jnp.where(low, other, block)


def rows_of(ref, idx):
    return ref[pl.ds(pl.multiple_of(idx * GROUP * 8, GROUP * 8), GROUP * 8), :].reshape(GROUP, 8, 128)


def attn_dots(hidden, w, raw):
    normed = rms(hidden.astype(F32), w["a_gain"][...].astype(F32))
    raw[1] = dot(normed, w["q"][...]).astype(BF16)
    raw[2, :, :512] = dot(normed, w["k"][...]).astype(BF16)
    raw[2, :, 512:] = dot(normed, w["v"][...]).astype(BF16)


def attn_rope(turn, raw, q3, k3, v3, kn, vn):
    cos_t, sin_t = turn[:, :128], turn[:, 128:]
    spread(q3, rope(raw[1].astype(F32), cos_t, sin_t).astype(BF16).astype(F32))
    k = rope(raw[2, :, :512].astype(F32), cos_t, sin_t).astype(BF16)
    kn[...] = k
    spread_heads(k3, k.astype(F32))
    v = raw[2, :, 512:]
    vn[...] = v
    spread_heads(v3, v.astype(F32))


def attn_scores(idx, q3, k3, k_rows):
    q = rows_of(q3, idx)
    lane3 = lax.broadcasted_iota(jnp.int32, (1, 1, 128), 2)
    prod = q * rows_of(k3, idx)
    self_a = jnp.sum(jnp.where(lane3 < 64, prod, 0.0), axis=-1, keepdims=True)
    self_b = jnp.sum(jnp.where(lane3 < 64, 0.0, prod), axis=-1, keepdims=True)
    wide = (GROUP, 8, 128)
    self_s = jnp.concatenate([jnp.broadcast_to(self_a, wide), jnp.broadcast_to(self_b, wide)], axis=1) * 0.125
    q_rows = jnp.concatenate([q, pltpu.roll(q, 64, 2)], axis=1).astype(BF16)[:, :, :64].reshape(GROUP * 16, 64)
    row0 = idx * (GROUP * 128)
    blocks = []
    for p in range(GROUP // 2):
        keys = k_rows[pl.ds(pl.multiple_of(row0 + p * 256, 256), 256), :]
        both = dot_nt(q_rows[p * 32:(p + 1) * 32], keys)
        blocks.append(both[:16, :128].reshape(1, 16, 128))
        blocks.append(both[16:, 128:].reshape(1, 16, 128))
    return jnp.concatenate(blocks, axis=0), self_s


def attn_weights(idx, scores, self_s, pos_ref):
    row_i = lax.broadcasted_iota(jnp.int32, (16, 128), 0)
    lane_i = lax.broadcasted_iota(jnp.int32, (16, 128), 1)
    step = jnp.where((row_i % 8) == (lane_i % 8), lane_i // 8, 1000).astype(F32)
    pos = pos_ref[pl.ds(pl.multiple_of(idx * GROUP, GROUP), GROUP), :].reshape(GROUP, 1, 128)
    scores = jnp.where(step.reshape(1, 16, 128) < pos, scores * 0.125, -jnp.inf)
    wide = (GROUP, 16, 128)
    top = jnp.maximum(jnp.broadcast_to(jnp.max(scores, axis=-1, keepdims=True), wide), self_s)
    weights = jnp.exp(scores - top)
    self_w = jnp.exp(self_s - top)
    inv = 1.0 / (jnp.broadcast_to(jnp.sum(weights, axis=-1, keepdims=True), wide) + self_w)
    return (weights * inv).astype(BF16), (self_w * inv).astype(BF16).astype(F32)


def attn_mix(idx, weights, self_w, v3, o3, v_rows):
    row0 = idx * (GROUP * 128)
    zeros = jnp.zeros((16, 128), BF16)
    outs = []
    for p in range(GROUP // 2):
        vals = v_rows[pl.ds(pl.multiple_of(row0 + p * 256, 256), 256), :]
        upper = jnp.concatenate([weights[2 * p], zeros], axis=1)
        lower = jnp.concatenate([zeros, weights[2 * p + 1]], axis=1)
        outs.append(dot(jnp.concatenate([upper, lower], axis=0), vals).reshape(2, 16, 64))
    out = jnp.concatenate(outs, axis=0)
    v_new = rows_of(v3, idx)[:, :, :64]
    out_a = out[:, :8] + self_w[:, :8, :64] * v_new
    out_b = out[:, 8:] + self_w[:, 8:, :64] * v_new
    o3[pl.ds(pl.multiple_of(idx * GROUP * 8, GROUP * 8), GROUP * 8), :] = jnp.concatenate([out_a, out_b], axis=-1).reshape(GROUP * 8, 128)


def plan_tiles(ids, first, tri, member_ref, rank_ref, table_ref):
    tokens = ids.shape[1]
    expert_i = lax.broadcasted_iota(jnp.int32, (32, tokens), 0)
    chosen = jnp.zeros((32, tokens), F32)
    for s in range(ids.shape[0]):
        chosen = jnp.where(ids[s:s + 1, :] == expert_i, 1.0, chosen)
    member_ref[...] = chosen
    rank = dot(chosen.astype(BF16), tri[...])
    rank_ref[...] = jnp.where(chosen > 0.0, rank, -1.0)
    local = member_ref[pl.ds(pl.multiple_of(first, 8), 8), :]
    counts = jnp.sum(local, axis=-1, keepdims=True).astype(jnp.int32)
    tiles = jnp.broadcast_to(lax.shift_right_logical(counts + (TILE - 1), 7), (8, 128))
    lane = lax.broadcasted_iota(jnp.int32, (1, 128), 1)
    end = jnp.zeros((1, 128), jnp.int32)
    start = jnp.zeros((1, 128), jnp.int32)
    expert = jnp.zeros((1, 128), jnp.int32)
    for e in range(8):
        end = end + tiles[e:e + 1, :]
        passed = lane >= end
        expert = jnp.where(passed, expert + 1, expert)
        start = jnp.where(passed, end, start)
    sub = jnp.where(expert < 8, lane - start, 1000)
    table_ref[0:1, :] = jnp.minimum(expert, 7)
    table_ref[1:2, :] = sub


def moe_gates(logits, rank_ref, gate_ref):
    chosen = rank_ref[...] >= 0.0
    top = jnp.max(jnp.where(chosen, logits, -jnp.inf), axis=0, keepdims=True)
    gates = jnp.where(chosen, jnp.exp(logits - top), 0.0)
    gate_ref[...] = gates / jnp.sum(gates, axis=0, keepdims=True)


def slot_of(u):
    return 0 if u == 0 else 1 + (u - 1) % 2


def moe_gather(j, u, expert, sub, first, normed, rank_ref, picks, x_buf):
    ranks = rank_ref[pl.ds(first + expert, 1), :]
    wanted = (lax.broadcasted_iota(jnp.int32, (TILE, 1), 0) + sub * TILE).astype(F32)
    picked = jnp.where(ranks == wanted, 1.0, 0.0)
    picks[:, pl.ds(pl.multiple_of(j * TILE, TILE), TILE)] = picked.T.astype(BF16)
    x_buf[slot_of(u)] = dot(picked.astype(BF16), normed[...]).astype(BF16)
    return picked


def moe_gate(picked, u, expert, first, gate_ref, g_buf):
    gate = jnp.sum(picked * gate_ref[pl.ds(first + expert, 1), :], axis=-1, keepdims=True)
    g_buf[u] = jnp.broadcast_to(gate, (TILE, 128))


def moe_expand(u, expert, w, x_buf, a_buf):
    rows = x_buf[slot_of(u)]
    a_buf[slot_of(u)] = (jax.nn.silu(dot(rows, w["gate"][expert])) * dot(rows, w["up"][expert])).astype(BF16)


def moe_contract(j, u, expert, w, a_buf, g_buf, terms):
    y = dot(a_buf[slot_of(u)], w["down"][expert])
    gate = g_buf[u]
    at = pl.ds(pl.multiple_of(j * TILE, TILE), TILE)
    for p in range(8):
        terms[at, p * 128:(p + 1) * 128] = (gate * y[:, p * 128:(p + 1) * 128]).astype(BF16)


def step_kernel(
    tile_count,
    hid, seq, k_cache, v_cache, ids_own, wq_h, wk_h, wv_h, wo_h, a_gain, m_gain, rope_ref, w_r, wg_h, wu_h, wd_h, tri,
    out, kn_out, vn_out,
    n_buf, hin, mid, ho, k_buf, v_buf, wq, wk, wv, wo, wg, wu, wd, part, rb1, rb2, picks, terms, x_buf, a_buf, g_buf, q3, k3, v3, o3, kn, vn, rank_buf, gate_ref, member, pos, turn, ids, table, smem_table,
    w_sem, ids_send, ids_recv, table_sem, hin_sem, kv_sem, new_sem, dx_send, dx_recv, dc_send, dc_recv, dr_send, dr_recv, r1_send, r1_recv, r2_send, r2_recv, hop_send, out_loc, out_recv, credit,
):
    chunks, tokens = hid.shape[0], hid.shape[1]
    gathered = 4 * tokens
    dp = lax.axis_index("dp")
    pp = lax.axis_index("pp")
    ep = lax.axis_index("ep")
    other_pp = (dp, 1 - pp, ep)
    across = (dp, pp, lax.rem(ep + 2, 4))
    beside = (dp, pp, ep + 1 - 2 * lax.rem(ep, 2))
    first = ep * 8

    diagonal = (dp, pp, lax.rem(ep + 3 - 2 * lax.rem(ep, 2), 4))

    attn_w = [(wq_h, wq), (wk_h, wk), (wv_h, wv), (wo_h, wo)]
    moe_w = [(wg_h, wg), (wu_h, wu), (wd_h, wd)]
    weight_copies = [pltpu.make_async_copy(s, d, w_sem.at[j]) for j, (s, d) in enumerate(attn_w + moe_w)]

    def hin_copies(c):
        h = lax.rem(c, HIN_SLOTS)
        return [pltpu.make_async_copy(hid.at[c, piece(p)], hin.at[h, piece(p)], hin_sem.at[h, p]) for p in range(PIECES)]

    def kv_copies(c):
        return (pltpu.make_async_copy(k_cache.at[c], k_buf, kv_sem.at[0]), pltpu.make_async_copy(v_cache.at[c], v_buf, kv_sem.at[1]))

    def new_copies(c):
        return (pltpu.make_async_copy(kn, kn_out.at[c], new_sem.at[0]), pltpu.make_async_copy(vn, vn_out.at[c], new_sem.at[1]))

    def remote(src, dst, send, recv, peer):
        return pltpu.make_async_remote_copy(src_ref=src, dst_ref=dst, send_sem=send, recv_sem=recv, device_id=peer, device_id_type=MESH)

    def rows_at(slot, part_idx):
        return n_buf.at[slot, pl.ds(part_idx * tokens, tokens)]

    def dx_copy(c):
        s = lax.rem(c, 3)
        return remote(rows_at(s, 0), rows_at(s, 1), dx_send.at[s], dx_recv.at[s], across)

    def dc_copy(c):
        s = lax.rem(c, 3)
        return remote(rows_at(s, 0), rows_at(s, 2), dc_send.at[s], dc_recv.at[s], beside)

    def dr_copy(c):
        s = lax.rem(c, 3)
        return remote(rows_at(s, 1), rows_at(s, 3), dr_send.at[s], dr_recv.at[s], beside)

    def r1_copy(c, home):
        s = lax.rem(c, 2)
        return remote(part.at[pl.ds((2 + home) * tokens, tokens)], rb1.at[s, pl.ds(home * tokens, tokens)], r1_send.at[s, home], r1_recv.at[s, home], beside)

    rows = tokens // PIECES

    def piece(p):
        return pl.ds(pl.multiple_of(p * rows, rows), rows)

    def r2_copy(c, p):
        s = lax.rem(c, 3)
        return remote(rb1.at[lax.rem(c, 2), pl.ds(tokens + p * rows, rows)], rb2.at[s, piece(p)], r2_send.at[s, p], r2_recv.at[s, p], across)

    def hop_copy(c, p):
        s = lax.rem(c, 2)
        h = lax.rem(c, HIN_SLOTS)
        return remote(ho.at[s, piece(p)], hin.at[h, piece(p)], hop_send.at[s, p], hin_sem.at[h, p], other_pp)

    def out_copy(c, p):
        s = lax.rem(c, 2)
        return remote(ho.at[s, piece(p)], out.at[c, piece(p)], hop_send.at[s, p], out_recv.at[c, p], other_pp)

    def out_local(c, p):
        s = lax.rem(c, 2)
        return pltpu.make_async_copy(ho.at[s, piece(p)], out.at[c, piece(p)], out_loc.at[s, p])

    def ids_copies(part_idx):
        some = pl.ds(0, 1) if part_idx == 0 else pl.ds(1, chunks - 1)
        return [remote(ids_own.at[some], ids.at[j, some], ids_send.at[part_idx, j], ids_recv.at[part_idx, j], peer) for j, peer in ((1, across), (2, beside), (3, diagonal))]

    def table_copy(c):
        s = lax.rem(c, 2)
        return pltpu.make_async_copy(table, smem_table.at[s], table_sem)

    smem_table[1, 0, 0] = 0
    smem_table[1, 1, 0] = 0

    @pl.when(pp == 0)
    def _():
        for copy in hin_copies(0):
            copy.start()

    for copy in weight_copies[:3]:
        copy.start()
    for copy in kv_copies(0):
        copy.start()
    weight_copies[3].start()

    @pl.when(pp == 0)
    def _():
        for copy in hin_copies(1):
            copy.start()

    barrier = pltpu.get_barrier_semaphore()
    for peer in (other_pp, across, beside, diagonal):
        pl.semaphore_signal(barrier, inc=1, device_id=peer, device_id_type=MESH)
    pl.semaphore_wait(barrier, 4)

    for part_idx in range(2):
        for copy in ids_copies(part_idx):
            copy.start()

    w = {"a_gain": a_gain, "rope": rope_ref, "q": wq, "k": wk, "v": wv, "gate": wg, "up": wu, "down": wd}

    def plan(c):
        @pl.when(c == 0)
        def _():
            ids[0] = ids_own[...]
            with scope("w_ids"):
                for copy in ids_copies(0):
                    copy.wait()

        @pl.when(c == 1)
        def _():
            for copy in ids_copies(1):
                copy.wait()

        chosen_ids = jnp.concatenate([ids[j, c] for j in range(4)], axis=1)
        plan_tiles(chosen_ids, first, tri, member, rank_buf.at[lax.rem(c, 2)], table)
        table_copy(c).start()

    def combine_near(from_col, to_col):
        half = pl.ds(0, 2 * tokens)
        part[half, from_col:to_col] = dot(picks[half, :], terms[:, from_col:to_col])

    def project(c, with_sums):
        plan(c)
        with scope("w_hin"):
            for copy in hin_copies(c):
                copy.wait()

        @pl.when(c == 0)
        def _():
            for copy in weight_copies[:3]:
                copy.wait()

        @pl.when(jnp.logical_and(pp == 0, c + 2 < chunks))
        def _():
            for copy in hin_copies(c + 2):
                copy.start()

        @pl.when(c > 0)
        def _():
            for copy in new_copies(c - 1):
                copy.wait()

        seq_row = seq[pl.ds(c, 1), :].astype(F32)
        pos[...] = jnp.broadcast_to(seq_row, (128, 128)).T
        turn[...] = rope_tables(pos[...], w["rope"])
        if with_sums:
            combine_near(0, 256)
        attn_dots(hin[lax.rem(c, HIN_SLOTS)], w, x_buf)
        if with_sums:
            combine_near(256, 1024)
        attn_rope(turn, x_buf, q3, k3, v3, kn, vn)
        for copy in new_copies(c):
            copy.start()

    def reduce_pair(c):
        s = lax.rem(c, 2)
        far = pl.ds(tokens, tokens)
        near = pl.ds(0, tokens)
        with scope("w_r1"):
            r1_copy(c, 1).wait_recv()
        rb1[s, far, :] = rb1[s, far, :] + part[far, :]
        for p in range(PIECES):
            r2_copy(c, p).start()
        r1_copy(c, 0).wait_recv()
        rb1[s, near, :] = rb1[s, near, :] + part[near, :]
        for home in (1, 0):
            r1_copy(c, home).wait_send()

    def relay(c):
        copy = dx_copy(c)
        with scope("w_dx"):
            copy.wait_recv()
        dr_copy(c).start()
        copy.wait_send()
        dc_copy(c).wait_send()

    def attend(c):
        table_copy(c).wait()
        with scope("w_kv"):
            for copy in kv_copies(c):
                copy.wait()

        @pl.when(c == 0)
        def _():
            weight_copies[4].start()

        @pl.when(c == 1)
        def _():
            for copy in weight_copies[5:]:
                copy.start()

        def body(idx, carry):
            base = idx * GROUP_UNROLL
            ahead = attn_scores(base, q3, k3, k_buf)
            for u in range(GROUP_UNROLL):
                scores = ahead
                if u + 1 < GROUP_UNROLL:
                    ahead = attn_scores(base + u + 1, q3, k3, k_buf)
                attn_mix(base + u, *attn_weights(base + u, *scores, pos), v3, o3, v_buf)
            return carry

        with scope("groups"):
            lax.fori_loop(0, tokens // (GROUP * GROUP_UNROLL), body, 0)

        @pl.when(c + 1 < chunks)
        def _():
            for copy in kv_copies(c + 1):
                copy.start()

        @pl.when(c == 0)
        def _():
            weight_copies[3].wait()

        @pl.when(c == 1)
        def _():
            relay(0)

        @pl.when(c >= 1)
        def _():
            dispatched(c - 1)

        hidden = hin[lax.rem(c, HIN_SLOTS)].astype(F32)
        attn_out = jnp.concatenate([o3[pl.ds(g, tokens, stride=8), :].astype(BF16) for g in range(8)], axis=1)
        before = c + 5
        mixed = dot(attn_out, wo[...])
        router = logits(before)
        picked = gather_rows(before, 0, 0)
        new_mid = (hidden + mixed).astype(BF16)
        mid[lax.rem(c, 3)] = new_mid
        n_buf[lax.rem(c, 3), pl.ds(0, tokens), :] = rms(new_mid.astype(F32), m_gain[...].astype(F32))
        gates(before, router)
        gather_gate(picked, before, 0, 0)
        dx_copy(c).start()
        dc_copy(c).start()

        @pl.when(jnp.logical_and(pp == 1, c + HIN_SLOTS < chunks))
        def _():
            pl.semaphore_signal(credit, inc=1, device_id=other_pp, device_id_type=MESH)

    def tile_at(c, row, j):
        return smem_table[lax.rem(c, 2), row, j]

    def gather_rows(c, j, u):
        normed = n_buf.at[lax.rem(c, 3)]
        return moe_gather(j, u, tile_at(c, 0, j), tile_at(c, 1, j), first, normed, rank_buf.at[lax.rem(c, 2)], picks, x_buf)

    def gather_gate(picked, c, j, u):
        moe_gate(picked, u, tile_at(c, 0, j), first, gate_ref, g_buf)

    def gather(c, j, u):
        gather_gate(gather_rows(c, j, u), c, j, u)

    def dispatched(c):
        with scope("w_disp"):
            dc_copy(c).wait_recv()
            dr_copy(c).wait_recv()

    def logits(c):
        return dot_nt(w_r[...], n_buf[lax.rem(c, 3)])

    def gates(c, router):
        moe_gates(router, rank_buf.at[lax.rem(c, 2)], gate_ref)

    def experts(c):
        @pl.when(c == 0)
        def _():
            with scope("w_wts"):
                for copy in weight_copies[4:]:
                    copy.wait()

        def expand(j, u):
            moe_expand(u, tile_at(c, 0, j), w, x_buf, a_buf)

        def contract(j, u):
            moe_contract(j, u, tile_at(c, 0, j), w, a_buf, g_buf, terms)

        def body(idx, carry):
            base = idx * TILE_UNROLL
            expand(base, 0)
            gather(c, base + 1, 1)
            for u in range(1, TILE_UNROLL):
                expand(base + u, u)
                if u + 1 < TILE_UNROLL:
                    gather(c, base + u + 1, u + 1)
                else:
                    gather(c, lax.rem(base + TILE_UNROLL, tile_count), 0)
                contract(base + u - 1, u - 1)
            contract(base + TILE_UNROLL - 1, TILE_UNROLL - 1)

            @pl.when(jnp.logical_and(c >= 1, idx >= 1))
            def _():
                finish(c - 1, idx - 1)

            return carry

        with scope("tiles"):
            lax.fori_loop(0, tile_count // TILE_UNROLL, body, 0)
        half = 2 * tokens
        part[pl.ds(half, half), :] = dot(picks[pl.ds(half, half), :], terms[...])
        dr_copy(c).wait_send()
        r1_copy(c, 1).start()
        r1_copy(c, 0).start()

    def finish(c, p):
        s = lax.rem(c, 2)
        at = piece(p)

        @pl.when(jnp.logical_and(jnp.logical_and(pp == 0, p == 0), c >= HIN_SLOTS))
        def _():
            pl.semaphore_wait(credit, 1)

        @pl.when(jnp.logical_and(pp == 0, c >= 2))
        def _():
            hop_copy(c - 2, p).wait_send()

        @pl.when(jnp.logical_and(pp == 1, c >= 2))
        def _():
            out_copy(c - 2, p).wait_send()
            out_local(c - 2, p).wait()

        with scope("w_r2"):
            r2_copy(c, p).wait_recv()
            r2_copy(c, p).wait_send()
        mixed = (rb1[s, at, :] + rb2[lax.rem(c, 3), at, :]).astype(BF16)
        ho[s, at, :] = (mid[lax.rem(c, 3), at, :].astype(F32) + mixed.astype(F32)).astype(BF16)

        @pl.when(pp == 0)
        def _():
            hop_copy(c, p).start()

        @pl.when(pp == 1)
        def _():
            out_copy(c, p).start()
            out_local(c, p).start()

    def step(i, carry):
        @pl.when(i < 2)
        def _():
            with scope("project"):
                project(i, False)

        @pl.when(jnp.logical_and(i >= 2, i < chunks))
        def _():
            with scope("project_sum"):
                project(i, True)

        @pl.when(i >= chunks)
        def _():
            combine_near(0, 1024)

        @pl.when(i >= 2)
        def _():
            with scope("reduce_pair"):
                reduce_pair(i - 2)

        @pl.when(jnp.logical_and(i >= 2, i <= chunks))
        def _():
            with scope("relay"):
                relay(i - 1)

        @pl.when(i < chunks)
        def _():
            with scope("attend"):
                attend(i)

        @pl.when(i == chunks)
        def _():
            dispatched(i - 1)
            gates(i - 1, logits(i - 1))
            gather(i - 1, 0, 0)

        @pl.when(jnp.logical_and(i >= 1, i <= chunks))
        def _():
            with scope("experts"):
                experts(i - 1)

        @pl.when(i == chunks + 1)
        def _():
            with scope("finish_last"):
                for p in range(PIECES):
                    finish(i - 2, p)

        return carry

    lax.fori_loop(0, chunks + 2, step, 0)

    for copy in new_copies(chunks - 1):
        copy.wait()

    @pl.when(pp == 0)
    def _():
        for c in (chunks - 2, chunks - 1):
            for p in range(PIECES):
                hop_copy(c, p).wait_send()

        def arrived(c, carry):
            for p in range(PIECES):
                out_copy(c, p).wait_recv()
            return carry

        with scope("w_out"):
            lax.fori_loop(0, chunks, arrived, 0)

    @pl.when(pp == 1)
    def _():
        for c in (chunks - 2, chunks - 1):
            for p in range(PIECES):
                out_copy(c, p).wait_send()
                out_local(c, p).wait()


def step_call(args, chunks, tokens, tile_count):
    vmem = pl.BlockSpec(memory_space=pltpu.VMEM)
    hbm = pl.BlockSpec(memory_space=pl.ANY)
    wide = 4 * tokens
    dma = pltpu.SemaphoreType.DMA
    return pl.pallas_call(
        functools.partial(step_kernel, tile_count),
        out_shape=(
            jax.ShapeDtypeStruct((chunks, tokens, 1024), BF16),
            jax.ShapeDtypeStruct((chunks, tokens, 512), BF16),
            jax.ShapeDtypeStruct((chunks, tokens, 512), BF16),
        ),
        in_specs=[hbm, vmem, hbm, hbm, vmem, hbm, hbm, hbm, hbm, vmem, vmem, vmem, vmem, hbm, hbm, hbm, vmem],
        out_specs=(hbm, hbm, hbm),
        scratch_shapes=[
            pltpu.VMEM((3, wide, 1024), BF16),
            pltpu.VMEM((HIN_SLOTS, tokens, 1024), BF16),
            pltpu.VMEM((3, tokens, 1024), BF16),
            pltpu.VMEM((2, tokens, 1024), BF16),
            pltpu.VMEM((tokens * 128, 64), BF16),
            pltpu.VMEM((tokens * 128, 64), BF16),
            pltpu.VMEM((1024, 1024), BF16),
            pltpu.VMEM((1024, 512), BF16),
            pltpu.VMEM((1024, 512), BF16),
            pltpu.VMEM((1024, 1024), BF16),
            pltpu.VMEM((8, 1024, 512), BF16),
            pltpu.VMEM((8, 1024, 512), BF16),
            pltpu.VMEM((8, 512, 1024), BF16),
            pltpu.VMEM((wide, 1024), F32),
            pltpu.VMEM((2, 2 * tokens, 1024), F32),
            pltpu.VMEM((3, tokens, 1024), F32),
            pltpu.VMEM((wide, tile_count * TILE), BF16),
            pltpu.VMEM((tile_count * TILE, 1024), BF16),
            pltpu.VMEM((3, TILE, 1024), BF16),
            pltpu.VMEM((3, TILE, 512), BF16),
            pltpu.VMEM((TILE_UNROLL, TILE, 128), F32),
            pltpu.VMEM((tokens * 8, 128), F32),
            pltpu.VMEM((tokens * 8, 128), F32),
            pltpu.VMEM((tokens * 8, 128), F32),
            pltpu.VMEM((tokens * 8, 128), F32),
            pltpu.VMEM((tokens, 512), BF16),
            pltpu.VMEM((tokens, 512), BF16),
            pltpu.VMEM((2, 32, wide), F32),
            pltpu.VMEM((32, wide), F32),
            pltpu.VMEM((32, wide), F32),
            pltpu.VMEM((tokens, 128), F32),
            pltpu.VMEM((tokens, 256), F32),
            pltpu.VMEM((4, chunks, 8, tokens), jnp.int32),
            pltpu.VMEM((8, 128), jnp.int32),
            pltpu.SMEM((2, 8, 128), jnp.int32),
            dma((7,)), dma((2, 4)), dma((2, 4)), dma(()), dma((HIN_SLOTS, PIECES)), dma((2,)), dma((2,)),
            dma((3,)), dma((3,)), dma((3,)), dma((3,)), dma((3,)), dma((3,)),
            dma((2, 2)), dma((2, 2)), dma((3, PIECES)), dma((3, PIECES)),
            dma((2, PIECES)), dma((2, PIECES)), dma((chunks, PIECES)),
            pltpu.SemaphoreType.REGULAR,
        ],
        compiler_params=pltpu.CompilerParams(collective_id=0, has_side_effects=True, vmem_limit_bytes=67043328),
        name="decode_step",
        cost_estimate=pl.CostEstimate(flops=2 * 10**11, bytes_accessed=2 * 10**8, transcendentals=0),
    )(*args)


def result_kernel(h_ref, k_ref, v_ref, gain_ref, out_ref, kn_ref, vn_ref, rows):
    tokens = rows.shape[1] // 8
    gain = gain_ref[...].astype(F32).reshape(1, 1024)

    def body(idx, carry):
        at = pl.ds(pl.multiple_of(idx * tokens, tokens), tokens)
        vals = h_ref[0, at, :].astype(F32)
        vals = vals * lax.rsqrt(jnp.mean(vals * vals, axis=-1, keepdims=True) + EPS)
        for g in range(8):
            out_ref[0, at, g * 128:(g + 1) * 128] = (vals[:, g * 128:(g + 1) * 128] * gain[:, g * 128:(g + 1) * 128]).astype(BF16)
        for j, (src, dst) in enumerate(((k_ref, kn_ref), (v_ref, vn_ref))):
            spread_heads(rows.at[j], src[0, at, :].astype(F32))
            dst[0, at] = rows[j].reshape(tokens, 8, 128)[:, :, :64].astype(BF16)
        return carry

    lax.fori_loop(0, h_ref.shape[1] // tokens, body, 0)


def result_call(hidden, k_rows, v_rows, gain):
    blocks = 4
    step = hidden.shape[1]
    tokens = hidden.shape[0] * step // blocks
    hidden, k_rows, v_rows = (x.reshape(blocks, tokens, x.shape[-1]) for x in (hidden, k_rows, v_rows))
    chunks = blocks
    wide = pl.BlockSpec((1, tokens, 1024), lambda i: (i, 0, 0))
    dense = pl.BlockSpec((1, tokens, 512), lambda i: (i, 0, 0))
    heads = pl.BlockSpec((1, tokens, 8, 64), lambda i: (i, 0, 0, 0))
    return pl.pallas_call(
        result_kernel,
        grid=(chunks,),
        out_shape=(
            jax.ShapeDtypeStruct((chunks, tokens, 1024), BF16),
            jax.ShapeDtypeStruct((chunks, tokens, 8, 64), BF16),
            jax.ShapeDtypeStruct((chunks, tokens, 8, 64), BF16),
        ),
        in_specs=[wide, dense, dense, pl.BlockSpec((1024,), lambda i: (0,))],
        out_specs=(wide, heads, heads),
        scratch_shapes=[pltpu.VMEM((2, step * 8, 128), F32)],
        name="results",
        cost_estimate=pl.CostEstimate(flops=10**7, bytes_accessed=2 * 10**7, transcendentals=0),
    )(hidden, k_rows, v_rows, gain)


def solution(mesh):
    rows_spec = ("dp", "ep")
    three_dim = P("pp", None, None)
    two_dim = P("pp", None)
    expert_spec = P("pp", "ep", None, None)
    cache_spec = P("pp", None, rows_spec, None, None, None)
    new_spec = P("pp", None, rows_spec, None, None)
    in_specs = (P(None, rows_spec, None), P(None, rows_spec), cache_spec, cache_spec, P("pp", None, rows_spec, None), three_dim, three_dim, three_dim, three_dim, two_dim, two_dim, three_dim, expert_spec, expert_spec, expert_spec, P(None))
    out_specs = (P(None, rows_spec, None), new_spec, new_spec)

    def device_fn(hidden_in, seq_pos, k_cache, v_cache, expert_ids, w_query, w_key, w_value, w_out, attn_gain, mlp_gain, w_router, w_gate, w_up, w_down, final_gain):
        micro, rows = seq_pos.shape
        chunks = micro // PER_CHUNK
        tokens = PER_CHUNK * rows
        wide = 4 * tokens
        tile_count = (wide * 2 - 8) // TILE + 8
        assert tile_count == TILE_UNROLL * (PIECES + 1)
        angles = np.arange(1, 17)[:, None] * THETA ** (-np.arange(32) / 32)
        both = np.concatenate([np.tile(np.cos(angles), (1, 4)), np.tile(np.concatenate([-np.sin(angles), np.sin(angles)], axis=1), (1, 2))], axis=1)
        both = np.concatenate([both, np.zeros((112, 256))], axis=0).astype(np.float32)
        table = []
        for _ in range(3):
            table.append(both.astype(BF16))
            both = both - table[-1].astype(np.float32)
        table = jnp.asarray(np.concatenate(table, axis=1))
        tri = jnp.asarray(np.triu(np.ones((wide, wide)), 1), BF16)
        ids = jnp.swapaxes(expert_ids[0].reshape(chunks, tokens, 8), 1, 2)
        args = (
            hidden_in.reshape(chunks, tokens, 1024), seq_pos.reshape(chunks, tokens), k_cache.reshape(chunks, tokens * 128, 64), v_cache.reshape(chunks, tokens * 128, 64),
            ids, w_query[0], w_key[0], w_value[0], w_out[0], attn_gain, mlp_gain, table, w_router[0].T,
            w_gate[0], w_up[0], w_down[0], tri,
        )
        out, k_new, v_new = result_call(*step_call(args, chunks, tokens, tile_count), final_gain)
        shape = (1,) + seq_pos.shape + (8, 64)
        return out.reshape(hidden_in.shape), k_new.reshape(shape), v_new.reshape(shape)

    return jax.shard_map(device_fn, mesh=mesh, in_specs=in_specs, out_specs=out_specs, check_vma=False)
```

```python
import functools

import jax
import jax.numpy as jnp
import numpy as np
from jax import lax
from jax.experimental import pallas as pl
from jax.experimental.pallas import tpu as pltpu
from jax.sharding import PartitionSpec as P

THETA = 1000000.0
EPS = 1e-05
F32 = jnp.float32
BF16 = jnp.bfloat16
TILE = 128
GROUP = 16
TILE_UNROLL = 3
PER_CHUNK = 4
HIN_SLOTS = 4
PIECES = 4
MESH = pl.DeviceIdType.MESH


def scope(name):
    return jax.named_scope(name)


def rms(vals, gain_row):
    inv = lax.rsqrt(jnp.mean(vals * vals, axis=-1, keepdims=True) + EPS)
    return (vals * inv * gain_row).astype(BF16)


def dot(lhs, rhs):
    return jnp.dot(lhs, rhs, preferred_element_type=F32)


def dot_nt(lhs, rhs):
    return lax.dot_general(lhs, rhs, (((1,), (1,)), ((), ())), preferred_element_type=F32)


def rope_tables(pos, table):
    lane = lax.broadcasted_iota(jnp.int32, pos.shape, 1).astype(F32)
    both = dot(jnp.where(lane + 1.0 == pos, 1.0, 0.0).astype(BF16), table[...])
    both = both[:, :256] + both[:, 256:512] + both[:, 512:]
    return both


def rope(vals, cos_t, sin_t):
    lane = lax.broadcasted_iota(jnp.int32, (1, 128), 1)
    first = (lane % 64) < 32
    parts = []
    for j in range(vals.shape[1] // 128):
        block = vals[:, j * 128:(j + 1) * 128]
        swapped = jnp.where(first, pltpu.roll(block, 96, 1), pltpu.roll(block, 32, 1))
        parts.append(block * cos_t + swapped * sin_t)
    return jnp.concatenate(parts, axis=1)


def spread(ref, vals):
    tokens = vals.shape[0]
    for g in range(8):
        ref[pl.ds(g, tokens, stride=8), :] = vals[:, g * 128:(g + 1) * 128]


def spread_heads(ref, vals):
    tokens = vals.shape[0]
    low = lax.broadcasted_iota(jnp.int32, (1, 128), 1) < 64
    for j in range(4):
        block = vals[:, j * 128:(j + 1) * 128]
        other = pltpu.roll(block, 64, 1)
        ref[pl.ds(2 * j, tokens, stride=8), :] = jnp.where(low, block, other)
        ref[pl.ds(2 * j + 1, tokens, stride=8), :] = jnp.where(low, other, block)


def rows_of(ref, idx):
    return ref[pl.ds(pl.multiple_of(idx * GROUP * 8, GROUP * 8), GROUP * 8), :].reshape(GROUP, 8, 128)


def attn_dots(hidden, w, raw):
    normed = rms(hidden.astype(F32), w["a_gain"][...].astype(F32))
    raw[1] = dot(normed, w["q"][...]).astype(BF16)
    raw[2, :, :512] = dot(normed, w["k"][...]).astype(BF16)
    raw[2, :, 512:] = dot(normed, w["v"][...]).astype(BF16)


def attn_rope(turn, raw, q3, k3, v3, kn, vn):
    cos_t, sin_t = turn[:, :128], turn[:, 128:]
    spread(q3, rope(raw[1].astype(F32), cos_t, sin_t).astype(BF16).astype(F32))
    k = rope(raw[2, :, :512].astype(F32), cos_t, sin_t).astype(BF16)
    kn[...] = k
    spread_heads(k3, k.astype(F32))
    v = raw[2, :, 512:]
    vn[...] = v
    spread_heads(v3, v.astype(F32))


def attn_scores(idx, q3, k3, k_rows):
    q = rows_of(q3, idx)
    lane3 = lax.broadcasted_iota(jnp.int32, (1, 1, 128), 2)
    prod = q * rows_of(k3, idx)
    self_a = jnp.sum(jnp.where(lane3 < 64, prod, 0.0), axis=-1, keepdims=True)
    self_b = jnp.sum(jnp.where(lane3 < 64, 0.0, prod), axis=-1, keepdims=True)
    wide = (GROUP, 8, 128)
    self_s = jnp.concatenate([jnp.broadcast_to(self_a, wide), jnp.broadcast_to(self_b, wide)], axis=1) * 0.125
    q_rows = jnp.concatenate([q, pltpu.roll(q, 64, 2)], axis=1).astype(BF16)[:, :, :64].reshape(GROUP * 16, 64)
    row0 = idx * (GROUP * 128)
    blocks = []
    for p in range(GROUP // 2):
        keys = k_rows[pl.ds(pl.multiple_of(row0 + p * 256, 256), 256), :]
        both = dot_nt(q_rows[p * 32:(p + 1) * 32], keys)
        blocks.append(both[:16, :128].reshape(1, 16, 128))
        blocks.append(both[16:, 128:].reshape(1, 16, 128))
    return jnp.concatenate(blocks, axis=0), self_s


def attn_weights(idx, scores, self_s, pos_ref):
    row_i = lax.broadcasted_iota(jnp.int32, (16, 128), 0)
    lane_i = lax.broadcasted_iota(jnp.int32, (16, 128), 1)
    step = jnp.where((row_i % 8) == (lane_i % 8), lane_i // 8, 1000).astype(F32)
    pos = pos_ref[pl.ds(pl.multiple_of(idx * GROUP, GROUP), GROUP), :].reshape(GROUP, 1, 128)
    scores = jnp.where(step.reshape(1, 16, 128) < pos, scores * 0.125, -jnp.inf)
    wide = (GROUP, 16, 128)
    top = jnp.maximum(jnp.broadcast_to(jnp.max(scores, axis=-1, keepdims=True), wide), self_s)
    weights = jnp.exp(scores - top)
    self_w = jnp.exp(self_s - top)
    inv = 1.0 / (jnp.broadcast_to(jnp.sum(weights, axis=-1, keepdims=True), wide) + self_w)
    return (weights * inv).astype(BF16), (self_w * inv).astype(BF16).astype(F32)


def attn_mix(idx, weights, self_w, v3, o3, v_rows):
    row0 = idx * (GROUP * 128)
    zeros = jnp.zeros((16, 128), BF16)
    outs = []
    for p in range(GROUP // 2):
        vals = v_rows[pl.ds(pl.multiple_of(row0 + p * 256, 256), 256), :]
        upper = jnp.concatenate([weights[2 * p], zeros], axis=1)
        lower = jnp.concatenate([zeros, weights[2 * p + 1]], axis=1)
        outs.append(dot(jnp.concatenate([upper, lower], axis=0), vals).reshape(2, 16, 64))
    out = jnp.concatenate(outs, axis=0)
    v_new = rows_of(v3, idx)[:, :, :64]
    out_a = out[:, :8] + self_w[:, :8, :64] * v_new
    out_b = out[:, 8:] + self_w[:, 8:, :64] * v_new
    o3[pl.ds(pl.multiple_of(idx * GROUP * 8, GROUP * 8), GROUP * 8), :] = jnp.concatenate([out_a, out_b], axis=-1).reshape(GROUP * 8, 128)


def plan_tiles(ids, first, tri, member_ref, rank_ref, table_ref):
    tokens = ids.shape[1]
    expert_i = lax.broadcasted_iota(jnp.int32, (32, tokens), 0)
    chosen = jnp.zeros((32, tokens), F32)
    for s in range(ids.shape[0]):
        chosen = jnp.where(ids[s:s + 1, :] == expert_i, 1.0, chosen)
    member_ref[...] = chosen
    rank = dot(chosen.astype(BF16), tri[...])
    rank_ref[...] = jnp.where(chosen > 0.0, rank, -1.0)
    local = member_ref[pl.ds(pl.multiple_of(first, 8), 8), :]
    counts = jnp.sum(local, axis=-1, keepdims=True).astype(jnp.int32)
    tiles = jnp.broadcast_to(lax.shift_right_logical(counts + (TILE - 1), 7), (8, 128))
    lane = lax.broadcasted_iota(jnp.int32, (1, 128), 1)
    end = jnp.zeros((1, 128), jnp.int32)
    start = jnp.zeros((1, 128), jnp.int32)
    expert = jnp.zeros((1, 128), jnp.int32)
    for e in range(8):
        end = end + tiles[e:e + 1, :]
        passed = lane >= end
        expert = jnp.where(passed, expert + 1, expert)
        start = jnp.where(passed, end, start)
    sub = jnp.where(expert < 8, lane - start, 1000)
    table_ref[0:1, :] = jnp.minimum(expert, 7)
    table_ref[1:2, :] = sub


def moe_gates(logits, rank_ref, gate_ref):
    chosen = rank_ref[...] >= 0.0
    top = jnp.max(jnp.where(chosen, logits, -jnp.inf), axis=0, keepdims=True)
    gates = jnp.where(chosen, jnp.exp(logits - top), 0.0)
    gate_ref[...] = gates / jnp.sum(gates, axis=0, keepdims=True)


def slot_of(u):
    return 0 if u == 0 else 1 + (u - 1) % 2


def moe_gather(j, u, expert, sub, first, normed, rank_ref, picks, x_buf):
    ranks = rank_ref[pl.ds(first + expert, 1), :]
    wanted = (lax.broadcasted_iota(jnp.int32, (TILE, 1), 0) + sub * TILE).astype(F32)
    picked = jnp.where(ranks == wanted, 1.0, 0.0)
    picks[:, pl.ds(pl.multiple_of(j * TILE, TILE), TILE)] = picked.T.astype(BF16)
    x_buf[slot_of(u)] = dot(picked.astype(BF16), normed[...]).astype(BF16)
    return picked


def moe_gate(picked, u, expert, first, gate_ref, g_buf):
    gate = jnp.sum(picked * gate_ref[pl.ds(first + expert, 1), :], axis=-1, keepdims=True)
    g_buf[u] = jnp.broadcast_to(gate, (TILE, 128))


def moe_expand(u, expert, w, x_buf, a_buf):
    rows = x_buf[slot_of(u)]
    a_buf[slot_of(u)] = (jax.nn.silu(dot(rows, w["gate"][expert])) * dot(rows, w["up"][expert])).astype(BF16)


def moe_contract(j, u, expert, w, a_buf, g_buf, terms):
    y = dot(a_buf[slot_of(u)], w["down"][expert])
    gate = g_buf[u]
    at = pl.ds(pl.multiple_of(j * TILE, TILE), TILE)
    for p in range(8):
        terms[at, p * 128:(p + 1) * 128] = (gate * y[:, p * 128:(p + 1) * 128]).astype(BF16)


def step_kernel(
    tile_count,
    hid, seq, k_cache, v_cache, ids_own, wq_h, wk_h, wv_h, wo_h, a_gain, m_gain, rope_ref, w_r, wg_h, wu_h, wd_h, tri,
    out, kn_out, vn_out,
    n_buf, hin, mid, ho, k_buf, v_buf, wq, wk, wv, wo, wg, wu, wd, part, rb1, rb2, picks, terms, x_buf, a_buf, g_buf, q3, k3, v3, o3, kn, vn, rank_buf, gate_ref, member, pos, turn, ids, table, smem_table,
    w_sem, ids_send, ids_recv, table_sem, hin_sem, kv_sem, new_sem, dx_send, dx_recv, dc_send, dc_recv, dr_send, dr_recv, r1_send, r1_recv, r2_send, r2_recv, hop_send, out_loc, out_recv, credit,
):
    chunks, tokens = hid.shape[0], hid.shape[1]
    gathered = 4 * tokens
    dp = lax.axis_index("dp")
    pp = lax.axis_index("pp")
    ep = lax.axis_index("ep")
    other_pp = (dp, 1 - pp, ep)
    across = (dp, pp, lax.rem(ep + 2, 4))
    beside = (dp, pp, ep + 1 - 2 * lax.rem(ep, 2))
    first = ep * 8

    diagonal = (dp, pp, lax.rem(ep + 3 - 2 * lax.rem(ep, 2), 4))

    attn_w = [(wq_h, wq), (wk_h, wk), (wv_h, wv), (wo_h, wo)]
    moe_w = [(wg_h, wg), (wu_h, wu), (wd_h, wd)]
    weight_copies = [pltpu.make_async_copy(s, d, w_sem.at[j]) for j, (s, d) in enumerate(attn_w + moe_w)]

    def hin_copies(c):
        h = lax.rem(c, HIN_SLOTS)
        return [pltpu.make_async_copy(hid.at[c, piece(p)], hin.at[h, piece(p)], hin_sem.at[h, p]) for p in range(PIECES)]

    def kv_copies(c):
        return (pltpu.make_async_copy(k_cache.at[c], k_buf, kv_sem.at[0]), pltpu.make_async_copy(v_cache.at[c], v_buf, kv_sem.at[1]))

    def new_copies(c):
        return (pltpu.make_async_copy(kn, kn_out.at[c], new_sem.at[0]), pltpu.make_async_copy(vn, vn_out.at[c], new_sem.at[1]))

    def remote(src, dst, send, recv, peer):
        return pltpu.make_async_remote_copy(src_ref=src, dst_ref=dst, send_sem=send, recv_sem=recv, device_id=peer, device_id_type=MESH)

    def rows_at(slot, part_idx):
        return n_buf.at[slot, pl.ds(part_idx * tokens, tokens)]

    def dx_copy(c):
        s = lax.rem(c, 3)
        return remote(rows_at(s, 0), rows_at(s, 1), dx_send.at[s], dx_recv.at[s], across)

    def dc_copy(c):
        s = lax.rem(c, 3)
        return remote(rows_at(s, 0), rows_at(s, 2), dc_send.at[s], dc_recv.at[s], beside)

    def dr_copy(c):
        s = lax.rem(c, 3)
        return remote(rows_at(s, 1), rows_at(s, 3), dr_send.at[s], dr_recv.at[s], beside)

    def r1_copy(c, home):
        s = lax.rem(c, 2)
        return remote(part.at[pl.ds((2 + home) * tokens, tokens)], rb1.at[s, pl.ds(home * tokens, tokens)], r1_send.at[s, home], r1_recv.at[s, home], beside)

    rows = tokens // PIECES

    def piece(p):
        return pl.ds(pl.multiple_of(p * rows, rows), rows)

    def r2_copy(c, p):
        s = lax.rem(c, 3)
        return remote(rb1.at[lax.rem(c, 2), pl.ds(tokens + p * rows, rows)], rb2.at[s, piece(p)], r2_send.at[s, p], r2_recv.at[s, p], across)

    def hop_copy(c, p):
        s = lax.rem(c, 2)
        h = lax.rem(c, HIN_SLOTS)
        return remote(ho.at[s, piece(p)], hin.at[h, piece(p)], hop_send.at[s, p], hin_sem.at[h, p], other_pp)

    def out_copy(c, p):
        s = lax.rem(c, 2)
        return remote(ho.at[s, piece(p)], out.at[c, piece(p)], hop_send.at[s, p], out_recv.at[c, p], other_pp)

    def out_local(c, p):
        s = lax.rem(c, 2)
        return pltpu.make_async_copy(ho.at[s, piece(p)], out.at[c, piece(p)], out_loc.at[s, p])

    def ids_copies(part_idx):
        some = pl.ds(0, 1) if part_idx == 0 else pl.ds(1, chunks - 1)
        return [remote(ids_own.at[some], ids.at[j, some], ids_send.at[part_idx, j], ids_recv.at[part_idx, j], peer) for j, peer in ((1, across), (2, beside), (3, diagonal))]

    def table_copy(c):
        s = lax.rem(c, 2)
        return pltpu.make_async_copy(table, smem_table.at[s], table_sem)

    smem_table[1, 0, 0] = 0
    smem_table[1, 1, 0] = 0

    @pl.when(pp == 0)
    def _():
        for copy in hin_copies(0):
            copy.start()

    for copy in weight_copies[:3]:
        copy.start()
    for copy in kv_copies(0):
        copy.start()
    weight_copies[3].start()

    @pl.when(pp == 0)
    def _():
        for copy in hin_copies(1):
            copy.start()

    barrier = pltpu.get_barrier_semaphore()
    for peer in (other_pp, across, beside, diagonal):
        pl.semaphore_signal(barrier, inc=1, device_id=peer, device_id_type=MESH)
    pl.semaphore_wait(barrier, 4)

    for part_idx in range(2):
        for copy in ids_copies(part_idx):
            copy.start()

    w = {"a_gain": a_gain, "rope": rope_ref, "q": wq, "k": wk, "v": wv, "gate": wg, "up": wu, "down": wd}

    def plan(c):
        @pl.when(c == 0)
        def _():
            ids[0] = ids_own[...]
            with scope("w_ids"):
                for copy in ids_copies(0):
                    copy.wait()

        @pl.when(c == 1)
        def _():
            for copy in ids_copies(1):
                copy.wait()

        chosen_ids = jnp.concatenate([ids[j, c] for j in range(4)], axis=1)
        plan_tiles(chosen_ids, first, tri, member, rank_buf.at[lax.rem(c, 2)], table)
        table_copy(c).start()

    def combine_near(from_col, to_col):
        half = pl.ds(0, 2 * tokens)
        part[half, from_col:to_col] = dot(picks[half, :], terms[:, from_col:to_col])

    def project(c, with_sums):
        plan(c)
        with scope("w_hin"):
            for copy in hin_copies(c):
                copy.wait()

        @pl.when(c == 0)
        def _():
            for copy in weight_copies[:3]:
                copy.wait()

        @pl.when(jnp.logical_and(pp == 0, c + 2 < chunks))
        def _():
            for copy in hin_copies(c + 2):
                copy.start()

        @pl.when(c > 0)
        def _():
            for copy in new_copies(c - 1):
                copy.wait()

        seq_row = seq[pl.ds(c, 1), :].astype(F32)
        pos[...] = jnp.broadcast_to(seq_row, (128, 128)).T
        turn[...] = rope_tables(pos[...], w["rope"])
        if with_sums:
            combine_near(0, 256)
        attn_dots(hin[lax.rem(c, HIN_SLOTS)], w, x_buf)
        if with_sums:
            combine_near(256, 1024)
        attn_rope(turn, x_buf, q3, k3, v3, kn, vn)
        for copy in new_copies(c):
            copy.start()

    def reduce_pair(c):
        s = lax.rem(c, 2)
        far = pl.ds(tokens, tokens)
        near = pl.ds(0, tokens)
        with scope("w_r1"):
            r1_copy(c, 1).wait_recv()
        rb1[s, far, :] = rb1[s, far, :] + part[far, :]
        for p in range(PIECES):
            r2_copy(c, p).start()
        r1_copy(c, 0).wait_recv()
        rb1[s, near, :] = rb1[s, near, :] + part[near, :]
        for home in (1, 0):
            r1_copy(c, home).wait_send()

    def relay(c):
        copy = dx_copy(c)
        with scope("w_dx"):
            copy.wait_recv()
        dr_copy(c).start()
        copy.wait_send()
        dc_copy(c).wait_send()

    def attend(c):
        table_copy(c).wait()
        with scope("w_kv"):
            for copy in kv_copies(c):
                copy.wait()

        @pl.when(c == 0)
        def _():
            weight_copies[4].start()

        @pl.when(c == 1 - pp)
        def _():
            for copy in weight_copies[5:]:
                copy.start()

        def groups(base, count):
            ahead = attn_scores(base, q3, k3, k_buf)
            for u in range(base, base + count):
                scores = ahead
                if u + 1 < base + count:
                    ahead = attn_scores(u + 1, q3, k3, k_buf)
                attn_mix(u, *attn_weights(u, *scores, pos), v3, o3, v_buf)

        half = tokens // GROUP // 2
        with scope("groups"):
            groups(0, half)

        @pl.when(c >= 2)
        def _():
            with scope("relay"):
                relay(c - 1)

        with scope("groups"):
            groups(half, half)

        @pl.when(c + 1 < chunks)
        def _():
            for copy in kv_copies(c + 1):
                copy.start()

        @pl.when(c == 0)
        def _():
            weight_copies[3].wait()

        @pl.when(c == 1)
        def _():
            relay(0)

        @pl.when(c >= 1)
        def _():
            dispatched(c - 1)

        hidden = hin[lax.rem(c, HIN_SLOTS)].astype(F32)
        attn_out = jnp.concatenate([o3[pl.ds(g, tokens, stride=8), :].astype(BF16) for g in range(8)], axis=1)
        before = c + 5
        mixed = dot(attn_out, wo[...])
        router = logits(before)
        picked = gather_rows(before, 0, 0)
        new_mid = (hidden + mixed).astype(BF16)
        mid[lax.rem(c, 3)] = new_mid
        n_buf[lax.rem(c, 3), pl.ds(0, tokens), :] = rms(new_mid.astype(F32), m_gain[...].astype(F32))
        gates(before, router)
        gather_gate(picked, before, 0, 0)
        dx_copy(c).start()
        dc_copy(c).start()

        @pl.when(jnp.logical_and(pp == 1, c + HIN_SLOTS < chunks))
        def _():
            pl.semaphore_signal(credit, inc=1, device_id=other_pp, device_id_type=MESH)

    def tile_at(c, row, j):
        return smem_table[lax.rem(c, 2), row, j]

    def gather_rows(c, j, u):
        normed = n_buf.at[lax.rem(c, 3)]
        return moe_gather(j, u, tile_at(c, 0, j), tile_at(c, 1, j), first, normed, rank_buf.at[lax.rem(c, 2)], picks, x_buf)

    def gather_gate(picked, c, j, u):
        moe_gate(picked, u, tile_at(c, 0, j), first, gate_ref, g_buf)

    def gather(c, j, u):
        gather_gate(gather_rows(c, j, u), c, j, u)

    def dispatched(c):
        with scope("w_disp"):
            dc_copy(c).wait_recv()
            dr_copy(c).wait_recv()

    def logits(c):
        return dot_nt(w_r[...], n_buf[lax.rem(c, 3)])

    def gates(c, router):
        moe_gates(router, rank_buf.at[lax.rem(c, 2)], gate_ref)

    def experts(c):
        @pl.when(c == 0)
        def _():
            with scope("w_wts"):
                for copy in weight_copies[4:]:
                    copy.wait()

        def expand(j, u):
            moe_expand(u, tile_at(c, 0, j), w, x_buf, a_buf)

        def contract(j, u):
            moe_contract(j, u, tile_at(c, 0, j), w, a_buf, g_buf, terms)

        def body(idx, carry):
            base = idx * TILE_UNROLL
            expand(base, 0)
            gather(c, base + 1, 1)
            for u in range(1, TILE_UNROLL):
                expand(base + u, u)
                if u + 1 < TILE_UNROLL:
                    gather(c, base + u + 1, u + 1)
                else:
                    gather(c, lax.rem(base + TILE_UNROLL, tile_count), 0)
                contract(base + u - 1, u - 1)
            contract(base + TILE_UNROLL - 1, TILE_UNROLL - 1)

            @pl.when(jnp.logical_and(c >= 1, idx >= 1))
            def _():
                finish(c - 1, idx - 1)

            return carry

        with scope("tiles"):
            lax.fori_loop(0, tile_count // TILE_UNROLL, body, 0)
        half = 2 * tokens
        part[pl.ds(half, half), :] = dot(picks[pl.ds(half, half), :], terms[...])
        dr_copy(c).wait_send()
        r1_copy(c, 1).start()
        r1_copy(c, 0).start()

    def finish(c, p):
        s = lax.rem(c, 2)
        at = piece(p)

        @pl.when(jnp.logical_and(jnp.logical_and(pp == 0, p == 0), c >= HIN_SLOTS))
        def _():
            pl.semaphore_wait(credit, 1)

        @pl.when(jnp.logical_and(pp == 0, c >= 2))
        def _():
            hop_copy(c - 2, p).wait_send()

        @pl.when(jnp.logical_and(pp == 1, c >= 2))
        def _():
            out_copy(c - 2, p).wait_send()
            out_local(c - 2, p).wait()

        with scope("w_r2"):
            r2_copy(c, p).wait_recv()
            r2_copy(c, p).wait_send()
        mixed = (rb1[s, at, :] + rb2[lax.rem(c, 3), at, :]).astype(BF16)
        ho[s, at, :] = (mid[lax.rem(c, 3), at, :].astype(F32) + mixed.astype(F32)).astype(BF16)

        @pl.when(pp == 0)
        def _():
            hop_copy(c, p).start()

        @pl.when(pp == 1)
        def _():
            out_copy(c, p).start()
            out_local(c, p).start()

    def step(i, carry):
        @pl.when(i < 2)
        def _():
            with scope("project"):
                project(i, False)

        @pl.when(jnp.logical_and(i >= 2, i < chunks))
        def _():
            with scope("project_sum"):
                project(i, True)

        @pl.when(i >= chunks)
        def _():
            combine_near(0, 1024)

        @pl.when(i >= 2)
        def _():
            with scope("reduce_pair"):
                reduce_pair(i - 2)

        @pl.when(i == chunks)
        def _():
            with scope("relay"):
                relay(i - 1)

        @pl.when(i < chunks)
        def _():
            with scope("attend"):
                attend(i)

        @pl.when(i == chunks)
        def _():
            dispatched(i - 1)
            gates(i - 1, logits(i - 1))
            gather(i - 1, 0, 0)

        @pl.when(jnp.logical_and(i >= 1, i <= chunks))
        def _():
            with scope("experts"):
                experts(i - 1)

        @pl.when(i == chunks + 1)
        def _():
            with scope("finish_last"):
                for p in range(PIECES):
                    finish(i - 2, p)

        return carry

    lax.fori_loop(0, chunks + 2, step, 0)

    for copy in new_copies(chunks - 1):
        copy.wait()

    @pl.when(pp == 0)
    def _():
        for c in (chunks - 2, chunks - 1):
            for p in range(PIECES):
                hop_copy(c, p).wait_send()

        def arrived(c, carry):
            for p in range(PIECES):
                out_copy(c, p).wait_recv()
            return carry

        with scope("w_out"):
            lax.fori_loop(0, chunks, arrived, 0)

    @pl.when(pp == 1)
    def _():
        for c in (chunks - 2, chunks - 1):
            for p in range(PIECES):
                out_copy(c, p).wait_send()
                out_local(c, p).wait()


def step_call(args, chunks, tokens, tile_count):
    vmem = pl.BlockSpec(memory_space=pltpu.VMEM)
    hbm = pl.BlockSpec(memory_space=pl.ANY)
    wide = 4 * tokens
    dma = pltpu.SemaphoreType.DMA
    return pl.pallas_call(
        functools.partial(step_kernel, tile_count),
        out_shape=(
            jax.ShapeDtypeStruct((chunks, tokens, 1024), BF16),
            jax.ShapeDtypeStruct((chunks, tokens, 512), BF16),
            jax.ShapeDtypeStruct((chunks, tokens, 512), BF16),
        ),
        in_specs=[hbm, vmem, hbm, hbm, vmem, hbm, hbm, hbm, hbm, vmem, vmem, vmem, vmem, hbm, hbm, hbm, vmem],
        out_specs=(hbm, hbm, hbm),
        scratch_shapes=[
            pltpu.VMEM((3, wide, 1024), BF16),
            pltpu.VMEM((HIN_SLOTS, tokens, 1024), BF16),
            pltpu.VMEM((3, tokens, 1024), BF16),
            pltpu.VMEM((2, tokens, 1024), BF16),
            pltpu.VMEM((tokens * 128, 64), BF16),
            pltpu.VMEM((tokens * 128, 64), BF16),
            pltpu.VMEM((1024, 1024), BF16),
            pltpu.VMEM((1024, 512), BF16),
            pltpu.VMEM((1024, 512), BF16),
            pltpu.VMEM((1024, 1024), BF16),
            pltpu.VMEM((8, 1024, 512), BF16),
            pltpu.VMEM((8, 1024, 512), BF16),
            pltpu.VMEM((8, 512, 1024), BF16),
            pltpu.VMEM((wide, 1024), F32),
            pltpu.VMEM((2, 2 * tokens, 1024), F32),
            pltpu.VMEM((3, tokens, 1024), F32),
            pltpu.VMEM((wide, tile_count * TILE), BF16),
            pltpu.VMEM((tile_count * TILE, 1024), BF16),
            pltpu.VMEM((3, TILE, 1024), BF16),
            pltpu.VMEM((3, TILE, 512), BF16),
            pltpu.VMEM((TILE_UNROLL, TILE, 128), F32),
            pltpu.VMEM((tokens * 8, 128), F32),
            pltpu.VMEM((tokens * 8, 128), F32),
            pltpu.VMEM((tokens * 8, 128), F32),
            pltpu.VMEM((tokens * 8, 128), F32),
            pltpu.VMEM((tokens, 512), BF16),
            pltpu.VMEM((tokens, 512), BF16),
            pltpu.VMEM((2, 32, wide), F32),
            pltpu.VMEM((32, wide), F32),
            pltpu.VMEM((32, wide), F32),
            pltpu.VMEM((tokens, 128), F32),
            pltpu.VMEM((tokens, 256), F32),
            pltpu.VMEM((4, chunks, 8, tokens), jnp.int32),
            pltpu.VMEM((8, 128), jnp.int32),
            pltpu.SMEM((2, 8, 128), jnp.int32),
            dma((7,)), dma((2, 4)), dma((2, 4)), dma(()), dma((HIN_SLOTS, PIECES)), dma((2,)), dma((2,)),
            dma((3,)), dma((3,)), dma((3,)), dma((3,)), dma((3,)), dma((3,)),
            dma((2, 2)), dma((2, 2)), dma((3, PIECES)), dma((3, PIECES)),
            dma((2, PIECES)), dma((2, PIECES)), dma((chunks, PIECES)),
            pltpu.SemaphoreType.REGULAR,
        ],
        compiler_params=pltpu.CompilerParams(collective_id=0, has_side_effects=True, vmem_limit_bytes=67043328),
        name="decode_step",
        cost_estimate=pl.CostEstimate(flops=2 * 10**11, bytes_accessed=2 * 10**8, transcendentals=0),
    )(*args)


def result_kernel(h_ref, k_ref, v_ref, gain_ref, out_ref, kn_ref, vn_ref, rows):
    tokens = rows.shape[1] // 8
    gain = gain_ref[...].astype(F32).reshape(1, 1024)

    def body(idx, carry):
        at = pl.ds(pl.multiple_of(idx * tokens, tokens), tokens)
        vals = h_ref[0, at, :].astype(F32)
        vals = vals * lax.rsqrt(jnp.mean(vals * vals, axis=-1, keepdims=True) + EPS)
        for g in range(8):
            out_ref[0, at, g * 128:(g + 1) * 128] = (vals[:, g * 128:(g + 1) * 128] * gain[:, g * 128:(g + 1) * 128]).astype(BF16)
        for j, (src, dst) in enumerate(((k_ref, kn_ref), (v_ref, vn_ref))):
            spread_heads(rows.at[j], src[0, at, :].astype(F32))
            dst[0, at] = rows[j].reshape(tokens, 8, 128)[:, :, :64].astype(BF16)
        return carry

    lax.fori_loop(0, h_ref.shape[1] // tokens, body, 0)


def result_call(hidden, k_rows, v_rows, gain):
    blocks = 4
    step = hidden.shape[1]
    tokens = hidden.shape[0] * step // blocks
    hidden, k_rows, v_rows = (x.reshape(blocks, tokens, x.shape[-1]) for x in (hidden, k_rows, v_rows))
    chunks = blocks
    wide = pl.BlockSpec((1, tokens, 1024), lambda i: (i, 0, 0))
    dense = pl.BlockSpec((1, tokens, 512), lambda i: (i, 0, 0))
    heads = pl.BlockSpec((1, tokens, 8, 64), lambda i: (i, 0, 0, 0))
    return pl.pallas_call(
        result_kernel,
        grid=(chunks,),
        out_shape=(
            jax.ShapeDtypeStruct((chunks, tokens, 1024), BF16),
            jax.ShapeDtypeStruct((chunks, tokens, 8, 64), BF16),
            jax.ShapeDtypeStruct((chunks, tokens, 8, 64), BF16),
        ),
        in_specs=[wide, dense, dense, pl.BlockSpec((1024,), lambda i: (0,))],
        out_specs=(wide, heads, heads),
        scratch_shapes=[pltpu.VMEM((2, step * 8, 128), F32)],
        name="results",
        cost_estimate=pl.CostEstimate(flops=10**7, bytes_accessed=2 * 10**7, transcendentals=0),
    )(hidden, k_rows, v_rows, gain)


def solution(mesh):
    rows_spec = ("dp", "ep")
    three_dim = P("pp", None, None)
    two_dim = P("pp", None)
    expert_spec = P("pp", "ep", None, None)
    cache_spec = P("pp", None, rows_spec, None, None, None)
    new_spec = P("pp", None, rows_spec, None, None)
    in_specs = (P(None, rows_spec, None), P(None, rows_spec), cache_spec, cache_spec, P("pp", None, rows_spec, None), three_dim, three_dim, three_dim, three_dim, two_dim, two_dim, three_dim, expert_spec, expert_spec, expert_spec, P(None))
    out_specs = (P(None, rows_spec, None), new_spec, new_spec)

    def device_fn(hidden_in, seq_pos, k_cache, v_cache, expert_ids, w_query, w_key, w_value, w_out, attn_gain, mlp_gain, w_router, w_gate, w_up, w_down, final_gain):
        micro, rows = seq_pos.shape
        chunks = micro // PER_CHUNK
        tokens = PER_CHUNK * rows
        wide = 4 * tokens
        tile_count = (wide * 2 - 8) // TILE + 8
        assert tile_count == TILE_UNROLL * (PIECES + 1)
        angles = np.arange(1, 17)[:, None] * THETA ** (-np.arange(32) / 32)
        both = np.concatenate([np.tile(np.cos(angles), (1, 4)), np.tile(np.concatenate([-np.sin(angles), np.sin(angles)], axis=1), (1, 2))], axis=1)
        both = np.concatenate([both, np.zeros((112, 256))], axis=0).astype(np.float32)
        table = []
        for _ in range(3):
            table.append(both.astype(BF16))
            both = both - table[-1].astype(np.float32)
        table = jnp.asarray(np.concatenate(table, axis=1))
        tri = jnp.asarray(np.triu(np.ones((wide, wide)), 1), BF16)
        ids = jnp.swapaxes(expert_ids[0].reshape(chunks, tokens, 8), 1, 2)
        args = (
            hidden_in.reshape(chunks, tokens, 1024), seq_pos.reshape(chunks, tokens), k_cache.reshape(chunks, tokens * 128, 64), v_cache.reshape(chunks, tokens * 128, 64),
            ids, w_query[0], w_key[0], w_value[0], w_out[0], attn_gain, mlp_gain, table, w_router[0].T,
            w_gate[0], w_up[0], w_down[0], tri,
        )
        out, k_new, v_new = result_call(*step_call(args, chunks, tokens, tile_count), final_gain)
        shape = (1,) + seq_pos.shape + (8, 64)
        return out.reshape(hidden_in.shape), k_new.reshape(shape), v_new.reshape(shape)

    return jax.shard_map(device_fn, mesh=mesh, in_specs=in_specs, out_specs=out_specs, check_vma=False)
```

```python
import functools

import jax
import jax.numpy as jnp
import numpy as np
from jax import lax
from jax.experimental import pallas as pl
from jax.experimental.pallas import tpu as pltpu
from jax.sharding import PartitionSpec as P

THETA = 1000000.0
EPS = 1e-05
F32 = jnp.float32
BF16 = jnp.bfloat16
TILE = 128
GROUP = 16
TILE_UNROLL = 3
PER_CHUNK = 4
HIN_SLOTS = 4
PIECES = 4
MESH = pl.DeviceIdType.MESH


def scope(name):
    return jax.named_scope(name)


def rms(vals, gain_row):
    inv = lax.rsqrt(jnp.mean(vals * vals, axis=-1, keepdims=True) + EPS)
    return (vals * inv * gain_row).astype(BF16)


def dot(lhs, rhs):
    return jnp.dot(lhs, rhs, preferred_element_type=F32)


def dot_nt(lhs, rhs):
    return lax.dot_general(lhs, rhs, (((1,), (1,)), ((), ())), preferred_element_type=F32)


def rope_tables(pos, table):
    lane = lax.broadcasted_iota(jnp.int32, pos.shape, 1).astype(F32)
    both = dot(jnp.where(lane + 1.0 == pos, 1.0, 0.0).astype(BF16), table[...])
    both = both[:, :256] + both[:, 256:512] + both[:, 512:]
    return both


def rope(vals, cos_t, sin_t):
    lane = lax.broadcasted_iota(jnp.int32, (1, 128), 1)
    first = (lane % 64) < 32
    parts = []
    for j in range(vals.shape[1] // 128):
        block = vals[:, j * 128:(j + 1) * 128]
        swapped = jnp.where(first, pltpu.roll(block, 96, 1), pltpu.roll(block, 32, 1))
        parts.append(block * cos_t + swapped * sin_t)
    return jnp.concatenate(parts, axis=1)


def spread(ref, vals):
    tokens = vals.shape[0]
    for g in range(8):
        ref[pl.ds(g, tokens, stride=8), :] = vals[:, g * 128:(g + 1) * 128]


def spread_heads(ref, vals):
    tokens = vals.shape[0]
    low = lax.broadcasted_iota(jnp.int32, (1, 128), 1) < 64
    for j in range(4):
        block = vals[:, j * 128:(j + 1) * 128]
        other = pltpu.roll(block, 64, 1)
        ref[pl.ds(2 * j, tokens, stride=8), :] = jnp.where(low, block, other)
        ref[pl.ds(2 * j + 1, tokens, stride=8), :] = jnp.where(low, other, block)


def rows_of(ref, idx):
    return ref[pl.ds(pl.multiple_of(idx * GROUP * 8, GROUP * 8), GROUP * 8), :].reshape(GROUP, 8, 128)


def attn_dots(hidden, w, raw):
    normed = rms(hidden.astype(F32), w["a_gain"][...].astype(F32))
    raw[1] = dot(normed, w["q"][...]).astype(BF16)
    raw[2, :, :512] = dot(normed, w["k"][...]).astype(BF16)
    raw[2, :, 512:] = dot(normed, w["v"][...]).astype(BF16)


def attn_rope(turn, raw, q3, k3, v3, kn, vn):
    cos_t, sin_t = turn[:, :128], turn[:, 128:]
    spread(q3, rope(raw[1].astype(F32), cos_t, sin_t).astype(BF16).astype(F32))
    k = rope(raw[2, :, :512].astype(F32), cos_t, sin_t).astype(BF16)
    kn[...] = k
    spread_heads(k3, k.astype(F32))
    v = raw[2, :, 512:]
    vn[...] = v
    spread_heads(v3, v.astype(F32))


def attn_scores(idx, q3, k3, k_rows):
    q = rows_of(q3, idx)
    lane3 = lax.broadcasted_iota(jnp.int32, (1, 1, 128), 2)
    prod = q * rows_of(k3, idx)
    self_a = jnp.sum(jnp.where(lane3 < 64, prod, 0.0), axis=-1, keepdims=True)
    self_b = jnp.sum(jnp.where(lane3 < 64, 0.0, prod), axis=-1, keepdims=True)
    wide = (GROUP, 8, 128)
    self_s = jnp.concatenate([jnp.broadcast_to(self_a, wide), jnp.broadcast_to(self_b, wide)], axis=1) * 0.125
    q_rows = jnp.concatenate([q, pltpu.roll(q, 64, 2)], axis=1).astype(BF16)[:, :, :64].reshape(GROUP * 16, 64)
    row0 = idx * (GROUP * 128)
    blocks = []
    for p in range(GROUP // 2):
        keys = k_rows[pl.ds(pl.multiple_of(row0 + p * 256, 256), 256), :]
        both = dot_nt(q_rows[p * 32:(p + 1) * 32], keys)
        blocks.append(both[:16, :128].reshape(1, 16, 128))
        blocks.append(both[16:, 128:].reshape(1, 16, 128))
    return jnp.concatenate(blocks, axis=0), self_s


def attn_weights(idx, scores, self_s, pos_ref):
    row_i = lax.broadcasted_iota(jnp.int32, (16, 128), 0)
    lane_i = lax.broadcasted_iota(jnp.int32, (16, 128), 1)
    step = jnp.where((row_i % 8) == (lane_i % 8), lane_i // 8, 1000).astype(F32)
    pos = pos_ref[pl.ds(pl.multiple_of(idx * GROUP, GROUP), GROUP), :].reshape(GROUP, 1, 128)
    scores = jnp.where(step.reshape(1, 16, 128) < pos, scores * 0.125, -jnp.inf)
    wide = (GROUP, 16, 128)
    top = jnp.maximum(jnp.broadcast_to(jnp.max(scores, axis=-1, keepdims=True), wide), self_s)
    weights = jnp.exp(scores - top)
    self_w = jnp.exp(self_s - top)
    inv = 1.0 / (jnp.broadcast_to(jnp.sum(weights, axis=-1, keepdims=True), wide) + self_w)
    return (weights * inv).astype(BF16), (self_w * inv).astype(BF16).astype(F32)


def attn_mix(idx, weights, self_w, v3, o3, v_rows):
    row0 = idx * (GROUP * 128)
    zeros = jnp.zeros((16, 128), BF16)
    outs = []
    for p in range(GROUP // 2):
        vals = v_rows[pl.ds(pl.multiple_of(row0 + p * 256, 256), 256), :]
        upper = jnp.concatenate([weights[2 * p], zeros], axis=1)
        lower = jnp.concatenate([zeros, weights[2 * p + 1]], axis=1)
        outs.append(dot(jnp.concatenate([upper, lower], axis=0), vals).reshape(2, 16, 64))
    out = jnp.concatenate(outs, axis=0)
    v_new = rows_of(v3, idx)[:, :, :64]
    out_a = out[:, :8] + self_w[:, :8, :64] * v_new
    out_b = out[:, 8:] + self_w[:, 8:, :64] * v_new
    o3[pl.ds(pl.multiple_of(idx * GROUP * 8, GROUP * 8), GROUP * 8), :] = jnp.concatenate([out_a, out_b], axis=-1).reshape(GROUP * 8, 128)


def plan_tiles(ids, first, tri, member_ref, rank_ref, table_ref):
    tokens = ids.shape[1]
    expert_i = lax.broadcasted_iota(jnp.int32, (32, tokens), 0)
    chosen = jnp.zeros((32, tokens), F32)
    for s in range(ids.shape[0]):
        chosen = jnp.where(ids[s:s + 1, :] == expert_i, 1.0, chosen)
    member_ref[...] = chosen
    rank = dot(chosen.astype(BF16), tri[...])
    rank_ref[...] = jnp.where(chosen > 0.0, rank, -1.0)
    local = member_ref[pl.ds(pl.multiple_of(first, 8), 8), :]
    counts = jnp.sum(local, axis=-1, keepdims=True).astype(jnp.int32)
    tiles = jnp.broadcast_to(lax.shift_right_logical(counts + (TILE - 1), 7), (8, 128))
    lane = lax.broadcasted_iota(jnp.int32, (1, 128), 1)
    end = jnp.zeros((1, 128), jnp.int32)
    start = jnp.zeros((1, 128), jnp.int32)
    expert = jnp.zeros((1, 128), jnp.int32)
    for e in range(8):
        end = end + tiles[e:e + 1, :]
        passed = lane >= end
        expert = jnp.where(passed, expert + 1, expert)
        start = jnp.where(passed, end, start)
    sub = jnp.where(expert < 8, lane - start, 1000)
    table_ref[0:1, :] = jnp.minimum(expert, 7)
    table_ref[1:2, :] = sub


def moe_gates(logits, rank_ref, gate_ref):
    chosen = rank_ref[...] >= 0.0
    top = jnp.max(jnp.where(chosen, logits, -jnp.inf), axis=0, keepdims=True)
    gates = jnp.where(chosen, jnp.exp(logits - top), 0.0)
    gate_ref[...] = gates / jnp.sum(gates, axis=0, keepdims=True)


def slot_of(u):
    return 0 if u == 0 else 1 + (u - 1) % 2


def moe_gather(j, u, expert, sub, first, normed, rank_ref, picks, x_buf):
    ranks = rank_ref[pl.ds(first + expert, 1), :]
    wanted = (lax.broadcasted_iota(jnp.int32, (TILE, 1), 0) + sub * TILE).astype(F32)
    picked = jnp.where(ranks == wanted, 1.0, 0.0)
    picks[:, pl.ds(pl.multiple_of(j * TILE, TILE), TILE)] = picked.T.astype(BF16)
    x_buf[slot_of(u)] = dot(picked.astype(BF16), normed[...]).astype(BF16)
    return picked


def moe_gate(picked, u, expert, first, gate_ref, g_buf):
    gate = jnp.sum(picked * gate_ref[pl.ds(first + expert, 1), :], axis=-1, keepdims=True)
    g_buf[u] = jnp.broadcast_to(gate, (TILE, 128))


def moe_expand(u, expert, w, x_buf, a_buf):
    rows = x_buf[slot_of(u)]
    a_buf[slot_of(u)] = (jax.nn.silu(dot(rows, w["gate"][expert])) * dot(rows, w["up"][expert])).astype(BF16)


def moe_contract(j, u, expert, w, a_buf, g_buf, terms):
    y = dot(a_buf[slot_of(u)], w["down"][expert])
    gate = g_buf[u]
    at = pl.ds(pl.multiple_of(j * TILE, TILE), TILE)
    for p in range(8):
        terms[at, p * 128:(p + 1) * 128] = (gate * y[:, p * 128:(p + 1) * 128]).astype(BF16)


def step_kernel(
    tile_count,
    hid, seq, k_cache, v_cache, ids_own, wq_h, wk_h, wv_h, wo_h, a_gain, m_gain, rope_ref, w_r, wg_h, wu_h, wd_h, tri,
    out, kn_out, vn_out,
    n_buf, hin, mid, ho, k_buf, v_buf, wq, wk, wv, wo, wg, wu, wd, part, rb1, rb2, picks, terms, x_buf, a_buf, g_buf, q3, k3, v3, o3, kn, vn, rank_buf, gate_ref, member, pos, turn, ids, table, smem_table,
    w_sem, ids_send, ids_recv, table_sem, hin_sem, kv_sem, new_sem, dx_send, dx_recv, dc_send, dc_recv, dr_send, dr_recv, r1_send, r1_recv, r2_send, r2_recv, hop_send, out_loc, out_recv, credit,
):
    chunks, tokens = hid.shape[0], hid.shape[1]
    gathered = 4 * tokens
    dp = lax.axis_index("dp")
    pp = lax.axis_index("pp")
    ep = lax.axis_index("ep")
    other_pp = (dp, 1 - pp, ep)
    across = (dp, pp, lax.rem(ep + 2, 4))
    beside = (dp, pp, ep + 1 - 2 * lax.rem(ep, 2))
    first = ep * 8

    diagonal = (dp, pp, lax.rem(ep + 3 - 2 * lax.rem(ep, 2), 4))

    attn_w = [(wq_h, wq), (wk_h, wk), (wv_h, wv), (wo_h, wo)]
    moe_w = [(wg_h, wg), (wu_h, wu), (wd_h, wd)]
    weight_copies = [pltpu.make_async_copy(s, d, w_sem.at[j]) for j, (s, d) in enumerate(attn_w + moe_w)]

    def hin_copies(c):
        h = lax.rem(c, HIN_SLOTS)
        return [pltpu.make_async_copy(hid.at[c, piece(p)], hin.at[h, piece(p)], hin_sem.at[h, p]) for p in range(PIECES)]

    def kv_copies(c):
        return (pltpu.make_async_copy(k_cache.at[c], k_buf, kv_sem.at[0]), pltpu.make_async_copy(v_cache.at[c], v_buf, kv_sem.at[1]))

    def new_copies(c):
        return (pltpu.make_async_copy(kn, kn_out.at[c], new_sem.at[0]), pltpu.make_async_copy(vn, vn_out.at[c], new_sem.at[1]))

    def remote(src, dst, send, recv, peer):
        return pltpu.make_async_remote_copy(src_ref=src, dst_ref=dst, send_sem=send, recv_sem=recv, device_id=peer, device_id_type=MESH)

    def rows_at(slot, part_idx):
        return n_buf.at[slot, pl.ds(part_idx * tokens, tokens)]

    def dx_copy(c):
        s = lax.rem(c, 3)
        return remote(rows_at(s, 0), rows_at(s, 1), dx_send.at[s], dx_recv.at[s], across)

    def dc_copy(c):
        s = lax.rem(c, 3)
        return remote(rows_at(s, 0), rows_at(s, 2), dc_send.at[s], dc_recv.at[s], beside)

    def dr_copy(c):
        s = lax.rem(c, 3)
        return remote(rows_at(s, 1), rows_at(s, 3), dr_send.at[s], dr_recv.at[s], beside)

    def r1_copy(c, home):
        s = lax.rem(c, 2)
        return remote(part.at[pl.ds((2 + home) * tokens, tokens)], rb1.at[s, pl.ds(home * tokens, tokens)], r1_send.at[s, home], r1_recv.at[s, home], beside)

    rows = tokens // PIECES

    def piece(p):
        return pl.ds(pl.multiple_of(p * rows, rows), rows)

    def r2_copy(c, p):
        s = lax.rem(c, 3)
        return remote(rb1.at[lax.rem(c, 2), pl.ds(tokens + p * rows, rows)], rb2.at[s, piece(p)], r2_send.at[s, p], r2_recv.at[s, p], across)

    def hop_copy(c, p):
        s = lax.rem(c, 2)
        h = lax.rem(c, HIN_SLOTS)
        return remote(ho.at[s, piece(p)], hin.at[h, piece(p)], hop_send.at[s, p], hin_sem.at[h, p], other_pp)

    def out_copy(c, p):
        s = lax.rem(c, 2)
        return remote(ho.at[s, piece(p)], out.at[c, piece(p)], hop_send.at[s, p], out_recv.at[c, p], other_pp)

    def out_local(c, p):
        s = lax.rem(c, 2)
        return pltpu.make_async_copy(ho.at[s, piece(p)], out.at[c, piece(p)], out_loc.at[s, p])

    def ids_copies(part_idx):
        some = pl.ds(0, 1) if part_idx == 0 else pl.ds(1, chunks - 1)
        return [remote(ids_own.at[some], ids.at[j, some], ids_send.at[part_idx, j], ids_recv.at[part_idx, j], peer) for j, peer in ((1, across), (2, beside), (3, diagonal))]

    def table_copy(c):
        s = lax.rem(c, 2)
        return pltpu.make_async_copy(table, smem_table.at[s], table_sem)

    smem_table[1, 0, 0] = 0
    smem_table[1, 1, 0] = 0

    @pl.when(pp == 0)
    def _():
        for copy in hin_copies(0):
            copy.start()

    for copy in weight_copies[:3]:
        copy.start()
    for copy in kv_copies(0):
        copy.start()
    weight_copies[3].start()

    @pl.when(pp == 0)
    def _():
        for copy in hin_copies(1):
            copy.start()

    barrier = pltpu.get_barrier_semaphore()
    for peer in (other_pp, across, beside, diagonal):
        pl.semaphore_signal(barrier, inc=1, device_id=peer, device_id_type=MESH)
    pl.semaphore_wait(barrier, 4)

    for part_idx in range(2):
        for copy in ids_copies(part_idx):
            copy.start()

    w = {"a_gain": a_gain, "rope": rope_ref, "q": wq, "k": wk, "v": wv, "gate": wg, "up": wu, "down": wd}

    def plan(c):
        @pl.when(c == 0)
        def _():
            ids[0] = ids_own[...]
            with scope("w_ids"):
                for copy in ids_copies(0):
                    copy.wait()

        @pl.when(c == 1)
        def _():
            for copy in ids_copies(1):
                copy.wait()

        chosen_ids = jnp.concatenate([ids[j, c] for j in range(4)], axis=1)
        plan_tiles(chosen_ids, first, tri, member, rank_buf.at[lax.rem(c, 2)], table)
        table_copy(c).start()

    def combine_near(from_col, to_col):
        half = pl.ds(0, 2 * tokens)
        part[half, from_col:to_col] = dot(picks[half, :], terms[:, from_col:to_col])

    def project(c, with_sums):
        plan(c)
        with scope("w_hin"):
            for copy in hin_copies(c):
                copy.wait()

        @pl.when(c == 0)
        def _():
            for copy in weight_copies[:3]:
                copy.wait()

        @pl.when(jnp.logical_and(pp == 0, c + 2 < chunks))
        def _():
            for copy in hin_copies(c + 2):
                copy.start()

        @pl.when(c > 0)
        def _():
            for copy in new_copies(c - 1):
                copy.wait()

        seq_row = seq[pl.ds(c, 1), :].astype(F32)
        pos[...] = jnp.broadcast_to(seq_row, (128, 128)).T
        turn[...] = rope_tables(pos[...], w["rope"])
        if with_sums:
            combine_near(0, 256)
        attn_dots(hin[lax.rem(c, HIN_SLOTS)], w, x_buf)
        if with_sums:
            combine_near(256, 1024)
        attn_rope(turn, x_buf, q3, k3, v3, kn, vn)
        for copy in new_copies(c):
            copy.start()

    def reduce_pair(c):
        s = lax.rem(c, 2)
        far = pl.ds(tokens, tokens)
        near = pl.ds(0, tokens)
        with scope("w_r1"):
            r1_copy(c, 1).wait_recv()
        rb1[s, far, :] = rb1[s, far, :] + part[far, :]
        for p in range(PIECES):
            r2_copy(c, p).start()
        r1_copy(c, 0).wait_recv()
        rb1[s, near, :] = rb1[s, near, :] + part[near, :]
        for home in (1, 0):
            r1_copy(c, home).wait_send()

    def relay(c):
        copy = dx_copy(c)
        with scope("w_dx"):
            copy.wait_recv()
        dr_copy(c).start()
        copy.wait_send()
        dc_copy(c).wait_send()

    def attend(c):
        table_copy(c).wait()
        with scope("w_kv"):
            for copy in kv_copies(c):
                copy.wait()

        @pl.when(c == 0)
        def _():
            weight_copies[4].start()

        @pl.when(c == 1 - pp)
        def _():
            for copy in weight_copies[5:]:
                copy.start()

        def groups(base, count):
            ahead = attn_scores(base, q3, k3, k_buf)
            for u in range(base, base + count):
                scores = ahead
                if u + 1 < base + count:
                    ahead = attn_scores(u + 1, q3, k3, k_buf)
                attn_mix(u, *attn_weights(u, *scores, pos), v3, o3, v_buf)

        half = tokens // GROUP // 2
        with scope("groups"):
            groups(0, half)

        @pl.when(c >= 2)
        def _():
            with scope("relay"):
                relay(c - 1)

        with scope("groups"):
            groups(half, half)

        @pl.when(c + 1 < chunks)
        def _():
            for copy in kv_copies(c + 1):
                copy.start()

        @pl.when(c == 0)
        def _():
            weight_copies[3].wait()

        @pl.when(c == 1)
        def _():
            relay(0)

        @pl.when(c >= 1)
        def _():
            dispatched(c - 1)

        hidden = hin[lax.rem(c, HIN_SLOTS)].astype(F32)
        attn_out = jnp.concatenate([o3[pl.ds(g, tokens, stride=8), :].astype(BF16) for g in range(8)], axis=1)
        before = c + 5
        mixed = dot(attn_out, wo[...])
        router = logits(before)
        picked = gather_rows(before, 0, 0)
        new_mid = (hidden + mixed).astype(BF16)
        mid[lax.rem(c, 3)] = new_mid
        n_buf[lax.rem(c, 3), pl.ds(0, tokens), :] = rms(new_mid.astype(F32), m_gain[...].astype(F32))
        gates(before, router)
        gather_gate(picked, before, 0, 0)
        dx_copy(c).start()
        dc_copy(c).start()

        @pl.when(jnp.logical_and(pp == 1, c + HIN_SLOTS < chunks))
        def _():
            pl.semaphore_signal(credit, inc=1, device_id=other_pp, device_id_type=MESH)

    def tile_at(c, row, j):
        return smem_table[lax.rem(c, 2), row, j]

    def gather_rows(c, j, u):
        normed = n_buf.at[lax.rem(c, 3)]
        return moe_gather(j, u, tile_at(c, 0, j), tile_at(c, 1, j), first, normed, rank_buf.at[lax.rem(c, 2)], picks, x_buf)

    def gather_gate(picked, c, j, u):
        moe_gate(picked, u, tile_at(c, 0, j), first, gate_ref, g_buf)

    def gather(c, j, u):
        gather_gate(gather_rows(c, j, u), c, j, u)

    def dispatched(c):
        with scope("w_disp"):
            dc_copy(c).wait_recv()
            dr_copy(c).wait_recv()

    def logits(c):
        return dot_nt(w_r[...], n_buf[lax.rem(c, 3)])

    def gates(c, router):
        moe_gates(router, rank_buf.at[lax.rem(c, 2)], gate_ref)

    def experts(c):
        @pl.when(c == 0)
        def _():
            with scope("w_wts"):
                for copy in weight_copies[4:]:
                    copy.wait()

        def expand(j, u):
            moe_expand(u, tile_at(c, 0, j), w, x_buf, a_buf)

        def contract(j, u):
            moe_contract(j, u, tile_at(c, 0, j), w, a_buf, g_buf, terms)

        def body(idx, carry):
            base = idx * TILE_UNROLL
            gather(c, base + 1, 1)
            expand(base, 0)
            for u in range(1, TILE_UNROLL):
                if u + 1 < TILE_UNROLL:
                    gather(c, base + u + 1, u + 1)
                expand(base + u, u)
                contract(base + u - 1, u - 1)
            gather(c, lax.rem(base + TILE_UNROLL, tile_count), 0)
            contract(base + TILE_UNROLL - 1, TILE_UNROLL - 1)

            @pl.when(jnp.logical_and(c >= 1, idx >= 1))
            def _():
                finish(c - 1, idx - 1)

            return carry

        with scope("tiles"):
            lax.fori_loop(0, tile_count // TILE_UNROLL, body, 0)
        half = 2 * tokens
        part[pl.ds(half, half), :] = dot(picks[pl.ds(half, half), :], terms[...])
        dr_copy(c).wait_send()
        r1_copy(c, 1).start()
        r1_copy(c, 0).start()

    def finish(c, p):
        s = lax.rem(c, 2)
        at = piece(p)

        @pl.when(jnp.logical_and(jnp.logical_and(pp == 0, p == 0), c >= HIN_SLOTS))
        def _():
            pl.semaphore_wait(credit, 1)

        @pl.when(jnp.logical_and(pp == 0, c >= 2))
        def _():
            hop_copy(c - 2, p).wait_send()

        @pl.when(jnp.logical_and(pp == 1, c >= 2))
        def _():
            out_copy(c - 2, p).wait_send()
            out_local(c - 2, p).wait()

        with scope("w_r2"):
            r2_copy(c, p).wait_recv()
            r2_copy(c, p).wait_send()
        mixed = (rb1[s, at, :] + rb2[lax.rem(c, 3), at, :]).astype(BF16)
        ho[s, at, :] = (mid[lax.rem(c, 3), at, :].astype(F32) + mixed.astype(F32)).astype(BF16)

        @pl.when(pp == 0)
        def _():
            hop_copy(c, p).start()

        @pl.when(pp == 1)
        def _():
            out_copy(c, p).start()
            out_local(c, p).start()

    def step(i, carry):
        @pl.when(i < 2)
        def _():
            with scope("project"):
                project(i, False)

        @pl.when(jnp.logical_and(i >= 2, i < chunks))
        def _():
            with scope("project_sum"):
                project(i, True)

        @pl.when(i >= chunks)
        def _():
            combine_near(0, 1024)

        @pl.when(i >= 2)
        def _():
            with scope("reduce_pair"):
                reduce_pair(i - 2)

        @pl.when(i == chunks)
        def _():
            with scope("relay"):
                relay(i - 1)

        @pl.when(i < chunks)
        def _():
            with scope("attend"):
                attend(i)

        @pl.when(i == chunks)
        def _():
            dispatched(i - 1)
            gates(i - 1, logits(i - 1))
            gather(i - 1, 0, 0)

        @pl.when(jnp.logical_and(i >= 1, i <= chunks))
        def _():
            with scope("experts"):
                experts(i - 1)

        @pl.when(i == chunks + 1)
        def _():
            with scope("finish_last"):
                for p in range(PIECES):
                    finish(i - 2, p)

        return carry

    lax.fori_loop(0, chunks + 2, step, 0)

    for copy in new_copies(chunks - 1):
        copy.wait()

    @pl.when(pp == 0)
    def _():
        for c in (chunks - 2, chunks - 1):
            for p in range(PIECES):
                hop_copy(c, p).wait_send()

        def arrived(c, carry):
            for p in range(PIECES):
                out_copy(c, p).wait_recv()
            return carry

        with scope("w_out"):
            lax.fori_loop(0, chunks, arrived, 0)

    @pl.when(pp == 1)
    def _():
        for c in (chunks - 2, chunks - 1):
            for p in range(PIECES):
                out_copy(c, p).wait_send()
                out_local(c, p).wait()


def step_call(args, chunks, tokens, tile_count):
    vmem = pl.BlockSpec(memory_space=pltpu.VMEM)
    hbm = pl.BlockSpec(memory_space=pl.ANY)
    wide = 4 * tokens
    dma = pltpu.SemaphoreType.DMA
    return pl.pallas_call(
        functools.partial(step_kernel, tile_count),
        out_shape=(
            jax.ShapeDtypeStruct((chunks, tokens, 1024), BF16),
            jax.ShapeDtypeStruct((chunks, tokens, 512), BF16),
            jax.ShapeDtypeStruct((chunks, tokens, 512), BF16),
        ),
        in_specs=[hbm, vmem, hbm, hbm, vmem, hbm, hbm, hbm, hbm, vmem, vmem, vmem, vmem, hbm, hbm, hbm, vmem],
        out_specs=(hbm, hbm, hbm),
        scratch_shapes=[
            pltpu.VMEM((3, wide, 1024), BF16),
            pltpu.VMEM((HIN_SLOTS, tokens, 1024), BF16),
            pltpu.VMEM((3, tokens, 1024), BF16),
            pltpu.VMEM((2, tokens, 1024), BF16),
            pltpu.VMEM((tokens * 128, 64), BF16),
            pltpu.VMEM((tokens * 128, 64), BF16),
            pltpu.VMEM((1024, 1024), BF16),
            pltpu.VMEM((1024, 512), BF16),
            pltpu.VMEM((1024, 512), BF16),
            pltpu.VMEM((1024, 1024), BF16),
            pltpu.VMEM((8, 1024, 512), BF16),
            pltpu.VMEM((8, 1024, 512), BF16),
            pltpu.VMEM((8, 512, 1024), BF16),
            pltpu.VMEM((wide, 1024), F32),
            pltpu.VMEM((2, 2 * tokens, 1024), F32),
            pltpu.VMEM((3, tokens, 1024), F32),
            pltpu.VMEM((wide, tile_count * TILE), BF16),
            pltpu.VMEM((tile_count * TILE, 1024), BF16),
            pltpu.VMEM((3, TILE, 1024), BF16),
            pltpu.VMEM((3, TILE, 512), BF16),
            pltpu.VMEM((TILE_UNROLL, TILE, 128), F32),
            pltpu.VMEM((tokens * 8, 128), F32),
            pltpu.VMEM((tokens * 8, 128), F32),
            pltpu.VMEM((tokens * 8, 128), F32),
            pltpu.VMEM((tokens * 8, 128), F32),
            pltpu.VMEM((tokens, 512), BF16),
            pltpu.VMEM((tokens, 512), BF16),
            pltpu.VMEM((2, 32, wide), F32),
            pltpu.VMEM((32, wide), F32),
            pltpu.VMEM((32, wide), F32),
            pltpu.VMEM((tokens, 128), F32),
            pltpu.VMEM((tokens, 256), F32),
            pltpu.VMEM((4, chunks, 8, tokens), jnp.int32),
            pltpu.VMEM((8, 128), jnp.int32),
            pltpu.SMEM((2, 8, 128), jnp.int32),
            dma((7,)), dma((2, 4)), dma((2, 4)), dma(()), dma((HIN_SLOTS, PIECES)), dma((2,)), dma((2,)),
            dma((3,)), dma((3,)), dma((3,)), dma((3,)), dma((3,)), dma((3,)),
            dma((2, 2)), dma((2, 2)), dma((3, PIECES)), dma((3, PIECES)),
            dma((2, PIECES)), dma((2, PIECES)), dma((chunks, PIECES)),
            pltpu.SemaphoreType.REGULAR,
        ],
        compiler_params=pltpu.CompilerParams(collective_id=0, has_side_effects=True, vmem_limit_bytes=67043328),
        name="decode_step",
        cost_estimate=pl.CostEstimate(flops=2 * 10**11, bytes_accessed=2 * 10**8, transcendentals=0),
    )(*args)


def result_kernel(h_ref, k_ref, v_ref, gain_ref, out_ref, kn_ref, vn_ref, rows):
    tokens = rows.shape[1] // 8
    gain = gain_ref[...].astype(F32).reshape(1, 1024)

    def body(idx, carry):
        at = pl.ds(pl.multiple_of(idx * tokens, tokens), tokens)
        vals = h_ref[0, at, :].astype(F32)
        vals = vals * lax.rsqrt(jnp.mean(vals * vals, axis=-1, keepdims=True) + EPS)
        for g in range(8):
            out_ref[0, at, g * 128:(g + 1) * 128] = (vals[:, g * 128:(g + 1) * 128] * gain[:, g * 128:(g + 1) * 128]).astype(BF16)
        for j, (src, dst) in enumerate(((k_ref, kn_ref), (v_ref, vn_ref))):
            spread_heads(rows.at[j], src[0, at, :].astype(F32))
            dst[0, at] = rows[j].reshape(tokens, 8, 128)[:, :, :64].astype(BF16)
        return carry

    lax.fori_loop(0, h_ref.shape[1] // tokens, body, 0)


def result_call(hidden, k_rows, v_rows, gain):
    blocks = 4
    step = hidden.shape[1]
    tokens = hidden.shape[0] * step // blocks
    hidden, k_rows, v_rows = (x.reshape(blocks, tokens, x.shape[-1]) for x in (hidden, k_rows, v_rows))
    chunks = blocks
    wide = pl.BlockSpec((1, tokens, 1024), lambda i: (i, 0, 0))
    dense = pl.BlockSpec((1, tokens, 512), lambda i: (i, 0, 0))
    heads = pl.BlockSpec((1, tokens, 8, 64), lambda i: (i, 0, 0, 0))
    return pl.pallas_call(
        result_kernel,
        grid=(chunks,),
        out_shape=(
            jax.ShapeDtypeStruct((chunks, tokens, 1024), BF16),
            jax.ShapeDtypeStruct((chunks, tokens, 8, 64), BF16),
            jax.ShapeDtypeStruct((chunks, tokens, 8, 64), BF16),
        ),
        in_specs=[wide, dense, dense, pl.BlockSpec((1024,), lambda i: (0,))],
        out_specs=(wide, heads, heads),
        scratch_shapes=[pltpu.VMEM((2, step * 8, 128), F32)],
        name="results",
        cost_estimate=pl.CostEstimate(flops=10**7, bytes_accessed=2 * 10**7, transcendentals=0),
    )(hidden, k_rows, v_rows, gain)


def solution(mesh):
    rows_spec = ("dp", "ep")
    three_dim = P("pp", None, None)
    two_dim = P("pp", None)
    expert_spec = P("pp", "ep", None, None)
    cache_spec = P("pp", None, rows_spec, None, None, None)
    new_spec = P("pp", None, rows_spec, None, None)
    in_specs = (P(None, rows_spec, None), P(None, rows_spec), cache_spec, cache_spec, P("pp", None, rows_spec, None), three_dim, three_dim, three_dim, three_dim, two_dim, two_dim, three_dim, expert_spec, expert_spec, expert_spec, P(None))
    out_specs = (P(None, rows_spec, None), new_spec, new_spec)

    def device_fn(hidden_in, seq_pos, k_cache, v_cache, expert_ids, w_query, w_key, w_value, w_out, attn_gain, mlp_gain, w_router, w_gate, w_up, w_down, final_gain):
        micro, rows = seq_pos.shape
        chunks = micro // PER_CHUNK
        tokens = PER_CHUNK * rows
        wide = 4 * tokens
        tile_count = (wide * 2 - 8) // TILE + 8
        assert tile_count == TILE_UNROLL * (PIECES + 1)
        angles = np.arange(1, 17)[:, None] * THETA ** (-np.arange(32) / 32)
        both = np.concatenate([np.tile(np.cos(angles), (1, 4)), np.tile(np.concatenate([-np.sin(angles), np.sin(angles)], axis=1), (1, 2))], axis=1)
        both = np.concatenate([both, np.zeros((112, 256))], axis=0).astype(np.float32)
        table = []
        for _ in range(3):
            table.append(both.astype(BF16))
            both = both - table[-1].astype(np.float32)
        table = jnp.asarray(np.concatenate(table, axis=1))
        tri = jnp.asarray(np.triu(np.ones((wide, wide)), 1), BF16)
        ids = jnp.swapaxes(expert_ids[0].reshape(chunks, tokens, 8), 1, 2)
        args = (
            hidden_in.reshape(chunks, tokens, 1024), seq_pos.reshape(chunks, tokens), k_cache.reshape(chunks, tokens * 128, 64), v_cache.reshape(chunks, tokens * 128, 64),
            ids, w_query[0], w_key[0], w_value[0], w_out[0], attn_gain, mlp_gain, table, w_router[0].T,
            w_gate[0], w_up[0], w_down[0], tri,
        )
        out, k_new, v_new = result_call(*step_call(args, chunks, tokens, tile_count), final_gain)
        shape = (1,) + seq_pos.shape + (8, 64)
        return out.reshape(hidden_in.shape), k_new.reshape(shape), v_new.reshape(shape)

    return jax.shard_map(device_fn, mesh=mesh, in_specs=in_specs, out_specs=out_specs, check_vma=False)
```

```python
import functools

import jax
import jax.numpy as jnp
import numpy as np
from jax import lax
from jax.experimental import pallas as pl
from jax.experimental.pallas import tpu as pltpu
from jax.sharding import PartitionSpec as P

THETA = 1000000.0
EPS = 1e-05
F32 = jnp.float32
BF16 = jnp.bfloat16
TILE = 128
GROUP = 16
TILE_UNROLL = 3
PER_CHUNK = 4
HIN_SLOTS = 4
PIECES = 4
MESH = pl.DeviceIdType.MESH


def scope(name):
    return jax.named_scope(name)


def rms(vals, gain_row):
    inv = lax.rsqrt(jnp.mean(vals * vals, axis=-1, keepdims=True) + EPS)
    return (vals * inv * gain_row).astype(BF16)


def dot(lhs, rhs):
    return jnp.dot(lhs, rhs, preferred_element_type=F32)


def dot_nt(lhs, rhs):
    return lax.dot_general(lhs, rhs, (((1,), (1,)), ((), ())), preferred_element_type=F32)


def rope_tables(pos, table):
    lane = lax.broadcasted_iota(jnp.int32, pos.shape, 1).astype(F32)
    both = dot(jnp.where(lane + 1.0 == pos, 1.0, 0.0).astype(BF16), table[...])
    both = both[:, :256] + both[:, 256:512] + both[:, 512:]
    return both


def rope(vals, cos_t, sin_t):
    lane = lax.broadcasted_iota(jnp.int32, (1, 128), 1)
    first = (lane % 64) < 32
    parts = []
    for j in range(vals.shape[1] // 128):
        block = vals[:, j * 128:(j + 1) * 128]
        swapped = jnp.where(first, pltpu.roll(block, 96, 1), pltpu.roll(block, 32, 1))
        parts.append(block * cos_t + swapped * sin_t)
    return jnp.concatenate(parts, axis=1)


def spread(ref, vals):
    tokens = vals.shape[0]
    for g in range(8):
        ref[pl.ds(g, tokens, stride=8), :] = vals[:, g * 128:(g + 1) * 128]


def spread_heads(ref, vals):
    tokens = vals.shape[0]
    low = lax.broadcasted_iota(jnp.int32, (1, 128), 1) < 64
    for j in range(4):
        block = vals[:, j * 128:(j + 1) * 128]
        other = pltpu.roll(block, 64, 1)
        ref[pl.ds(2 * j, tokens, stride=8), :] = jnp.where(low, block, other)
        ref[pl.ds(2 * j + 1, tokens, stride=8), :] = jnp.where(low, other, block)


def rows_of(ref, idx):
    return ref[pl.ds(pl.multiple_of(idx * GROUP * 8, GROUP * 8), GROUP * 8), :].reshape(GROUP, 8, 128)


def attn_dots(hidden, w, raw):
    normed = rms(hidden.astype(F32), w["a_gain"][...].astype(F32))
    raw[1] = dot(normed, w["q"][...]).astype(BF16)
    raw[2, :, :512] = dot(normed, w["k"][...]).astype(BF16)
    raw[2, :, 512:] = dot(normed, w["v"][...]).astype(BF16)


def attn_rope(turn, raw, q3, k3, v3, kn, vn):
    cos_t, sin_t = turn[:, :128], turn[:, 128:]
    spread(q3, rope(raw[1].astype(F32), cos_t, sin_t).astype(BF16).astype(F32))
    k = rope(raw[2, :, :512].astype(F32), cos_t, sin_t).astype(BF16)
    kn[...] = k
    spread_heads(k3, k.astype(F32))
    v = raw[2, :, 512:]
    vn[...] = v
    spread_heads(v3, v.astype(F32))


def attn_scores(idx, q3, k3, k_rows):
    q = rows_of(q3, idx)
    lane3 = lax.broadcasted_iota(jnp.int32, (1, 1, 128), 2)
    prod = q * rows_of(k3, idx)
    self_a = jnp.sum(jnp.where(lane3 < 64, prod, 0.0), axis=-1, keepdims=True)
    self_b = jnp.sum(jnp.where(lane3 < 64, 0.0, prod), axis=-1, keepdims=True)
    wide = (GROUP, 8, 128)
    self_s = jnp.concatenate([jnp.broadcast_to(self_a, wide), jnp.broadcast_to(self_b, wide)], axis=1) * 0.125
    q_rows = jnp.concatenate([q, pltpu.roll(q, 64, 2)], axis=1).astype(BF16)[:, :, :64].reshape(GROUP * 16, 64)
    row0 = idx * (GROUP * 128)
    blocks = []
    for p in range(GROUP // 2):
        keys = k_rows[pl.ds(pl.multiple_of(row0 + p * 256, 256), 256), :]
        both = dot_nt(q_rows[p * 32:(p + 1) * 32], keys)
        blocks.append(both[:16, :128].reshape(1, 16, 128))
        blocks.append(both[16:, 128:].reshape(1, 16, 128))
    return jnp.concatenate(blocks, axis=0), self_s


def attn_weights(idx, scores, self_s, pos_ref):
    row_i = lax.broadcasted_iota(jnp.int32, (16, 128), 0)
    lane_i = lax.broadcasted_iota(jnp.int32, (16, 128), 1)
    step = jnp.where((row_i % 8) == (lane_i % 8), lane_i // 8, 1000).astype(F32)
    pos = pos_ref[pl.ds(pl.multiple_of(idx * GROUP, GROUP), GROUP), :].reshape(GROUP, 1, 128)
    scores = jnp.where(step.reshape(1, 16, 128) < pos, scores * 0.125, -jnp.inf)
    wide = (GROUP, 16, 128)
    top = jnp.maximum(jnp.broadcast_to(jnp.max(scores, axis=-1, keepdims=True), wide), self_s)
    weights = jnp.exp(scores - top)
    self_w = jnp.exp(self_s - top)
    inv = 1.0 / (jnp.broadcast_to(jnp.sum(weights, axis=-1, keepdims=True), wide) + self_w)
    return (weights * inv).astype(BF16), (self_w * inv).astype(BF16).astype(F32)


def attn_mix(idx, weights, self_w, v3, o3, v_rows):
    row0 = idx * (GROUP * 128)
    zeros = jnp.zeros((16, 128), BF16)
    outs = []
    for p in range(GROUP // 2):
        vals = v_rows[pl.ds(pl.multiple_of(row0 + p * 256, 256), 256), :]
        upper = jnp.concatenate([weights[2 * p], zeros], axis=1)
        lower = jnp.concatenate([zeros, weights[2 * p + 1]], axis=1)
        outs.append(dot(jnp.concatenate([upper, lower], axis=0), vals).reshape(2, 16, 64))
    out = jnp.concatenate(outs, axis=0)
    v_new = rows_of(v3, idx)[:, :, :64]
    out_a = out[:, :8] + self_w[:, :8, :64] * v_new
    out_b = out[:, 8:] + self_w[:, 8:, :64] * v_new
    o3[pl.ds(pl.multiple_of(idx * GROUP * 8, GROUP * 8), GROUP * 8), :] = jnp.concatenate([out_a, out_b], axis=-1).reshape(GROUP * 8, 128)


def plan_tiles(ids, first, tri, member_ref, rank_ref, table_ref):
    tokens = ids.shape[1]
    expert_i = lax.broadcasted_iota(jnp.int32, (32, tokens), 0)
    chosen = jnp.zeros((32, tokens), F32)
    for s in range(ids.shape[0]):
        chosen = jnp.where(ids[s:s + 1, :] == expert_i, 1.0, chosen)
    member_ref[...] = chosen
    rank = dot(chosen.astype(BF16), tri[...])
    rank_ref[...] = jnp.where(chosen > 0.0, rank, -1.0)
    local = member_ref[pl.ds(pl.multiple_of(first, 8), 8), :]
    counts = jnp.sum(local, axis=-1, keepdims=True).astype(jnp.int32)
    tiles = jnp.broadcast_to(lax.shift_right_logical(counts + (TILE - 1), 7), (8, 128))
    lane = lax.broadcasted_iota(jnp.int32, (1, 128), 1)
    end = jnp.zeros((1, 128), jnp.int32)
    start = jnp.zeros((1, 128), jnp.int32)
    expert = jnp.zeros((1, 128), jnp.int32)
    for e in range(8):
        end = end + tiles[e:e + 1, :]
        passed = lane >= end
        expert = jnp.where(passed, expert + 1, expert)
        start = jnp.where(passed, end, start)
    sub = jnp.where(expert < 8, lane - start, 1000)
    table_ref[0:1, :] = jnp.minimum(expert, 7)
    table_ref[1:2, :] = sub


def moe_gates(logits, rank_ref, gate_ref):
    chosen = rank_ref[...] >= 0.0
    top = jnp.max(jnp.where(chosen, logits, -jnp.inf), axis=0, keepdims=True)
    gates = jnp.where(chosen, jnp.exp(logits - top), 0.0)
    gate_ref[...] = gates / jnp.sum(gates, axis=0, keepdims=True)


def slot_of(u):
    return 0 if u == 0 else 1 + (u - 1) % 2


def moe_gather(j, u, expert, sub, first, normed, rank_ref, picks, x_buf):
    ranks = rank_ref[pl.ds(first + expert, 1), :]
    wanted = (lax.broadcasted_iota(jnp.int32, (TILE, 1), 0) + sub * TILE).astype(F32)
    picked = jnp.where(ranks == wanted, 1.0, 0.0)
    picks[:, pl.ds(pl.multiple_of(j * TILE, TILE), TILE)] = picked.T.astype(BF16)
    x_buf[slot_of(u)] = dot(picked.astype(BF16), normed[...]).astype(BF16)
    return picked


def moe_gate(picked, u, expert, first, gate_ref, g_buf):
    gate = jnp.sum(picked * gate_ref[pl.ds(first + expert, 1), :], axis=-1, keepdims=True)
    g_buf[u] = jnp.broadcast_to(gate, (TILE, 128))


def moe_expand(u, expert, w, x_buf, a_buf):
    rows = x_buf[slot_of(u)]
    a_buf[slot_of(u)] = (jax.nn.silu(dot(rows, w["gate"][expert])) * dot(rows, w["up"][expert])).astype(BF16)


def moe_contract(j, u, expert, w, a_buf, g_buf, terms):
    y = dot(a_buf[slot_of(u)], w["down"][expert])
    gate = g_buf[u]
    at = pl.ds(pl.multiple_of(j * TILE, TILE), TILE)
    for p in range(8):
        terms[at, p * 128:(p + 1) * 128] = (gate * y[:, p * 128:(p + 1) * 128]).astype(BF16)


def step_kernel(
    tile_count,
    hid, seq, k_cache, v_cache, ids_own, wq_h, wk_h, wv_h, wo_h, a_gain, m_gain, rope_ref, w_r, wg_h, wu_h, wd_h, tri,
    out, kn_out, vn_out,
    n_buf, hin, mid, ho, k_buf, v_buf, wq, wk, wv, wo, wg, wu, wd, part, rb1, rb2, picks, terms, x_buf, a_buf, g_buf, q3, k3, v3, o3, kn, vn, rank_buf, gate_ref, member, pos, turn, ids, table, smem_table,
    w_sem, ids_send, ids_recv, table_sem, hin_sem, kv_sem, new_sem, dx_send, dx_recv, dc_send, dc_recv, dr_send, dr_recv, r1_send, r1_recv, r2_send, r2_recv, hop_send, out_loc, out_recv, credit,
):
    chunks, tokens = hid.shape[0], hid.shape[1]
    gathered = 4 * tokens
    dp = lax.axis_index("dp")
    pp = lax.axis_index("pp")
    ep = lax.axis_index("ep")
    other_pp = (dp, 1 - pp, ep)
    across = (dp, pp, lax.rem(ep + 2, 4))
    beside = (dp, pp, ep + 1 - 2 * lax.rem(ep, 2))
    first = ep * 8

    diagonal = (dp, pp, lax.rem(ep + 3 - 2 * lax.rem(ep, 2), 4))

    attn_w = [(wq_h, wq), (wk_h, wk), (wv_h, wv), (wo_h, wo)]
    moe_w = [(wg_h, wg), (wu_h, wu), (wd_h, wd)]
    weight_copies = [pltpu.make_async_copy(s, d, w_sem.at[j]) for j, (s, d) in enumerate(attn_w + moe_w)]

    def hin_copies(c):
        h = lax.rem(c, HIN_SLOTS)
        return [pltpu.make_async_copy(hid.at[c, piece(p)], hin.at[h, piece(p)], hin_sem.at[h, p]) for p in range(PIECES)]

    def kv_copies(c):
        return (pltpu.make_async_copy(k_cache.at[c], k_buf, kv_sem.at[0]), pltpu.make_async_copy(v_cache.at[c], v_buf, kv_sem.at[1]))

    def new_copies(c):
        return (pltpu.make_async_copy(kn, kn_out.at[c], new_sem.at[0]), pltpu.make_async_copy(vn, vn_out.at[c], new_sem.at[1]))

    def remote(src, dst, send, recv, peer):
        return pltpu.make_async_remote_copy(src_ref=src, dst_ref=dst, send_sem=send, recv_sem=recv, device_id=peer, device_id_type=MESH)

    def rows_at(slot, part_idx):
        return n_buf.at[slot, pl.ds(part_idx * tokens, tokens)]

    def dx_copy(c):
        s = lax.rem(c, 3)
        return remote(rows_at(s, 0), rows_at(s, 1), dx_send.at[s], dx_recv.at[s], across)

    def dc_copy(c):
        s = lax.rem(c, 3)
        return remote(rows_at(s, 0), rows_at(s, 2), dc_send.at[s], dc_recv.at[s], beside)

    def dr_copy(c):
        s = lax.rem(c, 3)
        return remote(rows_at(s, 1), rows_at(s, 3), dr_send.at[s], dr_recv.at[s], beside)

    def r1_copy(c, home):
        s = lax.rem(c, 2)
        return remote(part.at[pl.ds((2 + home) * tokens, tokens)], rb1.at[s, pl.ds(home * tokens, tokens)], r1_send.at[s, home], r1_recv.at[s, home], beside)

    rows = tokens // PIECES

    def piece(p):
        return pl.ds(pl.multiple_of(p * rows, rows), rows)

    def r2_copy(c, p):
        s = lax.rem(c, 3)
        return remote(rb1.at[lax.rem(c, 2), pl.ds(tokens + p * rows, rows)], rb2.at[s, piece(p)], r2_send.at[s, p], r2_recv.at[s, p], across)

    def hop_copy(c, p):
        s = lax.rem(c, 2)
        h = lax.rem(c, HIN_SLOTS)
        return remote(ho.at[s, piece(p)], hin.at[h, piece(p)], hop_send.at[s, p], hin_sem.at[h, p], other_pp)

    def out_copy(c, p):
        s = lax.rem(c, 2)
        return remote(ho.at[s, piece(p)], out.at[c, piece(p)], hop_send.at[s, p], out_recv.at[c, p], other_pp)

    def out_local(c, p):
        s = lax.rem(c, 2)
        return pltpu.make_async_copy(ho.at[s, piece(p)], out.at[c, piece(p)], out_loc.at[s, p])

    def ids_copies(part_idx):
        some = pl.ds(0, 1) if part_idx == 0 else pl.ds(1, chunks - 1)
        return [remote(ids_own.at[some], ids.at[j, some], ids_send.at[part_idx, j], ids_recv.at[part_idx, j], peer) for j, peer in ((1, across), (2, beside), (3, diagonal))]

    def table_copy(c):
        s = lax.rem(c, 2)
        return pltpu.make_async_copy(table, smem_table.at[s], table_sem)

    smem_table[1, 0, 0] = 0
    smem_table[1, 1, 0] = 0

    @pl.when(pp == 0)
    def _():
        for copy in hin_copies(0):
            copy.start()

    for copy in weight_copies[:3]:
        copy.start()
    for copy in kv_copies(0):
        copy.start()
    weight_copies[3].start()

    @pl.when(pp == 0)
    def _():
        for copy in hin_copies(1):
            copy.start()

    barrier = pltpu.get_barrier_semaphore()
    for peer in (other_pp, across, beside, diagonal):
        pl.semaphore_signal(barrier, inc=1, device_id=peer, device_id_type=MESH)
    pl.semaphore_wait(barrier, 4)

    for part_idx in range(2):
        for copy in ids_copies(part_idx):
            copy.start()

    w = {"a_gain": a_gain, "rope": rope_ref, "q": wq, "k": wk, "v": wv, "gate": wg, "up": wu, "down": wd}

    def plan(c):
        @pl.when(c == 0)
        def _():
            ids[0] = ids_own[...]
            with scope("w_ids"):
                for copy in ids_copies(0):
                    copy.wait()

        @pl.when(c == 1)
        def _():
            for copy in ids_copies(1):
                copy.wait()

        chosen_ids = jnp.concatenate([ids[j, c] for j in range(4)], axis=1)
        plan_tiles(chosen_ids, first, tri, member, rank_buf.at[lax.rem(c, 2)], table)
        table_copy(c).start()

    def combine_near(from_col, to_col):
        half = pl.ds(0, 2 * tokens)
        part[half, from_col:to_col] = dot(picks[half, :], terms[:, from_col:to_col])

    def project(c, with_sums):
        plan(c)
        with scope("w_hin"):
            for copy in hin_copies(c):
                copy.wait()

        @pl.when(c == 0)
        def _():
            for copy in weight_copies[:3]:
                copy.wait()

        @pl.when(jnp.logical_and(pp == 0, c + 2 < chunks))
        def _():
            for copy in hin_copies(c + 2):
                copy.start()

        @pl.when(c > 0)
        def _():
            for copy in new_copies(c - 1):
                copy.wait()

        seq_row = seq[pl.ds(c, 1), :].astype(F32)
        pos[...] = jnp.broadcast_to(seq_row, (128, 128)).T
        turn[...] = rope_tables(pos[...], w["rope"])
        if with_sums:
            combine_near(0, 256)
        attn_dots(hin[lax.rem(c, HIN_SLOTS)], w, x_buf)
        if with_sums:
            combine_near(256, 1024)
        attn_rope(turn, x_buf, q3, k3, v3, kn, vn)
        for copy in new_copies(c):
            copy.start()

    def reduce_pair(c):
        s = lax.rem(c, 2)
        far = pl.ds(tokens, tokens)
        with scope("w_r1"):
            r1_copy(c, 1).wait_recv()
        rb1[s, far, :] = rb1[s, far, :] + part[far, :]
        for p in range(PIECES):
            r2_copy(c, p).start()
        r1_copy(c, 0).wait_recv()
        for home in (1, 0):
            r1_copy(c, home).wait_send()

    def relay(c):
        copy = dx_copy(c)
        with scope("w_dx"):
            copy.wait_recv()
        dr_copy(c).start()
        copy.wait_send()
        dc_copy(c).wait_send()

    def attend(c):
        table_copy(c).wait()
        with scope("w_kv"):
            for copy in kv_copies(c):
                copy.wait()

        @pl.when(c == 0)
        def _():
            weight_copies[4].start()

        @pl.when(c == 1 - pp)
        def _():
            for copy in weight_copies[5:]:
                copy.start()

        def groups(base, count):
            ahead = attn_scores(base, q3, k3, k_buf)
            for u in range(base, base + count):
                scores = ahead
                if u + 1 < base + count:
                    ahead = attn_scores(u + 1, q3, k3, k_buf)
                attn_mix(u, *attn_weights(u, *scores, pos), v3, o3, v_buf)

        half = tokens // GROUP // 2
        with scope("groups"):
            groups(0, half)

        @pl.when(c >= 2)
        def _():
            with scope("relay"):
                relay(c - 1)

        with scope("groups"):
            groups(half, half)

        @pl.when(c + 1 < chunks)
        def _():
            for copy in kv_copies(c + 1):
                copy.start()

        @pl.when(c == 0)
        def _():
            weight_copies[3].wait()

        @pl.when(c == 1)
        def _():
            relay(0)

        @pl.when(c >= 1)
        def _():
            dispatched(c - 1)

        hidden = hin[lax.rem(c, HIN_SLOTS)].astype(F32)
        attn_out = jnp.concatenate([o3[pl.ds(g, tokens, stride=8), :].astype(BF16) for g in range(8)], axis=1)
        before = c + 5
        mixed = dot(attn_out, wo[...])
        router = logits(before)
        picked = gather_rows(before, 0, 0)
        new_mid = (hidden + mixed).astype(BF16)
        mid[lax.rem(c, 3)] = new_mid
        n_buf[lax.rem(c, 3), pl.ds(0, tokens), :] = rms(new_mid.astype(F32), m_gain[...].astype(F32))
        gates(before, router)
        gather_gate(picked, before, 0, 0)
        dx_copy(c).start()
        dc_copy(c).start()

        @pl.when(jnp.logical_and(pp == 1, c + HIN_SLOTS < chunks))
        def _():
            pl.semaphore_signal(credit, inc=1, device_id=other_pp, device_id_type=MESH)

    def tile_at(c, row, j):
        return smem_table[lax.rem(c, 2), row, j]

    def gather_rows(c, j, u):
        normed = n_buf.at[lax.rem(c, 3)]
        return moe_gather(j, u, tile_at(c, 0, j), tile_at(c, 1, j), first, normed, rank_buf.at[lax.rem(c, 2)], picks, x_buf)

    def gather_gate(picked, c, j, u):
        moe_gate(picked, u, tile_at(c, 0, j), first, gate_ref, g_buf)

    def gather(c, j, u):
        gather_gate(gather_rows(c, j, u), c, j, u)

    def dispatched(c):
        with scope("w_disp"):
            dc_copy(c).wait_recv()
            dr_copy(c).wait_recv()

    def logits(c):
        return dot_nt(w_r[...], n_buf[lax.rem(c, 3)])

    def gates(c, router):
        moe_gates(router, rank_buf.at[lax.rem(c, 2)], gate_ref)

    def experts(c):
        @pl.when(c == 0)
        def _():
            with scope("w_wts"):
                for copy in weight_copies[4:]:
                    copy.wait()

        def expand(j, u):
            moe_expand(u, tile_at(c, 0, j), w, x_buf, a_buf)

        def contract(j, u):
            moe_contract(j, u, tile_at(c, 0, j), w, a_buf, g_buf, terms)

        def body(idx, carry):
            base = idx * TILE_UNROLL
            gather(c, base + 1, 1)
            expand(base, 0)
            for u in range(1, TILE_UNROLL):
                if u + 1 < TILE_UNROLL:
                    gather(c, base + u + 1, u + 1)
                expand(base + u, u)
                contract(base + u - 1, u - 1)
            gather(c, lax.rem(base + TILE_UNROLL, tile_count), 0)
            contract(base + TILE_UNROLL - 1, TILE_UNROLL - 1)

            @pl.when(jnp.logical_and(c >= 1, idx >= 1))
            def _():
                finish(c - 1, idx - 1)

            return carry

        with scope("tiles"):
            lax.fori_loop(0, tile_count // TILE_UNROLL, body, 0)
        half = 2 * tokens
        part[pl.ds(half, half), :] = dot(picks[pl.ds(half, half), :], terms[...])
        dr_copy(c).wait_send()
        r1_copy(c, 1).start()
        r1_copy(c, 0).start()

    def finish(c, p):
        s = lax.rem(c, 2)
        at = piece(p)

        @pl.when(jnp.logical_and(jnp.logical_and(pp == 0, p == 0), c >= HIN_SLOTS))
        def _():
            pl.semaphore_wait(credit, 1)

        @pl.when(jnp.logical_and(pp == 0, c >= 2))
        def _():
            hop_copy(c - 2, p).wait_send()

        @pl.when(jnp.logical_and(pp == 1, c >= 2))
        def _():
            out_copy(c - 2, p).wait_send()
            out_local(c - 2, p).wait()

        with scope("w_r2"):
            r2_copy(c, p).wait_recv()
            r2_copy(c, p).wait_send()
        mixed = (rb1[s, at, :] + part[at, :] + rb2[lax.rem(c, 3), at, :]).astype(BF16)
        ho[s, at, :] = (mid[lax.rem(c, 3), at, :].astype(F32) + mixed.astype(F32)).astype(BF16)

        @pl.when(pp == 0)
        def _():
            hop_copy(c, p).start()

        @pl.when(pp == 1)
        def _():
            out_copy(c, p).start()
            out_local(c, p).start()

    def step(i, carry):
        @pl.when(i < 2)
        def _():
            with scope("project"):
                project(i, False)

        @pl.when(jnp.logical_and(i >= 2, i < chunks))
        def _():
            with scope("project_sum"):
                project(i, True)

        @pl.when(i >= chunks)
        def _():
            combine_near(0, 1024)

        @pl.when(i >= 2)
        def _():
            with scope("reduce_pair"):
                reduce_pair(i - 2)

        @pl.when(i == chunks)
        def _():
            with scope("relay"):
                relay(i - 1)

        @pl.when(i < chunks)
        def _():
            with scope("attend"):
                attend(i)

        @pl.when(i == chunks)
        def _():
            dispatched(i - 1)
            gates(i - 1, logits(i - 1))
            gather(i - 1, 0, 0)

        @pl.when(jnp.logical_and(i >= 1, i <= chunks))
        def _():
            with scope("experts"):
                experts(i - 1)

        @pl.when(i == chunks + 1)
        def _():
            with scope("finish_last"):
                for p in range(PIECES):
                    finish(i - 2, p)

        return carry

    lax.fori_loop(0, chunks + 2, step, 0)

    for copy in new_copies(chunks - 1):
        copy.wait()

    @pl.when(pp == 0)
    def _():
        for c in (chunks - 2, chunks - 1):
            for p in range(PIECES):
                hop_copy(c, p).wait_send()

        def arrived(c, carry):
            for p in range(PIECES):
                out_copy(c, p).wait_recv()
            return carry

        with scope("w_out"):
            lax.fori_loop(0, chunks, arrived, 0)

    @pl.when(pp == 1)
    def _():
        for c in (chunks - 2, chunks - 1):
            for p in range(PIECES):
                out_copy(c, p).wait_send()
                out_local(c, p).wait()


def step_call(args, chunks, tokens, tile_count):
    vmem = pl.BlockSpec(memory_space=pltpu.VMEM)
    hbm = pl.BlockSpec(memory_space=pl.ANY)
    wide = 4 * tokens
    dma = pltpu.SemaphoreType.DMA
    return pl.pallas_call(
        functools.partial(step_kernel, tile_count),
        out_shape=(
            jax.ShapeDtypeStruct((chunks, tokens, 1024), BF16),
            jax.ShapeDtypeStruct((chunks, tokens, 512), BF16),
            jax.ShapeDtypeStruct((chunks, tokens, 512), BF16),
        ),
        in_specs=[hbm, vmem, hbm, hbm, vmem, hbm, hbm, hbm, hbm, vmem, vmem, vmem, vmem, hbm, hbm, hbm, vmem],
        out_specs=(hbm, hbm, hbm),
        scratch_shapes=[
            pltpu.VMEM((3, wide, 1024), BF16),
            pltpu.VMEM((HIN_SLOTS, tokens, 1024), BF16),
            pltpu.VMEM((3, tokens, 1024), BF16),
            pltpu.VMEM((2, tokens, 1024), BF16),
            pltpu.VMEM((tokens * 128, 64), BF16),
            pltpu.VMEM((tokens * 128, 64), BF16),
            pltpu.VMEM((1024, 1024), BF16),
            pltpu.VMEM((1024, 512), BF16),
            pltpu.VMEM((1024, 512), BF16),
            pltpu.VMEM((1024, 1024), BF16),
            pltpu.VMEM((8, 1024, 512), BF16),
            pltpu.VMEM((8, 1024, 512), BF16),
            pltpu.VMEM((8, 512, 1024), BF16),
            pltpu.VMEM((wide, 1024), F32),
            pltpu.VMEM((2, 2 * tokens, 1024), F32),
            pltpu.VMEM((3, tokens, 1024), F32),
            pltpu.VMEM((wide, tile_count * TILE), BF16),
            pltpu.VMEM((tile_count * TILE, 1024), BF16),
            pltpu.VMEM((3, TILE, 1024), BF16),
            pltpu.VMEM((3, TILE, 512), BF16),
            pltpu.VMEM((TILE_UNROLL, TILE, 128), F32),
            pltpu.VMEM((tokens * 8, 128), F32),
            pltpu.VMEM((tokens * 8, 128), F32),
            pltpu.VMEM((tokens * 8, 128), F32),
            pltpu.VMEM((tokens * 8, 128), F32),
            pltpu.VMEM((tokens, 512), BF16),
            pltpu.VMEM((tokens, 512), BF16),
            pltpu.VMEM((2, 32, wide), F32),
            pltpu.VMEM((32, wide), F32),
            pltpu.VMEM((32, wide), F32),
            pltpu.VMEM((tokens, 128), F32),
            pltpu.VMEM((tokens, 256), F32),
            pltpu.VMEM((4, chunks, 8, tokens), jnp.int32),
            pltpu.VMEM((8, 128), jnp.int32),
            pltpu.SMEM((2, 8, 128), jnp.int32),
            dma((7,)), dma((2, 4)), dma((2, 4)), dma(()), dma((HIN_SLOTS, PIECES)), dma((2,)), dma((2,)),
            dma((3,)), dma((3,)), dma((3,)), dma((3,)), dma((3,)), dma((3,)),
            dma((2, 2)), dma((2, 2)), dma((3, PIECES)), dma((3, PIECES)),
            dma((2, PIECES)), dma((2, PIECES)), dma((chunks, PIECES)),
            pltpu.SemaphoreType.REGULAR,
        ],
        compiler_params=pltpu.CompilerParams(collective_id=0, has_side_effects=True, vmem_limit_bytes=67043328),
        name="decode_step",
        cost_estimate=pl.CostEstimate(flops=2 * 10**11, bytes_accessed=2 * 10**8, transcendentals=0),
    )(*args)


def result_kernel(h_ref, k_ref, v_ref, gain_ref, out_ref, kn_ref, vn_ref, rows):
    tokens = rows.shape[1] // 8
    gain = gain_ref[...].astype(F32).reshape(1, 1024)

    def body(idx, carry):
        at = pl.ds(pl.multiple_of(idx * tokens, tokens), tokens)
        vals = h_ref[0, at, :].astype(F32)
        vals = vals * lax.rsqrt(jnp.mean(vals * vals, axis=-1, keepdims=True) + EPS)
        for g in range(8):
            out_ref[0, at, g * 128:(g + 1) * 128] = (vals[:, g * 128:(g + 1) * 128] * gain[:, g * 128:(g + 1) * 128]).astype(BF16)
        for j, (src, dst) in enumerate(((k_ref, kn_ref), (v_ref, vn_ref))):
            spread_heads(rows.at[j], src[0, at, :].astype(F32))
            dst[0, at] = rows[j].reshape(tokens, 8, 128)[:, :, :64].astype(BF16)
        return carry

    lax.fori_loop(0, h_ref.shape[1] // tokens, body, 0)


def result_call(hidden, k_rows, v_rows, gain):
    blocks = 4
    step = hidden.shape[1]
    tokens = hidden.shape[0] * step // blocks
    hidden, k_rows, v_rows = (x.reshape(blocks, tokens, x.shape[-1]) for x in (hidden, k_rows, v_rows))
    chunks = blocks
    wide = pl.BlockSpec((1, tokens, 1024), lambda i: (i, 0, 0))
    dense = pl.BlockSpec((1, tokens, 512), lambda i: (i, 0, 0))
    heads = pl.BlockSpec((1, tokens, 8, 64), lambda i: (i, 0, 0, 0))
    return pl.pallas_call(
        result_kernel,
        grid=(chunks,),
        out_shape=(
            jax.ShapeDtypeStruct((chunks, tokens, 1024), BF16),
            jax.ShapeDtypeStruct((chunks, tokens, 8, 64), BF16),
            jax.ShapeDtypeStruct((chunks, tokens, 8, 64), BF16),
        ),
        in_specs=[wide, dense, dense, pl.BlockSpec((1024,), lambda i: (0,))],
        out_specs=(wide, heads, heads),
        scratch_shapes=[pltpu.VMEM((2, step * 8, 128), F32)],
        name="results",
        cost_estimate=pl.CostEstimate(flops=10**7, bytes_accessed=2 * 10**7, transcendentals=0),
    )(hidden, k_rows, v_rows, gain)


def solution(mesh):
    rows_spec = ("dp", "ep")
    three_dim = P("pp", None, None)
    two_dim = P("pp", None)
    expert_spec = P("pp", "ep", None, None)
    cache_spec = P("pp", None, rows_spec, None, None, None)
    new_spec = P("pp", None, rows_spec, None, None)
    in_specs = (P(None, rows_spec, None), P(None, rows_spec), cache_spec, cache_spec, P("pp", None, rows_spec, None), three_dim, three_dim, three_dim, three_dim, two_dim, two_dim, three_dim, expert_spec, expert_spec, expert_spec, P(None))
    out_specs = (P(None, rows_spec, None), new_spec, new_spec)

    def device_fn(hidden_in, seq_pos, k_cache, v_cache, expert_ids, w_query, w_key, w_value, w_out, attn_gain, mlp_gain, w_router, w_gate, w_up, w_down, final_gain):
        micro, rows = seq_pos.shape
        chunks = micro // PER_CHUNK
        tokens = PER_CHUNK * rows
        wide = 4 * tokens
        tile_count = (wide * 2 - 8) // TILE + 8
        assert tile_count == TILE_UNROLL * (PIECES + 1)
        angles = np.arange(1, 17)[:, None] * THETA ** (-np.arange(32) / 32)
        both = np.concatenate([np.tile(np.cos(angles), (1, 4)), np.tile(np.concatenate([-np.sin(angles), np.sin(angles)], axis=1), (1, 2))], axis=1)
        both = np.concatenate([both, np.zeros((112, 256))], axis=0).astype(np.float32)
        table = []
        for _ in range(3):
            table.append(both.astype(BF16))
            both = both - table[-1].astype(np.float32)
        table = jnp.asarray(np.concatenate(table, axis=1))
        tri = jnp.asarray(np.triu(np.ones((wide, wide)), 1), BF16)
        ids = jnp.swapaxes(expert_ids[0].reshape(chunks, tokens, 8), 1, 2)
        args = (
            hidden_in.reshape(chunks, tokens, 1024), seq_pos.reshape(chunks, tokens), k_cache.reshape(chunks, tokens * 128, 64), v_cache.reshape(chunks, tokens * 128, 64),
            ids, w_query[0], w_key[0], w_value[0], w_out[0], attn_gain, mlp_gain, table, w_router[0].T,
            w_gate[0], w_up[0], w_down[0], tri,
        )
        out, k_new, v_new = result_call(*step_call(args, chunks, tokens, tile_count), final_gain)
        shape = (1,) + seq_pos.shape + (8, 64)
        return out.reshape(hidden_in.shape), k_new.reshape(shape), v_new.reshape(shape)

    return jax.shard_map(device_fn, mesh=mesh, in_specs=in_specs, out_specs=out_specs, check_vma=False)
```
